32 devices in a mesh: dp: 4 (over z), ctx: 8 (over y, x, core).
Axes of the slice: x: 2, y: 2, z: 4, core: 2. Of those that a mesh axis runs over, the one named last changes fastest.
Arguments:
- layer_input: bfloat16 [4, 2048, 2048], P('dp', 'ctx'), may hold values from -6 to 6
- doc_ids: int32 [4, 2048], P('dp', 'ctx'), may hold values from 0 to 3, never falling along the last dimension, each value on 1 to 1024 neighbouring positions
- route_ids: int32 [4, 2048, 8], P('dp', 'ctx'), may hold values from 0 to 15, all different within a row; in each aligned block of 256 rows (0 to 255, 256 to 511, ..., all dimensions but the last counted through in order) at most 144 rows name the same one
- route_probs: float32 [4, 2048, 8], P('dp', 'ctx'), may hold values from 0.04 to 0.4
- attn_gain: bfloat16 [2048], P(('dp', 'ctx')), may hold values from 0.5 to 1.5
- ffn_gain: bfloat16 [2048], P(('dp', 'ctx')), may hold values from 0.5 to 1.5
- query_gain: bfloat16 [128], P(('dp', 'ctx')), may hold values from 0.5 to 1.5
- key_gain: bfloat16 [128], P(('dp', 'ctx')), may hold values from 0.5 to 1.5
- w_query: bfloat16 [2048, 4096], P(('dp', 'ctx')), may hold values from -0.125 to 0.125
- w_key: bfloat16 [2048, 512], P(('dp', 'ctx')), may hold values from -0.125 to 0.125
- w_value: bfloat16 [2048, 512], P(('dp', 'ctx')), may hold values from -0.125 to 0.125
- w_out: bfloat16 [4096, 2048], P(('dp', 'ctx')), may hold values from -1 to 1
- w_gate: bfloat16 [16, 2048, 768], P('ctx', 'dp'), may hold values from -0.125 to 0.125
- w_up: bfloat16 [16, 2048, 768], P('ctx', 'dp'), may hold values from -0.125 to 0.125
- w_down: bfloat16 [16, 768, 2048], P('ctx', None, 'dp'), may hold values from -0.875 to 0.875
- out_grad: bfloat16 [4, 2048, 2048], P('dp', 'ctx'), may hold values from -6 to 6
Outputs:
- layer_output: bfloat16 [4, 2048, 2048], P('dp', 'ctx')
- input_grad: float32 [4, 2048, 2048], P('dp', 'ctx')
- attn_gain_grad: float32 [2048], P(('dp', 'ctx'))
- ffn_gain_grad: float32 [2048], P(('dp', 'ctx'))
- query_gain_grad: float32 [128], P(('dp', 'ctx'))
- key_gain_grad: float32 [128], P(('dp', 'ctx'))
- w_query_grad: float32 [2048, 4096], P(('dp', 'ctx'))
- w_key_grad: float32 [2048, 512], P(('dp', 'ctx'))
- w_value_grad: float32 [2048, 512], P(('dp', 'ctx'))
- w_out_grad: float32 [4096, 2048], P(('dp', 'ctx'))
- w_gate_grad: float32 [16, 2048, 768], P('ctx', 'dp')
- w_up_grad: float32 [16, 2048, 768], P('ctx', 'dp')
- w_down_grad: float32 [16, 768, 2048], P('ctx', None, 'dp')
The draws below stay inside these ranges and needn't reach their ends.
Inputs may be any that keep to these rules, and one draw needn't show every extreme that they name: `doc_ids`: in each sequence the document numbers never fall; each document has 1 to 1024 tokens, some exactly 1024. `route_ids`: each token names 8 different experts; among the tokens of one device no expert is named more than 144 times, and in every draw some expert exactly 144 times.
All inputs are finite; a program needn't handle non-finite values.
Results may differ from the reference program's by a relative error of at most 0.017.
Values may be sent and summed in bfloat16 or wider, within the bound.
A program may use at most 384 MiB of HBM per device.

```python
import math
import jax
import jax.numpy as jnp
import numpy as np
from jax import lax

D = 2048
HQ = 32
KV = 4
HD = 128
FF = 768
TOP = 8
TOK_DEV = 256
MOST = 1024
LENGTH = 2048
SEQS = 4
EXPERTS = 16
CAP = 144
DOCS = 4


def strengthened(result, rng, source, target, parts, factor):
    def block_of(axis_at):
        return (jnp.arange(result.shape[axis_at]) // (result.shape[axis_at] // parts)).reshape((-1,) + (1,) * (result.ndim - 1 - axis_at))

    first = jax.random.permutation(rng, parts)[block_of(target)]
    far = (block_of(target) + parts // 2) % parts
    return jnp.where((block_of(source) == first) | (block_of(source) == far), factor * result, result)


def levels(stream_key, extent, cuts, low, top_value):
    level, own = 1.0, jax.random.fold_in(stream_key, 6)
    for position, shards_of in cuts:
        draws = jnp.exp(jax.random.uniform(jax.random.fold_in(own, position), (shards_of,), jnp.float32, low / len(cuts), top_value / len(cuts)))
        level = level * jnp.repeat(draws, extent[position] // shards_of).reshape([-1 if axis == position else 1 for axis in range(len(extent))])
    return level


def length_profile(count, total, limit, lean):
    portions = [(1 << 20) // math.isqrt(grade ** lean) + 1 for grade in range(2, count + 1)]
    spare, given = total - limit - (count - 1), [1] * (count - 1)
    while spare > 0:
        free = [i for i in range(count - 1) if given[i] < limit]
        whole, remaining = sum([portions[i] for i in free]), spare
        for i in free:
            more = min(limit - given[i], max(1, remaining * portions[i] // whole), spare)
            given[i] = given[i] + more
            spare = spare - more
    return np.array([limit] + given)


def uneven(key, amount, total, bound, skew):
    if amount == 2:
        one = jax.random.randint(key, (), max(1, total - bound), min(bound, total - 1) + 1)
        return jnp.stack([one, total - one])
    sizes = jnp.asarray(length_profile(amount, total, bound, skew), jnp.int32)
    pairs = (amount - 1) // 2
    donor, sink = sizes[1:1 + 2 * pairs:2], sizes[2:2 + 2 * pairs:2]
    room = jnp.minimum(donor - 1, bound - sink)
    moved = jax.random.randint(jax.random.fold_in(key, 1), (pairs,), 0, 1 << 20) % (room + 1)
    sizes = sizes.at[1:1 + 2 * pairs:2].set(donor - moved).at[2:2 + 2 * pairs:2].set(sink + moved)
    return sizes[jax.random.permutation(jax.random.fold_in(key, 2), amount)]


def deal_out(key, own, number, rows, number_of, top, reach, skew):
    ranking = jax.random.permutation(key, number_of)
    packed, usual = shares(number_of, rows * top, reach, skew, True), shares(number_of, rows * top, reach, skew, False)
    places = jnp.arange(number_of)

    def named(tallies, offset_by):
        used = int((tallies > 0).sum())
        fixed = max(1, used // 4)
        moved = fixed + (places - fixed + offset_by * (used - fixed)) % max(1, number_of - fixed)
        return jnp.zeros((number_of,), jnp.int32).at[ranking[jnp.where(places < fixed, places, moved)]].set(jnp.asarray(tallies, jnp.int32))

    tallies = jnp.where(number % 4 == 0, named(packed, number // 4), named(usual, number - number // 4 - 1))
    mixed = jax.random.permutation(jax.random.fold_in(own, 3), number_of)
    giver, sink = mixed[0:number_of // 2 * 2:2], mixed[1:number_of // 2 * 2:2]
    room = jnp.minimum(tallies[giver] - 1, reach - tallies[sink]) // 2
    room = jnp.where((giver == ranking[0]) | (sink == ranking[0]) | (tallies[sink] == 0), 0, jnp.maximum(room, 0))
    moved = jax.random.randint(jax.random.fold_in(own, 4), (number_of // 2,), 0, 1 << 20) % (room + 1)
    tallies = tallies.at[giver].add(-moved).at[sink].add(moved)
    labels = jnp.searchsorted(jnp.cumsum(tallies), jnp.arange(rows * top), side="right").astype(jnp.int32)
    listing = labels.reshape(top, rows).T
    listing = listing[jax.random.permutation(jax.random.fold_in(own, 1), rows)]
    offset_by = jax.random.randint(jax.random.fold_in(own, 2), (rows, 1), 0, top)
    return jnp.take_along_axis(listing, (jnp.arange(top)[None, :] + offset_by) % top, axis=1)


def shares(number_of, total, reach, lean, full):
    loads = [(1 << 20) // math.isqrt(rank ** lean) + 1 for rank in range(1, number_of + 1)]
    largest = reach if full else min(reach, max(-(-total // number_of), total * loads[0] // sum(loads)))
    least = 1 if total - largest >= number_of - 1 else 0
    counts, rest = [largest] + [least] * (number_of - 1), total - largest - least * (number_of - 1)
    while rest > 0:
        free = [i for i in range(1, number_of) if counts[i] < largest] or [i for i in range(1, number_of) if counts[i] < reach]
        mass, remaining = sum([loads[i] for i in free]), rest
        for i in free:
            addition = min(reach - counts[i], max(1, remaining * loads[i] // mass), rest)
            counts[i] = counts[i] + addition
            rest = rest - addition
    return np.array(counts)


def bell_draw(stream_key, dims, scale, reach, cuts=(), kind=jnp.bfloat16):
    array = jax.random.normal(stream_key, dims, jnp.float32) * scale
    if len(cuts) > 0:
        array = levels(stream_key, dims, cuts, -0.22, 0.18) * array
    return jnp.clip(array, min=-reach, max=reach).astype(kind)


def bell_draw_with(key, dims, spread, reach, cuts, heavy, kind=jnp.bfloat16):
    result = spread * jax.random.normal(key, dims, jnp.float32)
    if cuts:
        result = result * levels(key, dims, cuts, -0.22, 0.18)
    return jnp.clip(strengthened(result, jax.random.fold_in(key, 3), *heavy), -reach, reach).astype(kind)


def setup_inputs(seed: int = 0) -> dict:
    key_list = jax.random.split(jax.random.key(seed), 17)
    layer_input = bell_draw_with(key_list[0], (SEQS, LENGTH, D), 1.0, 6.0, ((0, 4), (1, 8)), (1, 2, 8, 2.0))
    doc_ids = jax.vmap(lambda own: jnp.searchsorted(jnp.cumsum(uneven(own, DOCS, LENGTH, MOST, 2)), jnp.arange(LENGTH), side="right"))(jax.random.split(key_list[1], SEQS)).reshape((SEQS, LENGTH)).astype(jnp.int32)
    route_ids_keys = jax.random.split(jax.random.fold_in(key_list[2], 1), SEQS * LENGTH // TOK_DEV)
    route_ids_turns = jax.random.permutation(jax.random.fold_in(key_list[2], 3), SEQS * LENGTH // TOK_DEV)
    route_ids = jax.vmap(lambda own, number: deal_out(jax.random.fold_in(key_list[2], 2), own, number, TOK_DEV, EXPERTS, TOP, CAP, 1))(route_ids_keys, route_ids_turns).reshape((SEQS, LENGTH, TOP))
    route_probs = jnp.clip(jnp.exp(math.log(0.4) - 2.3025851 * jax.random.uniform(key_list[3], (SEQS, LENGTH, TOP), jnp.float32) ** levels(key_list[3], (SEQS, LENGTH, TOP), ((0, 4), (1, 8)), -0.2, 0.2)), 0.04, 0.4)
    attn_gain = jnp.clip(1.0 + 0.1 * jax.random.normal(key_list[4], (D,), jnp.float32), 0.5, 1.5).astype(jnp.bfloat16)
    ffn_gain = jnp.clip(1.0 + 0.1 * jax.random.normal(key_list[5], (D,), jnp.float32), 0.5, 1.5).astype(jnp.bfloat16)
    query_gain = jnp.clip(1.0 + 0.1 * jax.random.normal(key_list[6], (HD,), jnp.float32), 0.5, 1.5).astype(jnp.bfloat16)
    key_gain = jnp.clip(1.0 + 0.1 * jax.random.normal(key_list[7], (HD,), jnp.float32), 0.5, 1.5).astype(jnp.bfloat16)
    w_query = bell_draw(key_list[8], (D, HQ * HD), D ** -0.5, 0.125, ((0, 32),))
    w_key = bell_draw(key_list[9], (D, KV * HD), D ** -0.5, 0.125, ((0, 32),))
    w_value = bell_draw(key_list[10], (D, KV * HD), D ** -0.5, 0.125, ((0, 32),))
    w_out = bell_draw(key_list[11], (HQ * HD, D), (HQ * HD // 128) ** -0.5, 1.0, ((0, 32),))
    w_gate = bell_draw(key_list[12], (EXPERTS, D, FF), D ** -0.5, 0.125, ((0, 8), (1, 4)))
    w_up = bell_draw(key_list[13], (EXPERTS, D, FF), D ** -0.5, 0.125, ((0, 8), (1, 4)))
    w_down = bell_draw(key_list[14], (EXPERTS, FF, D), (FF // 16) ** -0.5, 0.875, ((0, 8), (2, 4)))
    out_grad = bell_draw(key_list[15], (SEQS, LENGTH, D), 1.0, 6.0, ((0, 4), (1, 8)))
    return dict(layer_input=layer_input, doc_ids=doc_ids, route_ids=route_ids, route_probs=route_probs, attn_gain=attn_gain, ffn_gain=ffn_gain, query_gain=query_gain, key_gain=key_gain, w_query=w_query, w_key=w_key, w_value=w_value, w_out=w_out, w_gate=w_gate, w_up=w_up, w_down=w_down, out_grad=out_grad)


EPS = 1e-06
ROPE_BASE = 1000000.0
HIGH = lax.Precision.HIGHEST

@jax.custom_vjp
def low(v):
    return lax.optimization_barrier(v.astype(jnp.bfloat16)).astype(jnp.float32)

@jax.custom_vjp
def low_back(v):
    return v

def low_keep(v):
    return (low(v), None)

def low_pass(kept, grad):
    return (grad,)

def back_keep(v):
    return (v, None)

def back_low(kept, grad):
    return (low(grad),)
low.defvjp(low_keep, low_pass)
low_back.defvjp(back_keep, back_low)

def rms_scale(values, gain):
    return values * lax.rsqrt(lax.optimization_barrier(jnp.mean(values * values, axis=-1, keepdims=True)) + EPS) * gain

def rotate_heads(values, cosine, sine):
    half_width = values.shape[-1] // 2
    first_half = values[..., :half_width]
    second_half = values[..., half_width:]
    cos_b = cosine[:, None, :]
    sin_b = sine[:, None, :]
    return jnp.concatenate([first_half * cos_b - second_half * sin_b, second_half * cos_b + first_half * sin_b], axis=-1)

def matmul(left, right):
    return jnp.dot(left, right, precision=HIGH)

def attend(query_rot, key_rot, value_in, doc_seq):
    length = query_rot.shape[0]
    block = min(512, length)
    per_group = HQ // KV
    score_scale = 1.0 / math.sqrt(HD)
    key_wide = jnp.repeat(key_rot, per_group, axis=1)
    value_wide = jnp.repeat(value_in, per_group, axis=1)
    key_index = jnp.arange(length, dtype=jnp.int32)

    def one_block(start):
        query_blk = lax.dynamic_slice_in_dim(query_rot, start, block, 0)
        doc_blk = lax.dynamic_slice_in_dim(doc_seq, start, block, 0)
        query_index = start + jnp.arange(block, dtype=jnp.int32)
        scores = low_back(jnp.einsum('thd,shd->hts', query_blk, key_wide, precision=HIGH) * score_scale)
        allowed = (doc_blk[:, None] == doc_seq[None, :]) & (key_index[None, :] <= query_index[:, None])
        expo = jnp.where(allowed[None], jnp.exp(scores), 0.0)
        row_total = lax.optimization_barrier(jnp.sum(expo, axis=-1))
        summed = low_back(jnp.einsum('hts,shd->thd', low(expo), value_wide, precision=HIGH))
        return summed / jnp.transpose(row_total)[:, :, None]
    starts = jnp.arange(length // block, dtype=jnp.int32) * block
    pieces = lax.map(jax.checkpoint(one_block), starts)
    return pieces.reshape(length, HQ * HD)

def layer(weights, inputs, doc_seq, route_seq, prob_seq):
    attn_gain, ffn_gain, query_gain, key_gain, w_query, w_key, w_value, w_out, w_gate, w_up, w_down = weights
    length = inputs.shape[0]
    normed = low(rms_scale(inputs, attn_gain))
    query_lin = low_back(matmul(normed, w_query)).reshape(length, HQ, HD)
    key_lin = low_back(matmul(normed, w_key)).reshape(length, KV, HD)
    value_lin = low_back(matmul(normed, w_value)).reshape(length, KV, HD)
    positions = jnp.arange(length, dtype=jnp.float32)
    inverse = 1.0 / ROPE_BASE ** (jnp.arange(HD // 2, dtype=jnp.float32) * 2.0 / HD)
    angles = positions[:, None] * inverse[None, :]
    cosine = jnp.cos(angles)
    sine = jnp.sin(angles)
    query_rot = low(rotate_heads(rms_scale(query_lin, query_gain), cosine, sine))
    key_rot = low(rotate_heads(rms_scale(key_lin, key_gain), cosine, sine))
    value_low = low(value_lin)
    attn_low = low(attend(query_rot, key_rot, value_low, doc_seq))
    after_attn = inputs + low_back(matmul(attn_low, w_out))
    normed2 = low(rms_scale(after_attn, ffn_gain))

    def one_expert(running, item):
        expert_id, gate_w, up_w, down_w = item
        route_weight = lax.optimization_barrier(jnp.sum(jnp.where(route_seq == expert_id, prob_seq, 0.0), axis=-1))
        rows_in = low_back(normed2)
        gate_lin = low_back(matmul(rows_in, gate_w))
        up_lin = low_back(matmul(rows_in, up_w))
        act_low = low(jax.nn.silu(gate_lin) * up_lin)
        out_rows = low(low_back(matmul(act_low, down_w)))
        return (running + route_weight[:, None] * out_rows, None)
    moe_out, unused = lax.scan(jax.checkpoint(one_expert), jnp.zeros_like(after_attn), (jnp.arange(EXPERTS, dtype=jnp.int32), w_gate, w_up, w_down))
    return after_attn + moe_out

def reference(layer_input, doc_ids, route_ids, route_probs, attn_gain, ffn_gain, query_gain, key_gain, w_query, w_key, w_value, w_out, w_gate, w_up, w_down, out_grad):
    weights = (attn_gain.astype(jnp.float32), ffn_gain.astype(jnp.float32), query_gain.astype(jnp.float32), key_gain.astype(jnp.float32), w_query.astype(jnp.float32), w_key.astype(jnp.float32), w_value.astype(jnp.float32), w_out.astype(jnp.float32), w_gate.astype(jnp.float32), w_up.astype(jnp.float32), w_down.astype(jnp.float32))

    def forward(weight_set, inputs):

        def one_seq(carry, item):
            return (carry, jax.checkpoint(layer)(weight_set, item[0], item[1], item[2], item[3]))
        carry, outputs = lax.scan(one_seq, jnp.zeros((), jnp.float32), (inputs, doc_ids, route_ids, route_probs))
        return outputs
    outputs, pull = jax.vjp(forward, weights, layer_input.astype(jnp.float32))
    weight_grads, input_grad = pull(out_grad.astype(jnp.float32))
    return (outputs.astype(jnp.bfloat16), input_grad, weight_grads[0], weight_grads[1], weight_grads[2], weight_grads[3], weight_grads[4], weight_grads[5], weight_grads[6], weight_grads[7], weight_grads[8], weight_grads[9], weight_grads[10])
```

```python
import functools
import math

import jax
import jax.numpy as jnp
from jax import lax
from jax.experimental import pallas as pl
from jax.experimental.pallas import tpu as pltpu
from jax.sharding import PartitionSpec as P

HQ = 32
KV = 4
HD = 128
TOP = 8
MOST = 1024
EPS = 1e-06
ROPE_BASE = 1000000.0
F32 = jnp.float32
BF16 = jnp.bfloat16
SCALE = 1.0 / math.sqrt(HD)
VMEM_LIMIT = 60 * 1024 * 1024


def dot(left, right, dims=((1,), (0,))):
    return lax.dot_general(left, right, (dims, ((), ())), preferred_element_type=F32)


NT = ((1,), (1,))
TN = ((0,), (0,))


def rms_parts(values):
    return lax.rsqrt(jnp.mean(values * values, axis=-1, keepdims=True) + EPS)


def rms_back(grad, unit, inv, gain):
    scaled = grad * gain
    return inv * (scaled - unit * jnp.mean(scaled * unit, axis=-1, keepdims=True))


def head_forward(lin, gain, cosine, sine):
    unit = lin * rms_parts(lin) * gain
    return unit * cosine + pltpu.roll(unit, HD // 2, 1) * sine


def head_backward(lin, gain, cosine, sine, rot_grad):
    grad = rot_grad * cosine + pltpu.roll(rot_grad * sine, HD // 2, 1)
    inv = rms_parts(lin)
    unit = lin * inv
    return rms_back(grad, unit, inv, gain), jnp.sum(grad * unit, axis=0, keepdims=True)


def attn_forward_kernel(
    heads,
    back,
    normed_ref,
    wqkv_ref,
    wout_ref,
    cos_ref,
    sin_ref,
    qgain_ref,
    kgain_ref,
    docc_ref,
    docr_ref,
    qlin_ref,
    klin_ref,
    q_ref,
    k_ref,
    v_ref,
    attn_ref,
    total_ref,
    part_ref,
    acc_ref,
    sum_ref,
):
    step = pl.program_id(0)
    rows = normed_ref.shape[0]
    lin = dot(normed_ref[...], wqkv_ref[...])
    here = pl.ds(step * rows, rows)
    cosine = cos_ref[...]
    sine = sin_ref[...]
    qw = heads * HD
    for head in range(heads):
        cols = slice(head * HD, (head + 1) * HD)
        part = lin[:, cols]
        qlin_ref[:, cols] = part
        q_ref[:, cols] = head_forward(part, qgain_ref[...], cosine, sine).astype(BF16)
    key_lin = lin[:, qw : qw + HD]
    klin_ref[...] = key_lin
    k_ref[here, :] = head_forward(key_lin, kgain_ref[...], cosine, sine).astype(BF16)
    v_ref[here, :] = lin[:, qw + HD :].astype(BF16)
    acc_ref[...] = jnp.zeros_like(acc_ref)
    sum_ref[...] = jnp.zeros_like(sum_ref)
    row_pos = step * rows + lax.broadcasted_iota(jnp.int32, (rows, rows), 0)
    col_off = lax.broadcasted_iota(jnp.int32, (rows, rows), 1)

    def one(block, carry):
        at = pl.ds(pl.multiple_of(block * rows, rows), rows)
        key = k_ref[at, :]
        val = v_ref[at, :]
        allowed = (docc_ref[...] == docr_ref[:, at]) & (block * rows + col_off <= row_pos)
        for head in range(heads):
            cols = slice(head * HD, (head + 1) * HD)
            score = dot(q_ref[:, cols], key, NT) * SCALE
            expo = jnp.where(allowed, jnp.exp(score), 0.0)
            folded = expo[:, :HD]
            for piece in range(1, rows // HD):
                folded = folded + expo[:, piece * HD : (piece + 1) * HD]
            sum_ref[:, cols] += folded
            acc_ref[:, cols] += dot(expo.astype(BF16), val)
        return carry

    lax.fori_loop(jnp.maximum(step - back, 0), step + 1, one, 0)
    lane = lax.broadcasted_iota(jnp.int32, (rows, HD), 1)
    totals = jnp.ones((rows, HD), F32)
    for head in range(heads):
        cols = slice(head * HD, (head + 1) * HD)
        total = jnp.sum(sum_ref[:, cols], axis=-1, keepdims=True)
        totals = jnp.where(lane == head, total, totals)
        attn_ref[:, cols] = (acc_ref[:, cols] / total).astype(BF16)
    total_ref[...] = totals
    part_ref[...] = dot(attn_ref[...], wout_ref[...]).astype(BF16)


def attn_forward(normed, wqkv, wout, cosine, sine, qgain, kgain, doc, rows):
    length, width = normed.shape
    qw = wout.shape[0]
    heads = qw // HD
    blk = lambda cols: pl.BlockSpec((rows, cols), lambda i: (i, 0))
    whole = lambda shape: pl.BlockSpec(shape, lambda i: (0, 0))
    shape = jax.ShapeDtypeStruct
    return pl.pallas_call(
        functools.partial(attn_forward_kernel, heads, MOST // rows),
        grid=(length // rows,),
        in_specs=[
            blk(width),
            whole(wqkv.shape),
            whole(wout.shape),
            blk(HD),
            blk(HD),
            whole((1, HD)),
            whole((1, HD)),
            blk(1),
            whole((1, length)),
        ],
        out_specs=[
            blk(qw),
            blk(HD),
            blk(qw),
            whole((length, HD)),
            whole((length, HD)),
            blk(qw),
            blk(HD),
            blk(width),
        ],
        out_shape=[
            shape((length, qw), F32),
            shape((length, HD), F32),
            shape((length, qw), BF16),
            shape((length, HD), BF16),
            shape((length, HD), BF16),
            shape((length, qw), BF16),
            shape((length, HD), F32),
            shape((length, width), BF16),
        ],
        scratch_shapes=[pltpu.VMEM((rows, qw), F32), pltpu.VMEM((rows, qw), F32)],
        compiler_params=pltpu.CompilerParams(vmem_limit_bytes=VMEM_LIMIT),
        name="attn_forward",
    )(normed, wqkv, wout, cosine, sine, qgain, kgain, doc[:, None], doc[None, :])


def attn_backward_kernel(
    heads,
    back,
    branch_ref,
    wout_ref,
    attn_ref,
    total_ref,
    q_ref,
    k_ref,
    v_ref,
    qlin_ref,
    klin_ref,
    cos_ref,
    sin_ref,
    qgain_ref,
    kgain_ref,
    docc_ref,
    docr_ref,
    dq_ref,
    dkv_ref,
    gains_ref,
    dk_ref,
    dv_ref,
    dqa_ref,
):
    step = pl.program_id(0)
    rows = branch_ref.shape[0]
    here = pl.ds(pl.multiple_of(step * rows, rows), rows)

    @pl.when(step == 0)
    def _():
        gains_ref[...] = jnp.zeros_like(gains_ref)

    dk_ref[here, :] = jnp.zeros((rows, HD), F32)
    dv_ref[here, :] = jnp.zeros((rows, HD), F32)
    dqa_ref[...] = jnp.zeros_like(dqa_ref)
    attn_grad = dot(branch_ref[...], wout_ref[...], NT)
    grads = []
    shifts = []
    for head in range(heads):
        cols = slice(head * HD, (head + 1) * HD)
        part = attn_grad[:, cols]
        inv_total = 1.0 / total_ref[:, head : head + 1]
        delta = jnp.sum(part * attn_ref[:, cols].astype(F32), axis=-1, keepdims=True)
        grads.append((part * inv_total).astype(BF16))
        shifts.append(delta * inv_total)
    row_pos = step * rows + lax.broadcasted_iota(jnp.int32, (rows, rows), 0)
    col_off = lax.broadcasted_iota(jnp.int32, (rows, rows), 1)

    def one(block, carry):
        at = pl.ds(pl.multiple_of(block * rows, rows), rows)
        key = k_ref[at, :]
        val = v_ref[at, :]
        allowed = (docc_ref[...] == docr_ref[:, at]) & (block * rows + col_off <= row_pos)
        dk = jnp.zeros((rows, HD), F32)
        dv = jnp.zeros((rows, HD), F32)
        for head in range(heads):
            cols = slice(head * HD, (head + 1) * HD)
            query = q_ref[:, cols]
            score = dot(query, key, NT) * SCALE
            expo = jnp.where(allowed, jnp.exp(score), 0.0)
            prod = dot(grads[head], val, NT)
            score_grad = (expo * (prod - shifts[head])).astype(BF16)
            dv += dot(expo.astype(BF16), grads[head], TN)
            dk += dot(score_grad, query, TN)
            dqa_ref[:, cols] += dot(score_grad, key)
        dk_ref[at, :] += dk
        dv_ref[at, :] += dv
        return carry

    lax.fori_loop(jnp.maximum(step - back, 0), step + 1, one, 0)
    cosine = cos_ref[here, :]
    sine = sin_ref[here, :]
    for head in range(heads):
        cols = slice(head * HD, (head + 1) * HD)
        grad, gain_part = head_backward(
            qlin_ref[:, cols], qgain_ref[...], cosine, sine, dqa_ref[:, cols] * SCALE
        )
        dq_ref[:, cols] = grad.astype(BF16)
        gains_ref[0:1, :] += gain_part

    @pl.when(step == pl.num_programs(0) - 1)
    def _():
        def finish(block, carry):
            at = pl.ds(pl.multiple_of(block * rows, rows), rows)
            grad, gain_part = head_backward(
                klin_ref[at, :], kgain_ref[...], cos_ref[at, :], sin_ref[at, :], dk_ref[at, :] * SCALE
            )
            dkv_ref[at, :HD] = grad.astype(BF16)
            dkv_ref[at, HD:] = dv_ref[at, :].astype(BF16)
            gains_ref[1:2, :] += gain_part
            return carry

        lax.fori_loop(0, pl.num_programs(0), finish, 0)


def attn_backward(branch, wout, attn, total, q, k, v, qlin, klin, cosine, sine, qgain, kgain, doc, rows):
    length, width = branch.shape
    qw = wout.shape[0]
    heads = qw // HD
    blk = lambda cols: pl.BlockSpec((rows, cols), lambda i: (i, 0))
    whole = lambda shape: pl.BlockSpec(shape, lambda i: (0, 0))
    shape = jax.ShapeDtypeStruct
    full = whole((length, HD))
    return pl.pallas_call(
        functools.partial(attn_backward_kernel, heads, MOST // rows),
        grid=(length // rows,),
        in_specs=[
            blk(width),
            whole(wout.shape),
            blk(qw),
            blk(HD),
            blk(qw),
            full,
            full,
            blk(qw),
            full,
            full,
            full,
            whole((1, HD)),
            whole((1, HD)),
            blk(1),
            whole((1, length)),
        ],
        out_specs=[blk(qw), whole((length, 2 * HD)), whole((8, HD))],
        out_shape=[
            shape((length, qw), BF16),
            shape((length, 2 * HD), BF16),
            shape((8, HD), F32),
        ],
        scratch_shapes=[
            pltpu.VMEM((length, HD), F32),
            pltpu.VMEM((length, HD), F32),
            pltpu.VMEM((rows, qw), F32),
        ],
        compiler_params=pltpu.CompilerParams(vmem_limit_bytes=VMEM_LIMIT),
        name="attn_backward",
    )(branch, wout, attn, total, q, k, v, qlin, klin, cosine, sine, qgain, kgain, doc[:, None], doc[None, :])


MESH = pl.DeviceIdType.MESH
ANY = pl.BlockSpec(memory_space=pl.ANY)
VM = pl.BlockSpec(memory_space=pltpu.VMEM)
DMA = pltpu.SemaphoreType.DMA
CHUNK = 32


def flip(index, mask, count):
    result, bit = 0, 1
    while bit < count:
        digit = (index // bit) % 2
        result = result + bit * ((1 - digit) if mask & bit else digit)
        bit *= 2
    return result


def push(src, dst, send, recv, axis, peer):
    return pltpu.make_async_remote_copy(
        src_ref=src,
        dst_ref=dst,
        send_sem=send,
        recv_sem=recv,
        device_id={axis: peer},
        device_id_type=MESH,
    )


def meet(peers):
    barrier = pltpu.get_barrier_semaphore()
    for axis, peer in peers:
        pl.semaphore_signal(barrier, inc=1, device_id={axis: peer}, device_id_type=MESH)
    pl.semaphore_wait(barrier, len(peers))


class Plane:
    def __init__(self, n):
        self.n = n
        self.chips = n // 2
        self.me = lax.axis_index("ctx")
        self.core = self.me % 2
        self.chip = self.me // 2
        self.mate = self.me + 1 - 2 * self.core

    def same(self, s):
        return 2 * flip(self.chip, s, self.chips) + self.core

    def meet(self):
        meet([("ctx", self.same(s)) for s in range(1, self.chips)] + [("ctx", self.mate)])


def far_first(chips):
    return sorted(range(1, chips), key=lambda s: -bin(s).count("1"))


class Gather:
    def __init__(self, plane, src, out, send, recv, local):
        self.plane, self.out, self.send, self.recv = plane, out, send, recv
        self.own = pltpu.make_async_copy(src, out.at[plane.me], local)
        self.far = [
            push(src, out.at[plane.me], send.at[s], recv.at[s], "ctx", plane.same(s))
            for s in far_first(plane.chips)
        ]
        self.near = push(src, out.at[plane.me], send.at[0], recv.at[0], "ctx", plane.mate)

    def start(self):
        for copy in self.far:
            copy.start()
        self.near.start()
        self.own.start()

    def forward(self):
        plane, out = self.plane, self.out
        self.passed = []
        for s in sorted(range(1, plane.chips), key=lambda s: bin(s).count("1")):
            block = out.at[plane.same(s)]
            push(block, block, self.send.at[s], self.recv.at[s], "ctx", plane.mate).wait_recv()
            slot = plane.chips + s
            copy = push(block, block, self.send.at[slot], self.recv.at[slot], "ctx", plane.mate)
            copy.start()
            self.passed.append(copy)

    def finish(self):
        for copy in self.far:
            copy.wait_send()
        self.near.wait_send()
        self.near.wait_recv()
        for copy in self.passed:
            copy.wait_send()
            copy.wait_recv()
        self.own.wait()


def gather_sems(n):
    return [DMA((n,)), DMA((n,)), DMA(())]


def by_rows(rows, body):
    def one(index, carry):
        body(pl.ds(pl.multiple_of(index * CHUNK, CHUNK), CHUNK))
        return carry

    lax.fori_loop(0, rows // CHUNK, one, 0)


class Scatter:
    def __init__(self, plane, part, mine, other, landed, send, recv, local):
        self.plane, self.mine, self.other, self.landed = plane, mine, other, landed
        self.order = far_first(plane.chips) + [0]
        self.loads, self.across, self.far = {}, {}, {}
        mate_core = 1 - plane.core
        for s in self.order:
            block = plane.same(s)
            self.loads[s] = pltpu.make_async_copy(part.at[block], mine.at[s], local.at[s])
            self.across[s] = push(
                part.at[block + mate_core - plane.core],
                other.at[s],
                send.at[s],
                recv.at[s],
                "ctx",
                plane.mate,
            )
            slot = plane.chips + s
            if s:
                self.far[s] = push(
                    mine.at[s], landed.at[s], send.at[slot], recv.at[slot], "ctx", block
                )

    def start(self):
        for s in self.order:
            self.across[s].start()
            self.loads[s].start()

    def run(self):
        rows = self.mine.shape[1]
        mine, other = self.mine, self.other
        for s in self.order:
            self.loads[s].wait()
            self.across[s].wait_recv()
            if s:

                def add(at, s=s):
                    total = mine[s, at, :].astype(F32) + other[s, at, :].astype(F32)
                    mine[s, at, :] = total.astype(BF16)

                by_rows(rows, add)
                self.far[s].start()
        for s in self.order:
            if s:
                self.far[s].wait_recv()

    def total(self, at):
        value = self.mine[0, at, :].astype(F32) + self.other[0, at, :].astype(F32)
        for s in range(1, self.plane.chips):
            value = value + self.landed[s, at, :].astype(F32)
        return value

    def finish(self):
        for s in self.order:
            self.across[s].wait_send()
            if s:
                self.far[s].wait_send()


def scatter_scratch(n, rows, width):
    chips = n // 2
    return [pltpu.VMEM((chips, rows, width), BF16)] * 3 + [DMA((n,)), DMA((n,)), DMA((chips,))]


def comm_call(kernel, ident, name, outs, out_specs, in_specs, scratch, micros, *args):
    return pl.pallas_call(
        kernel,
        out_shape=outs,
        in_specs=in_specs,
        out_specs=out_specs,
        scratch_shapes=scratch,
        compiler_params=pltpu.CompilerParams(
            collective_id=ident, has_side_effects=True, vmem_limit_bytes=VMEM_LIMIT
        ),
        cost_estimate=pl.CostEstimate(
            flops=0, transcendentals=0, bytes_accessed=int(micros * 3.0e6)
        ),
        name=name,
    )(*args)


def swap_all(n, src, out, send, recv, local):
    me = lax.axis_index("ctx")
    own = pltpu.make_async_copy(src.at[me], out.at[me], local)
    own.start()
    copies = []
    for s in range(n - 1, 0, -1):
        peer = flip(me, s, n)
        copies.append(push(src.at[peer], out.at[me], send.at[s], recv.at[s], "ctx", peer))
        copies[-1].start()
    return own, copies


def prep_kernel(n, n_dp, cols_ref, small_ref, out_ref, all_ref, *sems):
    send, recv, local, gsend, grecv, zsend, zrecv = sems
    me, row = lax.axis_index("ctx"), lax.axis_index("dp")
    meet(
        [("ctx", flip(me, s, n)) for s in range(1, n)]
        + [("dp", flip(row, s, n_dp)) for s in range(1, n_dp)]
    )
    all_ref[row, me] = small_ref[...]
    smalls = []
    for s in range(1, n):
        peer = flip(me, s, n)
        smalls.append(push(small_ref, all_ref.at[row, me], gsend.at[s], grecv.at[s], "ctx", peer))
        smalls[-1].start()
    own, copies = swap_all(n, cols_ref, out_ref, send, recv, local)
    for copy in smalls:
        copy.wait_recv()
    planes = []
    for s in range(1, n_dp):
        peer = flip(row, s, n_dp)
        planes.append(push(all_ref.at[row], all_ref.at[row], zsend.at[s], zrecv.at[s], "dp", peer))
        planes[-1].start()
    for copy in copies + planes:
        copy.wait_recv()
    for copy in copies + planes + smalls:
        copy.wait_send()
    own.wait()


def post_kernel(n, n_dp, cols_ref, small_ref, out_ref, sum_ref, first, mid, second, *sems):
    send, recv, local, gsend, grecv, zsend, zrecv = sems
    me, row = lax.axis_index("ctx"), lax.axis_index("dp")
    meet(
        [("ctx", flip(me, s, n)) for s in range(1, n)]
        + [("dp", flip(row, s, n_dp)) for s in range(1, n_dp)]
    )
    smalls = []
    for s in range(1, n):
        peer = flip(me, s, n)
        smalls.append(push(small_ref.at[peer], first.at[s], gsend.at[s], grecv.at[s], "ctx", peer))
        smalls[-1].start()
    own, copies = swap_all(n, cols_ref, out_ref, send, recv, local)
    value = small_ref[me]
    for copy, s in zip(smalls, range(1, n)):
        copy.wait_recv()
        value = value + first[s]
    mid[...] = value
    planes = []
    for s in range(1, n_dp):
        peer = flip(row, s, n_dp)
        planes.append(push(mid.at[peer], second.at[s], zsend.at[s], zrecv.at[s], "dp", peer))
        planes[-1].start()
    value = mid[row]
    for copy, s in zip(planes, range(1, n_dp)):
        copy.wait_recv()
        value = value + second[s]
    sum_ref[...] = value
    for copy in copies:
        copy.wait_recv()
    for copy in copies + planes + smalls:
        copy.wait_send()
    own.wait()


def swap_sems(n, n_dp):
    return [DMA((n,)), DMA((n,)), DMA(()), DMA((n,)), DMA((n,)), DMA((n_dp,)), DMA((n_dp,))]


def prep(n, n_dp, cols, small):
    shape = jax.ShapeDtypeStruct
    return comm_call(
        functools.partial(prep_kernel, n, n_dp),
        0,
        "prep",
        [shape(cols.shape, cols.dtype), shape((n_dp, n) + small.shape, F32)],
        [ANY, VM],
        [ANY, VM],
        swap_sems(n, n_dp),
        8,
        cols,
        small,
    )


def post(n, n_dp, cols, small):
    shape = jax.ShapeDtypeStruct
    tile = small.shape[2:]
    return comm_call(
        functools.partial(post_kernel, n, n_dp),
        1,
        "post",
        [shape(cols.shape, cols.dtype), shape(tile, F32)],
        [ANY, VM],
        [ANY, VM],
        [
            pltpu.VMEM((n, n_dp) + tile, F32),
            pltpu.VMEM((n_dp,) + tile, F32),
            pltpu.VMEM((n_dp,) + tile, F32),
        ]
        + swap_sems(n, n_dp),
        8,
        cols,
        small,
    )


def first_kernel(n, x_ref, gain_ref, grad_ref, info_ref, nall_ref, gall_ref, iall_ref, low, *sems):
    plane = Plane(n)
    plane.meet()
    grads = Gather(plane, grad_ref, gall_ref, *sems[0:3])
    infos = Gather(plane, info_ref, iall_ref, *sems[3:6])
    infos.start()

    def norm(at):
        value = x_ref[at, :].astype(F32)
        low[at, :] = (value * rms_parts(value) * gain_ref[...]).astype(BF16)

    by_rows(x_ref.shape[0], norm)
    normed = Gather(plane, low, nall_ref, *sems[6:9])
    normed.start()
    grads.start()
    infos.forward()
    normed.forward()
    grads.forward()
    for each in (infos, normed, grads):
        each.finish()


def first(n, x, gain, grad, info):
    shape = jax.ShapeDtypeStruct
    many = lambda array, kind: shape((n,) + array.shape, kind)
    return comm_call(
        functools.partial(first_kernel, n),
        2,
        "first",
        [many(x, BF16), many(grad, BF16), many(info, F32)],
        [ANY] * 3,
        [VM] * 4,
        [pltpu.VMEM(x.shape, BF16)] + gather_sems(n) * 3,
        90,
        x,
        gain,
        grad,
        info,
    )


def middle_kernel(n, part_ref, x_ref, gain_ref, after_ref, all_ref, low, *scratch):
    plane = Plane(n)
    plane.meet()
    sums = Scatter(plane, part_ref, *scratch[:6])
    sums.start()
    sums.run()

    def norm(at):
        value = x_ref[at, :].astype(F32) + sums.total(at)
        after_ref[at, :] = value
        low[at, :] = (value * rms_parts(value) * gain_ref[...]).astype(BF16)

    by_rows(x_ref.shape[0], norm)
    normed = Gather(plane, low, all_ref, *scratch[6:])
    normed.start()
    normed.forward()
    sums.finish()
    normed.finish()


def middle(n, part, x, gain):
    shape = jax.ShapeDtypeStruct
    return comm_call(
        functools.partial(middle_kernel, n),
        3,
        "middle",
        [shape(x.shape, F32), shape((n,) + x.shape, BF16)],
        [VM, ANY],
        [ANY, VM, VM],
        [pltpu.VMEM(x.shape, BF16)] + scatter_scratch(n, *x.shape) + gather_sems(n),
        95,
        part,
        x,
        gain,
    )


def turn_kernel(
    n, part_ref, after_ref, grad_ref, gain_ref, mid_ref, fpart_ref, all_ref, low, *scratch
):
    plane = Plane(n)
    plane.meet()
    sums = Scatter(plane, part_ref, *scratch[:6])
    sums.start()
    fpart_ref[...] = jnp.zeros_like(fpart_ref)
    sums.run()

    def norm(at):
        value = after_ref[at, :]
        inv = rms_parts(value)
        unit = value * inv
        grad = sums.total(at)
        fpart_ref[0:1, :] += jnp.sum(grad * unit, axis=0, keepdims=True)
        mid = grad_ref[at, :].astype(F32) + rms_back(grad, unit, inv, gain_ref[...])
        mid_ref[at, :] = mid
        low[at, :] = mid.astype(BF16)

    by_rows(after_ref.shape[0], norm)
    branch = Gather(plane, low, all_ref, *scratch[6:])
    branch.start()
    branch.forward()
    sums.finish()
    branch.finish()


def turn(n, part, after, grad, gain):
    shape = jax.ShapeDtypeStruct
    return comm_call(
        functools.partial(turn_kernel, n),
        4,
        "turn",
        [
            shape(after.shape, F32),
            shape((8, after.shape[1]), F32),
            shape((n,) + after.shape, BF16),
        ],
        [VM, VM, ANY],
        [ANY, VM, VM, VM],
        [pltpu.VMEM(after.shape, BF16)] + scatter_scratch(n, *after.shape) + gather_sems(n),
        95,
        part,
        after,
        grad,
        gain,
    )


def last_kernel(n, part_ref, x_ref, mid_ref, gain_ref, out_ref, apart_ref, *scratch):
    plane = Plane(n)
    plane.meet()
    sums = Scatter(plane, part_ref, *scratch[:6])
    sums.start()
    apart_ref[...] = jnp.zeros_like(apart_ref)
    sums.run()

    def norm(at):
        value = x_ref[at, :].astype(F32)
        inv = rms_parts(value)
        unit = value * inv
        grad = sums.total(at)
        apart_ref[0:1, :] += jnp.sum(grad * unit, axis=0, keepdims=True)
        out_ref[at, :] = mid_ref[at, :] + rms_back(grad, unit, inv, gain_ref[...])

    by_rows(x_ref.shape[0], norm)
    sums.finish()


def last(n, part, x, mid, gain):
    shape = jax.ShapeDtypeStruct
    return comm_call(
        functools.partial(last_kernel, n),
        5,
        "last",
        [shape(mid.shape, F32), shape((8, mid.shape[1]), F32)],
        [VM, VM],
        [ANY, VM, VM, VM],
        scatter_scratch(n, *mid.shape),
        50,
        part,
        x,
        mid,
        gain,
    )


def close_kernel(n, part_ref, after_ref, out_ref, *scratch):
    plane = Plane(n)
    plane.meet()
    sums = Scatter(plane, part_ref, *scratch[:6])
    sums.start()
    sums.run()

    def add(at):
        out_ref[at, :] = (after_ref[at, :] + sums.total(at)).astype(BF16)

    by_rows(after_ref.shape[0], add)
    sums.finish()


def close(n, part, after):
    return comm_call(
        functools.partial(close_kernel, n),
        6,
        "close",
        jax.ShapeDtypeStruct(after.shape, BF16),
        VM,
        [ANY, VM],
        scatter_scratch(n, *after.shape),
        50,
        part,
        after,
    )


def scatter_dp(partial):
    return lax.psum_scatter(partial.astype(BF16), "dp", scatter_dimension=0, tiled=True)


def per_device(
    layer_input,
    doc_ids,
    route_ids,
    route_probs,
    attn_gain,
    ffn_gain,
    query_gain,
    key_gain,
    w_query,
    w_key,
    w_value,
    w_out,
    w_gate,
    w_up,
    w_down,
    out_grad,
):
    tokens, width = layer_input.shape[1:]
    n_dp = lax.axis_size("dp")
    n_ctx = lax.axis_size("ctx")
    ctx_index = lax.axis_index("ctx")
    length = tokens * n_ctx
    heads = HQ // n_ctx
    share = n_ctx // KV
    qw = heads * HD
    both = ("dp", "ctx")
    depth = w_query.shape[0]
    own_e = w_gate.shape[0]

    cut = attn_gain.shape[0]
    hcut = query_gain.shape[0]
    kinds = 2 * (cut + hcut)
    small = jnp.concatenate([attn_gain, ffn_gain, query_gain, key_gain]).astype(F32)
    small = jnp.pad(small, (0, 1024 - kinds)).reshape(8, HD)
    cols = jnp.concatenate(
        [
            w_query.reshape(depth, n_ctx, qw),
            jnp.repeat(w_key.reshape(depth, KV, HD), share, axis=1),
            jnp.repeat(w_value.reshape(depth, KV, HD), share, axis=1),
        ],
        axis=2,
    ).transpose(1, 0, 2)
    cols, small = prep(n_ctx, n_dp, cols, small)
    small = small.reshape(n_dp * n_ctx, 1024)
    gain_attn = small[:, :cut].reshape(1, width)
    gain_ffn = small[:, cut : 2 * cut].reshape(1, width)
    gain_query = small[:, 2 * cut : 2 * cut + hcut].reshape(1, HD)
    gain_key = small[:, 2 * cut + hcut : kinds].reshape(1, HD)
    wqkv = lax.all_gather(cols.reshape(n_ctx * depth, qw + 2 * HD), "dp", axis=0, tiled=True)
    forth = [(c * n_dp + d, d * n_ctx + c) for d in range(n_dp) for c in range(n_ctx)]
    wout = lax.all_gather(lax.ppermute(w_out, both, forth), "dp", axis=0, tiled=True)

    inputs = layer_input.reshape(tokens, width)
    top_own = out_grad.reshape(tokens, width)
    n_experts = own_e * n_ctx
    match = route_ids.reshape(1, tokens, TOP) == jnp.arange(n_experts, dtype=jnp.int32)[:, None, None]
    probs = jnp.sum(jnp.where(match, route_probs.reshape(1, tokens, TOP), 0.0), axis=2)
    info = jnp.concatenate(
        [probs, doc_ids.reshape(1, tokens).astype(F32), jnp.zeros((7, tokens), F32)], axis=0
    )
    normed, top_all, info = first(n_ctx, inputs, gain_attn, top_own, info)
    normed = normed.reshape(length, width)
    top_all = top_all.reshape(length, width)
    doc = info[:, n_experts].reshape(length).astype(jnp.int32)
    my_probs = lax.dynamic_slice_in_dim(info, ctx_index * own_e, own_e, 1)
    my_probs = my_probs.transpose(0, 2, 1).reshape(length, own_e)

    inverse = 1.0 / ROPE_BASE ** (jnp.arange(HD // 2, dtype=F32) * 2.0 / HD)
    angles = jnp.arange(length, dtype=F32)[:, None] * inverse[None, :]
    cosine = jnp.cos(angles)
    sine = jnp.sin(angles)
    cosine = jnp.concatenate([cosine, cosine], axis=1)
    sine = jnp.concatenate([-sine, sine], axis=1)
    qlin, klin, q, k, v, attn, total, part = attn_forward(
        normed, wqkv, wout, cosine, sine, gain_query, gain_key, doc, tokens
    )
    blocks = (n_ctx, tokens, width)
    after, normed2 = middle(n_ctx, part.reshape(blocks), inputs, gain_ffn)
    normed2 = normed2.reshape(length, width)

    moe = 0.0
    row_sum = 0.0
    expert_grads = []
    for e in range(own_e):
        wg = lax.all_gather(w_gate[e], "dp", axis=0, tiled=True)
        wu = lax.all_gather(w_up[e], "dp", axis=0, tiled=True)
        wd = lax.all_gather(w_down[e], "dp", axis=0, tiled=False)
        prob = my_probs[:, e : e + 1]
        gate = dot(normed2, wg)
        up = dot(normed2, wu)
        sig = jax.nn.sigmoid(gate)
        silu = gate * sig
        act = (silu * up).astype(BF16)
        out = jnp.einsum("rf,zfd->rzd", act, wd, preferred_element_type=F32).astype(BF16)
        moe = moe + prob * out.reshape(length, width).astype(F32)
        route_grad = (top_all.astype(F32) * prob).astype(BF16)
        route3 = route_grad.reshape(length, n_dp, width // n_dp)
        act_grad = jnp.einsum("rzd,zfd->rf", route3, wd, preferred_element_type=F32)
        down_grad = jnp.einsum("rf,rzd->zfd", act, route3, preferred_element_type=F32)
        gate_grad = (act_grad * up * sig * (1.0 + gate * (1.0 - sig))).astype(BF16)
        up_grad = (act_grad * silu).astype(BF16)
        row_sum = row_sum + dot(gate_grad, wg, NT) + dot(up_grad, wu, NT)
        raw = (
            dot(normed2, gate_grad, TN).astype(BF16),
            dot(normed2, up_grad, TN).astype(BF16),
            down_grad.astype(BF16),
        )
        raw, normed2, top_all = lax.optimization_barrier((raw, normed2, top_all))
        expert_grads.append((scatter_dp(raw[0]), scatter_dp(raw[1]), scatter_dp(raw[2])[0]))
    mid, ffn_part, branch = turn(
        n_ctx, row_sum.astype(BF16).reshape(blocks), after, top_own, gain_ffn
    )
    branch = branch.reshape(length, width)
    layer_output = close(n_ctx, moe.astype(BF16).reshape(blocks), after)

    dq, dkv, gains = attn_backward(
        branch, wout, attn, total, q, k, v, qlin, klin, cosine, sine, gain_query, gain_key, doc, tokens
    )
    dqkv = jnp.concatenate([dq, dkv], axis=1)
    normed_grad = dot(dqkv, wqkv, NT).astype(BF16).reshape(blocks)
    input_grad, attn_part = last(n_ctx, normed_grad, inputs, mid, gain_attn)

    out_w = scatter_dp(dot(attn, branch, TN))
    out_w = lax.ppermute(out_w, both, [(b, a) for a, b in forth]).astype(F32)
    qkv_w = scatter_dp(dot(normed, dqkv, TN))
    n_all = n_dp * n_ctx
    packed = jnp.concatenate(
        [
            attn_part[0].reshape(n_all, cut),
            ffn_part[0].reshape(n_all, cut),
            gains[0].reshape(n_all, hcut),
            gains[1].reshape(n_all, hcut),
            jnp.zeros((n_all, 1024 - kinds), F32),
        ],
        axis=1,
    )
    packed = packed.reshape(n_dp, n_ctx, 8, HD).transpose(1, 0, 2, 3)
    qkv_w, packed = post(n_ctx, n_dp, qkv_w.reshape(n_ctx, depth, qw + 2 * HD), packed)
    packed = packed.reshape(1024)
    query_w = qkv_w[:, :, :qw].transpose(1, 0, 2).reshape(depth, HQ * HD).astype(F32)
    kv_w = jnp.sum(qkv_w[:, :, qw:].astype(F32).reshape(KV, share, depth, 2 * HD), axis=1)
    key_w = kv_w[:, :, :HD].transpose(1, 0, 2).reshape(depth, KV * HD)
    value_w = kv_w[:, :, HD:].transpose(1, 0, 2).reshape(depth, KV * HD)

    stack = lambda index: jnp.stack([g[index] for g in expert_grads]).astype(F32)
    return (
        layer_output.reshape(1, tokens, width),
        input_grad.reshape(1, tokens, width),
        packed[:cut],
        packed[cut : 2 * cut],
        packed[2 * cut : 2 * cut + hcut],
        packed[2 * cut + hcut : kinds],
        query_w,
        key_w,
        value_w,
        out_w,
        stack(0),
        stack(1),
        stack(2),
    )


def solution(mesh):
    both = ("dp", "ctx")
    seq = P("dp", "ctx", None)
    in_specs = (
        seq,
        P("dp", "ctx"),
        seq,
        seq,
        P(both),
        P(both),
        P(both),
        P(both),
        P(both, None),
        P(both, None),
        P(both, None),
        P(both, None),
        P("ctx", "dp", None),
        P("ctx", "dp", None),
        P("ctx", None, "dp"),
        seq,
    )
    out_specs = (
        seq,
        seq,
        P(both),
        P(both),
        P(both),
        P(both),
        P(both, None),
        P(both, None),
        P(both, None),
        P(both, None),
        P("ctx", "dp", None),
        P("ctx", "dp", None),
        P("ctx", None, "dp"),
    )
    return jax.shard_map(
        per_device, mesh=mesh, in_specs=in_specs, out_specs=out_specs, check_vma=False
    )
```

```python
import functools
import math

import jax
import jax.numpy as jnp
from jax import lax
from jax.experimental import pallas as pl
from jax.experimental.pallas import tpu as pltpu
from jax.sharding import PartitionSpec as P


HQ = 32
KV = 4
HD = 128
TOP = 8
MOST = 1024
EPS = 1e-06
ROPE_BASE = 1000000.0
F32 = jnp.float32
BF16 = jnp.bfloat16
SCALE = 1.0 / math.sqrt(HD)
VMEM_LIMIT = 60 * 1024 * 1024


def dot(left, right, dims=((1,), (0,))):
    return lax.dot_general(left, right, (dims, ((), ())), preferred_element_type=F32)


NT = ((1,), (1,))
TN = ((0,), (0,))


def rms_parts(values):
    return lax.rsqrt(jnp.mean(values * values, axis=-1, keepdims=True) + EPS)


def rms_back(grad, unit, inv, gain):
    scaled = grad * gain
    return inv * (scaled - unit * jnp.mean(scaled * unit, axis=-1, keepdims=True))


def head_forward(lin, gain, cosine, sine):
    unit = lin * rms_parts(lin) * gain
    return unit * cosine + pltpu.roll(unit, HD // 2, 1) * sine


def head_backward(lin, gain, cosine, sine, rot_grad):
    grad = rot_grad * cosine + pltpu.roll(rot_grad * sine, HD // 2, 1)
    inv = rms_parts(lin)
    unit = lin * inv
    return rms_back(grad, unit, inv, gain), jnp.sum(grad * unit, axis=0, keepdims=True)


def attn_forward_kernel(
    heads,
    back,
    normed_ref,
    wqkv_ref,
    cos_ref,
    sin_ref,
    qgain_ref,
    kgain_ref,
    docc_ref,
    docr_ref,
    qlin_ref,
    klin_ref,
    q_ref,
    k_ref,
    v_ref,
    attn_ref,
    total_ref,
    acc_ref,
    sum_ref,
):
    step = pl.program_id(0)
    rows = normed_ref.shape[0]
    lin = dot(normed_ref[...], wqkv_ref[...])
    here = pl.ds(step * rows, rows)
    cosine = cos_ref[...]
    sine = sin_ref[...]
    qw = heads * HD
    for head in range(heads):
        cols = slice(head * HD, (head + 1) * HD)
        part = lin[:, cols]
        qlin_ref[:, cols] = part
        q_ref[:, cols] = head_forward(part, qgain_ref[...], cosine, sine).astype(BF16)
    key_lin = lin[:, qw : qw + HD]
    klin_ref[...] = key_lin
    k_ref[here, :] = head_forward(key_lin, kgain_ref[...], cosine, sine).astype(BF16)
    v_ref[here, :] = lin[:, qw + HD :].astype(BF16)
    acc_ref[...] = jnp.zeros_like(acc_ref)
    sum_ref[...] = jnp.zeros_like(sum_ref)
    row_pos = step * rows + lax.broadcasted_iota(jnp.int32, (rows, rows), 0)
    col_off = lax.broadcasted_iota(jnp.int32, (rows, rows), 1)

    def one(block, carry):
        at = pl.ds(pl.multiple_of(block * rows, rows), rows)
        key = k_ref[at, :]
        val = v_ref[at, :]
        allowed = (docc_ref[...] == docr_ref[:, at]) & (block * rows + col_off <= row_pos)
        for head in range(heads):
            cols = slice(head * HD, (head + 1) * HD)
            score = dot(q_ref[:, cols], key, NT) * SCALE
            expo = jnp.where(allowed, jnp.exp(score), 0.0)
            folded = expo[:, :HD]
            for piece in range(1, rows // HD):
                folded = folded + expo[:, piece * HD : (piece + 1) * HD]
            sum_ref[:, cols] += folded
            acc_ref[:, cols] += dot(expo.astype(BF16), val)
        return carry

    lax.fori_loop(jnp.maximum(step - back, 0), step + 1, one, 0)
    lane = lax.broadcasted_iota(jnp.int32, (rows, HD), 1)
    totals = jnp.ones((rows, HD), F32)
    for head in range(heads):
        cols = slice(head * HD, (head + 1) * HD)
        total = jnp.sum(sum_ref[:, cols], axis=-1, keepdims=True)
        totals = jnp.where(lane == head, total, totals)
        attn_ref[:, cols] = (acc_ref[:, cols] / total).astype(BF16)
    total_ref[...] = totals


def attn_forward(normed, wqkv, cosine, sine, qgain, kgain, doc, rows):
    length, width = normed.shape
    qw = wqkv.shape[1] - 2 * HD
    heads = qw // HD
    blk = lambda cols: pl.BlockSpec((rows, cols), lambda i: (i, 0))
    whole = lambda shape: pl.BlockSpec(shape, lambda i: (0, 0))
    shape = jax.ShapeDtypeStruct
    return pl.pallas_call(
        functools.partial(attn_forward_kernel, heads, MOST // rows),
        grid=(length // rows,),
        in_specs=[
            blk(width),
            whole(wqkv.shape),
            blk(HD),
            blk(HD),
            whole((1, HD)),
            whole((1, HD)),
            blk(1),
            whole((1, length)),
        ],
        out_specs=[
            blk(qw),
            blk(HD),
            blk(qw),
            whole((length, HD)),
            whole((length, HD)),
            blk(qw),
            blk(HD),
        ],
        out_shape=[
            shape((length, qw), F32),
            shape((length, HD), F32),
            shape((length, qw), BF16),
            shape((length, HD), BF16),
            shape((length, HD), BF16),
            shape((length, qw), BF16),
            shape((length, HD), F32),
        ],
        scratch_shapes=[pltpu.VMEM((rows, qw), F32), pltpu.VMEM((rows, qw), F32)],
        compiler_params=pltpu.CompilerParams(vmem_limit_bytes=VMEM_LIMIT),
        cost_estimate=pl.CostEstimate(
            flops=35 * 10**9, transcendentals=0, bytes_accessed=30 * 2**20
        ),
        name="attn_forward",
    )(normed, wqkv, cosine, sine, qgain, kgain, doc[:, None], doc[None, :])


def attn_backward_kernel(
    heads,
    back,
    branch_ref,
    wout_ref,
    attn_ref,
    total_ref,
    q_ref,
    k_ref,
    v_ref,
    qlin_ref,
    klin_ref,
    cos_ref,
    sin_ref,
    qgain_ref,
    kgain_ref,
    docc_ref,
    docr_ref,
    dqkv_ref,
    gains_ref,
    dk_ref,
    dv_ref,
    dqa_ref,
):
    step = pl.program_id(0)
    rows = branch_ref.shape[0]
    here = pl.ds(pl.multiple_of(step * rows, rows), rows)

    @pl.when(step == 0)
    def _():
        gains_ref[...] = jnp.zeros_like(gains_ref)

    dk_ref[here, :] = jnp.zeros((rows, HD), F32)
    dv_ref[here, :] = jnp.zeros((rows, HD), F32)
    dqa_ref[...] = jnp.zeros_like(dqa_ref)
    attn_grad = dot(branch_ref[...], wout_ref[...], NT)
    grads = []
    shifts = []
    for head in range(heads):
        cols = slice(head * HD, (head + 1) * HD)
        part = attn_grad[:, cols]
        inv_total = 1.0 / total_ref[:, head : head + 1]
        delta = jnp.sum(part * attn_ref[:, cols].astype(F32), axis=-1, keepdims=True)
        grads.append((part * inv_total).astype(BF16))
        shifts.append(delta * inv_total)
    row_pos = step * rows + lax.broadcasted_iota(jnp.int32, (rows, rows), 0)
    col_off = lax.broadcasted_iota(jnp.int32, (rows, rows), 1)

    def one(block, carry):
        at = pl.ds(pl.multiple_of(block * rows, rows), rows)
        key = k_ref[at, :]
        val = v_ref[at, :]
        allowed = (docc_ref[...] == docr_ref[:, at]) & (block * rows + col_off <= row_pos)
        dk = jnp.zeros((rows, HD), F32)
        dv = jnp.zeros((rows, HD), F32)
        for head in range(heads):
            cols = slice(head * HD, (head + 1) * HD)
            query = q_ref[:, cols]
            score = dot(query, key, NT) * SCALE
            expo = jnp.where(allowed, jnp.exp(score), 0.0)
            prod = dot(grads[head], val, NT)
            score_grad = (expo * (prod - shifts[head])).astype(BF16)
            dv += dot(expo.astype(BF16), grads[head], TN)
            dk += dot(score_grad, query, TN)
            dqa_ref[:, cols] += dot(score_grad, key)
        dk_ref[at, :] += dk
        dv_ref[at, :] += dv
        return carry

    lax.fori_loop(jnp.maximum(step - back, 0), step + 1, one, 0)
    cosine = cos_ref[here, :]
    sine = sin_ref[here, :]
    for head in range(heads):
        cols = slice(head * HD, (head + 1) * HD)
        grad, gain_part = head_backward(
            qlin_ref[:, cols], qgain_ref[...], cosine, sine, dqa_ref[:, cols] * SCALE
        )
        dqkv_ref[here, cols] = grad.astype(BF16)
        gains_ref[0:1, :] += gain_part

    @pl.when(step == pl.num_programs(0) - 1)
    def _():
        def finish(block, carry):
            at = pl.ds(pl.multiple_of(block * rows, rows), rows)
            grad, gain_part = head_backward(
                klin_ref[at, :], kgain_ref[...], cos_ref[at, :], sin_ref[at, :], dk_ref[at, :] * SCALE
            )
            qw = heads * HD
            dqkv_ref[at, qw : qw + HD] = grad.astype(BF16)
            dqkv_ref[at, qw + HD :] = dv_ref[at, :].astype(BF16)
            gains_ref[1:2, :] += gain_part
            return carry

        lax.fori_loop(0, pl.num_programs(0), finish, 0)


def attn_backward(branch, wout, attn, total, q, k, v, qlin, klin, cosine, sine, qgain, kgain, doc, rows):
    length, width = branch.shape
    qw = wout.shape[0]
    heads = qw // HD
    blk = lambda cols: pl.BlockSpec((rows, cols), lambda i: (i, 0))
    whole = lambda shape: pl.BlockSpec(shape, lambda i: (0, 0))
    shape = jax.ShapeDtypeStruct
    full = whole((length, HD))
    return pl.pallas_call(
        functools.partial(attn_backward_kernel, heads, MOST // rows),
        grid=(length // rows,),
        in_specs=[
            blk(width),
            whole(wout.shape),
            blk(qw),
            blk(HD),
            blk(qw),
            full,
            full,
            blk(qw),
            full,
            full,
            full,
            whole((1, HD)),
            whole((1, HD)),
            blk(1),
            whole((1, length)),
        ],
        out_specs=[whole((length, qw + 2 * HD)), whole((8, HD))],
        out_shape=[
            shape((length, qw + 2 * HD), BF16),
            shape((8, HD), F32),
        ],
        scratch_shapes=[
            pltpu.VMEM((length, HD), F32),
            pltpu.VMEM((length, HD), F32),
            pltpu.VMEM((rows, qw), F32),
        ],
        compiler_params=pltpu.CompilerParams(vmem_limit_bytes=VMEM_LIMIT),
        cost_estimate=pl.CostEstimate(
            flops=60 * 10**9, transcendentals=0, bytes_accessed=30 * 2**20
        ),
        name="attn_backward",
    )(branch, wout, attn, total, q, k, v, qlin, klin, cosine, sine, qgain, kgain, doc[:, None], doc[None, :])


MESH = pl.DeviceIdType.MESH
ANY = pl.BlockSpec(memory_space=pl.ANY)
VM = pl.BlockSpec(memory_space=pltpu.VMEM)
DMA = pltpu.SemaphoreType.DMA
CHUNK = 32


def flip(index, mask, count):
    result, bit = 0, 1
    while bit < count:
        digit = (index // bit) % 2
        result = result + bit * ((1 - digit) if mask & bit else digit)
        bit *= 2
    return result


def push(src, dst, send, recv, axis, peer):
    return pltpu.make_async_remote_copy(
        src_ref=src,
        dst_ref=dst,
        send_sem=send,
        recv_sem=recv,
        device_id={axis: peer},
        device_id_type=MESH,
    )


def meet(peers):
    barrier = pltpu.get_barrier_semaphore()
    for axis, peer in peers:
        pl.semaphore_signal(barrier, inc=1, device_id={axis: peer}, device_id_type=MESH)
    pl.semaphore_wait(barrier, len(peers))


class Plane:
    def __init__(self, n):
        self.chips = n // 2
        self.me = lax.axis_index("ctx")
        self.core = self.me % 2
        self.chip = self.me // 2
        self.mate = self.me + 1 - 2 * self.core

    def same(self, s):
        return 2 * flip(self.chip, s, self.chips) + self.core

    def meet(self):
        meet([("ctx", self.same(s)) for s in range(1, self.chips)] + [("ctx", self.mate)])


def far_first(chips):
    return sorted(range(1, chips), key=lambda s: -bin(s).count("1"))


class Gather:
    def __init__(self, plane, src, out, send, recv, local):
        self.plane, self.out, self.send, self.recv = plane, out, send, recv
        self.own = pltpu.make_async_copy(src, out.at[plane.me], local)
        self.far = [
            push(src, out.at[plane.me], send.at[s], recv.at[s], "ctx", plane.same(s))
            for s in far_first(plane.chips)
        ]
        self.near = push(src, out.at[plane.me], send.at[0], recv.at[0], "ctx", plane.mate)

    def start(self):
        for copy in self.far:
            copy.start()
        self.near.start()
        self.own.start()

    def forward(self):
        plane, out = self.plane, self.out
        self.passed = []
        for s in sorted(range(1, plane.chips), key=lambda s: bin(s).count("1")):
            block = out.at[plane.same(s)]
            push(block, block, self.send.at[s], self.recv.at[s], "ctx", plane.mate).wait_recv()
            slot = plane.chips + s
            copy = push(block, block, self.send.at[slot], self.recv.at[slot], "ctx", plane.mate)
            copy.start()
            self.passed.append(copy)

    def finish(self):
        for copy in self.far:
            copy.wait_send()
        self.near.wait_send()
        self.near.wait_recv()
        for copy in self.passed:
            copy.wait_send()
            copy.wait_recv()
        self.own.wait()


def gather_sems(n):
    return [DMA((n,)), DMA((n,)), DMA(())]


def by_rows(rows, body):
    def one(index, carry):
        body(pl.ds(pl.multiple_of(index * CHUNK, CHUNK), CHUNK))
        return carry

    lax.fori_loop(0, rows // CHUNK, one, 0)


class Scatter:
    def __init__(self, plane, part, mine, other, landed, send, recv, local):
        self.plane, self.mine, self.other, self.landed = plane, mine, other, landed
        self.order = far_first(plane.chips) + [0]
        self.loads, self.across, self.far = {}, {}, {}
        mate_core = 1 - plane.core
        for s in self.order:
            block = plane.same(s)
            self.loads[s] = pltpu.make_async_copy(part.at[block], mine.at[s], local.at[s])
            self.across[s] = push(
                part.at[block + mate_core - plane.core],
                other.at[s],
                send.at[s],
                recv.at[s],
                "ctx",
                plane.mate,
            )
            slot = plane.chips + s
            if s:
                self.far[s] = push(
                    mine.at[s], landed.at[s], send.at[slot], recv.at[slot], "ctx", block
                )

    def start(self):
        for s in self.order:
            self.across[s].start()
            self.loads[s].start()

    def run(self):
        rows = self.mine.shape[1]
        mine, other = self.mine, self.other
        for s in self.order:
            self.loads[s].wait()
            self.across[s].wait_recv()
            if s:

                def add(at, s=s):
                    total = mine[s, at, :].astype(F32) + other[s, at, :].astype(F32)
                    mine[s, at, :] = total.astype(BF16)

                by_rows(rows, add)
                self.far[s].start()
        for s in self.order:
            if s:
                self.far[s].wait_recv()

    def total(self, at):
        value = self.mine[0, at, :].astype(F32) + self.other[0, at, :].astype(F32)
        for s in range(1, self.plane.chips):
            value = value + self.landed[s, at, :].astype(F32)
        return value

    def finish(self):
        for s in self.order:
            self.across[s].wait_send()
            if s:
                self.far[s].wait_send()


class Product:
    def __init__(self, plane, value, mine, other, landed, given, send, recv):
        self.plane, self.value = plane, value
        self.mine, self.other, self.landed, self.given = mine, other, landed, given
        self.order = far_first(plane.chips) + [0]
        self.across, self.far = {}, {}
        for s in self.order:
            self.across[s] = push(
                given.at[s], other.at[s], send.at[s], recv.at[s], "ctx", plane.mate
            )
            slot = plane.chips + s
            if s:
                self.far[s] = push(
                    mine.at[s], landed.at[s], send.at[slot], recv.at[slot], "ctx", plane.same(s)
                )

    def start(self):
        plane = self.plane
        width = self.mine.shape[2]
        for s in self.order:
            block = plane.same(s) + 1 - 2 * plane.core

            def fill(at, s=s, block=block):
                self.given[s, :, at] = self.value(block, at).astype(BF16)

            by_cols(width, fill)
            self.across[s].start()

    def run(self):
        plane, mine, other = self.plane, self.mine, self.other
        width = mine.shape[2]
        for s in self.order:
            block = plane.same(s)
            self.across[s].wait_recv()

            def fill(at, s=s, block=block):
                total = self.value(block, at) + other[s, :, at].astype(F32)
                mine[s, :, at] = total.astype(BF16)

            by_cols(width, fill)
            if s:
                self.far[s].start()
        for s in self.order:
            if s:
                self.far[s].wait_recv()

    def total(self, at):
        value = self.mine[0, at, :].astype(F32)
        for s in range(1, self.plane.chips):
            value = value + self.landed[s, at, :].astype(F32)
        return value

    finish = Scatter.finish


def by_cols(width, body):
    span = 512

    def one(index, carry):
        body(pl.ds(pl.multiple_of(index * span, span), span))
        return carry

    lax.fori_loop(0, width // span, one, 0)


def product_scratch(n, rows, width):
    chips = n // 2
    return [pltpu.VMEM((chips, rows, width), BF16)] * 4 + [DMA((n,)), DMA((n,))]


def scatter_scratch(n, rows, width):
    chips = n // 2
    return [pltpu.VMEM((chips, rows, width), BF16)] * 3 + [DMA((n,)), DMA((n,)), DMA((chips,))]


def comm_call(kernel, ident, outs, out_specs, in_specs, scratch, micros, *args):
    return pl.pallas_call(
        kernel,
        out_shape=outs,
        in_specs=in_specs,
        out_specs=out_specs,
        scratch_shapes=scratch,
        compiler_params=pltpu.CompilerParams(
            collective_id=ident, has_side_effects=True, vmem_limit_bytes=VMEM_LIMIT
        ),
        cost_estimate=pl.CostEstimate(
            flops=0, transcendentals=0, bytes_accessed=int(micros * 3.0e6)
        ),
    )(*args)


def swap_all(n, src, out, send, recv, local):
    me = lax.axis_index("ctx")
    own = pltpu.make_async_copy(src.at[me], out.at[me], local)
    own.start()
    copies = []
    for s in range(n - 1, 0, -1):
        peer = flip(me, s, n)
        copies.append(push(src.at[peer], out.at[me], send.at[s], recv.at[s], "ctx", peer))
        copies[-1].start()
    return own, copies


def prep_kernel(n, n_dp, cols_ref, small_ref, out_ref, all_ref, *sems):
    send, recv, local, gsend, grecv, zsend, zrecv = sems
    me, row = lax.axis_index("ctx"), lax.axis_index("dp")
    meet(
        [("ctx", flip(me, s, n)) for s in range(1, n)]
        + [("dp", flip(row, s, n_dp)) for s in range(1, n_dp)]
    )
    all_ref[row, me] = small_ref[...]
    smalls = []
    for s in range(1, n):
        peer = flip(me, s, n)
        smalls.append(push(small_ref, all_ref.at[row, me], gsend.at[s], grecv.at[s], "ctx", peer))
        smalls[-1].start()
    own, copies = swap_all(n, cols_ref, out_ref, send, recv, local)
    for copy in smalls:
        copy.wait_recv()
    planes = []
    for s in range(1, n_dp):
        peer = flip(row, s, n_dp)
        planes.append(push(all_ref.at[row], all_ref.at[row], zsend.at[s], zrecv.at[s], "dp", peer))
        planes[-1].start()
    for copy in copies + planes:
        copy.wait_recv()
    for copy in copies + planes + smalls:
        copy.wait_send()
    own.wait()


def post_kernel(n, n_dp, cols_ref, small_ref, out_ref, sum_ref, first, mid, second, *sems):
    send, recv, local, gsend, grecv, zsend, zrecv = sems
    me, row = lax.axis_index("ctx"), lax.axis_index("dp")
    meet(
        [("ctx", flip(me, s, n)) for s in range(1, n)]
        + [("dp", flip(row, s, n_dp)) for s in range(1, n_dp)]
    )
    smalls = []
    for s in range(1, n):
        peer = flip(me, s, n)
        smalls.append(push(small_ref.at[peer], first.at[s], gsend.at[s], grecv.at[s], "ctx", peer))
        smalls[-1].start()
    own, copies = swap_all(n, cols_ref, out_ref, send, recv, local)
    value = small_ref[me]
    for copy, s in zip(smalls, range(1, n)):
        copy.wait_recv()
        value = value + first[s]
    mid[...] = value
    planes = []
    for s in range(1, n_dp):
        peer = flip(row, s, n_dp)
        planes.append(push(mid.at[peer], second.at[s], zsend.at[s], zrecv.at[s], "dp", peer))
        planes[-1].start()
    value = mid[row]
    for copy, s in zip(planes, range(1, n_dp)):
        copy.wait_recv()
        value = value + second[s]
    sum_ref[...] = value
    for copy in copies:
        copy.wait_recv()
    for copy in copies + planes + smalls:
        copy.wait_send()
    own.wait()


def swap_sems(n, n_dp):
    return [DMA((n,)), DMA((n,)), DMA(()), DMA((n,)), DMA((n,)), DMA((n_dp,)), DMA((n_dp,))]


def prep(n, n_dp, cols, small):
    shape = jax.ShapeDtypeStruct
    return comm_call(
        functools.partial(prep_kernel, n, n_dp),
        0,
        [shape(cols.shape, cols.dtype), shape((n_dp, n) + small.shape, F32)],
        [ANY, VM],
        [ANY, VM],
        swap_sems(n, n_dp),
        8,
        cols,
        small,
    )


def post(n, n_dp, cols, small):
    shape = jax.ShapeDtypeStruct
    tile = small.shape[2:]
    return comm_call(
        functools.partial(post_kernel, n, n_dp),
        1,
        [shape(cols.shape, cols.dtype), shape(tile, F32)],
        [ANY, VM],
        [ANY, VM],
        [
            pltpu.VMEM((n, n_dp) + tile, F32),
            pltpu.VMEM((n_dp,) + tile, F32),
            pltpu.VMEM((n_dp,) + tile, F32),
        ]
        + swap_sems(n, n_dp),
        8,
        cols,
        small,
    )


def first_kernel(n, x_ref, gain_ref, grad_ref, info_ref, nall_ref, gall_ref, iall_ref, low, *sems):
    plane = Plane(n)
    plane.meet()
    grads = Gather(plane, grad_ref, gall_ref, *sems[0:3])
    infos = Gather(plane, info_ref, iall_ref, *sems[3:6])
    infos.start()

    def norm(at):
        value = x_ref[at, :].astype(F32)
        low[at, :] = (value * rms_parts(value) * gain_ref[...]).astype(BF16)

    by_rows(x_ref.shape[0], norm)
    normed = Gather(plane, low, nall_ref, *sems[6:9])
    normed.start()
    grads.start()
    infos.forward()
    normed.forward()
    grads.forward()
    for each in (infos, normed, grads):
        each.finish()


def first(n, x, gain, grad, info):
    shape = jax.ShapeDtypeStruct
    many = lambda array, kind: shape((n,) + array.shape, kind)
    return comm_call(
        functools.partial(first_kernel, n),
        2,
        [many(x, BF16), many(grad, BF16), many(info, F32)],
        [ANY] * 3,
        [VM] * 4,
        [pltpu.VMEM(x.shape, BF16)] + gather_sems(n) * 3,
        90,
        x,
        gain,
        grad,
        info,
    )


def middle_kernel(n, attn_ref, wout_ref, x_ref, gain_ref, after_ref, all_ref, low, *scratch):
    plane = Plane(n)
    plane.meet()
    rows = x_ref.shape[0]

    def value(block, at):
        left = attn_ref[pl.ds(pl.multiple_of(block * rows, rows), rows), :]
        return dot(left, wout_ref[:, at])

    sums = Product(plane, value, *scratch[:6])
    sums.start()
    sums.run()

    def norm(at):
        value = x_ref[at, :].astype(F32) + sums.total(at)
        after_ref[at, :] = value
        low[at, :] = (value * rms_parts(value) * gain_ref[...]).astype(BF16)

    by_rows(rows, norm)
    normed = Gather(plane, low, all_ref, *scratch[6:])
    normed.start()
    normed.forward()
    sums.finish()
    normed.finish()


def middle(n, attn, wout, x, gain):
    shape = jax.ShapeDtypeStruct
    return comm_call(
        functools.partial(middle_kernel, n),
        3,
        [shape(x.shape, F32), shape((n,) + x.shape, BF16)],
        [VM, ANY],
        [VM, VM, VM, VM],
        [pltpu.VMEM(x.shape, BF16)] + product_scratch(n, *x.shape) + gather_sems(n),
        105,
        attn,
        wout,
        x,
        gain,
    )


def turn_kernel(
    n, part_ref, after_ref, grad_ref, gain_ref, mid_ref, fpart_ref, all_ref, low, *scratch
):
    plane = Plane(n)
    plane.meet()
    sums = Scatter(plane, part_ref, *scratch[:6])
    sums.start()
    fpart_ref[...] = jnp.zeros_like(fpart_ref)
    sums.run()

    def norm(at):
        value = after_ref[at, :]
        inv = rms_parts(value)
        unit = value * inv
        grad = sums.total(at)
        fpart_ref[0:1, :] += jnp.sum(grad * unit, axis=0, keepdims=True)
        mid = grad_ref[at, :].astype(F32) + rms_back(grad, unit, inv, gain_ref[...])
        mid_ref[at, :] = mid
        low[at, :] = mid.astype(BF16)

    by_rows(after_ref.shape[0], norm)
    branch = Gather(plane, low, all_ref, *scratch[6:])
    branch.start()
    branch.forward()
    sums.finish()
    branch.finish()


def turn(n, part, after, grad, gain):
    shape = jax.ShapeDtypeStruct
    return comm_call(
        functools.partial(turn_kernel, n),
        4,
        [
            shape(after.shape, F32),
            shape((8, after.shape[1]), F32),
            shape((n,) + after.shape, BF16),
        ],
        [VM, VM, ANY],
        [ANY, VM, VM, VM],
        [pltpu.VMEM(after.shape, BF16)] + scatter_scratch(n, *after.shape) + gather_sems(n),
        95,
        part,
        after,
        grad,
        gain,
    )


def last_kernel(
    n, grad_ref, wqkv_ref, x_ref, mid_ref, gain_ref, out_ref, apart_ref, *scratch
):
    plane = Plane(n)
    plane.meet()
    apart_ref[...] = jnp.zeros_like(apart_ref)
    rows = x_ref.shape[0]

    def value(block, at):
        left = grad_ref[pl.ds(pl.multiple_of(block * rows, rows), rows), :]
        return dot(left, wqkv_ref[at, :], NT)

    sums = Product(plane, value, *scratch[:6])
    sums.start()
    sums.run()

    def norm(at):
        value = x_ref[at, :].astype(F32)
        inv = rms_parts(value)
        unit = value * inv
        grad = sums.total(at)
        apart_ref[0:1, :] += jnp.sum(grad * unit, axis=0, keepdims=True)
        out_ref[at, :] = mid_ref[at, :] + rms_back(grad, unit, inv, gain_ref[...])

    by_rows(rows, norm)
    sums.finish()


def last(n, grad, wqkv, x, mid, gain):
    shape = jax.ShapeDtypeStruct
    return comm_call(
        functools.partial(last_kernel, n),
        5,
        [shape(mid.shape, F32), shape((8, mid.shape[1]), F32)],
        [VM, VM],
        [VM] * 5,
        product_scratch(n, *mid.shape),
        60,
        grad,
        wqkv,
        x,
        mid,
        gain,
    )


def close_kernel(n, part_ref, after_ref, out_ref, *scratch):
    plane = Plane(n)
    plane.meet()
    sums = Scatter(plane, part_ref, *scratch[:6])
    sums.start()
    sums.run()

    def add(at):
        out_ref[at, :] = (after_ref[at, :] + sums.total(at)).astype(BF16)

    by_rows(after_ref.shape[0], add)
    sums.finish()


def close(n, part, after):
    return comm_call(
        functools.partial(close_kernel, n),
        6,
        jax.ShapeDtypeStruct(after.shape, BF16),
        VM,
        [ANY, VM],
        scatter_scratch(n, *after.shape),
        50,
        part,
        after,
    )


def expert_kernel(chained, plan, z_ref, n2_ref, top_ref, prob_ref, *rest):
    if chained:
        moe_in, row_in = rest[:2]
        rest = rest[2:]
    sources, rest = rest[: len(plan)], rest[len(plan) :]
    moe_ref, row_ref, grads_ref, wg_ref, wu_ref, wd_ref = rest[:6]
    ag_ref, au_ref, ad_ref, stage, wsem, sem = rest[6:]
    step = pl.program_id(0)
    rows, width = n2_ref.shape
    parts, cut, hidden = wd_ref.shape
    weights = (wg_ref, wu_ref, wd_ref)

    @pl.when(step == 0)
    def _():
        z = z_ref[0]
        for source, (kind, amount, start) in zip(sources, plan):
            count = source.shape[-2] // cut
            for k in range(parts) if kind == "all" else [amount]:
                if kind == "all":
                    src, owner, wanted = source.at[k], k, None
                elif kind == "up":
                    src, owner, wanted = source, z - k, z >= k
                else:
                    src, owner, wanted = source, z + k, z + k < parts

                def load(src=src, owner=owner, start=start, count=count):
                    for piece in range(count):
                        pltpu.make_async_copy(
                            src.at[pl.ds(piece * cut, cut), :],
                            weights[start + piece].at[owner],
                            wsem.at[start + piece, owner],
                        ).start()

                if wanted is None:
                    load()
                else:
                    pl.when(wanted)(load)
        ag_ref[...] = jnp.zeros_like(ag_ref)
        au_ref[...] = jnp.zeros_like(au_ref)
        ad_ref[...] = jnp.zeros_like(ad_ref)
        for index in range(3):
            for owner in range(parts):
                block = weights[index].at[owner]
                pltpu.make_async_copy(block, block, wsem.at[index, owner]).wait()

    n2 = n2_ref[...]
    prob = prob_ref[...]
    wg = wg_ref[...].reshape(width, hidden)
    wu = wu_ref[...].reshape(width, hidden)
    gate = dot(n2, wg)
    up = dot(n2, wu)
    sig = 1.0 / (1.0 + jnp.exp(-gate))
    silu = gate * sig
    act = (silu * up).astype(BF16)
    act_grad = jnp.zeros((rows, hidden), F32)
    for z in range(parts):
        cols = slice(z * cut, (z + 1) * cut)
        out = dot(act, wd_ref[z], NT).astype(BF16).astype(F32) * prob
        if chained:
            out = out + moe_in[:, cols].astype(F32)
        moe_ref[:, cols] = out.astype(BF16)
        route = (top_ref[:, cols].astype(F32) * prob).astype(BF16)
        act_grad += dot(route, wd_ref[z])
        ad_ref[z] += dot(route, act, TN)
    gate_grad = (act_grad * up * sig * (1.0 + gate * (1.0 - sig))).astype(BF16)
    up_grad = (act_grad * silu).astype(BF16)
    row = dot(gate_grad, wg, NT) + dot(up_grad, wu, NT)
    if chained:
        row = row + row_in[...].astype(F32)
    row_ref[...] = row.astype(BF16)
    ag_ref[...] += dot(n2, gate_grad, TN).reshape(parts, cut, hidden)
    au_ref[...] += dot(n2, up_grad, TN).reshape(parts, cut, hidden)

    @pl.when(step == pl.num_programs(0) - 1)
    def _():
        copies = []
        pieces = [
            (acc, place, z) for z in range(parts) for place, acc in enumerate((ag_ref, au_ref, ad_ref))
        ]
        for index, (acc, place, z) in enumerate(pieces):
            slot = index % 2
            if index >= 2:
                copies[index - 2].wait()
            stage[slot] = acc[z].astype(BF16)
            copies.append(
                pltpu.make_async_copy(
                    stage.at[slot], grads_ref.at[z, pl.ds(place * cut, cut), :], sem.at[slot]
                )
            )
            copies[-1].start()
        copies[-2].wait()
        copies[-1].wait()


def expert(z, n2, top, prob, n_dp, sources, before, rows):
    length, width = n2.shape
    cut = width // n_dp
    hidden = sources[0][0].shape[-1]
    blk = pl.BlockSpec((rows, width), lambda i: (i, 0))
    col = pl.BlockSpec((rows, 1), lambda i: (i, 0))
    shape = jax.ShapeDtypeStruct
    plan = tuple(entry[1:] for entry in sources)
    weight = pltpu.VMEM((n_dp, cut, hidden), BF16)
    total = pltpu.VMEM((n_dp, cut, hidden), F32)
    return pl.pallas_call(
        functools.partial(expert_kernel, len(before) > 0, plan),
        grid=(length // rows,),
        in_specs=[pl.BlockSpec(memory_space=pltpu.SMEM), blk, blk, col]
        + [blk] * len(before)
        + [ANY] * len(sources),
        out_specs=[blk, blk, ANY],
        out_shape=[
            shape((length, width), BF16),
            shape((length, width), BF16),
            shape((n_dp, 3 * cut, hidden), BF16),
        ],
        scratch_shapes=[weight] * 3
        + [total] * 3
        + [pltpu.VMEM((2, cut, hidden), BF16), DMA((3, n_dp)), DMA((2,))],
        compiler_params=pltpu.CompilerParams(vmem_limit_bytes=VMEM_LIMIT),
        cost_estimate=pl.CostEstimate(
            flops=18 * length * width * hidden,
            transcendentals=length * hidden,
            bytes_accessed=5 * length * width * 2,
        ),
        name="expert",
    )(z, n2, top, prob, *before, *[entry[0] for entry in sources])


def pack_kernel(up_ref, down_ref, out_ref):
    cut = up_ref.shape[0]
    out_ref[:cut, :] = up_ref[...]
    out_ref[cut:, :] = jnp.transpose(down_ref[...].astype(F32)).astype(BF16)


def pack(w_up, w_down):
    cut, hidden = w_up.shape
    return pl.pallas_call(
        pack_kernel,
        in_specs=[VM] * 2,
        out_specs=VM,
        out_shape=jax.ShapeDtypeStruct((2 * cut, hidden), BF16),
        name="pack",
    )(w_up, w_down)


def unpack_kernel(own, *refs):
    gate_ref, up_ref, down_ref = refs[own:]
    cut = gate_ref.shape[1]
    for e in range(own):
        gate_ref[e] = refs[e][:cut, :].astype(F32)
        up_ref[e] = refs[e][cut : 2 * cut, :].astype(F32)
        down_ref[e] = jnp.transpose(refs[e][2 * cut :, :].astype(F32))


def unpack(grads):
    own = len(grads)
    rows, hidden = grads[0].shape
    cut = rows // 3
    shape = jax.ShapeDtypeStruct
    return pl.pallas_call(
        functools.partial(unpack_kernel, own),
        in_specs=[VM] * own,
        out_specs=[VM] * 3,
        out_shape=[
            shape((own, cut, hidden), F32),
            shape((own, cut, hidden), F32),
            shape((own, hidden, cut), F32),
        ],
        compiler_params=pltpu.CompilerParams(vmem_limit_bytes=VMEM_LIMIT),
        name="unpack",
    )(*grads)


def line_hop(block_up, block_down, n_dp):
    up = [(i, i + 1) for i in range(n_dp - 1)]
    down = [(i + 1, i) for i in range(n_dp - 1)]
    return lax.ppermute(block_up, "dp", up), lax.ppermute(block_down, "dp", down)


def after_of(value, *others):
    return lax.optimization_barrier((value,) + others)[0]


def scatter_dp(partial):
    return lax.psum_scatter(partial.astype(BF16), "dp", scatter_dimension=0, tiled=True)


def per_device(
    layer_input,
    doc_ids,
    route_ids,
    route_probs,
    attn_gain,
    ffn_gain,
    query_gain,
    key_gain,
    w_query,
    w_key,
    w_value,
    w_out,
    w_gate,
    w_up,
    w_down,
    out_grad,
):
    tokens, width = layer_input.shape[1:]
    n_dp = lax.axis_size("dp")
    n_ctx = lax.axis_size("ctx")
    ctx_index = lax.axis_index("ctx")
    length = tokens * n_ctx
    heads = HQ // n_ctx
    share = n_ctx // KV
    qw = heads * HD
    both = ("dp", "ctx")
    depth = w_query.shape[0]
    own_e = w_gate.shape[0]

    cut = attn_gain.shape[0]
    hcut = query_gain.shape[0]
    kinds = 2 * (cut + hcut)
    small = jnp.concatenate([attn_gain, ffn_gain, query_gain, key_gain]).astype(F32)
    small = jnp.pad(small, (0, 1024 - kinds)).reshape(8, HD)
    cols = jnp.concatenate(
        [
            w_query.reshape(depth, n_ctx, qw),
            jnp.repeat(w_key.reshape(depth, KV, HD), share, axis=1),
            jnp.repeat(w_value.reshape(depth, KV, HD), share, axis=1),
        ],
        axis=2,
    ).transpose(1, 0, 2)
    cols, small = prep(n_ctx, n_dp, cols, small)
    small = small.reshape(n_dp * n_ctx, 1024)
    gain_attn = small[:, :cut].reshape(1, width)
    gain_ffn = small[:, cut : 2 * cut].reshape(1, width)
    gain_query = small[:, 2 * cut : 2 * cut + hcut].reshape(1, HD)
    gain_key = small[:, 2 * cut + hcut : kinds].reshape(1, HD)
    wqkv = lax.all_gather(cols.reshape(n_ctx * depth, qw + 2 * HD), "dp", axis=0, tiled=True)
    forth = [(c * n_dp + d, d * n_ctx + c) for d in range(n_dp) for c in range(n_ctx)]
    wout = lax.ppermute(after_of(w_out, small), both, forth)
    wout = lax.all_gather(wout, "dp", axis=0, tiled=True)

    inputs = layer_input.reshape(tokens, width)
    top_own = out_grad.reshape(tokens, width)
    n_experts = own_e * n_ctx
    match = route_ids.reshape(1, tokens, TOP) == jnp.arange(n_experts, dtype=jnp.int32)[:, None, None]
    probs = jnp.sum(jnp.where(match, route_probs.reshape(1, tokens, TOP), 0.0), axis=2)
    info = jnp.concatenate(
        [probs, doc_ids.reshape(1, tokens).astype(F32), jnp.zeros((7, tokens), F32)], axis=0
    )
    normed, top_all, info = first(n_ctx, inputs, gain_attn, top_own, info)
    normed = normed.reshape(length, width)
    top_all = top_all.reshape(length, width)
    doc = info[:, n_experts].reshape(length).astype(jnp.int32)
    my_probs = lax.dynamic_slice_in_dim(info, ctx_index * own_e, own_e, 1)
    my_probs = my_probs.transpose(0, 2, 1).reshape(length, own_e)

    inverse = 1.0 / ROPE_BASE ** (jnp.arange(HD // 2, dtype=F32) * 2.0 / HD)
    angles = jnp.arange(length, dtype=F32)[:, None] * inverse[None, :]
    cosine = jnp.cos(angles)
    sine = jnp.sin(angles)
    cosine = jnp.concatenate([cosine, cosine], axis=1)
    sine = jnp.concatenate([-sine, sine], axis=1)
    qlin, klin, q, k, v, attn, total = attn_forward(
        normed, wqkv, cosine, sine, gain_query, gain_key, doc, tokens
    )
    blocks = (n_ctx, tokens, width)
    after, normed2 = middle(n_ctx, attn, wout, inputs, gain_ffn)
    normed2 = normed2.reshape(length, width)

    z = lax.axis_index("dp").astype(jnp.int32).reshape(1)
    carried, expert_grads = (), []
    for e in range(own_e):
        pair = pack(w_up[e], w_down[e])
        if e == 0:
            one = lax.all_gather(w_gate[e], "dp", axis=0, tiled=False)
            two = lax.all_gather(pair, "dp", axis=0, tiled=False)
            sources = [(one, "all", 0, 0), (two, "all", 0, 1)]
        else:
            sources = []
            for block, start in ((w_gate[e], 0), (pair, 1)):
                sources.append((block, "up", 0, start))
                up = down = after_of(block, after)
                for hop in range(1, n_dp):
                    if hop == 2:
                        up, down = after_of(up, *carried), after_of(down, *carried)
                    up, down = line_hop(up, down, n_dp)
                    sources += [(up, "up", hop, start), (down, "down", hop, start)]
        moe, rows_grad, grads = expert(
            z, normed2, top_all, my_probs[:, e : e + 1], n_dp, sources, carried, tokens
        )
        carried = (moe, rows_grad)
        grads = grads.reshape(3 * width, w_gate.shape[2])
        expert_grads.append(lax.psum_scatter(grads, "dp", scatter_dimension=0, tiled=True))
    mid, ffn_part, branch = turn(
        n_ctx, rows_grad.reshape(blocks), after, top_own, gain_ffn
    )
    branch = branch.reshape(length, width)
    layer_output = close(n_ctx, moe.reshape(blocks), after)

    out_w = dot(attn, branch, TN).astype(BF16)
    out_w = scatter_dp(out_w)
    dqkv, gains = attn_backward(
        branch, wout, attn, total, q, k, v, qlin, klin, cosine, sine, gain_query, gain_key, doc, tokens
    )
    input_grad, attn_part = last(n_ctx, dqkv, wqkv, inputs, mid, gain_attn)

    out_w = lax.ppermute(out_w, both, [(b, a) for a, b in forth]).astype(F32)
    qkv_w = dot(normed, dqkv, TN).astype(BF16)
    qkv_w = scatter_dp(qkv_w)
    n_all = n_dp * n_ctx
    packed = jnp.concatenate(
        [
            attn_part[0].reshape(n_all, cut),
            ffn_part[0].reshape(n_all, cut),
            gains[0].reshape(n_all, hcut),
            gains[1].reshape(n_all, hcut),
            jnp.zeros((n_all, 1024 - kinds), F32),
        ],
        axis=1,
    )
    packed = packed.reshape(n_dp, n_ctx, 8, HD).transpose(1, 0, 2, 3)
    qkv_w, packed = post(n_ctx, n_dp, qkv_w.reshape(n_ctx, depth, qw + 2 * HD), packed)
    packed = packed.reshape(1024)
    query_w = qkv_w[:, :, :qw].transpose(1, 0, 2).reshape(depth, HQ * HD).astype(F32)
    kv_w = jnp.sum(qkv_w[:, :, qw:].astype(F32).reshape(KV, share, depth, 2 * HD), axis=1)
    key_w = kv_w[:, :, :HD].transpose(1, 0, 2).reshape(depth, KV * HD)
    value_w = kv_w[:, :, HD:].transpose(1, 0, 2).reshape(depth, KV * HD)

    gate_w, up_w, down_w = unpack(expert_grads)
    return (
        layer_output.reshape(1, tokens, width),
        input_grad.reshape(1, tokens, width),
        packed[:cut],
        packed[cut : 2 * cut],
        packed[2 * cut : 2 * cut + hcut],
        packed[2 * cut + hcut : kinds],
        query_w,
        key_w,
        value_w,
        out_w,
        gate_w,
        up_w,
        down_w,
    )


def solution(mesh):
    both = ("dp", "ctx")
    seq = P("dp", "ctx", None)
    in_specs = (
        seq,
        P("dp", "ctx"),
        seq,
        seq,
        P(both),
        P(both),
        P(both),
        P(both),
        P(both, None),
        P(both, None),
        P(both, None),
        P(both, None),
        P("ctx", "dp", None),
        P("ctx", "dp", None),
        P("ctx", None, "dp"),
        seq,
    )
    out_specs = (
        seq,
        seq,
        P(both),
        P(both),
        P(both),
        P(both),
        P(both, None),
        P(both, None),
        P(both, None),
        P(both, None),
        P("ctx", "dp", None),
        P("ctx", "dp", None),
        P("ctx", None, "dp"),
    )

    return jax.shard_map(
        per_device, mesh=mesh, in_specs=in_specs, out_specs=out_specs, check_vma=False
    )
```

```python
import functools
import math

import jax
import jax.numpy as jnp
from jax import lax
from jax.experimental import pallas as pl
from jax.experimental.pallas import tpu as pltpu
from jax.sharding import PartitionSpec as P


HQ = 32
KV = 4
HD = 128
TOP = 8
MOST = 1024
EPS = 1e-06
ROPE_BASE = 1000000.0
F32 = jnp.float32
BF16 = jnp.bfloat16
SCALE = 1.0 / math.sqrt(HD)
VMEM_LIMIT = 60 * 1024 * 1024


def dot(left, right, dims=((1,), (0,))):
    return lax.dot_general(left, right, (dims, ((), ())), preferred_element_type=F32)


NT = ((1,), (1,))
TN = ((0,), (0,))


def rms_parts(values):
    return lax.rsqrt(jnp.mean(values * values, axis=-1, keepdims=True) + EPS)


def rms_back(grad, unit, inv, gain):
    scaled = grad * gain
    return inv * (scaled - unit * jnp.mean(scaled * unit, axis=-1, keepdims=True))


def head_forward(lin, gain, cosine, sine):
    unit = lin * rms_parts(lin) * gain
    return unit * cosine + pltpu.roll(unit, HD // 2, 1) * sine


def head_backward(lin, gain, cosine, sine, rot_grad):
    grad = rot_grad * cosine + pltpu.roll(rot_grad * sine, HD // 2, 1)
    inv = rms_parts(lin)
    unit = lin * inv
    return rms_back(grad, unit, inv, gain), jnp.sum(grad * unit, axis=0, keepdims=True)


MESH = pl.DeviceIdType.MESH
ANY = pl.BlockSpec(memory_space=pl.ANY)
VM = pl.BlockSpec(memory_space=pltpu.VMEM)
DMA = pltpu.SemaphoreType.DMA
CHUNK = 32


def flip(index, mask, count):
    result, bit = 0, 1
    while bit < count:
        digit = (index // bit) % 2
        result = result + bit * ((1 - digit) if mask & bit else digit)
        bit *= 2
    return result


def push(src, dst, send, recv, axis, peer):
    return pltpu.make_async_remote_copy(
        src_ref=src,
        dst_ref=dst,
        send_sem=send,
        recv_sem=recv,
        device_id={axis: peer},
        device_id_type=MESH,
    )


def meet(peers):
    barrier = pltpu.get_barrier_semaphore()
    for axis, peer in peers:
        pl.semaphore_signal(barrier, inc=1, device_id={axis: peer}, device_id_type=MESH)
    pl.semaphore_wait(barrier, len(peers))


class Plane:
    def __init__(self, n):
        self.chips = n // 2
        self.me = lax.axis_index("ctx")
        self.core = self.me % 2
        self.chip = self.me // 2
        self.mate = self.me + 1 - 2 * self.core

    def same(self, s):
        return 2 * flip(self.chip, s, self.chips) + self.core

    def meet(self):
        meet([("ctx", self.same(s)) for s in range(1, self.chips)] + [("ctx", self.mate)])


def far_first(chips):
    return sorted(range(1, chips), key=lambda s: -bin(s).count("1"))


class Gather:
    def __init__(self, plane, src, out, send, recv, local):
        self.plane, self.out, self.send, self.recv = plane, out, send, recv
        self.own = pltpu.make_async_copy(src, out.at[plane.me], local)
        self.far = [
            push(src, out.at[plane.me], send.at[s], recv.at[s], "ctx", plane.same(s))
            for s in far_first(plane.chips)
        ]
        self.near = push(src, out.at[plane.me], send.at[0], recv.at[0], "ctx", plane.mate)

    def start(self):
        for copy in self.far:
            copy.start()
        self.near.start()
        self.own.start()

    def forward(self):
        plane, out = self.plane, self.out
        self.passed = []
        for s in sorted(range(1, plane.chips), key=lambda s: bin(s).count("1")):
            block = out.at[plane.same(s)]
            push(block, block, self.send.at[s], self.recv.at[s], "ctx", plane.mate).wait_recv()
            slot = plane.chips + s
            copy = push(block, block, self.send.at[slot], self.recv.at[slot], "ctx", plane.mate)
            copy.start()
            self.passed.append(copy)

    def finish(self):
        for copy in self.far:
            copy.wait_send()
        self.near.wait_send()
        self.near.wait_recv()
        for copy in self.passed:
            copy.wait_send()
            copy.wait_recv()
        self.own.wait()


def by_rows(rows, body):
    def one(index, carry):
        body(pl.ds(pl.multiple_of(index * CHUNK, CHUNK), CHUNK))
        return carry

    lax.fori_loop(0, rows // CHUNK, one, 0)


class SquareGather:
    def __init__(self, plane, src, out, send, recv, local):
        self.plane, self.out, self.send, self.recv = plane, out, send, recv
        half = src.shape[0] // 2
        self.halves = [pl.ds(0, half), pl.ds(half, half)]
        mine = out.at[plane.me]
        self.own = pltpu.make_async_copy(src, mine, local)
        self.near = push(src, mine, send.at[0], recv.at[0], "ctx", plane.mate)
        self.far = []
        for s, h in ((1, 0), (2, 1), (1, 1), (2, 0)):
            part, slot = self.halves[h], 2 * s + h
            self.far.append(
                push(
                    src.at[part, :],
                    mine.at[part, :],
                    send.at[slot],
                    recv.at[slot],
                    "ctx",
                    plane.same(s),
                )
            )

    def start(self):
        for copy in self.far:
            copy.start()
        self.near.start()
        self.own.start()

    def arrived(self, s, h):
        block = self.out.at[self.plane.same(s)].at[self.halves[h], :]
        slot = 2 * s + h
        push(block, block, self.send.at[slot], self.recv.at[slot], "ctx", self.plane.mate).wait_recv()
        return block

    def forward(self):
        plane = self.plane
        self.passed = []
        for s, h in ((1, 0), (2, 1)):
            block = self.arrived(s, h)
            slot = 6 + h
            copy = push(block, block, self.send.at[slot], self.recv.at[slot], "ctx", plane.same(3 - s))
            copy.start()
            self.far.append(copy)
        for s in (1, 2, 3):
            if s < 3:
                self.arrived(s, 2 - s)
            else:
                self.arrived(3, 0)
                self.arrived(3, 1)
            block, slot = self.out.at[plane.same(s)], 7 + s
            copy = push(block, block, self.send.at[slot], self.recv.at[slot], "ctx", plane.mate)
            copy.start()
            self.passed.append(copy)

    def finish(self):
        for copy in self.far:
            copy.wait_send()
        self.near.wait_send()
        self.near.wait_recv()
        for copy in self.passed:
            copy.wait_send()
            copy.wait_recv()
        self.own.wait()


def gather_of(plane, src, out, send, recv, local):
    kind = SquareGather if plane.chips == 4 else Gather
    return kind(plane, src, out, send, recv, local)


class Spread:
    def __init__(self, plane, mine, landed, send, recv):
        self.plane, self.mine, self.landed = plane, mine, landed
        self.square = plane.chips == 4
        self.order = [3, 1, 2, 0] if self.square else far_first(plane.chips) + [0]
        self.send, self.recv = send, recv
        self.sent = []
        half = mine.shape[1] // 2
        self.halves = [pl.ds(0, half), pl.ds(half, half)]

    def copy(self, s, h, to):
        part, slot = self.halves[h], 2 * s + h
        return push(
            self.mine.at[s].at[part, :],
            self.landed.at[s].at[part, :],
            self.send.at[slot],
            self.recv.at[slot],
            "ctx",
            self.plane.same(to),
        )

    def go(self, s, h, to):
        copy = self.copy(s, h, to)
        copy.start()
        self.sent.append(copy)

    def ready(self, s):
        if self.square:
            if s == 3:
                self.go(3, 0, 1)
                self.go(3, 1, 2)
            elif s == 1:
                self.go(1, 0, 1)
            elif s == 2:
                self.go(2, 1, 2)
        elif s:
            copy = push(
                self.mine.at[s],
                self.landed.at[s],
                self.send.at[s],
                self.recv.at[s],
                "ctx",
                self.plane.same(s),
            )
            copy.start()
            self.sent.append(copy)

    def settle(self):
        mine, landed = self.mine, self.landed
        half = mine.shape[1] // 2
        if not self.square:
            for copy in self.sent:
                copy.wait_recv()
            return
        for s, h in ((2, 0), (1, 1)):
            self.copy(3, h, 1).wait_recv()

            def add(at, s=s, h=h):
                rows = pl.ds(h * half + at.start, CHUNK)
                total = mine[s, rows, :].astype(F32) + landed[3, rows, :].astype(F32)
                mine[s, rows, :] = total.astype(BF16)

            by_rows(half, add)
            self.go(s, h, s)
        for s in (1, 2):
            for h in (0, 1):
                self.copy(s, h, s).wait_recv()

    def total(self, at):
        value = self.mine[0, at, :].astype(F32)
        for s in (1, 2) if self.square else range(1, self.plane.chips):
            value = value + self.landed[s, at, :].astype(F32)
        return value

    def finish(self):
        for copy in self.sent:
            copy.wait_send()


class Scatter:
    def __init__(self, plane, part, mine, other, landed, send, recv, send2, recv2, local):
        self.plane, self.mine, self.other = plane, mine, other
        self.spread = Spread(plane, mine, landed, send2, recv2)
        self.order = self.spread.order
        self.loads, self.across = {}, {}
        for s in self.order:
            block = plane.same(s)
            self.loads[s] = pltpu.make_async_copy(part.at[block], mine.at[s], local.at[s])
            self.across[s] = push(
                part.at[block + 1 - 2 * plane.core],
                other.at[s],
                send.at[s],
                recv.at[s],
                "ctx",
                plane.mate,
            )

    def start(self):
        for s in self.order:
            self.across[s].start()
            self.loads[s].start()

    def run(self):
        mine, other = self.mine, self.other
        for s in self.order:
            self.loads[s].wait()
            self.across[s].wait_recv()

            def add(at, s=s):
                total = mine[s, at, :].astype(F32) + other[s, at, :].astype(F32)
                mine[s, at, :] = total.astype(BF16)

            by_rows(mine.shape[1], add)
            self.spread.ready(s)
        self.spread.settle()

    def total(self, at):
        return self.spread.total(at)

    def finish(self):
        for s in self.order:
            self.across[s].wait_send()
        self.spread.finish()


class Product:
    def __init__(self, plane, value, mine, other, landed, given, send, recv, send2, recv2):
        self.plane, self.value = plane, value
        self.mine, self.other, self.given = mine, other, given
        self.spread = Spread(plane, mine, landed, send2, recv2)
        self.order = self.spread.order
        self.across = {
            s: push(given.at[s], other.at[s], send.at[s], recv.at[s], "ctx", plane.mate)
            for s in self.order
        }

    def start(self):
        plane = self.plane
        for s in self.order:
            block = plane.same(s) + 1 - 2 * plane.core

            def fill(at, s=s, block=block):
                self.given[s, :, at] = self.value(block, at).astype(BF16)

            by_cols(self.mine.shape[2], fill)
            self.across[s].start()

    def run(self):
        plane, mine, other = self.plane, self.mine, self.other
        for s in self.order:
            block = plane.same(s)
            self.across[s].wait_recv()

            def fill(at, s=s, block=block):
                total = self.value(block, at) + other[s, :, at].astype(F32)
                mine[s, :, at] = total.astype(BF16)

            by_cols(mine.shape[2], fill)
            self.spread.ready(s)
        self.spread.settle()

    total = Scatter.total
    finish = Scatter.finish


def by_cols(width, body):
    span = 512

    def one(index, carry):
        body(pl.ds(pl.multiple_of(index * span, span), span))
        return carry

    lax.fori_loop(0, width // span, one, 0)


def gather_sems(n):
    return [DMA((12 if n == 8 else n,)), DMA((12 if n == 8 else n,)), DMA(())]


def scatter_scratch(n, rows, width):
    chips = n // 2
    return (
        [pltpu.VMEM((chips, rows, width), BF16)] * 3
        + [DMA((chips,)), DMA((chips,)), DMA((n,)), DMA((n,))]
        + [DMA((chips,))]
    )


def product_scratch(n, rows, width):
    chips = n // 2
    return [pltpu.VMEM((chips, rows, width), BF16)] * 4 + [
        DMA((chips,)),
        DMA((chips,)),
        DMA((n,)),
        DMA((n,)),
    ]


def comm_call(kernel, ident, outs, out_specs, in_specs, scratch, micros, *args):
    return pl.pallas_call(
        kernel,
        out_shape=outs,
        in_specs=in_specs,
        out_specs=out_specs,
        scratch_shapes=scratch,
        compiler_params=pltpu.CompilerParams(
            collective_id=ident, has_side_effects=True, vmem_limit_bytes=VMEM_LIMIT
        ),
        cost_estimate=pl.CostEstimate(
            flops=0, transcendentals=0, bytes_accessed=int(micros * 3.0e6)
        ),
    )(*args)


def swap_all(n, src, out, send, recv, local):
    me = lax.axis_index("ctx")
    own = pltpu.make_async_copy(src.at[me], out.at[me], local)
    own.start()
    copies = []
    for s in range(n - 1, 0, -1):
        peer = flip(me, s, n)
        copies.append(push(src.at[peer], out.at[me], send.at[s], recv.at[s], "ctx", peer))
        copies[-1].start()
    return own, copies


def prep_kernel(n, n_dp, cols_ref, small_ref, out_ref, all_ref, *sems):
    send, recv, local, gsend, grecv, zsend, zrecv = sems
    me, row = lax.axis_index("ctx"), lax.axis_index("dp")
    meet(
        [("ctx", flip(me, s, n)) for s in range(1, n)]
        + [("dp", flip(row, s, n_dp)) for s in range(1, n_dp)]
    )
    all_ref[row, me] = small_ref[...]
    smalls = []
    for s in range(1, n):
        peer = flip(me, s, n)
        smalls.append(push(small_ref, all_ref.at[row, me], gsend.at[s], grecv.at[s], "ctx", peer))
        smalls[-1].start()
    own, copies = swap_all(n, cols_ref, out_ref, send, recv, local)
    for copy in smalls:
        copy.wait_recv()
    planes = []
    for s in range(1, n_dp):
        peer = flip(row, s, n_dp)
        planes.append(push(all_ref.at[row], all_ref.at[row], zsend.at[s], zrecv.at[s], "dp", peer))
        planes[-1].start()
    for copy in copies + planes:
        copy.wait_recv()
    for copy in copies + planes + smalls:
        copy.wait_send()
    own.wait()


def post_kernel(n, n_dp, cols_ref, small_ref, out_ref, sum_ref, first, mid, second, *sems):
    send, recv, local, gsend, grecv, zsend, zrecv = sems
    me, row = lax.axis_index("ctx"), lax.axis_index("dp")
    meet(
        [("ctx", flip(me, s, n)) for s in range(1, n)]
        + [("dp", flip(row, s, n_dp)) for s in range(1, n_dp)]
    )
    smalls = []
    for s in range(1, n):
        peer = flip(me, s, n)
        smalls.append(push(small_ref.at[peer], first.at[s], gsend.at[s], grecv.at[s], "ctx", peer))
        smalls[-1].start()
    own, copies = swap_all(n, cols_ref, out_ref, send, recv, local)
    value = small_ref[me]
    for copy, s in zip(smalls, range(1, n)):
        copy.wait_recv()
        value = value + first[s]
    mid[...] = value
    planes = []
    for s in range(1, n_dp):
        peer = flip(row, s, n_dp)
        planes.append(push(mid.at[peer], second.at[s], zsend.at[s], zrecv.at[s], "dp", peer))
        planes[-1].start()
    value = mid[row]
    for copy, s in zip(planes, range(1, n_dp)):
        copy.wait_recv()
        value = value + second[s]
    sum_ref[...] = value
    for copy in copies:
        copy.wait_recv()
    for copy in copies + planes + smalls:
        copy.wait_send()
    own.wait()


def swap_sems(n, n_dp):
    return [DMA((n,)), DMA((n,)), DMA(()), DMA((n,)), DMA((n,)), DMA((n_dp,)), DMA((n_dp,))]


def prep(n, n_dp, cols, small):
    shape = jax.ShapeDtypeStruct
    return comm_call(
        functools.partial(prep_kernel, n, n_dp),
        0,
        [shape(cols.shape, cols.dtype), shape((n_dp, n) + small.shape, F32)],
        [ANY, VM],
        [ANY, VM],
        swap_sems(n, n_dp),
        8,
        cols,
        small,
    )


def post(n, n_dp, cols, small):
    shape = jax.ShapeDtypeStruct
    tile = small.shape[2:]
    return comm_call(
        functools.partial(post_kernel, n, n_dp),
        1,
        [shape(cols.shape, cols.dtype), shape(tile, F32)],
        [ANY, VM],
        [ANY, VM],
        [
            pltpu.VMEM((n, n_dp) + tile, F32),
            pltpu.VMEM((n_dp,) + tile, F32),
            pltpu.VMEM((n_dp,) + tile, F32),
        ]
        + swap_sems(n, n_dp),
        8,
        cols,
        small,
    )


def first_kernel(n, x_ref, gain_ref, info_ref, nall_ref, iall_ref, low, *sems):
    plane = Plane(n)
    plane.meet()
    infos = Gather(plane, info_ref, iall_ref, *sems[0:3])
    infos.start()

    def norm(at):
        value = x_ref[at, :].astype(F32)
        low[at, :] = (value * rms_parts(value) * gain_ref[...]).astype(BF16)

    by_rows(x_ref.shape[0], norm)
    normed = gather_of(plane, low, nall_ref, *sems[3:6])
    normed.start()
    infos.forward()
    normed.forward()
    infos.finish()
    normed.finish()


def first(n, x, gain, info):
    shape = jax.ShapeDtypeStruct
    many = lambda array, kind: shape((n,) + array.shape, kind)
    return comm_call(
        functools.partial(first_kernel, n),
        2,
        [many(x, BF16), many(info, F32)],
        [ANY] * 2,
        [VM] * 3,
        [pltpu.VMEM(x.shape, BF16)] + [DMA((n,)), DMA((n,)), DMA(())] + gather_sems(n),
        50,
        x,
        gain,
        info,
    )


def middle_kernel(n, attn_ref, wout_ref, x_ref, gain_ref, after_ref, all_ref, low, *scratch):
    plane = Plane(n)
    plane.meet()
    rows = x_ref.shape[0]

    def value(block, at):
        left = attn_ref[pl.ds(pl.multiple_of(block * rows, rows), rows), :]
        return dot(left, wout_ref[:, at])

    sums = Product(plane, value, *scratch[:8])
    sums.start()
    sums.run()

    def norm(at):
        value = x_ref[at, :].astype(F32) + sums.total(at)
        after_ref[at, :] = value
        low[at, :] = (value * rms_parts(value) * gain_ref[...]).astype(BF16)

    by_rows(rows, norm)
    normed = gather_of(plane, low, all_ref, *scratch[8:])
    normed.start()
    normed.forward()
    sums.finish()
    normed.finish()


def middle(n, attn, wout, x, gain):
    shape = jax.ShapeDtypeStruct
    return comm_call(
        functools.partial(middle_kernel, n),
        3,
        [shape(x.shape, F32), shape((n,) + x.shape, BF16)],
        [VM, ANY],
        [VM, VM, VM, VM],
        [pltpu.VMEM(x.shape, BF16)] + product_scratch(n, *x.shape) + gather_sems(n),
        105,
        attn,
        wout,
        x,
        gain,
    )


def turn_kernel(
    n, part_ref, after_ref, grad_ref, gain_ref, mid_ref, fpart_ref, all_ref, low, *scratch
):
    plane = Plane(n)
    plane.meet()
    sums = Scatter(plane, part_ref, *scratch[:8])
    sums.start()
    fpart_ref[...] = jnp.zeros_like(fpart_ref)
    sums.run()

    def norm(at):
        value = after_ref[at, :]
        inv = rms_parts(value)
        unit = value * inv
        grad = sums.total(at)
        fpart_ref[0:1, :] += jnp.sum(grad * unit, axis=0, keepdims=True)
        mid = grad_ref[at, :].astype(F32) + rms_back(grad, unit, inv, gain_ref[...])
        mid_ref[at, :] = mid
        low[at, :] = mid.astype(BF16)

    by_rows(after_ref.shape[0], norm)
    branch = gather_of(plane, low, all_ref, *scratch[8:])
    branch.start()
    branch.forward()
    sums.finish()
    branch.finish()


def turn(n, part, after, grad, gain):
    shape = jax.ShapeDtypeStruct
    return comm_call(
        functools.partial(turn_kernel, n),
        4,
        [
            shape(after.shape, F32),
            shape((8, after.shape[1]), F32),
            shape((n,) + after.shape, BF16),
        ],
        [VM, VM, ANY],
        [ANY, VM, VM, VM],
        [pltpu.VMEM(after.shape, BF16)] + scatter_scratch(n, *after.shape) + gather_sems(n),
        95,
        part,
        after,
        grad,
        gain,
    )


def last_kernel(
    n, grad_ref, wqkv_ref, x_ref, mid_ref, gain_ref, out_ref, apart_ref, *scratch
):
    plane = Plane(n)
    plane.meet()
    apart_ref[...] = jnp.zeros_like(apart_ref)
    rows = x_ref.shape[0]

    def value(block, at):
        left = grad_ref[pl.ds(pl.multiple_of(block * rows, rows), rows), :]
        return dot(left, wqkv_ref[at, :], NT)

    sums = Product(plane, value, *scratch[:8])
    sums.start()
    sums.run()

    def norm(at):
        value = x_ref[at, :].astype(F32)
        inv = rms_parts(value)
        unit = value * inv
        grad = sums.total(at)
        apart_ref[0:1, :] += jnp.sum(grad * unit, axis=0, keepdims=True)
        out_ref[at, :] = mid_ref[at, :] + rms_back(grad, unit, inv, gain_ref[...])

    by_rows(rows, norm)
    sums.finish()


def last(n, grad, wqkv, x, mid, gain):
    shape = jax.ShapeDtypeStruct
    return comm_call(
        functools.partial(last_kernel, n),
        5,
        [shape(mid.shape, F32), shape((8, mid.shape[1]), F32)],
        [VM, VM],
        [VM] * 5,
        product_scratch(n, *mid.shape),
        60,
        grad,
        wqkv,
        x,
        mid,
        gain,
    )


def close_kernel(n, part_ref, after_ref, out_ref, *scratch):
    plane = Plane(n)
    plane.meet()
    sums = Scatter(plane, part_ref, *scratch[:8])
    sums.start()
    sums.run()

    def add(at):
        out_ref[at, :] = (after_ref[at, :] + sums.total(at)).astype(BF16)

    by_rows(after_ref.shape[0], add)
    sums.finish()


def close(n, part, after):
    return comm_call(
        functools.partial(close_kernel, n),
        6,
        jax.ShapeDtypeStruct(after.shape, BF16),
        VM,
        [ANY, VM],
        scatter_scratch(n, *after.shape),
        50,
        part,
        after,
    )


def attn_forward_kernel(
    n,
    heads,
    back,
    normed_ref,
    wqkv_ref,
    cos_ref,
    sin_ref,
    qgain_ref,
    kgain_ref,
    docc_ref,
    docr_ref,
    grad_ref,
    qlin_ref,
    klin_ref,
    q_ref,
    k_ref,
    v_ref,
    attn_ref,
    total_ref,
    gall_ref,
    acc_ref,
    sum_ref,
    *sems,
):
    step = pl.program_id(0)

    @pl.when(step == 0)
    def _():
        plane = Plane(n)
        plane.meet()
        gather_of(plane, grad_ref, gall_ref, *sems).start()

    rows = normed_ref.shape[0]
    lin = dot(normed_ref[...], wqkv_ref[...])
    here = pl.ds(step * rows, rows)
    cosine = cos_ref[...]
    sine = sin_ref[...]
    qw = heads * HD
    for head in range(heads):
        cols = slice(head * HD, (head + 1) * HD)
        part = lin[:, cols]
        qlin_ref[:, cols] = part
        q_ref[:, cols] = head_forward(part, qgain_ref[...], cosine, sine).astype(BF16)
    key_lin = lin[:, qw : qw + HD]
    klin_ref[...] = key_lin
    k_ref[here, :] = head_forward(key_lin, kgain_ref[...], cosine, sine).astype(BF16)
    v_ref[here, :] = lin[:, qw + HD :].astype(BF16)
    acc_ref[...] = jnp.zeros_like(acc_ref)
    sum_ref[...] = jnp.zeros_like(sum_ref)
    row_pos = step * rows + lax.broadcasted_iota(jnp.int32, (rows, rows), 0)
    col_off = lax.broadcasted_iota(jnp.int32, (rows, rows), 1)

    def one(block, carry):
        at = pl.ds(pl.multiple_of(block * rows, rows), rows)
        key = k_ref[at, :]
        val = v_ref[at, :]
        allowed = (docc_ref[...] == docr_ref[:, at]) & (block * rows + col_off <= row_pos)
        for head in range(heads):
            cols = slice(head * HD, (head + 1) * HD)
            score = dot(q_ref[:, cols], key, NT) * SCALE
            expo = jnp.where(allowed, jnp.exp(score), 0.0)
            folded = expo[:, :HD]
            for piece in range(1, rows // HD):
                folded = folded + expo[:, piece * HD : (piece + 1) * HD]
            sum_ref[:, cols] += folded
            acc_ref[:, cols] += dot(expo.astype(BF16), val)
        return carry

    lax.fori_loop(jnp.maximum(step - back, 0), step + 1, one, 0)
    lane = lax.broadcasted_iota(jnp.int32, (rows, HD), 1)
    totals = jnp.ones((rows, HD), F32)
    for head in range(heads):
        cols = slice(head * HD, (head + 1) * HD)
        total = jnp.sum(sum_ref[:, cols], axis=-1, keepdims=True)
        totals = jnp.where(lane == head, total, totals)
        attn_ref[:, cols] = (acc_ref[:, cols] / total).astype(BF16)
    total_ref[...] = totals

    @pl.when(step == pl.num_programs(0) - 1)
    def _():
        grads = gather_of(Plane(n), grad_ref, gall_ref, *sems)
        grads.forward()
        grads.finish()


def attn_forward(n, normed, wqkv, cosine, sine, qgain, kgain, doc, grad, rows):
    length, width = normed.shape
    qw = wqkv.shape[1] - 2 * HD
    heads = qw // HD
    blk = lambda cols: pl.BlockSpec((rows, cols), lambda i: (i, 0))
    whole = lambda shape: pl.BlockSpec(shape, lambda i: (0, 0))
    shape = jax.ShapeDtypeStruct
    return pl.pallas_call(
        functools.partial(attn_forward_kernel, n, heads, MOST // rows),
        grid=(length // rows,),
        in_specs=[
            blk(width),
            whole(wqkv.shape),
            blk(HD),
            blk(HD),
            whole((1, HD)),
            whole((1, HD)),
            blk(1),
            whole((1, length)),
            whole(grad.shape),
        ],
        out_specs=[
            blk(qw),
            blk(HD),
            blk(qw),
            whole((length, HD)),
            whole((length, HD)),
            blk(qw),
            blk(HD),
            ANY,
        ],
        out_shape=[
            shape((length, qw), F32),
            shape((length, HD), F32),
            shape((length, qw), BF16),
            shape((length, HD), BF16),
            shape((length, HD), BF16),
            shape((length, qw), BF16),
            shape((length, HD), F32),
            shape((n,) + grad.shape, BF16),
        ],
        scratch_shapes=[pltpu.VMEM((rows, qw), F32), pltpu.VMEM((rows, qw), F32)]
        + gather_sems(n),
        compiler_params=pltpu.CompilerParams(
            collective_id=7, has_side_effects=True, vmem_limit_bytes=VMEM_LIMIT
        ),
        cost_estimate=pl.CostEstimate(
            flops=35 * 10**9, transcendentals=0, bytes_accessed=30 * 2**20
        ),
        name="attn_forward",
    )(normed, wqkv, cosine, sine, qgain, kgain, doc[:, None], doc[None, :], grad)


def attn_backward_kernel(
    heads,
    back,
    branch_ref,
    wout_ref,
    attn_ref,
    total_ref,
    q_ref,
    k_ref,
    v_ref,
    qlin_ref,
    klin_ref,
    cos_ref,
    sin_ref,
    qgain_ref,
    kgain_ref,
    docc_ref,
    docr_ref,
    dqkv_ref,
    gains_ref,
    dk_ref,
    dv_ref,
    dqa_ref,
):
    step = pl.program_id(0)
    rows = branch_ref.shape[0]
    here = pl.ds(pl.multiple_of(step * rows, rows), rows)

    @pl.when(step == 0)
    def _():
        gains_ref[...] = jnp.zeros_like(gains_ref)

    dk_ref[here, :] = jnp.zeros((rows, HD), F32)
    dv_ref[here, :] = jnp.zeros((rows, HD), F32)
    dqa_ref[...] = jnp.zeros_like(dqa_ref)
    attn_grad = dot(branch_ref[...], wout_ref[...], NT)
    grads = []
    shifts = []
    for head in range(heads):
        cols = slice(head * HD, (head + 1) * HD)
        part = attn_grad[:, cols]
        inv_total = 1.0 / total_ref[:, head : head + 1]
        delta = jnp.sum(part * attn_ref[:, cols].astype(F32), axis=-1, keepdims=True)
        grads.append((part * inv_total).astype(BF16))
        shifts.append(delta * inv_total)
    row_pos = step * rows + lax.broadcasted_iota(jnp.int32, (rows, rows), 0)
    col_off = lax.broadcasted_iota(jnp.int32, (rows, rows), 1)

    def one(block, carry):
        at = pl.ds(pl.multiple_of(block * rows, rows), rows)
        key = k_ref[at, :]
        val = v_ref[at, :]
        allowed = (docc_ref[...] == docr_ref[:, at]) & (block * rows + col_off <= row_pos)
        dk = jnp.zeros((rows, HD), F32)
        dv = jnp.zeros((rows, HD), F32)
        for head in range(heads):
            cols = slice(head * HD, (head + 1) * HD)
            query = q_ref[:, cols]
            score = dot(query, key, NT) * SCALE
            expo = jnp.where(allowed, jnp.exp(score), 0.0)
            prod = dot(grads[head], val, NT)
            score_grad = (expo * (prod - shifts[head])).astype(BF16)
            dv += dot(expo.astype(BF16), grads[head], TN)
            dk += dot(score_grad, query, TN)
            dqa_ref[:, cols] += dot(score_grad, key)
        dk_ref[at, :] += dk
        dv_ref[at, :] += dv
        return carry

    lax.fori_loop(jnp.maximum(step - back, 0), step + 1, one, 0)
    cosine = cos_ref[here, :]
    sine = sin_ref[here, :]
    for head in range(heads):
        cols = slice(head * HD, (head + 1) * HD)
        grad, gain_part = head_backward(
            qlin_ref[:, cols], qgain_ref[...], cosine, sine, dqa_ref[:, cols] * SCALE
        )
        dqkv_ref[here, cols] = grad.astype(BF16)
        gains_ref[0:1, :] += gain_part

    @pl.when(step == pl.num_programs(0) - 1)
    def _():
        def finish(block, carry):
            at = pl.ds(pl.multiple_of(block * rows, rows), rows)
            grad, gain_part = head_backward(
                klin_ref[at, :], kgain_ref[...], cos_ref[at, :], sin_ref[at, :], dk_ref[at, :] * SCALE
            )
            qw = heads * HD
            dqkv_ref[at, qw : qw + HD] = grad.astype(BF16)
            dqkv_ref[at, qw + HD :] = dv_ref[at, :].astype(BF16)
            gains_ref[1:2, :] += gain_part
            return carry

        lax.fori_loop(0, pl.num_programs(0), finish, 0)


def attn_backward(branch, wout, attn, total, q, k, v, qlin, klin, cosine, sine, qgain, kgain, doc, rows):
    length, width = branch.shape
    qw = wout.shape[0]
    heads = qw // HD
    blk = lambda cols: pl.BlockSpec((rows, cols), lambda i: (i, 0))
    whole = lambda shape: pl.BlockSpec(shape, lambda i: (0, 0))
    shape = jax.ShapeDtypeStruct
    full = whole((length, HD))
    return pl.pallas_call(
        functools.partial(attn_backward_kernel, heads, MOST // rows),
        grid=(length // rows,),
        in_specs=[
            blk(width),
            whole(wout.shape),
            blk(qw),
            blk(HD),
            blk(qw),
            full,
            full,
            blk(qw),
            full,
            full,
            full,
            whole((1, HD)),
            whole((1, HD)),
            blk(1),
            whole((1, length)),
        ],
        out_specs=[whole((length, qw + 2 * HD)), whole((8, HD))],
        out_shape=[
            shape((length, qw + 2 * HD), BF16),
            shape((8, HD), F32),
        ],
        scratch_shapes=[
            pltpu.VMEM((length, HD), F32),
            pltpu.VMEM((length, HD), F32),
            pltpu.VMEM((rows, qw), F32),
        ],
        compiler_params=pltpu.CompilerParams(vmem_limit_bytes=VMEM_LIMIT),
        cost_estimate=pl.CostEstimate(
            flops=60 * 10**9, transcendentals=0, bytes_accessed=30 * 2**20
        ),
        name="attn_backward",
    )(branch, wout, attn, total, q, k, v, qlin, klin, cosine, sine, qgain, kgain, doc[:, None], doc[None, :])


def expert_kernel(chained, plan, z_ref, n2_ref, top_ref, prob_ref, *rest):
    if chained:
        moe_in, row_in = rest[:2]
        rest = rest[2:]
    sources, rest = rest[: len(plan)], rest[len(plan) :]
    moe_ref, row_ref, grads_ref, wg_ref, wu_ref, wd_ref = rest[:6]
    ag_ref, au_ref, ad_ref, stage, wsem, sem = rest[6:]
    step = pl.program_id(0)
    rows, width = n2_ref.shape
    parts, cut, hidden = wd_ref.shape
    weights = (wg_ref, wu_ref, wd_ref)

    @pl.when(step == 0)
    def _():
        z = z_ref[0]
        for source, (kind, amount, start) in zip(sources, plan):
            count = source.shape[-2] // cut
            for k in range(parts) if kind == "all" else [amount]:
                if kind == "all":
                    src, owner, wanted = source.at[k], k, None
                elif kind == "up":
                    src, owner, wanted = source, z - k, z >= k
                else:
                    src, owner, wanted = source, z + k, z + k < parts

                def load(src=src, owner=owner, start=start, count=count):
                    for piece in range(count):
                        pltpu.make_async_copy(
                            src.at[pl.ds(piece * cut, cut), :],
                            weights[start + piece].at[owner],
                            wsem.at[start + piece, owner],
                        ).start()

                if wanted is None:
                    load()
                else:
                    pl.when(wanted)(load)
        ag_ref[...] = jnp.zeros_like(ag_ref)
        au_ref[...] = jnp.zeros_like(au_ref)
        ad_ref[...] = jnp.zeros_like(ad_ref)
        for index in range(3):
            for owner in range(parts):
                block = weights[index].at[owner]
                pltpu.make_async_copy(block, block, wsem.at[index, owner]).wait()

    n2 = n2_ref[...]
    prob = prob_ref[...]
    wg = wg_ref[...].reshape(width, hidden)
    wu = wu_ref[...].reshape(width, hidden)
    gate = dot(n2, wg)
    up = dot(n2, wu)
    sig = 1.0 / (1.0 + jnp.exp(-gate))
    silu = gate * sig
    act = (silu * up).astype(BF16)
    act_grad = jnp.zeros((rows, hidden), F32)
    for z in range(parts):
        cols = slice(z * cut, (z + 1) * cut)
        out = dot(act, wd_ref[z], NT).astype(BF16).astype(F32) * prob
        if chained:
            out = out + moe_in[:, cols].astype(F32)
        moe_ref[:, cols] = out.astype(BF16)
        route = (top_ref[:, cols].astype(F32) * prob).astype(BF16)
        act_grad += dot(route, wd_ref[z])
        ad_ref[z] += dot(route, act, TN)
    gate_grad = (act_grad * up * sig * (1.0 + gate * (1.0 - sig))).astype(BF16)
    up_grad = (act_grad * silu).astype(BF16)
    row = dot(gate_grad, wg, NT) + dot(up_grad, wu, NT)
    if chained:
        row = row + row_in[...].astype(F32)
    row_ref[...] = row.astype(BF16)
    ag_ref[...] += dot(n2, gate_grad, TN).reshape(parts, cut, hidden)
    au_ref[...] += dot(n2, up_grad, TN).reshape(parts, cut, hidden)

    @pl.when(step == pl.num_programs(0) - 1)
    def _():
        copies = []
        pieces = [
            (acc, place, z) for z in range(parts) for place, acc in enumerate((ag_ref, au_ref, ad_ref))
        ]
        for index, (acc, place, z) in enumerate(pieces):
            slot = index % 2
            if index >= 2:
                copies[index - 2].wait()
            stage[slot] = acc[z].astype(BF16)
            copies.append(
                pltpu.make_async_copy(
                    stage.at[slot], grads_ref.at[z, pl.ds(place * cut, cut), :], sem.at[slot]
                )
            )
            copies[-1].start()
        copies[-2].wait()
        copies[-1].wait()


def expert(z, n2, top, prob, n_dp, sources, before, rows):
    length, width = n2.shape
    cut = width // n_dp
    hidden = sources[0][0].shape[-1]
    blk = pl.BlockSpec((rows, width), lambda i: (i, 0))
    col = pl.BlockSpec((rows, 1), lambda i: (i, 0))
    shape = jax.ShapeDtypeStruct
    plan = tuple(entry[1:] for entry in sources)
    weight = pltpu.VMEM((n_dp, cut, hidden), BF16)
    total = pltpu.VMEM((n_dp, cut, hidden), F32)
    return pl.pallas_call(
        functools.partial(expert_kernel, len(before) > 0, plan),
        grid=(length // rows,),
        in_specs=[pl.BlockSpec(memory_space=pltpu.SMEM), blk, blk, col]
        + [blk] * len(before)
        + [ANY] * len(sources),
        out_specs=[blk, blk, ANY],
        out_shape=[
            shape((length, width), BF16),
            shape((length, width), BF16),
            shape((n_dp, 3 * cut, hidden), BF16),
        ],
        scratch_shapes=[weight] * 3
        + [total] * 3
        + [pltpu.VMEM((2, cut, hidden), BF16), DMA((3, n_dp)), DMA((2,))],
        compiler_params=pltpu.CompilerParams(vmem_limit_bytes=VMEM_LIMIT),
        cost_estimate=pl.CostEstimate(
            flops=18 * length * width * hidden,
            transcendentals=length * hidden,
            bytes_accessed=5 * length * width * 2,
        ),
        name="expert",
    )(z, n2, top, prob, *before, *[entry[0] for entry in sources])


def pack_kernel(cuts, gate_ref, up_ref, down_ref, *outs):
    cut = gate_ref.shape[0]
    for (low, high), out in zip(cuts, outs):
        out[:cut, :] = gate_ref[:, low:high]
        out[cut : 2 * cut, :] = up_ref[:, low:high]
        out[2 * cut :, :] = jnp.transpose(down_ref[low:high, :].astype(F32)).astype(BF16)


def pack(cuts, w_gate, w_up, w_down):
    cut = w_gate.shape[0]
    return pl.pallas_call(
        functools.partial(pack_kernel, cuts),
        in_specs=[VM] * 3,
        out_specs=[VM] * len(cuts),
        out_shape=[jax.ShapeDtypeStruct((3 * cut, high - low), BF16) for low, high in cuts],
        name="pack",
    )(w_gate, w_up, w_down)


def unpack_kernel(chunks, *refs):
    gate_ref, up_ref, down_ref = refs[len(chunks) :]
    cut = gate_ref.shape[1]
    for (e, low, high), ref in zip(chunks, refs):
        gate_ref[e, :, low:high] = ref[:cut, :].astype(F32)
        up_ref[e, :, low:high] = ref[cut : 2 * cut, :].astype(F32)
        down_ref[e, low:high, :] = jnp.transpose(ref[2 * cut :, :].astype(F32))


def unpack(own, chunks, grads, hidden):
    cut = grads[0].shape[0] // 3
    shape = jax.ShapeDtypeStruct
    return pl.pallas_call(
        functools.partial(unpack_kernel, chunks),
        in_specs=[VM] * len(grads),
        out_specs=[VM] * 3,
        out_shape=[
            shape((own, cut, hidden), F32),
            shape((own, cut, hidden), F32),
            shape((own, hidden, cut), F32),
        ],
        compiler_params=pltpu.CompilerParams(vmem_limit_bytes=VMEM_LIMIT),
        name="unpack",
    )(*grads)


def line_hop(block_up, block_down, n_dp, hop):
    up = [(i, i + 1) for i in range(hop - 1, n_dp - 1)]
    down = [(i + 1, i) for i in range(n_dp - hop)]
    return lax.ppermute(block_up, "dp", up), lax.ppermute(block_down, "dp", down)


def after_of(value, *others):
    return lax.optimization_barrier((value,) + others)[0]


def scatter_dp(partial):
    return lax.psum_scatter(partial.astype(BF16), "dp", scatter_dimension=0, tiled=True)


def per_device(
    layer_input,
    doc_ids,
    route_ids,
    route_probs,
    attn_gain,
    ffn_gain,
    query_gain,
    key_gain,
    w_query,
    w_key,
    w_value,
    w_out,
    w_gate,
    w_up,
    w_down,
    out_grad,
):
    tokens, width = layer_input.shape[1:]
    n_dp = lax.axis_size("dp")
    n_ctx = lax.axis_size("ctx")
    ctx_index = lax.axis_index("ctx")
    length = tokens * n_ctx
    heads = HQ // n_ctx
    share = n_ctx // KV
    qw = heads * HD
    both = ("dp", "ctx")
    depth = w_query.shape[0]
    own_e = w_gate.shape[0]

    cut = attn_gain.shape[0]
    hcut = query_gain.shape[0]
    kinds = 2 * (cut + hcut)
    small = jnp.concatenate([attn_gain, ffn_gain, query_gain, key_gain]).astype(F32)
    small = jnp.pad(small, (0, 1024 - kinds)).reshape(8, HD)
    cols = jnp.concatenate(
        [
            w_query.reshape(depth, n_ctx, qw),
            jnp.repeat(w_key.reshape(depth, KV, HD), share, axis=1),
            jnp.repeat(w_value.reshape(depth, KV, HD), share, axis=1),
        ],
        axis=2,
    ).transpose(1, 0, 2)
    cols, small = prep(n_ctx, n_dp, cols, small)
    small = small.reshape(n_dp * n_ctx, 1024)
    gain_attn = small[:, :cut].reshape(1, width)
    gain_ffn = small[:, cut : 2 * cut].reshape(1, width)
    gain_query = small[:, 2 * cut : 2 * cut + hcut].reshape(1, HD)
    gain_key = small[:, 2 * cut + hcut : kinds].reshape(1, HD)
    wqkv = lax.all_gather(cols.reshape(n_ctx * depth, qw + 2 * HD), "dp", axis=0, tiled=True)
    forth = [(c * n_dp + d, d * n_ctx + c) for d in range(n_dp) for c in range(n_ctx)]
    wout = lax.ppermute(after_of(w_out, small), both, forth)
    wout = lax.all_gather(wout, "dp", axis=0, tiled=True)

    inputs = layer_input.reshape(tokens, width)
    top_own = out_grad.reshape(tokens, width)
    n_experts = own_e * n_ctx
    match = route_ids.reshape(1, tokens, TOP) == jnp.arange(n_experts, dtype=jnp.int32)[:, None, None]
    probs = jnp.sum(jnp.where(match, route_probs.reshape(1, tokens, TOP), 0.0), axis=2)
    info = jnp.concatenate(
        [probs, doc_ids.reshape(1, tokens).astype(F32), jnp.zeros((7, tokens), F32)], axis=0
    )
    normed, info = first(n_ctx, inputs, gain_attn, info)
    normed = normed.reshape(length, width)
    doc = info[:, n_experts].reshape(length).astype(jnp.int32)
    my_probs = lax.dynamic_slice_in_dim(info, ctx_index * own_e, own_e, 1)
    my_probs = my_probs.transpose(0, 2, 1).reshape(length, own_e)

    inverse = 1.0 / ROPE_BASE ** (jnp.arange(HD // 2, dtype=F32) * 2.0 / HD)
    angles = jnp.arange(length, dtype=F32)[:, None] * inverse[None, :]
    cosine = jnp.cos(angles)
    sine = jnp.sin(angles)
    cosine = jnp.concatenate([cosine, cosine], axis=1)
    sine = jnp.concatenate([-sine, sine], axis=1)
    qlin, klin, q, k, v, attn, total, top_all = attn_forward(
        n_ctx, normed, wqkv, cosine, sine, gain_query, gain_key, doc, top_own, tokens
    )
    top_all = top_all.reshape(length, width)
    blocks = (n_ctx, tokens, width)
    after, normed2 = middle(n_ctx, attn, wout, inputs, gain_ffn)
    normed2 = normed2.reshape(length, width)

    z = lax.axis_index("dp").astype(jnp.int32).reshape(1)
    carried, chunk_grads = (), []
    hidden = w_gate.shape[2]
    chunks = [(0, 0, 256), (0, 256, hidden)] + [(e, 0, hidden) for e in range(1, own_e)]
    for e, low, high in chunks:
        if low == 0:
            cuts = [(f, g) for o, f, g in chunks if o == e]
            packed_e = pack(cuts, w_gate[e], w_up[e], w_down[e])
        block = packed_e[cuts.index((low, high))]
        if e == 0:
            sources = [(lax.all_gather(block, "dp", axis=0, tiled=False), "all", 0, 0)]
        else:
            sources = [(block, "up", 0, 0)]
            up = down = after_of(block, after)
            for hop in range(1, n_dp):
                if hop == 2:
                    up, down = after_of(up, *carried), after_of(down, *carried)
                up, down = line_hop(up, down, n_dp, hop)
                sources += [(up, "up", hop, 0), (down, "down", hop, 0)]
        moe, rows_grad, grads = expert(
            z, normed2, top_all, my_probs[:, e : e + 1], n_dp, sources, carried, tokens
        )
        carried = (moe, rows_grad)
        grads = grads.reshape(3 * width, high - low)
        chunk_grads.append(lax.psum_scatter(grads, "dp", scatter_dimension=0, tiled=True))
    mid, ffn_part, branch = turn(
        n_ctx, rows_grad.reshape(blocks), after, top_own, gain_ffn
    )
    branch = branch.reshape(length, width)

    out_w = dot(attn, branch, TN).astype(BF16)
    out_w = scatter_dp(out_w)
    dqkv, gains = attn_backward(
        branch, wout, attn, total, q, k, v, qlin, klin, cosine, sine, gain_query, gain_key, doc, tokens
    )
    input_grad, attn_part = last(n_ctx, dqkv, wqkv, inputs, mid, gain_attn)
    moe = after_of(moe, attn_part)
    layer_output = close(n_ctx, moe.reshape(blocks), after)

    out_w = lax.ppermute(out_w, both, [(b, a) for a, b in forth]).astype(F32)
    qkv_w = dot(normed, dqkv, TN).astype(BF16)
    qkv_w = scatter_dp(qkv_w)
    n_all = n_dp * n_ctx
    packed = jnp.concatenate(
        [
            attn_part[0].reshape(n_all, cut),
            ffn_part[0].reshape(n_all, cut),
            gains[0].reshape(n_all, hcut),
            gains[1].reshape(n_all, hcut),
            jnp.zeros((n_all, 1024 - kinds), F32),
        ],
        axis=1,
    )
    packed = packed.reshape(n_dp, n_ctx, 8, HD).transpose(1, 0, 2, 3)
    qkv_w, packed = post(n_ctx, n_dp, qkv_w.reshape(n_ctx, depth, qw + 2 * HD), packed)
    packed = packed.reshape(1024)
    query_w = qkv_w[:, :, :qw].transpose(1, 0, 2).reshape(depth, HQ * HD).astype(F32)
    kv_w = jnp.sum(qkv_w[:, :, qw:].astype(F32).reshape(KV, share, depth, 2 * HD), axis=1)
    key_w = kv_w[:, :, :HD].transpose(1, 0, 2).reshape(depth, KV * HD)
    value_w = kv_w[:, :, HD:].transpose(1, 0, 2).reshape(depth, KV * HD)

    gate_w, up_w, down_w = unpack(own_e, chunks, chunk_grads, hidden)
    return (
        layer_output.reshape(1, tokens, width),
        input_grad.reshape(1, tokens, width),
        packed[:cut],
        packed[cut : 2 * cut],
        packed[2 * cut : 2 * cut + hcut],
        packed[2 * cut + hcut : kinds],
        query_w,
        key_w,
        value_w,
        out_w,
        gate_w,
        up_w,
        down_w,
    )


def solution(mesh):
    both = ("dp", "ctx")
    seq = P("dp", "ctx", None)
    in_specs = (
        seq,
        P("dp", "ctx"),
        seq,
        seq,
        P(both),
        P(both),
        P(both),
        P(both),
        P(both, None),
        P(both, None),
        P(both, None),
        P(both, None),
        P("ctx", "dp", None),
        P("ctx", "dp", None),
        P("ctx", None, "dp"),
        seq,
    )
    out_specs = (
        seq,
        seq,
        P(both),
        P(both),
        P(both),
        P(both),
        P(both, None),
        P(both, None),
        P(both, None),
        P(both, None),
        P("ctx", "dp", None),
        P("ctx", "dp", None),
        P("ctx", None, "dp"),
    )

    return jax.shard_map(
        per_device, mesh=mesh, in_specs=in_specs, out_specs=out_specs, check_vma=False
    )
```

```python
import functools
import math

import jax
import jax.numpy as jnp
from jax import lax
from jax.experimental import pallas as pl
from jax.experimental.pallas import tpu as pltpu
from jax.sharding import PartitionSpec as P


HQ = 32
KV = 4
HD = 128
TOP = 8
MOST = 1024
EPS = 1e-06
ROPE_BASE = 1000000.0
F32 = jnp.float32
BF16 = jnp.bfloat16
SCALE = 1.0 / math.sqrt(HD)
VMEM_LIMIT = 60 * 1024 * 1024


def dot(left, right, dims=((1,), (0,))):
    return lax.dot_general(left, right, (dims, ((), ())), preferred_element_type=F32)


NT = ((1,), (1,))
TN = ((0,), (0,))


def rms_parts(values):
    return lax.rsqrt(jnp.mean(values * values, axis=-1, keepdims=True) + EPS)


def rms_back(grad, unit, inv, gain):
    scaled = grad * gain
    return inv * (scaled - unit * jnp.mean(scaled * unit, axis=-1, keepdims=True))


def head_forward(lin, gain, cosine, sine):
    unit = lin * rms_parts(lin) * gain
    return unit * cosine + pltpu.roll(unit, HD // 2, 1) * sine


def head_backward(lin, gain, cosine, sine, rot_grad):
    grad = rot_grad * cosine + pltpu.roll(rot_grad * sine, HD // 2, 1)
    inv = rms_parts(lin)
    unit = lin * inv
    return rms_back(grad, unit, inv, gain), jnp.sum(grad * unit, axis=0, keepdims=True)


MESH = pl.DeviceIdType.MESH
ANY = pl.BlockSpec(memory_space=pl.ANY)
VM = pl.BlockSpec(memory_space=pltpu.VMEM)
DMA = pltpu.SemaphoreType.DMA
CHUNK = 32


def flip(index, mask, count):
    result, bit = 0, 1
    while bit < count:
        digit = (index // bit) % 2
        result = result + bit * ((1 - digit) if mask & bit else digit)
        bit *= 2
    return result


def push(src, dst, send, recv, axis, peer):
    return pltpu.make_async_remote_copy(
        src_ref=src,
        dst_ref=dst,
        send_sem=send,
        recv_sem=recv,
        device_id={axis: peer},
        device_id_type=MESH,
    )


def meet(peers):
    barrier = pltpu.get_barrier_semaphore()
    for axis, peer in peers:
        pl.semaphore_signal(barrier, inc=1, device_id={axis: peer}, device_id_type=MESH)
    pl.semaphore_wait(barrier, len(peers))


class Plane:
    def __init__(self, n):
        self.chips = n // 2
        self.me = lax.axis_index("ctx")
        self.core = self.me % 2
        self.chip = self.me // 2
        self.mate = self.me + 1 - 2 * self.core

    def same(self, s):
        return 2 * flip(self.chip, s, self.chips) + self.core

    def meet(self):
        meet([("ctx", self.same(s)) for s in range(1, self.chips)] + [("ctx", self.mate)])


def far_first(chips):
    return sorted(range(1, chips), key=lambda s: -bin(s).count("1"))


class Gather:
    def __init__(self, plane, src, out, send, recv, local):
        self.plane, self.out, self.send, self.recv = plane, out, send, recv
        self.own = pltpu.make_async_copy(src, out.at[plane.me], local)
        self.far = [
            push(src, out.at[plane.me], send.at[s], recv.at[s], "ctx", plane.same(s))
            for s in far_first(plane.chips)
        ]
        self.near = push(src, out.at[plane.me], send.at[0], recv.at[0], "ctx", plane.mate)

    def start(self):
        for copy in self.far:
            copy.start()
        self.near.start()
        self.own.start()

    def forward(self):
        plane, out = self.plane, self.out
        self.passed = []
        for s in sorted(range(1, plane.chips), key=lambda s: bin(s).count("1")):
            block = out.at[plane.same(s)]
            push(block, block, self.send.at[s], self.recv.at[s], "ctx", plane.mate).wait_recv()
            slot = plane.chips + s
            copy = push(block, block, self.send.at[slot], self.recv.at[slot], "ctx", plane.mate)
            copy.start()
            self.passed.append(copy)

    def finish(self):
        for copy in self.far:
            copy.wait_send()
        self.near.wait_send()
        self.near.wait_recv()
        for copy in self.passed:
            copy.wait_send()
            copy.wait_recv()
        self.own.wait()


def by_rows(rows, body):
    def one(index, carry):
        body(pl.ds(pl.multiple_of(index * CHUNK, CHUNK), CHUNK))
        return carry

    lax.fori_loop(0, rows // CHUNK, one, 0)


class SquareGather:
    def __init__(self, plane, src, out, send, recv, local):
        self.plane, self.out, self.send, self.recv = plane, out, send, recv
        half = src.shape[0] // 2
        self.halves = [pl.ds(0, half), pl.ds(half, half)]
        mine = out.at[plane.me]
        self.own = pltpu.make_async_copy(src, mine, local)
        self.near = push(src, mine, send.at[0], recv.at[0], "ctx", plane.mate)
        self.far = []
        for s, h in ((1, 0), (2, 1), (1, 1), (2, 0)):
            part, slot = self.halves[h], 2 * s + h
            self.far.append(
                push(
                    src.at[part, :],
                    mine.at[part, :],
                    send.at[slot],
                    recv.at[slot],
                    "ctx",
                    plane.same(s),
                )
            )

    def start(self):
        for copy in self.far:
            copy.start()
        self.near.start()
        self.own.start()

    def arrived(self, s, h):
        block = self.out.at[self.plane.same(s)].at[self.halves[h], :]
        slot = 2 * s + h
        push(block, block, self.send.at[slot], self.recv.at[slot], "ctx", self.plane.mate).wait_recv()
        return block

    def forward(self):
        plane = self.plane
        self.passed = []
        for s, h in ((1, 0), (2, 1)):
            block = self.arrived(s, h)
            slot = 6 + h
            copy = push(block, block, self.send.at[slot], self.recv.at[slot], "ctx", plane.same(3 - s))
            copy.start()
            self.far.append(copy)
        for s in (1, 2, 3):
            if s < 3:
                self.arrived(s, 2 - s)
            else:
                self.arrived(3, 0)
                self.arrived(3, 1)
            block, slot = self.out.at[plane.same(s)], 7 + s
            copy = push(block, block, self.send.at[slot], self.recv.at[slot], "ctx", plane.mate)
            copy.start()
            self.passed.append(copy)

    def finish(self):
        for copy in self.far:
            copy.wait_send()
        self.near.wait_send()
        self.near.wait_recv()
        for copy in self.passed:
            copy.wait_send()
            copy.wait_recv()
        self.own.wait()


def gather_of(plane, src, out, send, recv, local):
    kind = SquareGather if plane.chips == 4 else Gather
    return kind(plane, src, out, send, recv, local)


class Spread:
    def __init__(self, plane, mine, landed, send, recv):
        self.plane, self.mine, self.landed = plane, mine, landed
        self.square = plane.chips == 4
        self.order = [3, 1, 2, 0] if self.square else far_first(plane.chips) + [0]
        self.send, self.recv = send, recv
        self.sent = []
        half = mine.shape[1] // 2
        self.halves = [pl.ds(0, half), pl.ds(half, half)]

    def copy(self, s, h, to):
        part, slot = self.halves[h], 2 * s + h
        return push(
            self.mine.at[s].at[part, :],
            self.landed.at[s].at[part, :],
            self.send.at[slot],
            self.recv.at[slot],
            "ctx",
            self.plane.same(to),
        )

    def go(self, s, h, to):
        copy = self.copy(s, h, to)
        copy.start()
        self.sent.append(copy)

    def ready(self, s):
        if self.square:
            if s == 3:
                self.go(3, 0, 1)
                self.go(3, 1, 2)
            elif s == 1:
                self.go(1, 0, 1)
            elif s == 2:
                self.go(2, 1, 2)
        elif s:
            copy = push(
                self.mine.at[s],
                self.landed.at[s],
                self.send.at[s],
                self.recv.at[s],
                "ctx",
                self.plane.same(s),
            )
            copy.start()
            self.sent.append(copy)

    def settle(self):
        mine, landed = self.mine, self.landed
        half = mine.shape[1] // 2
        if not self.square:
            for copy in self.sent:
                copy.wait_recv()
            return
        for s, h in ((2, 0), (1, 1)):
            self.copy(3, h, 1).wait_recv()

            def add(at, s=s, h=h):
                rows = pl.ds(h * half + at.start, CHUNK)
                total = mine[s, rows, :].astype(F32) + landed[3, rows, :].astype(F32)
                mine[s, rows, :] = total.astype(BF16)

            by_rows(half, add)
            self.go(s, h, s)
        for s in (1, 2):
            for h in (0, 1):
                self.copy(s, h, s).wait_recv()

    def total(self, at):
        value = self.mine[0, at, :].astype(F32)
        for s in (1, 2) if self.square else range(1, self.plane.chips):
            value = value + self.landed[s, at, :].astype(F32)
        return value

    def finish(self):
        for copy in self.sent:
            copy.wait_send()


class Scatter:
    def __init__(self, plane, part, mine, other, landed, send, recv, send2, recv2, local):
        self.plane, self.mine, self.other = plane, mine, other
        self.spread = Spread(plane, mine, landed, send2, recv2)
        self.order = self.spread.order
        self.loads, self.across = {}, {}
        for s in self.order:
            block = plane.same(s)
            self.loads[s] = pltpu.make_async_copy(part.at[block], mine.at[s], local.at[s])
            self.across[s] = push(
                part.at[block + 1 - 2 * plane.core],
                other.at[s],
                send.at[s],
                recv.at[s],
                "ctx",
                plane.mate,
            )

    def start(self):
        for s in self.order:
            self.across[s].start()
            self.loads[s].start()

    def run(self):
        mine, other = self.mine, self.other
        for s in self.order:
            self.loads[s].wait()
            self.across[s].wait_recv()

            def add(at, s=s):
                total = mine[s, at, :].astype(F32) + other[s, at, :].astype(F32)
                mine[s, at, :] = total.astype(BF16)

            by_rows(mine.shape[1], add)
            self.spread.ready(s)
        self.spread.settle()

    def total(self, at):
        return self.spread.total(at)

    def finish(self):
        for s in self.order:
            self.across[s].wait_send()
        self.spread.finish()


class Product:
    def __init__(self, plane, value, mine, other, landed, given, send, recv, send2, recv2):
        self.plane, self.value = plane, value
        self.mine, self.other, self.given = mine, other, given
        self.spread = Spread(plane, mine, landed, send2, recv2)
        self.order = self.spread.order
        self.across = {
            s: push(given.at[s], other.at[s], send.at[s], recv.at[s], "ctx", plane.mate)
            for s in self.order
        }

    def start(self):
        plane = self.plane
        for s in self.order:
            block = plane.same(s) + 1 - 2 * plane.core

            def fill(at, s=s, block=block):
                self.given[s, :, at] = self.value(block, at).astype(BF16)

            by_cols(self.mine.shape[2], fill)
            self.across[s].start()

    def run(self):
        plane, mine, other = self.plane, self.mine, self.other
        for s in self.order:
            block = plane.same(s)
            self.across[s].wait_recv()

            def fill(at, s=s, block=block):
                total = self.value(block, at) + other[s, :, at].astype(F32)
                mine[s, :, at] = total.astype(BF16)

            by_cols(mine.shape[2], fill)
            self.spread.ready(s)
        self.spread.settle()

    total = Scatter.total
    finish = Scatter.finish


def by_cols(width, body):
    span = 512

    def one(index, carry):
        body(pl.ds(pl.multiple_of(index * span, span), span))
        return carry

    lax.fori_loop(0, width // span, one, 0)


def gather_sems(n):
    return [DMA((12 if n == 8 else n,)), DMA((12 if n == 8 else n,)), DMA(())]


def scatter_scratch(n, rows, width):
    chips = n // 2
    return (
        [pltpu.VMEM((chips, rows, width), BF16)] * 3
        + [DMA((chips,)), DMA((chips,)), DMA((n,)), DMA((n,))]
        + [DMA((chips,))]
    )


def product_scratch(n, rows, width):
    chips = n // 2
    return [pltpu.VMEM((chips, rows, width), BF16)] * 4 + [
        DMA((chips,)),
        DMA((chips,)),
        DMA((n,)),
        DMA((n,)),
    ]


def comm_call(kernel, ident, outs, out_specs, in_specs, scratch, micros, *args):
    return pl.pallas_call(
        kernel,
        out_shape=outs,
        in_specs=in_specs,
        out_specs=out_specs,
        scratch_shapes=scratch,
        compiler_params=pltpu.CompilerParams(
            collective_id=ident, has_side_effects=True, vmem_limit_bytes=VMEM_LIMIT
        ),
        cost_estimate=pl.CostEstimate(
            flops=0, transcendentals=0, bytes_accessed=int(micros * 3.0e6)
        ),
    )(*args)


def swap_all(n, src, out, send, recv, local):
    me = lax.axis_index("ctx")
    own = pltpu.make_async_copy(src.at[me], out.at[me], local)
    own.start()
    copies = []
    for s in range(n - 1, 0, -1):
        peer = flip(me, s, n)
        copies.append(push(src.at[peer], out.at[me], send.at[s], recv.at[s], "ctx", peer))
        copies[-1].start()
    return own, copies


def prep_kernel(n, n_dp, cols_ref, small_ref, out_ref, all_ref, *sems):
    send, recv, local, gsend, grecv, zsend, zrecv = sems
    me, row = lax.axis_index("ctx"), lax.axis_index("dp")
    meet(
        [("ctx", flip(me, s, n)) for s in range(1, n)]
        + [("dp", flip(row, s, n_dp)) for s in range(1, n_dp)]
    )
    all_ref[row, me] = small_ref[...]
    smalls = []
    for s in range(1, n):
        peer = flip(me, s, n)
        smalls.append(push(small_ref, all_ref.at[row, me], gsend.at[s], grecv.at[s], "ctx", peer))
        smalls[-1].start()
    own, copies = swap_all(n, cols_ref, out_ref, send, recv, local)
    for copy in smalls:
        copy.wait_recv()
    planes = []
    for s in range(1, n_dp):
        peer = flip(row, s, n_dp)
        planes.append(push(all_ref.at[row], all_ref.at[row], zsend.at[s], zrecv.at[s], "dp", peer))
        planes[-1].start()
    for copy in copies + planes:
        copy.wait_recv()
    for copy in copies + planes + smalls:
        copy.wait_send()
    own.wait()


def gains_kernel(n, n_dp, small_ref, sum_ref, landed, mid, second, *sems):
    gsend, grecv, zsend, zrecv = sems
    me, row = lax.axis_index("ctx"), lax.axis_index("dp")
    meet(
        [("ctx", flip(me, s, n)) for s in range(1, n)]
        + [("dp", flip(row, s, n_dp)) for s in range(1, n_dp)]
    )
    smalls = []
    for s in range(1, n):
        peer = flip(me, s, n)
        smalls.append(push(small_ref.at[peer], landed.at[s], gsend.at[s], grecv.at[s], "ctx", peer))
        smalls[-1].start()
    value = small_ref[me]
    for copy, s in zip(smalls, range(1, n)):
        copy.wait_recv()
        value = value + landed[s]
    mid[...] = value
    planes = []
    for s in range(1, n_dp):
        peer = flip(row, s, n_dp)
        planes.append(push(mid.at[peer], second.at[s], zsend.at[s], zrecv.at[s], "dp", peer))
        planes[-1].start()
    value = mid[row]
    for copy, s in zip(planes, range(1, n_dp)):
        copy.wait_recv()
        value = value + second[s]
    sum_ref[...] = value
    for copy in planes + smalls:
        copy.wait_send()


def post_kernel(n, src_ref, query_ref, key_ref, value_ref, blocks, send, recv, local):
    me = lax.axis_index("ctx")
    meet([("ctx", flip(me, s, n)) for s in range(1, n)])
    own, copies = swap_all(n, src_ref, blocks, send, recv, local)
    for copy in copies:
        copy.wait_recv()
    own.wait()
    share = n // KV
    qw = HQ * HD // n
    for c in range(n):
        query_ref[:, c * qw : (c + 1) * qw] = blocks[c, :, :qw].astype(F32)
    for g in range(KV):
        for out, at in ((key_ref, qw), (value_ref, qw + HD)):
            total = blocks[g * share, :, at : at + HD].astype(F32)
            for c in range(1, share):
                total = total + blocks[g * share + c, :, at : at + HD].astype(F32)
            out[:, g * HD : (g + 1) * HD] = total
    for copy in copies:
        copy.wait_send()


def swap_sems(n, n_dp):
    return [DMA((n,)), DMA((n,)), DMA(()), DMA((n,)), DMA((n,)), DMA((n_dp,)), DMA((n_dp,))]


def prep(n, n_dp, cols, small):
    shape = jax.ShapeDtypeStruct
    return comm_call(
        functools.partial(prep_kernel, n, n_dp),
        0,
        [shape(cols.shape, cols.dtype), shape((n_dp, n) + small.shape, F32)],
        [ANY, VM],
        [ANY, VM],
        swap_sems(n, n_dp),
        8,
        cols,
        small,
    )


def gains_sum(n, n_dp, small):
    tile = small.shape[2:]
    return comm_call(
        functools.partial(gains_kernel, n, n_dp),
        8,
        jax.ShapeDtypeStruct(tile, F32),
        VM,
        [VM],
        [
            pltpu.VMEM((n, n_dp) + tile, F32),
            pltpu.VMEM((n_dp,) + tile, F32),
            pltpu.VMEM((n_dp,) + tile, F32),
            DMA((n,)),
            DMA((n,)),
            DMA((n_dp,)),
            DMA((n_dp,)),
        ],
        10,
        small,
    )


def post(n, cols):
    shape = jax.ShapeDtypeStruct
    depth = cols.shape[1]
    return comm_call(
        functools.partial(post_kernel, n),
        1,
        [
            shape((depth, HQ * HD), F32),
            shape((depth, KV * HD), F32),
            shape((depth, KV * HD), F32),
        ],
        [VM] * 3,
        [VM],
        [pltpu.VMEM(cols.shape, BF16), DMA((n,)), DMA((n,)), DMA(())],
        10,
        cols,
    )


def first_kernel(n, x_ref, gain_ref, info_ref, nall_ref, iall_ref, low, *sems):
    plane = Plane(n)
    plane.meet()
    infos = Gather(plane, info_ref, iall_ref, *sems[0:3])
    infos.start()

    def norm(at):
        value = x_ref[at, :].astype(F32)
        low[at, :] = (value * rms_parts(value) * gain_ref[...]).astype(BF16)

    by_rows(x_ref.shape[0], norm)
    normed = gather_of(plane, low, nall_ref, *sems[3:6])
    normed.start()
    infos.forward()
    normed.forward()
    infos.finish()
    normed.finish()


def first(n, x, gain, info):
    shape = jax.ShapeDtypeStruct
    many = lambda array, kind: shape((n,) + array.shape, kind)
    return comm_call(
        functools.partial(first_kernel, n),
        2,
        [many(x, BF16), many(info, F32)],
        [ANY] * 2,
        [VM] * 3,
        [pltpu.VMEM(x.shape, BF16)] + [DMA((n,)), DMA((n,)), DMA(())] + gather_sems(n),
        50,
        x,
        gain,
        info,
    )


def middle_kernel(n, attn_ref, wout_ref, x_ref, gain_ref, after_ref, all_ref, low, *scratch):
    plane = Plane(n)
    plane.meet()
    rows = x_ref.shape[0]

    def value(block, at):
        left = attn_ref[pl.ds(pl.multiple_of(block * rows, rows), rows), :]
        return dot(left, wout_ref[:, at])

    sums = Product(plane, value, *scratch[:8])
    sums.start()
    sums.run()

    def norm(at):
        value = x_ref[at, :].astype(F32) + sums.total(at)
        after_ref[at, :] = value
        low[at, :] = (value * rms_parts(value) * gain_ref[...]).astype(BF16)

    by_rows(rows, norm)
    normed = gather_of(plane, low, all_ref, *scratch[8:])
    normed.start()
    normed.forward()
    sums.finish()
    normed.finish()


def middle(n, attn, wout, x, gain):
    shape = jax.ShapeDtypeStruct
    return comm_call(
        functools.partial(middle_kernel, n),
        3,
        [shape(x.shape, F32), shape((n,) + x.shape, BF16)],
        [VM, ANY],
        [VM, VM, VM, VM],
        [pltpu.VMEM(x.shape, BF16)] + product_scratch(n, *x.shape) + gather_sems(n),
        105,
        attn,
        wout,
        x,
        gain,
    )


def turn_kernel(
    n, part_ref, after_ref, grad_ref, gain_ref, mid_ref, fpart_ref, all_ref, low, *scratch
):
    plane = Plane(n)
    plane.meet()
    sums = Scatter(plane, part_ref, *scratch[:8])
    sums.start()
    fpart_ref[...] = jnp.zeros_like(fpart_ref)
    sums.run()

    def norm(at):
        value = after_ref[at, :]
        inv = rms_parts(value)
        unit = value * inv
        grad = sums.total(at)
        fpart_ref[0:1, :] += jnp.sum(grad * unit, axis=0, keepdims=True)
        mid = grad_ref[at, :].astype(F32) + rms_back(grad, unit, inv, gain_ref[...])
        mid_ref[at, :] = mid
        low[at, :] = mid.astype(BF16)

    by_rows(after_ref.shape[0], norm)
    branch = gather_of(plane, low, all_ref, *scratch[8:])
    branch.start()
    branch.forward()
    sums.finish()
    branch.finish()


def turn(n, part, after, grad, gain):
    shape = jax.ShapeDtypeStruct
    return comm_call(
        functools.partial(turn_kernel, n),
        4,
        [
            shape(after.shape, F32),
            shape((8, after.shape[1]), F32),
            shape((n,) + after.shape, BF16),
        ],
        [VM, VM, ANY],
        [ANY, VM, VM, VM],
        [pltpu.VMEM(after.shape, BF16)] + scatter_scratch(n, *after.shape) + gather_sems(n),
        95,
        part,
        after,
        grad,
        gain,
    )


def last_kernel(
    n, grad_ref, wqkv_ref, x_ref, mid_ref, gain_ref, out_ref, apart_ref, *scratch
):
    plane = Plane(n)
    plane.meet()
    apart_ref[...] = jnp.zeros_like(apart_ref)
    rows = x_ref.shape[0]

    def value(block, at):
        left = grad_ref[pl.ds(pl.multiple_of(block * rows, rows), rows), :]
        return dot(left, wqkv_ref[at, :], NT)

    sums = Product(plane, value, *scratch[:8])
    sums.start()
    sums.run()

    def norm(at):
        value = x_ref[at, :].astype(F32)
        inv = rms_parts(value)
        unit = value * inv
        grad = sums.total(at)
        apart_ref[0:1, :] += jnp.sum(grad * unit, axis=0, keepdims=True)
        out_ref[at, :] = mid_ref[at, :] + rms_back(grad, unit, inv, gain_ref[...])

    by_rows(rows, norm)
    sums.finish()


def last(n, grad, wqkv, x, mid, gain):
    shape = jax.ShapeDtypeStruct
    return comm_call(
        functools.partial(last_kernel, n),
        5,
        [shape(mid.shape, F32), shape((8, mid.shape[1]), F32)],
        [VM, VM],
        [VM] * 5,
        product_scratch(n, *mid.shape),
        60,
        grad,
        wqkv,
        x,
        mid,
        gain,
    )


def close_kernel(n, part_ref, after_ref, out_ref, *scratch):
    plane = Plane(n)
    plane.meet()
    sums = Scatter(plane, part_ref, *scratch[:8])
    sums.start()
    sums.run()

    def add(at):
        out_ref[at, :] = (after_ref[at, :] + sums.total(at)).astype(BF16)

    by_rows(after_ref.shape[0], add)
    sums.finish()


def close(n, part, after):
    return comm_call(
        functools.partial(close_kernel, n),
        6,
        jax.ShapeDtypeStruct(after.shape, BF16),
        VM,
        [ANY, VM],
        scatter_scratch(n, *after.shape),
        50,
        part,
        after,
    )


def attn_forward_kernel(
    n,
    heads,
    back,
    normed_ref,
    wqkv_ref,
    cos_ref,
    sin_ref,
    qgain_ref,
    kgain_ref,
    docc_ref,
    docr_ref,
    grad_ref,
    qlin_ref,
    klin_ref,
    q_ref,
    k_ref,
    v_ref,
    attn_ref,
    total_ref,
    gall_ref,
    acc_ref,
    sum_ref,
    *sems,
):
    step = pl.program_id(0)

    @pl.when(step == 0)
    def _():
        plane = Plane(n)
        plane.meet()
        gather_of(plane, grad_ref, gall_ref, *sems).start()

    rows = normed_ref.shape[0]
    lin = dot(normed_ref[...], wqkv_ref[...])
    here = pl.ds(step * rows, rows)
    cosine = cos_ref[...]
    sine = sin_ref[...]
    qw = heads * HD
    for head in range(heads):
        cols = slice(head * HD, (head + 1) * HD)
        part = lin[:, cols]
        qlin_ref[:, cols] = part
        q_ref[:, cols] = head_forward(part, qgain_ref[...], cosine, sine).astype(BF16)
    key_lin = lin[:, qw : qw + HD]
    klin_ref[...] = key_lin
    k_ref[here, :] = head_forward(key_lin, kgain_ref[...], cosine, sine).astype(BF16)
    v_ref[here, :] = lin[:, qw + HD :].astype(BF16)
    acc_ref[...] = jnp.zeros_like(acc_ref)
    sum_ref[...] = jnp.zeros_like(sum_ref)
    row_pos = step * rows + lax.broadcasted_iota(jnp.int32, (rows, rows), 0)
    col_off = lax.broadcasted_iota(jnp.int32, (rows, rows), 1)

    def one(block, carry):
        at = pl.ds(pl.multiple_of(block * rows, rows), rows)
        key = k_ref[at, :]
        val = v_ref[at, :]
        allowed = (docc_ref[...] == docr_ref[:, at]) & (block * rows + col_off <= row_pos)
        for head in range(heads):
            cols = slice(head * HD, (head + 1) * HD)
            score = dot(q_ref[:, cols], key, NT) * SCALE
            expo = jnp.where(allowed, jnp.exp(score), 0.0)
            folded = expo[:, :HD]
            for piece in range(1, rows // HD):
                folded = folded + expo[:, piece * HD : (piece + 1) * HD]
            sum_ref[:, cols] += folded
            acc_ref[:, cols] += dot(expo.astype(BF16), val)
        return carry

    lax.fori_loop(jnp.maximum(step - back, 0), step + 1, one, 0)
    lane = lax.broadcasted_iota(jnp.int32, (rows, HD), 1)
    totals = jnp.ones((rows, HD), F32)
    for head in range(heads):
        cols = slice(head * HD, (head + 1) * HD)
        total = jnp.sum(sum_ref[:, cols], axis=-1, keepdims=True)
        totals = jnp.where(lane == head, total, totals)
        attn_ref[:, cols] = (acc_ref[:, cols] / total).astype(BF16)
    total_ref[...] = totals

    @pl.when(step == pl.num_programs(0) - 1)
    def _():
        grads = gather_of(Plane(n), grad_ref, gall_ref, *sems)
        grads.forward()
        grads.finish()


def attn_forward(n, normed, wqkv, cosine, sine, qgain, kgain, doc, grad, rows):
    length, width = normed.shape
    qw = wqkv.shape[1] - 2 * HD
    heads = qw // HD
    blk = lambda cols: pl.BlockSpec((rows, cols), lambda i: (i, 0))
    whole = lambda shape: pl.BlockSpec(shape, lambda i: (0, 0))
    shape = jax.ShapeDtypeStruct
    return pl.pallas_call(
        functools.partial(attn_forward_kernel, n, heads, MOST // rows),
        grid=(length // rows,),
        in_specs=[
            blk(width),
            whole(wqkv.shape),
            blk(HD),
            blk(HD),
            whole((1, HD)),
            whole((1, HD)),
            blk(1),
            whole((1, length)),
            whole(grad.shape),
        ],
        out_specs=[
            blk(qw),
            blk(HD),
            blk(qw),
            whole((length, HD)),
            whole((length, HD)),
            blk(qw),
            blk(HD),
            ANY,
        ],
        out_shape=[
            shape((length, qw), F32),
            shape((length, HD), F32),
            shape((length, qw), BF16),
            shape((length, HD), BF16),
            shape((length, HD), BF16),
            shape((length, qw), BF16),
            shape((length, HD), F32),
            shape((n,) + grad.shape, BF16),
        ],
        scratch_shapes=[pltpu.VMEM((rows, qw), F32), pltpu.VMEM((rows, qw), F32)]
        + gather_sems(n),
        compiler_params=pltpu.CompilerParams(
            collective_id=7, has_side_effects=True, vmem_limit_bytes=VMEM_LIMIT
        ),
        cost_estimate=pl.CostEstimate(
            flops=35 * 10**9, transcendentals=0, bytes_accessed=30 * 2**20
        ),
        name="attn_forward",
    )(normed, wqkv, cosine, sine, qgain, kgain, doc[:, None], doc[None, :], grad)


def attn_backward_kernel(
    heads,
    back,
    branch_ref,
    wout_ref,
    attn_ref,
    total_ref,
    q_ref,
    k_ref,
    v_ref,
    qlin_ref,
    klin_ref,
    cos_ref,
    sin_ref,
    qgain_ref,
    kgain_ref,
    docc_ref,
    docr_ref,
    dqkv_ref,
    gains_ref,
    dk_ref,
    dv_ref,
    dqa_ref,
):
    step = pl.program_id(0)
    rows = branch_ref.shape[0]
    here = pl.ds(pl.multiple_of(step * rows, rows), rows)

    @pl.when(step == 0)
    def _():
        gains_ref[...] = jnp.zeros_like(gains_ref)

    dk_ref[here, :] = jnp.zeros((rows, HD), F32)
    dv_ref[here, :] = jnp.zeros((rows, HD), F32)
    dqa_ref[...] = jnp.zeros_like(dqa_ref)
    attn_grad = dot(branch_ref[...], wout_ref[...], NT)
    grads = []
    shifts = []
    for head in range(heads):
        cols = slice(head * HD, (head + 1) * HD)
        part = attn_grad[:, cols]
        inv_total = 1.0 / total_ref[:, head : head + 1]
        delta = jnp.sum(part * attn_ref[:, cols].astype(F32), axis=-1, keepdims=True)
        grads.append((part * inv_total).astype(BF16))
        shifts.append(delta * inv_total)
    row_pos = step * rows + lax.broadcasted_iota(jnp.int32, (rows, rows), 0)
    col_off = lax.broadcasted_iota(jnp.int32, (rows, rows), 1)

    def one(block, carry):
        at = pl.ds(pl.multiple_of(block * rows, rows), rows)
        key = k_ref[at, :]
        val = v_ref[at, :]
        allowed = (docc_ref[...] == docr_ref[:, at]) & (block * rows + col_off <= row_pos)
        dk = jnp.zeros((rows, HD), F32)
        dv = jnp.zeros((rows, HD), F32)
        for head in range(heads):
            cols = slice(head * HD, (head + 1) * HD)
            query = q_ref[:, cols]
            score = dot(query, key, NT) * SCALE
            expo = jnp.where(allowed, jnp.exp(score), 0.0)
            prod = dot(grads[head], val, NT)
            score_grad = (expo * (prod - shifts[head])).astype(BF16)
            dv += dot(expo.astype(BF16), grads[head], TN)
            dk += dot(score_grad, query, TN)
            dqa_ref[:, cols] += dot(score_grad, key)
        dk_ref[at, :] += dk
        dv_ref[at, :] += dv
        return carry

    lax.fori_loop(jnp.maximum(step - back, 0), step + 1, one, 0)
    cosine = cos_ref[here, :]
    sine = sin_ref[here, :]
    for head in range(heads):
        cols = slice(head * HD, (head + 1) * HD)
        grad, gain_part = head_backward(
            qlin_ref[:, cols], qgain_ref[...], cosine, sine, dqa_ref[:, cols] * SCALE
        )
        dqkv_ref[here, cols] = grad.astype(BF16)
        gains_ref[0:1, :] += gain_part

    @pl.when(step == pl.num_programs(0) - 1)
    def _():
        def finish(block, carry):
            at = pl.ds(pl.multiple_of(block * rows, rows), rows)
            grad, gain_part = head_backward(
                klin_ref[at, :], kgain_ref[...], cos_ref[at, :], sin_ref[at, :], dk_ref[at, :] * SCALE
            )
            qw = heads * HD
            dqkv_ref[at, qw : qw + HD] = grad.astype(BF16)
            dqkv_ref[at, qw + HD :] = dv_ref[at, :].astype(BF16)
            gains_ref[1:2, :] += gain_part
            return carry

        lax.fori_loop(0, pl.num_programs(0), finish, 0)


def attn_backward(branch, wout, attn, total, q, k, v, qlin, klin, cosine, sine, qgain, kgain, doc, rows):
    length, width = branch.shape
    qw = wout.shape[0]
    heads = qw // HD
    blk = lambda cols: pl.BlockSpec((rows, cols), lambda i: (i, 0))
    whole = lambda shape: pl.BlockSpec(shape, lambda i: (0, 0))
    shape = jax.ShapeDtypeStruct
    full = whole((length, HD))
    return pl.pallas_call(
        functools.partial(attn_backward_kernel, heads, MOST // rows),
        grid=(length // rows,),
        in_specs=[
            blk(width),
            whole(wout.shape),
            blk(qw),
            blk(HD),
            blk(qw),
            full,
            full,
            blk(qw),
            full,
            full,
            full,
            whole((1, HD)),
            whole((1, HD)),
            blk(1),
            whole((1, length)),
        ],
        out_specs=[whole((length, qw + 2 * HD)), whole((8, HD))],
        out_shape=[
            shape((length, qw + 2 * HD), BF16),
            shape((8, HD), F32),
        ],
        scratch_shapes=[
            pltpu.VMEM((length, HD), F32),
            pltpu.VMEM((length, HD), F32),
            pltpu.VMEM((rows, qw), F32),
        ],
        compiler_params=pltpu.CompilerParams(vmem_limit_bytes=VMEM_LIMIT),
        cost_estimate=pl.CostEstimate(
            flops=60 * 10**9, transcendentals=0, bytes_accessed=30 * 2**20
        ),
        name="attn_backward",
    )(branch, wout, attn, total, q, k, v, qlin, klin, cosine, sine, qgain, kgain, doc[:, None], doc[None, :])


def expert_kernel(chained, low, aliased, plan, z_ref, n2_ref, top_ref, prob_ref, *rest):
    if aliased:
        rest = rest[1:]
    if chained:
        moe_in, row_in = rest[:2]
        rest = rest[2:]
    sources, rest = rest[: len(plan)], rest[len(plan) :]
    moe_ref, row_ref, grads_ref, wg_ref, wu_ref, wd_ref = rest[:6]
    ag_ref, au_ref, ad_ref, stage, wsem, sem = rest[6:]
    step = pl.program_id(0)
    rows, width = n2_ref.shape
    parts, cut, hidden = wd_ref.shape
    weights = (wg_ref, wu_ref, wd_ref)

    @pl.when(step == 0)
    def _():
        z = z_ref[0]
        for source, (kind, amount, start) in zip(sources, plan):
            count = source.shape[-2] // cut
            for k in range(parts) if kind == "all" else [amount]:
                if kind == "all":
                    src, owner, wanted = source.at[k], k, None
                elif kind == "up":
                    src, owner, wanted = source, z - k, z >= k
                else:
                    src, owner, wanted = source, z + k, z + k < parts

                def load(src=src, owner=owner, start=start, count=count):
                    for piece in range(count):
                        pltpu.make_async_copy(
                            src.at[pl.ds(piece * cut, cut), :],
                            weights[start + piece].at[owner],
                            wsem.at[start + piece, owner],
                        ).start()

                if wanted is None:
                    load()
                else:
                    pl.when(wanted)(load)
        ag_ref[...] = jnp.zeros_like(ag_ref)
        au_ref[...] = jnp.zeros_like(au_ref)
        ad_ref[...] = jnp.zeros_like(ad_ref)
        for index in range(3):
            for owner in range(parts):
                block = weights[index].at[owner]
                pltpu.make_async_copy(block, block, wsem.at[index, owner]).wait()

    n2 = n2_ref[...]
    prob = prob_ref[...]
    wg = wg_ref[...].reshape(width, hidden)
    wu = wu_ref[...].reshape(width, hidden)
    gate = dot(n2, wg)
    up = dot(n2, wu)
    sig = 1.0 / (1.0 + jnp.exp(-gate))
    silu = gate * sig
    act = (silu * up).astype(BF16)
    act_grad = jnp.zeros((rows, hidden), F32)
    for z in range(parts):
        cols = slice(z * cut, (z + 1) * cut)
        out = dot(act, wd_ref[z], NT).astype(BF16).astype(F32) * prob
        if chained:
            out = out + moe_in[:, cols].astype(F32)
        moe_ref[:, cols] = out.astype(BF16)
        route = (top_ref[:, cols].astype(F32) * prob).astype(BF16)
        act_grad += dot(route, wd_ref[z])
        ad_ref[z] += dot(route, act, TN)
    gate_grad = (act_grad * up * sig * (1.0 + gate * (1.0 - sig))).astype(BF16)
    up_grad = (act_grad * silu).astype(BF16)
    row = dot(gate_grad, wg, NT) + dot(up_grad, wu, NT)
    if chained:
        row = row + row_in[...].astype(F32)
    row_ref[...] = row.astype(BF16)
    ag_ref[...] += dot(n2, gate_grad, TN).reshape(parts, cut, hidden)
    au_ref[...] += dot(n2, up_grad, TN).reshape(parts, cut, hidden)

    @pl.when(step == pl.num_programs(0) - 1)
    def _():
        copies = []
        pieces = [
            (acc, place, z) for z in range(parts) for place, acc in enumerate((ag_ref, au_ref, ad_ref))
        ]
        for index, (acc, place, z) in enumerate(pieces):
            slot = index % 2
            if index >= 2:
                copies[index - 2].wait()
            stage[slot] = acc[z].astype(BF16)
            copies.append(
                pltpu.make_async_copy(
                    stage.at[slot],
                    grads_ref.at[z, pl.ds(place * cut, cut), pl.ds(low, acc.shape[2])],
                    sem.at[slot],
                )
            )
            copies[-1].start()
        copies[-2].wait()
        copies[-1].wait()


def expert(z, n2, top, prob, n_dp, sources, before, rows, low, full, grads):
    length, width = n2.shape
    cut = width // n_dp
    hidden = sources[0][0].shape[-1]
    blk = pl.BlockSpec((rows, width), lambda i: (i, 0))
    col = pl.BlockSpec((rows, 1), lambda i: (i, 0))
    shape = jax.ShapeDtypeStruct
    plan = tuple(entry[1:] for entry in sources)
    weight = pltpu.VMEM((n_dp, cut, hidden), BF16)
    total = pltpu.VMEM((n_dp, cut, hidden), F32)
    return pl.pallas_call(
        functools.partial(expert_kernel, len(before) > 0, low, len(grads) > 0, plan),
        grid=(length // rows,),
        in_specs=[pl.BlockSpec(memory_space=pltpu.SMEM), blk, blk, col]
        + [ANY] * len(grads)
        + [blk] * len(before)
        + [ANY] * len(sources),
        out_specs=[blk, blk, ANY],
        out_shape=[
            shape((length, width), BF16),
            shape((length, width), BF16),
            shape((n_dp, 3 * cut, full), BF16),
        ],
        input_output_aliases={4: 2} if grads else {},
        scratch_shapes=[weight] * 3
        + [total] * 3
        + [pltpu.VMEM((2, cut, hidden), BF16), DMA((3, n_dp)), DMA((2,))],
        compiler_params=pltpu.CompilerParams(vmem_limit_bytes=VMEM_LIMIT),
        cost_estimate=pl.CostEstimate(
            flops=18 * length * width * hidden,
            transcendentals=length * hidden,
            bytes_accessed=5 * length * width * 2,
        ),
        name="expert",
    )(z, n2, top, prob, *grads, *before, *[entry[0] for entry in sources])


def pack_kernel(cuts, gate_ref, up_ref, down_ref, *outs):
    cut = gate_ref.shape[0]
    for (low, high), out in zip(cuts, outs):
        out[:cut, :] = gate_ref[:, low:high]
        out[cut : 2 * cut, :] = up_ref[:, low:high]
        out[2 * cut :, :] = jnp.transpose(down_ref[low:high, :].astype(F32)).astype(BF16)


def pack(cuts, w_gate, w_up, w_down):
    cut = w_gate.shape[0]
    return pl.pallas_call(
        functools.partial(pack_kernel, cuts),
        in_specs=[VM] * 3,
        out_specs=[VM] * len(cuts),
        out_shape=[jax.ShapeDtypeStruct((3 * cut, high - low), BF16) for low, high in cuts],
        name="pack",
    )(w_gate, w_up, w_down)


def unpack_kernel(chunks, *refs):
    gate_ref, up_ref, down_ref = refs[len(chunks) :]
    cut = gate_ref.shape[1]
    for (e, low, high), ref in zip(chunks, refs):
        gate_ref[e, :, low:high] = ref[:cut, :].astype(F32)
        up_ref[e, :, low:high] = ref[cut : 2 * cut, :].astype(F32)
        down_ref[e, low:high, :] = jnp.transpose(ref[2 * cut :, :].astype(F32))


def unpack(own, chunks, grads, hidden):
    cut = grads[0].shape[0] // 3
    shape = jax.ShapeDtypeStruct
    return pl.pallas_call(
        functools.partial(unpack_kernel, chunks),
        in_specs=[VM] * len(grads),
        out_specs=[VM] * 3,
        out_shape=[
            shape((own, cut, hidden), F32),
            shape((own, cut, hidden), F32),
            shape((own, hidden, cut), F32),
        ],
        compiler_params=pltpu.CompilerParams(vmem_limit_bytes=VMEM_LIMIT),
        name="unpack",
    )(*grads)


def line_hop(block_up, block_down, n_dp, hop):
    up = [(i, i + 1) for i in range(hop - 1, n_dp - 1)]
    down = [(i + 1, i) for i in range(n_dp - hop)]
    return lax.ppermute(block_up, "dp", up), lax.ppermute(block_down, "dp", down)


def reduce_hop(grads, got, n_dp, hop):
    place = lax.axis_index("dp")
    reach = n_dp - hop
    spots = (jnp.minimum(place + reach, n_dp - 1), jnp.maximum(place - reach, 0))
    blocks = [lax.dynamic_index_in_dim(grads, spot, 0, False) for spot in spots]
    if got is not None:
        blocks = [(b.astype(F32) + g.astype(F32)).astype(BF16) for b, g in zip(blocks, got)]
    up = [(i, i + 1) for i in range(hop)]
    down = [(i, i - 1) for i in range(n_dp - hop, n_dp)]
    return lax.ppermute(blocks[0], "dp", up), lax.ppermute(blocks[1], "dp", down)


def after_of(value, *others):
    return lax.optimization_barrier((value,) + others)[0]


def scatter_dp(partial):
    return lax.psum_scatter(partial.astype(BF16), "dp", scatter_dimension=0, tiled=True)


def per_device(
    layer_input,
    doc_ids,
    route_ids,
    route_probs,
    attn_gain,
    ffn_gain,
    query_gain,
    key_gain,
    w_query,
    w_key,
    w_value,
    w_out,
    w_gate,
    w_up,
    w_down,
    out_grad,
):
    tokens, width = layer_input.shape[1:]
    n_dp = lax.axis_size("dp")
    n_ctx = lax.axis_size("ctx")
    ctx_index = lax.axis_index("ctx")
    length = tokens * n_ctx
    heads = HQ // n_ctx
    share = n_ctx // KV
    qw = heads * HD
    both = ("dp", "ctx")
    depth = w_query.shape[0]
    own_e = w_gate.shape[0]

    cut = attn_gain.shape[0]
    hcut = query_gain.shape[0]
    kinds = 2 * (cut + hcut)
    small = jnp.concatenate([attn_gain, ffn_gain, query_gain, key_gain]).astype(F32)
    small = jnp.pad(small, (0, 1024 - kinds)).reshape(8, HD)
    cols = jnp.concatenate(
        [
            w_query.reshape(depth, n_ctx, qw),
            jnp.repeat(w_key.reshape(depth, KV, HD), share, axis=1),
            jnp.repeat(w_value.reshape(depth, KV, HD), share, axis=1),
        ],
        axis=2,
    ).transpose(1, 0, 2)
    cols, small = prep(n_ctx, n_dp, cols, small)
    small = small.reshape(n_dp * n_ctx, 1024)
    gain_attn = small[:, :cut].reshape(1, width)
    gain_ffn = small[:, cut : 2 * cut].reshape(1, width)
    gain_query = small[:, 2 * cut : 2 * cut + hcut].reshape(1, HD)
    gain_key = small[:, 2 * cut + hcut : kinds].reshape(1, HD)
    wqkv = lax.all_gather(cols.reshape(n_ctx * depth, qw + 2 * HD), "dp", axis=0, tiled=True)
    forth = [(c * n_dp + d, d * n_ctx + c) for d in range(n_dp) for c in range(n_ctx)]
    wout = lax.ppermute(after_of(w_out, small), both, forth)
    wout = lax.all_gather(wout, "dp", axis=0, tiled=True)

    inputs = layer_input.reshape(tokens, width)
    top_own = out_grad.reshape(tokens, width)
    n_experts = own_e * n_ctx
    match = route_ids.reshape(1, tokens, TOP) == jnp.arange(n_experts, dtype=jnp.int32)[:, None, None]
    probs = jnp.sum(jnp.where(match, route_probs.reshape(1, tokens, TOP), 0.0), axis=2)
    info = jnp.concatenate(
        [probs, doc_ids.reshape(1, tokens).astype(F32), jnp.zeros((7, tokens), F32)], axis=0
    )
    normed, info = first(n_ctx, inputs, gain_attn, info)
    normed = normed.reshape(length, width)
    doc = info[:, n_experts].reshape(length).astype(jnp.int32)
    my_probs = lax.dynamic_slice_in_dim(info, ctx_index * own_e, own_e, 1)
    my_probs = my_probs.transpose(0, 2, 1).reshape(length, own_e)

    inverse = 1.0 / ROPE_BASE ** (jnp.arange(HD // 2, dtype=F32) * 2.0 / HD)
    angles = jnp.arange(length, dtype=F32)[:, None] * inverse[None, :]
    cosine = jnp.cos(angles)
    sine = jnp.sin(angles)
    cosine = jnp.concatenate([cosine, cosine], axis=1)
    sine = jnp.concatenate([-sine, sine], axis=1)
    qlin, klin, q, k, v, attn, total, top_all = attn_forward(
        n_ctx, normed, wqkv, cosine, sine, gain_query, gain_key, doc, top_own, tokens
    )
    top_all = top_all.reshape(length, width)
    blocks = (n_ctx, tokens, width)
    after, normed2 = middle(n_ctx, attn, wout, inputs, gain_ffn)
    normed2 = normed2.reshape(length, width)

    z = lax.axis_index("dp").astype(jnp.int32).reshape(1)
    hidden = w_gate.shape[2]

    def run(e, sources, carried, low, grads):
        moe, rows_grad, grads = expert(
            z,
            normed2,
            top_all,
            my_probs[:, e : e + 1],
            n_dp,
            sources,
            carried,
            tokens,
            low,
            hidden,
            grads,
        )
        return (moe, rows_grad), grads

    cuts = [(0, 256), (256, hidden)]
    blocks0 = pack(cuts, w_gate[0], w_up[0], w_down[0])
    carried, grads0 = (), ()
    for index, (low, high) in enumerate(cuts):
        full = lax.all_gather(blocks0[index], "dp", axis=0, tiled=False)
        if index == 1:
            (block1,) = pack([(0, hidden)], w_gate[1], w_up[1], w_down[1])
            sources1 = [(block1, "up", 0, 0)]
            up = down = after_of(block1, full)
            up, down = line_hop(up, down, n_dp, 1)
            sources1 += [(up, "up", 1, 0), (down, "down", 1, 0)]
        carried, grads = run(0, [(full, "all", 0, 0)], carried, low, grads0)
        grads0 = (grads,)
    got = None
    for hop in range(2, n_dp + 1):
        if hop == 2:
            up, down, grads = lax.optimization_barrier((up, down, grads))
        else:
            up, down, got = lax.optimization_barrier((up, down, got))
        if hop < n_dp:
            up, down = line_hop(up, down, n_dp, hop)
            sources1 += [(up, "up", hop, 0), (down, "down", hop, 0)]
        got = reduce_hop(grads, got, n_dp, hop - 1)
    (moe, rows_grad), grads1 = run(1, sources1, carried, 0, ())
    own0 = lax.dynamic_index_in_dim(grads, lax.axis_index("dp"), 0, False).astype(F32)
    done1 = lax.psum_scatter(
        grads1.reshape(3 * width, hidden), "dp", scatter_dimension=0, tiled=True
    )
    done0 = own0 + got[0].astype(F32) + got[1].astype(F32)
    mid, ffn_part, branch = turn(
        n_ctx, rows_grad.reshape(blocks), after, top_own, gain_ffn
    )
    branch = branch.reshape(length, width)

    out_w = dot(attn, branch, TN).astype(BF16)
    out_w = scatter_dp(out_w)
    dqkv, gains = attn_backward(
        branch, wout, attn, total, q, k, v, qlin, klin, cosine, sine, gain_query, gain_key, doc, tokens
    )
    input_grad, attn_part = last(n_ctx, dqkv, wqkv, inputs, mid, gain_attn)
    moe = after_of(moe, attn_part)
    layer_output = close(n_ctx, moe.reshape(blocks), after)

    out_w = lax.ppermute(out_w, both, [(b, a) for a, b in forth])
    out_w = out_w.astype(F32)
    qkv_w = dot(normed, dqkv, TN).astype(BF16)
    qkv_w = scatter_dp(qkv_w)
    n_all = n_dp * n_ctx
    packed = jnp.concatenate(
        [
            attn_part[0].reshape(n_all, cut),
            ffn_part[0].reshape(n_all, cut),
            gains[0].reshape(n_all, hcut),
            gains[1].reshape(n_all, hcut),
            jnp.zeros((n_all, 1024 - kinds), F32),
        ],
        axis=1,
    )
    packed = packed.reshape(n_dp, n_ctx, 8, HD).transpose(1, 0, 2, 3)
    packed = gains_sum(n_ctx, n_dp, after_of(packed, layer_output)).reshape(1024)
    query_w, key_w, value_w = post(n_ctx, qkv_w.reshape(n_ctx, depth, qw + 2 * HD))

    gate_w, up_w, down_w = unpack(own_e, [(0, 0, hidden), (1, 0, hidden)], [done0, done1], hidden)
    return (
        layer_output.reshape(1, tokens, width),
        input_grad.reshape(1, tokens, width),
        packed[:cut],
        packed[cut : 2 * cut],
        packed[2 * cut : 2 * cut + hcut],
        packed[2 * cut + hcut : kinds],
        query_w,
        key_w,
        value_w,
        out_w,
        gate_w,
        up_w,
        down_w,
    )


def solution(mesh):
    both = ("dp", "ctx")
    seq = P("dp", "ctx", None)
    in_specs = (
        seq,
        P("dp", "ctx"),
        seq,
        seq,
        P(both),
        P(both),
        P(both),
        P(both),
        P(both, None),
        P(both, None),
        P(both, None),
        P(both, None),
        P("ctx", "dp", None),
        P("ctx", "dp", None),
        P("ctx", None, "dp"),
        seq,
    )
    out_specs = (
        seq,
        seq,
        P(both),
        P(both),
        P(both),
        P(both),
        P(both, None),
        P(both, None),
        P(both, None),
        P(both, None),
        P("ctx", "dp", None),
        P("ctx", "dp", None),
        P("ctx", None, "dp"),
    )

    return jax.shard_map(
        per_device, mesh=mesh, in_specs=in_specs, out_specs=out_specs, check_vma=False
    )
```

```python
import functools
import math

import jax
import jax.numpy as jnp
from jax import lax
from jax.experimental import pallas as pl
from jax.experimental.pallas import tpu as pltpu
from jax.sharding import PartitionSpec as P


HQ = 32
KV = 4
HD = 128
TOP = 8
MOST = 1024
EPS = 1e-06
ROPE_BASE = 1000000.0
F32 = jnp.float32
BF16 = jnp.bfloat16
SCALE = 1.0 / math.sqrt(HD)
SCALE2 = SCALE / math.log(2.0)
VMEM_LIMIT = 60 * 1024 * 1024


def dot(left, right, dims=((1,), (0,))):
    return lax.dot_general(left, right, (dims, ((), ())), preferred_element_type=F32)


NT = ((1,), (1,))
TN = ((0,), (0,))


def rms_parts(values):
    return lax.rsqrt(jnp.mean(values * values, axis=-1, keepdims=True) + EPS)


def rms_back(grad, unit, inv, gain):
    scaled = grad * gain
    return inv * (scaled - unit * jnp.mean(scaled * unit, axis=-1, keepdims=True))


def head_forward(lin, gain, cosine, sine):
    unit = lin * rms_parts(lin) * gain
    return unit * cosine + pltpu.roll(unit, HD // 2, 1) * sine


def head_backward(lin, gain, cosine, sine, rot_grad):
    grad = rot_grad * cosine + pltpu.roll(rot_grad * sine, HD // 2, 1)
    inv = rms_parts(lin)
    unit = lin * inv
    return rms_back(grad, unit, inv, gain), jnp.sum(grad * unit, axis=0, keepdims=True)


MESH = pl.DeviceIdType.MESH
ANY = pl.BlockSpec(memory_space=pl.ANY)
VM = pl.BlockSpec(memory_space=pltpu.VMEM)
DMA = pltpu.SemaphoreType.DMA
CHUNK = 32


def flip(index, mask, count):
    result, bit = 0, 1
    while bit < count:
        digit = (index // bit) % 2
        result = result + bit * ((1 - digit) if mask & bit else digit)
        bit *= 2
    return result


def push(src, dst, send, recv, axis, peer):
    return pltpu.make_async_remote_copy(
        src_ref=src,
        dst_ref=dst,
        send_sem=send,
        recv_sem=recv,
        device_id={axis: peer},
        device_id_type=MESH,
    )


def meet(peers):
    barrier = pltpu.get_barrier_semaphore()
    for axis, peer in peers:
        pl.semaphore_signal(barrier, inc=1, device_id={axis: peer}, device_id_type=MESH)
    pl.semaphore_wait(barrier, len(peers))


class Plane:
    def __init__(self, n):
        self.chips = n // 2
        self.me = lax.axis_index("ctx")
        self.core = self.me % 2
        self.chip = self.me // 2
        self.mate = self.me + 1 - 2 * self.core

    def same(self, s):
        return 2 * flip(self.chip, s, self.chips) + self.core

    def meet(self):
        meet([("ctx", self.same(s)) for s in range(1, self.chips)] + [("ctx", self.mate)])


def far_first(chips):
    return sorted(range(1, chips), key=lambda s: -bin(s).count("1"))


class Gather:
    def __init__(self, plane, src, out, send, recv, local):
        self.plane, self.out, self.send, self.recv = plane, out, send, recv
        self.own = pltpu.make_async_copy(src, out.at[plane.me], local)
        self.far = [
            push(src, out.at[plane.me], send.at[s], recv.at[s], "ctx", plane.same(s))
            for s in far_first(plane.chips)
        ]
        self.near = push(src, out.at[plane.me], send.at[0], recv.at[0], "ctx", plane.mate)

    def start(self):
        for copy in self.far:
            copy.start()
        self.near.start()
        self.own.start()

    def forward(self):
        plane, out = self.plane, self.out
        self.passed = []
        for s in sorted(range(1, plane.chips), key=lambda s: bin(s).count("1")):
            block = out.at[plane.same(s)]
            push(block, block, self.send.at[s], self.recv.at[s], "ctx", plane.mate).wait_recv()
            slot = plane.chips + s
            copy = push(block, block, self.send.at[slot], self.recv.at[slot], "ctx", plane.mate)
            copy.start()
            self.passed.append(copy)

    def finish(self):
        for copy in self.far:
            copy.wait_send()
        self.near.wait_send()
        self.near.wait_recv()
        for copy in self.passed:
            copy.wait_send()
            copy.wait_recv()
        self.own.wait()


def by_rows(rows, body):
    def one(index, carry):
        body(pl.ds(pl.multiple_of(index * CHUNK, CHUNK), CHUNK))
        return carry

    lax.fori_loop(0, rows // CHUNK, one, 0)


class SquareGather:
    def __init__(self, plane, src, out, send, recv, local):
        self.plane, self.out, self.send, self.recv = plane, out, send, recv
        half = src.shape[0] // 2
        self.halves = [pl.ds(0, half), pl.ds(half, half)]
        mine = out.at[plane.me]
        self.own = pltpu.make_async_copy(src, mine, local)
        self.near = push(src, mine, send.at[0], recv.at[0], "ctx", plane.mate)
        self.far = []
        for s, h in ((1, 0), (2, 1), (1, 1), (2, 0)):
            part, slot = self.halves[h], 2 * s + h
            self.far.append(
                push(
                    src.at[part, :],
                    mine.at[part, :],
                    send.at[slot],
                    recv.at[slot],
                    "ctx",
                    plane.same(s),
                )
            )

    def start(self):
        for copy in self.far:
            copy.start()
        self.near.start()
        self.own.start()

    def arrived(self, s, h):
        block = self.out.at[self.plane.same(s)].at[self.halves[h], :]
        slot = 2 * s + h
        push(block, block, self.send.at[slot], self.recv.at[slot], "ctx", self.plane.mate).wait_recv()
        return block

    def forward(self):
        plane = self.plane
        self.passed = []
        for s, h in ((1, 0), (2, 1)):
            block = self.arrived(s, h)
            slot = 6 + h
            copy = push(block, block, self.send.at[slot], self.recv.at[slot], "ctx", plane.same(3 - s))
            copy.start()
            self.far.append(copy)
        for s in (1, 2, 3):
            if s < 3:
                self.arrived(s, 2 - s)
            else:
                self.arrived(3, 0)
                self.arrived(3, 1)
            block, slot = self.out.at[plane.same(s)], 7 + s
            copy = push(block, block, self.send.at[slot], self.recv.at[slot], "ctx", plane.mate)
            copy.start()
            self.passed.append(copy)

    def finish(self):
        for copy in self.far:
            copy.wait_send()
        self.near.wait_send()
        self.near.wait_recv()
        for copy in self.passed:
            copy.wait_send()
            copy.wait_recv()
        self.own.wait()


def gather_of(plane, src, out, send, recv, local):
    kind = SquareGather if plane.chips == 4 else Gather
    return kind(plane, src, out, send, recv, local)


class Spread:
    def __init__(self, plane, mine, landed, send, recv):
        self.plane, self.mine, self.landed = plane, mine, landed
        self.square = plane.chips == 4
        self.order = [3, 1, 2, 0] if self.square else far_first(plane.chips) + [0]
        self.send, self.recv = send, recv
        self.sent = []
        half = mine.shape[1] // 2
        self.halves = [pl.ds(0, half), pl.ds(half, half)]

    def copy(self, s, h, to):
        part, slot = self.halves[h], 2 * s + h
        return push(
            self.mine.at[s].at[part, :],
            self.landed.at[s].at[part, :],
            self.send.at[slot],
            self.recv.at[slot],
            "ctx",
            self.plane.same(to),
        )

    def go(self, s, h, to):
        copy = self.copy(s, h, to)
        copy.start()
        self.sent.append(copy)

    def ready(self, s):
        if self.square:
            if s == 3:
                self.go(3, 0, 1)
                self.go(3, 1, 2)
            elif s == 1:
                self.go(1, 0, 1)
            elif s == 2:
                self.go(2, 1, 2)
        elif s:
            copy = push(
                self.mine.at[s],
                self.landed.at[s],
                self.send.at[s],
                self.recv.at[s],
                "ctx",
                self.plane.same(s),
            )
            copy.start()
            self.sent.append(copy)

    def settle(self, extra=None):
        mine, landed = self.mine, self.landed
        half = mine.shape[1] // 2
        if not self.square:
            if extra is not None:
                extra()
            for copy in self.sent:
                copy.wait_recv()
            return
        for s, h in ((2, 0), (1, 1)):
            self.copy(3, h, 1).wait_recv()

            def add(at, s=s, h=h):
                rows = pl.ds(h * half + at.start, CHUNK)
                total = mine[s, rows, :].astype(F32) + landed[3, rows, :].astype(F32)
                mine[s, rows, :] = total.astype(BF16)

            by_rows(half, add)
            self.go(s, h, s)
        if extra is not None:
            extra()
        for s in (1, 2):
            for h in (0, 1):
                self.copy(s, h, s).wait_recv()

    def total(self, at):
        value = self.mine[0, at, :].astype(F32)
        for s in (1, 2) if self.square else range(1, self.plane.chips):
            value = value + self.landed[s, at, :].astype(F32)
        return value

    def finish(self):
        for copy in self.sent:
            copy.wait_send()


class Scatter:
    def __init__(self, plane, part, mine, other, landed, send, recv, send2, recv2, local):
        self.plane, self.mine, self.other = plane, mine, other
        self.spread = Spread(plane, mine, landed, send2, recv2)
        self.order = self.spread.order
        self.loads, self.across = {}, {}
        for s in self.order:
            block = plane.same(s)
            self.loads[s] = pltpu.make_async_copy(part.at[block], mine.at[s], local.at[s])
            self.across[s] = push(
                part.at[block + 1 - 2 * plane.core],
                other.at[s],
                send.at[s],
                recv.at[s],
                "ctx",
                plane.mate,
            )

    def start(self):
        for s in self.order:
            self.across[s].start()
            self.loads[s].start()

    def run(self, extra=None):
        mine, other = self.mine, self.other
        for s in self.order:
            self.loads[s].wait()
            self.across[s].wait_recv()

            def add(at, s=s):
                total = mine[s, at, :].astype(F32) + other[s, at, :].astype(F32)
                mine[s, at, :] = total.astype(BF16)

            by_rows(mine.shape[1], add)
            self.spread.ready(s)
        if extra is not None:
            extra()
        self.spread.settle()

    def total(self, at):
        return self.spread.total(at)

    def finish(self):
        for s in self.order:
            self.across[s].wait_send()
        self.spread.finish()


class Product:
    def __init__(self, plane, value, mine, other, landed, given, send, recv, send2, recv2):
        self.plane, self.value = plane, value
        self.mine, self.other, self.given = mine, other, given
        self.spread = Spread(plane, mine, landed, send2, recv2)
        self.order = self.spread.order
        self.across = {
            s: push(given.at[s], other.at[s], send.at[s], recv.at[s], "ctx", plane.mate)
            for s in self.order
        }

    def start(self):
        plane = self.plane
        for s in self.order:
            block = plane.same(s) + 1 - 2 * plane.core

            def fill(at, s=s, block=block):
                self.given[s, :, at] = self.value(block, at).astype(BF16)

            by_cols(self.mine.shape[2], fill)
            self.across[s].start()

    def run(self, extra=None):
        plane, mine, other = self.plane, self.mine, self.other
        for s in self.order:
            block = plane.same(s)
            self.across[s].wait_recv()

            def fill(at, s=s, block=block):
                total = self.value(block, at) + other[s, :, at].astype(F32)
                mine[s, :, at] = total.astype(BF16)

            by_cols(mine.shape[2], fill)
            self.spread.ready(s)
        self.spread.settle(extra)

    total = Scatter.total
    finish = Scatter.finish


def by_cols(width, body):
    span = 512

    def one(index, carry):
        body(pl.ds(pl.multiple_of(index * span, span), span))
        return carry

    lax.fori_loop(0, width // span, one, 0)


def gather_sems(n):
    return [DMA((12 if n == 8 else n,)), DMA((12 if n == 8 else n,)), DMA(())]


def scatter_scratch(n, rows, width):
    chips = n // 2
    return (
        [pltpu.VMEM((chips, rows, width), BF16)] * 3
        + [DMA((chips,)), DMA((chips,)), DMA((n,)), DMA((n,))]
        + [DMA((chips,))]
    )


def product_scratch(n, rows, width):
    chips = n // 2
    return [pltpu.VMEM((chips, rows, width), BF16)] * 4 + [
        DMA((chips,)),
        DMA((chips,)),
        DMA((n,)),
        DMA((n,)),
    ]


def comm_call(kernel, ident, outs, out_specs, in_specs, scratch, micros, *args):
    return pl.pallas_call(
        kernel,
        out_shape=outs,
        in_specs=in_specs,
        out_specs=out_specs,
        scratch_shapes=scratch,
        compiler_params=pltpu.CompilerParams(
            collective_id=ident, has_side_effects=True, vmem_limit_bytes=VMEM_LIMIT
        ),
        cost_estimate=pl.CostEstimate(
            flops=0, transcendentals=0, bytes_accessed=int(micros * 3.0e6)
        ),
    )(*args)


def swap_all(n, src, out, send, recv, local):
    me = lax.axis_index("ctx")
    own = pltpu.make_async_copy(src.at[me], out.at[me], local)
    own.start()
    copies = []
    for s in range(n - 1, 0, -1):
        peer = flip(me, s, n)
        copies.append(push(src.at[peer], out.at[me], send.at[s], recv.at[s], "ctx", peer))
        copies[-1].start()
    return own, copies


class RowSwap:
    def __init__(self, n, n_dp, src, dst, send, recv, spread):
        self.me = lax.axis_index("ctx")
        self.dst, self.send, self.recv, self.n_dp = dst, send, recv, n_dp
        self.entries = []
        for k in range(n_dp):
            flat = self.me * n_dp + k if spread else k * n + self.me
            peer = flat % n if spread else flat // n_dp
            slot = flat // n if spread else flat % n_dp
            far = push(src.at[k], dst.at[slot], send.at[k], recv.at[slot], "ctx", peer)
            near = pltpu.make_async_copy(src.at[k], dst.at[slot], recv.at[slot])
            self.entries.append((peer, far, near))

    def start(self):
        for peer, far, near in self.entries:
            pl.when(peer != self.me)(far.start)
            pl.when(peer == self.me)(near.start)

    def arrive(self):
        for slot in range(self.n_dp):
            block = self.dst.at[slot]
            pltpu.make_async_copy(block, block, self.recv.at[slot]).wait()

    def finish(self):
        for peer, far, near in self.entries:
            pl.when(peer != self.me)(far.wait_send)


def meet_all(n):
    me = lax.axis_index("ctx")
    meet([("ctx", flip(me, s, n)) for s in range(1, n)])


def prep_kernel(n, n_dp, cols_ref, small_ref, out_ref, all_ref, *sems):
    send, recv, local, gsend, grecv, zsend, zrecv = sems
    me, row = lax.axis_index("ctx"), lax.axis_index("dp")
    meet(
        [("ctx", flip(me, s, n)) for s in range(1, n)]
        + [("dp", flip(row, s, n_dp)) for s in range(1, n_dp)]
    )
    all_ref[row, me] = small_ref[...]
    smalls = []
    for s in range(1, n):
        peer = flip(me, s, n)
        smalls.append(push(small_ref, all_ref.at[row, me], gsend.at[s], grecv.at[s], "ctx", peer))
        smalls[-1].start()
    own, copies = swap_all(n, cols_ref, out_ref, send, recv, local)
    for copy in smalls:
        copy.wait_recv()
    planes = []
    for s in range(1, n_dp):
        peer = flip(row, s, n_dp)
        planes.append(push(all_ref.at[row], all_ref.at[row], zsend.at[s], zrecv.at[s], "dp", peer))
        planes[-1].start()
    for copy in copies + planes:
        copy.wait_recv()
    for copy in copies + planes + smalls:
        copy.wait_send()
    own.wait()


class Gains:
    def __init__(self, n, n_dp, small, landed, mid, second, gsend, grecv, zsend, zrecv):
        self.me, self.row = lax.axis_index("ctx"), lax.axis_index("dp")
        self.small, self.landed, self.mid, self.second = small, landed, mid, second
        self.near, self.far = [], []
        for s in range(1, n):
            peer = flip(self.me, s, n)
            self.near.append(push(small.at[peer], landed.at[s], gsend.at[s], grecv.at[s], "ctx", peer))
        for s in range(1, n_dp):
            peer = flip(self.row, s, n_dp)
            self.far.append(push(mid.at[peer], second.at[s], zsend.at[s], zrecv.at[s], "dp", peer))

    def start(self):
        for copy in self.near:
            copy.start()

    def middle(self):
        value = self.small[self.me]
        for s, copy in enumerate(self.near, 1):
            copy.wait_recv()
            value = value + self.landed[s]
        self.mid[...] = value
        for copy in self.far:
            copy.start()

    def finish(self):
        value = self.mid[self.row]
        for s, copy in enumerate(self.far, 1):
            copy.wait_recv()
            value = value + self.second[s]
        for copy in self.near + self.far:
            copy.wait_send()
        return value


def post_kernel(n, src_ref, query_ref, key_ref, value_ref, blocks, send, recv, local):
    me = lax.axis_index("ctx")
    meet([("ctx", flip(me, s, n)) for s in range(1, n)])
    own, copies = swap_all(n, src_ref, blocks, send, recv, local)
    for copy in copies:
        copy.wait_recv()
    own.wait()
    share = n // KV
    qw = HQ * HD // n
    for c in range(n):
        query_ref[:, c * qw : (c + 1) * qw] = blocks[c, :, :qw].astype(F32)
    for g in range(KV):
        for out, at in ((key_ref, qw), (value_ref, qw + HD)):
            total = blocks[g * share, :, at : at + HD].astype(F32)
            for c in range(1, share):
                total = total + blocks[g * share + c, :, at : at + HD].astype(F32)
            out[:, g * HD : (g + 1) * HD] = total
    for copy in copies:
        copy.wait_send()


def swap_sems(n, n_dp):
    return [DMA((n,)), DMA((n,)), DMA(()), DMA((n,)), DMA((n,)), DMA((n_dp,)), DMA((n_dp,))]


def prep(n, n_dp, cols, small):
    shape = jax.ShapeDtypeStruct
    return comm_call(
        functools.partial(prep_kernel, n, n_dp),
        0,
        [shape(cols.shape, cols.dtype), shape((n_dp, n) + small.shape, F32)],
        [ANY, VM],
        [ANY, VM],
        swap_sems(n, n_dp),
        8,
        cols,
        small,
    )


def post(n, cols):
    shape = jax.ShapeDtypeStruct
    depth = cols.shape[1]
    return comm_call(
        functools.partial(post_kernel, n),
        1,
        [
            shape((depth, HQ * HD), F32),
            shape((depth, KV * HD), F32),
            shape((depth, KV * HD), F32),
        ],
        [VM] * 3,
        [VM],
        [pltpu.VMEM(cols.shape, BF16), DMA((n,)), DMA((n,)), DMA(())],
        10,
        cols,
    )


def first_kernel(n, x_ref, gain_ref, info_ref, nall_ref, iall_ref, low, *sems):
    plane = Plane(n)
    plane.meet()
    infos = Gather(plane, info_ref, iall_ref, *sems[0:3])
    infos.start()

    def norm(at):
        value = x_ref[at, :].astype(F32)
        low[at, :] = (value * rms_parts(value) * gain_ref[...]).astype(BF16)

    by_rows(x_ref.shape[0], norm)
    normed = gather_of(plane, low, nall_ref, *sems[3:6])
    normed.start()
    infos.forward()
    normed.forward()
    infos.finish()
    normed.finish()


def first(n, x, gain, info):
    shape = jax.ShapeDtypeStruct
    many = lambda array, kind: shape((n,) + array.shape, kind)
    return comm_call(
        functools.partial(first_kernel, n),
        2,
        [many(x, BF16), many(info, F32)],
        [ANY] * 2,
        [VM] * 3,
        [pltpu.VMEM(x.shape, BF16)] + [DMA((n,)), DMA((n,)), DMA(())] + gather_sems(n),
        50,
        x,
        gain,
        info,
    )


def middle_kernel(
    n, n_dp, attn_ref, rows_ref, x_ref, gain_ref, after_ref, all_ref, wout_ref, low, *scratch
):
    meet_all(n)
    plane = Plane(n)
    swap = RowSwap(n, n_dp, rows_ref, wout_ref, *scratch[:2], False)
    swap.start()
    scratch = scratch[2:]
    rows = x_ref.shape[0]
    deep = wout_ref.shape[1]
    swap.arrive()

    def value(block, at):
        here = pl.ds(pl.multiple_of(block * rows, rows), rows)
        total = dot(attn_ref[here, :deep], wout_ref[0, :, at])
        for k in range(1, n_dp):
            total = total + dot(attn_ref[here, k * deep : (k + 1) * deep], wout_ref[k, :, at])
        return total

    sums = Product(plane, value, *scratch[:8])
    sums.start()
    sums.run()

    def norm(at):
        value = x_ref[at, :].astype(F32) + sums.total(at)
        after_ref[at, :] = value
        low[at, :] = (value * rms_parts(value) * gain_ref[...]).astype(BF16)

    by_rows(rows, norm)
    normed = gather_of(plane, low, all_ref, *scratch[8:])
    normed.start()
    normed.forward()
    sums.finish()
    normed.finish()
    swap.finish()


def middle(n, n_dp, attn, wrows, x, gain):
    shape = jax.ShapeDtypeStruct
    return comm_call(
        functools.partial(middle_kernel, n, n_dp),
        3,
        [shape(x.shape, F32), shape((n,) + x.shape, BF16), shape(wrows.shape, BF16)],
        [VM, ANY, VM],
        [VM, ANY, VM, VM],
        [pltpu.VMEM(x.shape, BF16), DMA((n_dp,)), DMA((n_dp,))]
        + product_scratch(n, *x.shape)
        + gather_sems(n),
        105,
        attn,
        wrows,
        x,
        gain,
    )


def turn_kernel(
    n, part_ref, after_ref, grad_ref, gain_ref, mid_ref, fpart_ref, all_ref, low, *scratch
):
    plane = Plane(n)
    plane.meet()
    sums = Scatter(plane, part_ref, *scratch[:8])
    sums.start()
    fpart_ref[...] = jnp.zeros_like(fpart_ref)
    sums.run()

    def norm(at):
        value = after_ref[at, :]
        inv = rms_parts(value)
        unit = value * inv
        grad = sums.total(at)
        fpart_ref[0:1, :] += jnp.sum(grad * unit, axis=0, keepdims=True)
        mid = grad_ref[at, :].astype(F32) + rms_back(grad, unit, inv, gain_ref[...])
        mid_ref[at, :] = mid
        low[at, :] = mid.astype(BF16)

    by_rows(after_ref.shape[0], norm)
    branch = gather_of(plane, low, all_ref, *scratch[8:])
    branch.start()
    branch.forward()
    sums.finish()
    branch.finish()


def turn(n, part, after, grad, gain):
    shape = jax.ShapeDtypeStruct
    return comm_call(
        functools.partial(turn_kernel, n),
        4,
        [
            shape(after.shape, F32),
            shape((8, after.shape[1]), F32),
            shape((n,) + after.shape, BF16),
        ],
        [VM, VM, ANY],
        [ANY, VM, VM, VM],
        [pltpu.VMEM(after.shape, BF16)] + scatter_scratch(n, *after.shape) + gather_sems(n),
        95,
        part,
        after,
        grad,
        gain,
    )


def last_kernel(
    n,
    grad_ref,
    wqkv_ref,
    x_ref,
    mid_ref,
    gain_ref,
    *rest,
):
    fused = n == 8
    normed_ref, rest = (rest[0], rest[1:]) if fused else (None, rest)
    out_ref, apart_ref, rest = rest[0], rest[1], rest[2:]
    wgrad_ref, scratch = (rest[0], rest[1:]) if fused else (None, rest)
    plane = Plane(n)
    plane.meet()
    apart_ref[...] = jnp.zeros_like(apart_ref)
    rows = x_ref.shape[0]

    def value(block, at):
        left = grad_ref[pl.ds(pl.multiple_of(block * rows, rows), rows), :]
        return dot(left, wqkv_ref[at, :], NT)

    sums = Product(plane, value, *scratch[:8])
    sums.start()

    def weights():
        def fill(at):
            wgrad_ref[at, :] = dot(normed_ref[:, at], grad_ref[...], TN).astype(BF16)

        by_cols(normed_ref.shape[1], fill)

    sums.run(weights if fused else None)

    def norm(at):
        value = x_ref[at, :].astype(F32)
        inv = rms_parts(value)
        unit = value * inv
        grad = sums.total(at)
        apart_ref[0:1, :] += jnp.sum(grad * unit, axis=0, keepdims=True)
        out_ref[at, :] = mid_ref[at, :] + rms_back(grad, unit, inv, gain_ref[...])

    by_rows(rows, norm)
    sums.finish()


def last(n, grad, wqkv, x, mid, gain, normed):
    shape = jax.ShapeDtypeStruct
    outs = [shape(mid.shape, F32), shape((8, mid.shape[1]), F32)]
    more = [normed] if n == 8 else []
    outs += [shape(wqkv.shape, BF16) for _ in more]
    got = comm_call(
        functools.partial(last_kernel, n),
        5,
        outs,
        [VM] * len(outs),
        [VM] * (5 + len(more)),
        product_scratch(n, *mid.shape),
        60,
        grad,
        wqkv,
        x,
        mid,
        gain,
        *more,
    )
    return got if more else (*got, dot(normed, grad, TN).astype(BF16))


def close_kernel(n, n_dp, part_ref, after_ref, small_ref, out_ref, sum_ref, *scratch):
    meet(
        [("ctx", flip(lax.axis_index("ctx"), s, n)) for s in range(1, n)]
        + [("dp", flip(lax.axis_index("dp"), s, n_dp)) for s in range(1, n_dp)]
    )
    plane = Plane(n)
    sums = Scatter(plane, part_ref, *scratch[:8])
    sums.start()
    gains = Gains(n, n_dp, small_ref, *scratch[8:])
    gains.start()
    sums.run(gains.middle)

    def add(at):
        out_ref[at, :] = (after_ref[at, :] + sums.total(at)).astype(BF16)

    by_rows(after_ref.shape[0], add)
    sums.finish()
    sum_ref[...] = gains.finish()


def close(n, n_dp, part, after, small):
    shape = jax.ShapeDtypeStruct
    tile = small.shape[2:]
    return comm_call(
        functools.partial(close_kernel, n, n_dp),
        6,
        [shape(after.shape, BF16), shape(tile, F32)],
        [VM, VM],
        [ANY, VM, VM],
        scatter_scratch(n, *after.shape)
        + [
            pltpu.VMEM((n, n_dp) + tile, F32),
            pltpu.VMEM((n_dp,) + tile, F32),
            pltpu.VMEM((n_dp,) + tile, F32),
            DMA((n,)),
            DMA((n,)),
            DMA((n_dp,)),
            DMA((n_dp,)),
        ],
        50,
        part,
        after,
        small,
    )


def attn_forward_kernel(
    n,
    heads,
    back,
    normed_ref,
    wqkv_ref,
    cos_ref,
    sin_ref,
    qgain_ref,
    kgain_ref,
    docc_ref,
    docr_ref,
    grad_ref,
    qlin_ref,
    klin_ref,
    q_ref,
    k_ref,
    v_ref,
    attn_ref,
    total_ref,
    gall_ref,
    acc_ref,
    sum_ref,
    *sems,
):
    step = pl.program_id(0)

    @pl.when(step == 0)
    def _():
        plane = Plane(n)
        plane.meet()
        gather_of(plane, grad_ref, gall_ref, *sems).start()

    rows = normed_ref.shape[0]
    lin = dot(normed_ref[...], wqkv_ref[...])
    here = pl.ds(step * rows, rows)
    cosine = cos_ref[...]
    sine = sin_ref[...]
    qw = heads * HD
    for head in range(heads):
        cols = slice(head * HD, (head + 1) * HD)
        part = lin[:, cols]
        qlin_ref[:, cols] = part
        q_ref[:, cols] = head_forward(part, qgain_ref[...], cosine, sine).astype(BF16)
    key_lin = lin[:, qw : qw + HD]
    klin_ref[...] = key_lin
    k_ref[here, :] = head_forward(key_lin, kgain_ref[...], cosine, sine).astype(BF16)
    v_ref[here, :] = lin[:, qw + HD :].astype(BF16)
    acc_ref[...] = jnp.zeros_like(acc_ref)
    sum_ref[...] = jnp.zeros_like(sum_ref)
    row_pos = step * rows + lax.broadcasted_iota(jnp.int32, (rows, rows), 0)
    col_off = lax.broadcasted_iota(jnp.int32, (rows, rows), 1)

    def one(block, carry):
        at = pl.ds(pl.multiple_of(block * rows, rows), rows)
        key = k_ref[at, :]
        val = v_ref[at, :]
        allowed = (docc_ref[...] == docr_ref[:, at]) & (block * rows + col_off <= row_pos)
        for head in range(heads):
            cols = slice(head * HD, (head + 1) * HD)
            score = dot(q_ref[:, cols], key, NT) * SCALE2
            expo = jnp.where(allowed, jnp.exp2(score), 0.0)
            folded = expo[:, :HD]
            for piece in range(1, rows // HD):
                folded = folded + expo[:, piece * HD : (piece + 1) * HD]
            sum_ref[:, cols] += folded
            acc_ref[:, cols] += dot(expo.astype(BF16), val)
        return carry

    lax.fori_loop(jnp.maximum(step - back, 0), step + 1, one, 0)
    lane = lax.broadcasted_iota(jnp.int32, (rows, HD), 1)
    totals = jnp.ones((rows, HD), F32)
    for head in range(heads):
        cols = slice(head * HD, (head + 1) * HD)
        total = jnp.sum(sum_ref[:, cols], axis=-1, keepdims=True)
        totals = jnp.where(lane == head, total, totals)
        attn_ref[:, cols] = (acc_ref[:, cols] / total).astype(BF16)
    total_ref[...] = totals

    @pl.when(step == pl.num_programs(0) - 1)
    def _():
        grads = gather_of(Plane(n), grad_ref, gall_ref, *sems)
        grads.forward()
        grads.finish()


def attn_forward(n, normed, wqkv, cosine, sine, qgain, kgain, doc, grad, rows):
    length, width = normed.shape
    qw = wqkv.shape[1] - 2 * HD
    heads = qw // HD
    blk = lambda cols: pl.BlockSpec((rows, cols), lambda i: (i, 0))
    whole = lambda shape: pl.BlockSpec(shape, lambda i: (0, 0))
    shape = jax.ShapeDtypeStruct
    return pl.pallas_call(
        functools.partial(attn_forward_kernel, n, heads, MOST // rows),
        grid=(length // rows,),
        in_specs=[
            blk(width),
            whole(wqkv.shape),
            blk(HD),
            blk(HD),
            whole((1, HD)),
            whole((1, HD)),
            blk(1),
            whole((1, length)),
            whole(grad.shape),
        ],
        out_specs=[
            blk(qw),
            blk(HD),
            blk(qw),
            whole((length, HD)),
            whole((length, HD)),
            blk(qw),
            blk(HD),
            ANY,
        ],
        out_shape=[
            shape((length, qw), F32),
            shape((length, HD), F32),
            shape((length, qw), BF16),
            shape((length, HD), BF16),
            shape((length, HD), BF16),
            shape((length, qw), BF16),
            shape((length, HD), F32),
            shape((n,) + grad.shape, BF16),
        ],
        scratch_shapes=[pltpu.VMEM((rows, qw), F32), pltpu.VMEM((rows, qw), F32)]
        + gather_sems(n),
        compiler_params=pltpu.CompilerParams(
            collective_id=7, has_side_effects=True, vmem_limit_bytes=VMEM_LIMIT
        ),
        cost_estimate=pl.CostEstimate(
            flops=35 * 10**9, transcendentals=0, bytes_accessed=30 * 2**20
        ),
        name="attn_forward",
    )(normed, wqkv, cosine, sine, qgain, kgain, doc[:, None], doc[None, :], grad)


def attn_backward_kernel(
    n,
    n_dp,
    heads,
    back,
    branch_ref,
    wout_ref,
    attn_ref,
    total_ref,
    q_ref,
    k_ref,
    v_ref,
    qlin_ref,
    klin_ref,
    cos_ref,
    sin_ref,
    qgain_ref,
    kgain_ref,
    docc_ref,
    docr_ref,
    wgrad_ref,
    dqkv_ref,
    gains_ref,
    swapped_ref,
    dk_ref,
    dv_ref,
    dqa_ref,
    *sems,
):
    step = pl.program_id(0)

    @pl.when(step == 0)
    def _():
        meet_all(n)
        RowSwap(n, n_dp, wgrad_ref, swapped_ref, *sems, True).start()

    @pl.when(step == pl.num_programs(0) - 1)
    def _():
        swap = RowSwap(n, n_dp, wgrad_ref, swapped_ref, *sems, True)
        swap.arrive()
        swap.finish()

    rows = branch_ref.shape[0]
    here = pl.ds(pl.multiple_of(step * rows, rows), rows)

    @pl.when(step == 0)
    def _():
        gains_ref[...] = jnp.zeros_like(gains_ref)

    dk_ref[here, :] = jnp.zeros((rows, HD), F32)
    dv_ref[here, :] = jnp.zeros((rows, HD), F32)
    dqa_ref[...] = jnp.zeros_like(dqa_ref)
    attn_grad = dot(branch_ref[...], wout_ref[...], NT)
    grads = []
    shifts = []
    for head in range(heads):
        cols = slice(head * HD, (head + 1) * HD)
        part = attn_grad[:, cols]
        inv_total = 1.0 / total_ref[:, head : head + 1]
        delta = jnp.sum(part * attn_ref[:, cols].astype(F32), axis=-1, keepdims=True)
        grads.append((part * inv_total).astype(BF16))
        shifts.append(delta * inv_total)
    row_pos = step * rows + lax.broadcasted_iota(jnp.int32, (rows, rows), 0)
    col_off = lax.broadcasted_iota(jnp.int32, (rows, rows), 1)

    def one(block, carry):
        at = pl.ds(pl.multiple_of(block * rows, rows), rows)
        key = k_ref[at, :]
        val = v_ref[at, :]
        allowed = (docc_ref[...] == docr_ref[:, at]) & (block * rows + col_off <= row_pos)
        dk = jnp.zeros((rows, HD), F32)
        dv = jnp.zeros((rows, HD), F32)
        for head in range(heads):
            cols = slice(head * HD, (head + 1) * HD)
            query = q_ref[:, cols]
            score = dot(query, key, NT) * SCALE2
            expo = jnp.where(allowed, jnp.exp2(score), 0.0)
            prod = dot(grads[head], val, NT)
            score_grad = (expo * (prod - shifts[head])).astype(BF16)
            dv += dot(expo.astype(BF16), grads[head], TN)
            dk += dot(score_grad, query, TN)
            dqa_ref[:, cols] += dot(score_grad, key)
        dk_ref[at, :] += dk
        dv_ref[at, :] += dv
        return carry

    lax.fori_loop(jnp.maximum(step - back, 0), step + 1, one, 0)
    cosine = cos_ref[here, :]
    sine = sin_ref[here, :]
    for head in range(heads):
        cols = slice(head * HD, (head + 1) * HD)
        grad, gain_part = head_backward(
            qlin_ref[:, cols], qgain_ref[...], cosine, sine, dqa_ref[:, cols] * SCALE
        )
        dqkv_ref[here, cols] = grad.astype(BF16)
        gains_ref[0:1, :] += gain_part

    @pl.when(step == pl.num_programs(0) - 1)
    def _():
        def finish(block, carry):
            at = pl.ds(pl.multiple_of(block * rows, rows), rows)
            grad, gain_part = head_backward(
                klin_ref[at, :], kgain_ref[...], cos_ref[at, :], sin_ref[at, :], dk_ref[at, :] * SCALE
            )
            qw = heads * HD
            dqkv_ref[at, qw : qw + HD] = grad.astype(BF16)
            dqkv_ref[at, qw + HD :] = dv_ref[at, :].astype(BF16)
            gains_ref[1:2, :] += gain_part
            return carry

        lax.fori_loop(0, pl.num_programs(0), finish, 0)


def attn_backward(n, n_dp, wgrad, branch, wout, attn, total, q, k, v, qlin, klin, cosine, sine, qgain, kgain, doc, rows):
    length, width = branch.shape
    qw = wout.shape[0]
    heads = qw // HD
    blk = lambda cols: pl.BlockSpec((rows, cols), lambda i: (i, 0))
    whole = lambda shape: pl.BlockSpec(shape, lambda i: (0, 0))
    shape = jax.ShapeDtypeStruct
    full = whole((length, HD))
    return pl.pallas_call(
        functools.partial(attn_backward_kernel, n, n_dp, heads, MOST // rows),
        grid=(length // rows,),
        in_specs=[
            blk(width),
            whole(wout.shape),
            blk(qw),
            blk(HD),
            blk(qw),
            full,
            full,
            blk(qw),
            full,
            full,
            full,
            whole((1, HD)),
            whole((1, HD)),
            blk(1),
            whole((1, length)),
            ANY,
        ],
        out_specs=[whole((length, qw + 2 * HD)), whole((8, HD)), ANY],
        out_shape=[
            shape((length, qw + 2 * HD), BF16),
            shape((8, HD), F32),
            shape(wgrad.shape, BF16),
        ],
        scratch_shapes=[
            pltpu.VMEM((length, HD), F32),
            pltpu.VMEM((length, HD), F32),
            pltpu.VMEM((rows, qw), F32),
            DMA((n_dp,)),
            DMA((n_dp,)),
        ],
        compiler_params=pltpu.CompilerParams(
            collective_id=9, has_side_effects=True, vmem_limit_bytes=VMEM_LIMIT
        ),
        cost_estimate=pl.CostEstimate(
            flops=60 * 10**9, transcendentals=0, bytes_accessed=30 * 2**20
        ),
        name="attn_backward",
    )(branch, wout, attn, total, q, k, v, qlin, klin, cosine, sine, qgain, kgain, doc[:, None], doc[None, :], wgrad)


def expert_kernel(chained, low, aliased, plan, z_ref, n2_ref, top_ref, prob_ref, *rest):
    if aliased:
        rest = rest[1:]
    if chained:
        moe_in, row_in = rest[:2]
        rest = rest[2:]
    sources, rest = rest[: len(plan)], rest[len(plan) :]
    moe_ref, row_ref, grads_ref, wg_ref, wu_ref, wd_ref = rest[:6]
    ag_ref, au_ref, ad_ref, stage, wsem, sem = rest[6:]
    step = pl.program_id(0)
    rows, width = n2_ref.shape
    parts, cut, hidden = wd_ref.shape
    weights = (wg_ref, wu_ref, wd_ref)

    @pl.when(step == 0)
    def _():
        z = z_ref[0]
        for source, (kind, amount, start) in zip(sources, plan):
            count = source.shape[-2] // cut
            for k in range(parts) if kind == "all" else [amount]:
                if kind == "all":
                    src, owner, wanted = source.at[k], k, None
                elif kind == "up":
                    src, owner, wanted = source, z - k, z >= k
                else:
                    src, owner, wanted = source, z + k, z + k < parts

                def load(src=src, owner=owner, start=start, count=count):
                    for piece in range(count):
                        pltpu.make_async_copy(
                            src.at[pl.ds(piece * cut, cut), :],
                            weights[start + piece].at[owner],
                            wsem.at[start + piece, owner],
                        ).start()

                if wanted is None:
                    load()
                else:
                    pl.when(wanted)(load)
        ag_ref[...] = jnp.zeros_like(ag_ref)
        au_ref[...] = jnp.zeros_like(au_ref)
        ad_ref[...] = jnp.zeros_like(ad_ref)
        for index in range(3):
            for owner in range(parts):
                block = weights[index].at[owner]
                pltpu.make_async_copy(block, block, wsem.at[index, owner]).wait()

    n2 = n2_ref[...]
    prob = prob_ref[...]
    wg = wg_ref[...].reshape(width, hidden)
    wu = wu_ref[...].reshape(width, hidden)
    gate = dot(n2, wg)
    up = dot(n2, wu)
    sig = 1.0 / (1.0 + jnp.exp(-gate))
    silu = gate * sig
    act = (silu * up).astype(BF16)
    act_grad = jnp.zeros((rows, hidden), F32)
    for z in range(parts):
        cols = slice(z * cut, (z + 1) * cut)
        out = dot(act, wd_ref[z], NT).astype(BF16).astype(F32) * prob
        if chained:
            out = out + moe_in[:, cols].astype(F32)
        moe_ref[:, cols] = out.astype(BF16)
        route = (top_ref[:, cols].astype(F32) * prob).astype(BF16)
        act_grad += dot(route, wd_ref[z])
        ad_ref[z] += dot(route, act, TN)
    gate_grad = (act_grad * up * sig * (1.0 + gate * (1.0 - sig))).astype(BF16)
    up_grad = (act_grad * silu).astype(BF16)
    row = dot(gate_grad, wg, NT) + dot(up_grad, wu, NT)
    if chained:
        row = row + row_in[...].astype(F32)
    row_ref[...] = row.astype(BF16)
    ag_ref[...] += dot(n2, gate_grad, TN).reshape(parts, cut, hidden)
    au_ref[...] += dot(n2, up_grad, TN).reshape(parts, cut, hidden)

    @pl.when(step == pl.num_programs(0) - 1)
    def _():
        copies = []
        pieces = [
            (acc, place, z) for z in range(parts) for place, acc in enumerate((ag_ref, au_ref, ad_ref))
        ]
        for index, (acc, place, z) in enumerate(pieces):
            slot = index % 2
            if index >= 2:
                copies[index - 2].wait()
            stage[slot] = acc[z].astype(BF16)
            copies.append(
                pltpu.make_async_copy(
                    stage.at[slot],
                    grads_ref.at[z, pl.ds(place * cut, cut), pl.ds(low, acc.shape[2])],
                    sem.at[slot],
                )
            )
            copies[-1].start()
        copies[-2].wait()
        copies[-1].wait()


def expert(z, n2, top, prob, n_dp, sources, before, rows, low, full, grads):
    length, width = n2.shape
    cut = width // n_dp
    hidden = sources[0][0].shape[-1]
    blk = pl.BlockSpec((rows, width), lambda i: (i, 0))
    col = pl.BlockSpec((rows, 1), lambda i: (i, 0))
    shape = jax.ShapeDtypeStruct
    plan = tuple(entry[1:] for entry in sources)
    weight = pltpu.VMEM((n_dp, cut, hidden), BF16)
    total = pltpu.VMEM((n_dp, cut, hidden), F32)
    return pl.pallas_call(
        functools.partial(expert_kernel, len(before) > 0, low, len(grads) > 0, plan),
        grid=(length // rows,),
        in_specs=[pl.BlockSpec(memory_space=pltpu.SMEM), blk, blk, col]
        + [ANY] * len(grads)
        + [blk] * len(before)
        + [ANY] * len(sources),
        out_specs=[blk, blk, ANY],
        out_shape=[
            shape((length, width), BF16),
            shape((length, width), BF16),
            shape((n_dp, 3 * cut, full), BF16),
        ],
        input_output_aliases={4: 2} if grads else {},
        scratch_shapes=[weight] * 3
        + [total] * 3
        + [pltpu.VMEM((2, cut, hidden), BF16), DMA((3, n_dp)), DMA((2,))],
        compiler_params=pltpu.CompilerParams(vmem_limit_bytes=VMEM_LIMIT),
        cost_estimate=pl.CostEstimate(
            flops=18 * length * width * hidden,
            transcendentals=length * hidden,
            bytes_accessed=5 * length * width * 2,
        ),
        name="expert",
    )(z, n2, top, prob, *grads, *before, *[entry[0] for entry in sources])


def pack_kernel(cuts, gate_ref, up_ref, down_ref, *outs):
    cut = gate_ref.shape[0]
    for (low, high), out in zip(cuts, outs):
        out[:cut, :] = gate_ref[:, low:high]
        out[cut : 2 * cut, :] = up_ref[:, low:high]
        out[2 * cut :, :] = jnp.transpose(down_ref[low:high, :].astype(F32)).astype(BF16)


def pack(cuts, w_gate, w_up, w_down):
    cut = w_gate.shape[0]
    return pl.pallas_call(
        functools.partial(pack_kernel, cuts),
        in_specs=[VM] * 3,
        out_specs=[VM] * len(cuts),
        out_shape=[jax.ShapeDtypeStruct((3 * cut, high - low), BF16) for low, high in cuts],
        name="pack",
    )(w_gate, w_up, w_down)


def unpack_kernel(z_ref, one_ref, all_ref, up_ref, down_ref, dg_ref, du_ref, dd_ref, own, sem):
    copy = pltpu.make_async_copy(all_ref.at[z_ref[0]], own, sem)
    copy.start()
    cut = dg_ref.shape[1]
    piece = [slice(k * cut, (k + 1) * cut) for k in range(3)]
    dg_ref[1] = one_ref[piece[0], :].astype(F32)
    du_ref[1] = one_ref[piece[1], :].astype(F32)
    dd_ref[1] = jnp.transpose(one_ref[piece[2], :].astype(F32))
    copy.wait()

    def total(at):
        return own[at, :].astype(F32) + up_ref[at, :].astype(F32) + down_ref[at, :].astype(F32)

    dg_ref[0] = total(piece[0])
    du_ref[0] = total(piece[1])
    dd_ref[0] = jnp.transpose(total(piece[2]))


def unpack(z, one, grads, got):
    rows, hidden = one.shape
    cut = rows // 3
    shape = jax.ShapeDtypeStruct
    return pl.pallas_call(
        unpack_kernel,
        in_specs=[pl.BlockSpec(memory_space=pltpu.SMEM), VM, ANY, VM, VM],
        out_specs=[VM] * 3,
        out_shape=[
            shape((2, cut, hidden), F32),
            shape((2, cut, hidden), F32),
            shape((2, hidden, cut), F32),
        ],
        scratch_shapes=[pltpu.VMEM((rows, hidden), BF16), DMA(())],
        compiler_params=pltpu.CompilerParams(vmem_limit_bytes=VMEM_LIMIT),
        name="unpack",
    )(z, one, grads, *got)


def line_hop(block_up, block_down, n_dp, hop):
    up = [(i, i + 1) for i in range(hop - 1, n_dp - 1)]
    down = [(i + 1, i) for i in range(n_dp - hop)]
    return lax.ppermute(block_up, "dp", up), lax.ppermute(block_down, "dp", down)


def reduce_hop(grads, got, n_dp, hop):
    place = lax.axis_index("dp")
    reach = n_dp - hop
    spots = (jnp.minimum(place + reach, n_dp - 1), jnp.maximum(place - reach, 0))
    blocks = [lax.dynamic_index_in_dim(grads, spot, 0, False) for spot in spots]
    if got is not None:
        blocks = [(b.astype(F32) + g.astype(F32)).astype(BF16) for b, g in zip(blocks, got)]
    up = [(i, i + 1) for i in range(hop)]
    down = [(i, i - 1) for i in range(n_dp - hop, n_dp)]
    return lax.ppermute(blocks[0], "dp", up), lax.ppermute(blocks[1], "dp", down)


def after_of(value, *others):
    return lax.optimization_barrier((value,) + others)[0]


def per_device(
    layer_input,
    doc_ids,
    route_ids,
    route_probs,
    attn_gain,
    ffn_gain,
    query_gain,
    key_gain,
    w_query,
    w_key,
    w_value,
    w_out,
    w_gate,
    w_up,
    w_down,
    out_grad,
):
    tokens, width = layer_input.shape[1:]
    n_dp = lax.axis_size("dp")
    n_ctx = lax.axis_size("ctx")
    ctx_index = lax.axis_index("ctx")
    length = tokens * n_ctx
    heads = HQ // n_ctx
    share = n_ctx // KV
    qw = heads * HD
    depth = w_query.shape[0]
    own_e = w_gate.shape[0]

    cut = attn_gain.shape[0]
    hcut = query_gain.shape[0]
    kinds = 2 * (cut + hcut)
    small = jnp.concatenate([attn_gain, ffn_gain, query_gain, key_gain]).astype(F32)
    small = jnp.pad(small, (0, 1024 - kinds)).reshape(8, HD)
    cols = jnp.concatenate(
        [
            w_query.reshape(depth, n_ctx, qw),
            jnp.repeat(w_key.reshape(depth, KV, HD), share, axis=1),
            jnp.repeat(w_value.reshape(depth, KV, HD), share, axis=1),
        ],
        axis=2,
    ).transpose(1, 0, 2)
    cols, small = prep(n_ctx, n_dp, cols, small)
    small = small.reshape(n_dp * n_ctx, 1024)
    gain_attn = small[:, :cut].reshape(1, width)
    gain_ffn = small[:, cut : 2 * cut].reshape(1, width)
    gain_query = small[:, 2 * cut : 2 * cut + hcut].reshape(1, HD)
    gain_key = small[:, 2 * cut + hcut : kinds].reshape(1, HD)
    wqkv = lax.all_gather(cols.reshape(n_ctx * depth, qw + 2 * HD), "dp", axis=0, tiled=True)
    wrows = lax.all_gather(after_of(w_out, small), "dp", axis=0, tiled=False)

    inputs = layer_input.reshape(tokens, width)
    top_own = out_grad.reshape(tokens, width)
    n_experts = own_e * n_ctx
    match = route_ids.reshape(1, tokens, TOP) == jnp.arange(n_experts, dtype=jnp.int32)[:, None, None]
    probs = jnp.sum(jnp.where(match, route_probs.reshape(1, tokens, TOP), 0.0), axis=2)
    info = jnp.concatenate(
        [probs, doc_ids.reshape(1, tokens).astype(F32), jnp.zeros((7, tokens), F32)], axis=0
    )
    normed, info = first(n_ctx, inputs, gain_attn, info)
    normed = normed.reshape(length, width)
    doc = info[:, n_experts].reshape(length).astype(jnp.int32)
    my_probs = lax.dynamic_slice_in_dim(info, ctx_index * own_e, own_e, 1)
    my_probs = my_probs.transpose(0, 2, 1).reshape(length, own_e)

    inverse = 1.0 / ROPE_BASE ** (jnp.arange(HD // 2, dtype=F32) * 2.0 / HD)
    angles = jnp.arange(length, dtype=F32)[:, None] * inverse[None, :]
    cosine = jnp.cos(angles)
    sine = jnp.sin(angles)
    cosine = jnp.concatenate([cosine, cosine], axis=1)
    sine = jnp.concatenate([-sine, sine], axis=1)
    qlin, klin, q, k, v, attn, total, top_all = attn_forward(
        n_ctx, normed, wqkv, cosine, sine, gain_query, gain_key, doc, top_own, tokens
    )
    top_all = top_all.reshape(length, width)
    blocks = (n_ctx, tokens, width)
    after, normed2, wout = middle(n_ctx, n_dp, attn, wrows, inputs, gain_ffn)
    wout = wout.reshape(qw, width)
    normed2 = normed2.reshape(length, width)

    z = lax.axis_index("dp").astype(jnp.int32).reshape(1)
    hidden = w_gate.shape[2]

    def run(e, sources, carried, low, grads):
        moe, rows_grad, grads = expert(
            z,
            normed2,
            top_all,
            my_probs[:, e : e + 1],
            n_dp,
            sources,
            carried,
            tokens,
            low,
            hidden,
            grads,
        )
        return (moe, rows_grad), grads

    cuts = [(0, 256), (256, hidden)]
    blocks0 = pack(cuts, w_gate[0], w_up[0], w_down[0])
    carried, grads0 = (), ()
    for index, (low, high) in enumerate(cuts):
        full = lax.all_gather(blocks0[index], "dp", axis=0, tiled=False)
        if index == 1:
            (block1,) = pack([(0, hidden)], w_gate[1], w_up[1], w_down[1])
            sources1 = [(block1, "up", 0, 0)]
            up = down = after_of(block1, full)
            up, down = line_hop(up, down, n_dp, 1)
            sources1 += [(up, "up", 1, 0), (down, "down", 1, 0)]
        carried, grads = run(0, [(full, "all", 0, 0)], carried, low, grads0)
        grads0 = (grads,)
    got = None
    for hop in range(2, n_dp + 1):
        if hop == 2:
            up, down, grads = lax.optimization_barrier((up, down, grads))
        else:
            up, down, got = lax.optimization_barrier((up, down, got))
        if hop < n_dp:
            up, down = line_hop(up, down, n_dp, hop)
            sources1 += [(up, "up", hop, 0), (down, "down", hop, 0)]
        got = reduce_hop(grads, got, n_dp, hop - 1)
    (moe, rows_grad), grads1 = run(1, sources1, carried, 0, ())
    done1 = lax.psum_scatter(
        grads1.reshape(3 * width, hidden), "dp", scatter_dimension=0, tiled=True
    )
    mid, ffn_part, branch = turn(
        n_ctx, rows_grad.reshape(blocks), after, top_own, gain_ffn
    )
    branch = branch.reshape(length, width)

    out_w = dot(attn, branch, TN).astype(BF16).reshape(n_dp, qw // n_dp, width)
    dqkv, gains, out_w = attn_backward(
        n_ctx,
        n_dp,
        out_w,
        branch,
        wout,
        attn,
        total,
        q,
        k,
        v,
        qlin,
        klin,
        cosine,
        sine,
        gain_query,
        gain_key,
        doc,
        tokens,
    )
    out_w = lax.psum_scatter(out_w.reshape(qw, width), "dp", scatter_dimension=0, tiled=True)
    out_w = out_w.astype(F32)
    input_grad, attn_part, qkv_w = last(n_ctx, dqkv, wqkv, inputs, mid, gain_attn, normed)
    qkv_w = lax.psum_scatter(qkv_w, "dp", scatter_dimension=0, tiled=True)
    n_all = n_dp * n_ctx
    packed = jnp.concatenate(
        [
            attn_part[0].reshape(n_all, cut),
            ffn_part[0].reshape(n_all, cut),
            gains[0].reshape(n_all, hcut),
            gains[1].reshape(n_all, hcut),
            jnp.zeros((n_all, 1024 - kinds), F32),
        ],
        axis=1,
    )
    packed = packed.reshape(n_dp, n_ctx, 8, HD).transpose(1, 0, 2, 3)
    layer_output, packed = close(n_ctx, n_dp, moe.reshape(blocks), after, packed)
    packed = packed.reshape(1024)
    query_w, key_w, value_w = post(n_ctx, qkv_w.reshape(n_ctx, depth, qw + 2 * HD))
    gate_w, up_w, down_w = unpack(z, done1, grads, got)
    return (
        layer_output.reshape(1, tokens, width),
        input_grad.reshape(1, tokens, width),
        packed[:cut],
        packed[cut : 2 * cut],
        packed[2 * cut : 2 * cut + hcut],
        packed[2 * cut + hcut : kinds],
        query_w,
        key_w,
        value_w,
        out_w,
        gate_w,
        up_w,
        down_w,
    )


def solution(mesh):
    both = ("dp", "ctx")
    seq = P("dp", "ctx", None)
    in_specs = (
        seq,
        P("dp", "ctx"),
        seq,
        seq,
        P(both),
        P(both),
        P(both),
        P(both),
        P(both, None),
        P(both, None),
        P(both, None),
        P(both, None),
        P("ctx", "dp", None),
        P("ctx", "dp", None),
        P("ctx", None, "dp"),
        seq,
    )
    out_specs = (
        seq,
        seq,
        P(both),
        P(both),
        P(both),
        P(both),
        P(both, None),
        P(both, None),
        P(both, None),
        P(both, None),
        P("ctx", "dp", None),
        P("ctx", "dp", None),
        P("ctx", None, "dp"),
    )

    return jax.shard_map(
        per_device, mesh=mesh, in_specs=in_specs, out_specs=out_specs, check_vma=False
    )
```

```python
import functools
import math

import jax
import jax.numpy as jnp
from jax import lax
from jax.experimental import pallas as pl
from jax.experimental.pallas import tpu as pltpu
from jax.sharding import PartitionSpec as P


HQ = 32
KV = 4
HD = 128
TOP = 8
MOST = 1024
EPS = 1e-06
ROPE_BASE = 1000000.0
F32 = jnp.float32
BF16 = jnp.bfloat16
SCALE = 1.0 / math.sqrt(HD)
SCALE2 = SCALE / math.log(2.0)
VMEM_LIMIT = 60 * 1024 * 1024


def dot(left, right, dims=((1,), (0,))):
    return lax.dot_general(left, right, (dims, ((), ())), preferred_element_type=F32)


NT = ((1,), (1,))
TN = ((0,), (0,))


def rms_parts(values):
    return lax.rsqrt(jnp.mean(values * values, axis=-1, keepdims=True) + EPS)


def rms_back(grad, unit, inv, gain):
    scaled = grad * gain
    return inv * (scaled - unit * jnp.mean(scaled * unit, axis=-1, keepdims=True))


def head_forward(lin, gain, cosine, sine):
    unit = lin * rms_parts(lin) * gain
    return unit * cosine + pltpu.roll(unit, HD // 2, 1) * sine


def head_backward(lin, gain, cosine, sine, rot_grad):
    grad = rot_grad * cosine + pltpu.roll(rot_grad * sine, HD // 2, 1)
    inv = rms_parts(lin)
    unit = lin * inv
    return rms_back(grad, unit, inv, gain), jnp.sum(grad * unit, axis=0, keepdims=True)


MESH = pl.DeviceIdType.MESH
ANY = pl.BlockSpec(memory_space=pl.ANY)
VM = pl.BlockSpec(memory_space=pltpu.VMEM)
DMA = pltpu.SemaphoreType.DMA
CHUNK = 32


def flip(index, mask, count):
    result, bit = 0, 1
    while bit < count:
        digit = (index // bit) % 2
        result = result + bit * ((1 - digit) if mask & bit else digit)
        bit *= 2
    return result


def push(src, dst, send, recv, axis, peer):
    return pltpu.make_async_remote_copy(
        src_ref=src,
        dst_ref=dst,
        send_sem=send,
        recv_sem=recv,
        device_id={axis: peer},
        device_id_type=MESH,
    )


def meet(peers):
    barrier = pltpu.get_barrier_semaphore()
    for axis, peer in peers:
        pl.semaphore_signal(barrier, inc=1, device_id={axis: peer}, device_id_type=MESH)
    pl.semaphore_wait(barrier, len(peers))


class Plane:
    def __init__(self, n):
        self.chips = n // 2
        self.me = lax.axis_index("ctx")
        self.core = self.me % 2
        self.chip = self.me // 2
        self.mate = self.me + 1 - 2 * self.core

    def same(self, s):
        return 2 * flip(self.chip, s, self.chips) + self.core

    def meet(self):
        meet([("ctx", self.same(s)) for s in range(1, self.chips)] + [("ctx", self.mate)])


def far_first(chips):
    return sorted(range(1, chips), key=lambda s: -bin(s).count("1"))


class Gather:
    def __init__(self, plane, src, out, send, recv, local):
        self.plane, self.out, self.send, self.recv = plane, out, send, recv
        self.own = pltpu.make_async_copy(src, out.at[plane.me], local)
        self.far = [
            push(src, out.at[plane.me], send.at[s], recv.at[s], "ctx", plane.same(s))
            for s in far_first(plane.chips)
        ]
        self.near = push(src, out.at[plane.me], send.at[0], recv.at[0], "ctx", plane.mate)

    def start(self):
        for copy in self.far:
            copy.start()
        self.near.start()
        self.own.start()

    def forward(self):
        plane, out = self.plane, self.out
        self.passed = []
        for s in sorted(range(1, plane.chips), key=lambda s: bin(s).count("1")):
            block = out.at[plane.same(s)]
            push(block, block, self.send.at[s], self.recv.at[s], "ctx", plane.mate).wait_recv()
            slot = plane.chips + s
            copy = push(block, block, self.send.at[slot], self.recv.at[slot], "ctx", plane.mate)
            copy.start()
            self.passed.append(copy)

    def finish(self):
        for copy in self.far:
            copy.wait_send()
        self.near.wait_send()
        self.near.wait_recv()
        for copy in self.passed:
            copy.wait_send()
            copy.wait_recv()
        self.own.wait()


def by_rows(rows, body):
    def one(index, carry):
        body(pl.ds(pl.multiple_of(index * CHUNK, CHUNK), CHUNK))
        return carry

    lax.fori_loop(0, rows // CHUNK, one, 0)


class SquareGather:
    def __init__(self, plane, src, out, send, recv, local):
        self.plane, self.out, self.send, self.recv = plane, out, send, recv
        half = src.shape[0] // 2
        self.halves = [pl.ds(0, half), pl.ds(half, half)]
        mine = out.at[plane.me]
        self.own = pltpu.make_async_copy(src, mine, local)
        self.near = push(src, mine, send.at[0], recv.at[0], "ctx", plane.mate)
        self.far = []
        for s, h in ((1, 0), (2, 1), (1, 1), (2, 0)):
            part, slot = self.halves[h], 2 * s + h
            self.far.append(
                push(
                    src.at[part, :],
                    mine.at[part, :],
                    send.at[slot],
                    recv.at[slot],
                    "ctx",
                    plane.same(s),
                )
            )

    def start(self):
        for copy in self.far:
            copy.start()
        self.near.start()
        self.own.start()

    def arrived(self, s, h):
        block = self.out.at[self.plane.same(s)].at[self.halves[h], :]
        slot = 2 * s + h
        push(block, block, self.send.at[slot], self.recv.at[slot], "ctx", self.plane.mate).wait_recv()
        return block

    def forward(self):
        plane = self.plane
        self.passed = []
        for s, h in ((1, 0), (2, 1)):
            block = self.arrived(s, h)
            slot = 6 + h
            copy = push(block, block, self.send.at[slot], self.recv.at[slot], "ctx", plane.same(3 - s))
            copy.start()
            self.far.append(copy)
        for s in (1, 2, 3):
            if s < 3:
                self.arrived(s, 2 - s)
            else:
                self.arrived(3, 0)
                self.arrived(3, 1)
            block, slot = self.out.at[plane.same(s)], 7 + s
            copy = push(block, block, self.send.at[slot], self.recv.at[slot], "ctx", plane.mate)
            copy.start()
            self.passed.append(copy)

    def finish(self):
        for copy in self.far:
            copy.wait_send()
        self.near.wait_send()
        self.near.wait_recv()
        for copy in self.passed:
            copy.wait_send()
            copy.wait_recv()
        self.own.wait()


def gather_of(plane, src, out, send, recv, local):
    kind = SquareGather if plane.chips == 4 else Gather
    return kind(plane, src, out, send, recv, local)


class Spread:
    def __init__(self, plane, mine, landed, send, recv):
        self.plane, self.mine, self.landed = plane, mine, landed
        self.square = plane.chips == 4
        self.order = [3, 1, 2, 0] if self.square else far_first(plane.chips) + [0]
        self.send, self.recv = send, recv
        self.sent = []
        half = mine.shape[1] // 2
        self.halves = [pl.ds(0, half), pl.ds(half, half)]

    def copy(self, s, h, to):
        part, slot = self.halves[h], 2 * s + h
        return push(
            self.mine.at[s].at[part, :],
            self.landed.at[s].at[part, :],
            self.send.at[slot],
            self.recv.at[slot],
            "ctx",
            self.plane.same(to),
        )

    def go(self, s, h, to):
        copy = self.copy(s, h, to)
        copy.start()
        self.sent.append(copy)

    def ready(self, s):
        if self.square:
            if s == 3:
                self.go(3, 0, 1)
                self.go(3, 1, 2)
            elif s == 1:
                self.go(1, 0, 1)
            elif s == 2:
                self.go(2, 1, 2)
        elif s:
            copy = push(
                self.mine.at[s],
                self.landed.at[s],
                self.send.at[s],
                self.recv.at[s],
                "ctx",
                self.plane.same(s),
            )
            copy.start()
            self.sent.append(copy)

    def settle(self, extra=None):
        mine, landed = self.mine, self.landed
        half = mine.shape[1] // 2
        if not self.square:
            if extra is not None:
                extra()
            for copy in self.sent:
                copy.wait_recv()
            return
        for s, h in ((2, 0), (1, 1)):
            self.copy(3, h, 1).wait_recv()

            def add(at, s=s, h=h):
                rows = pl.ds(h * half + at.start, CHUNK)
                total = mine[s, rows, :].astype(F32) + landed[3, rows, :].astype(F32)
                mine[s, rows, :] = total.astype(BF16)

            by_rows(half, add)
            self.go(s, h, s)
        if extra is not None:
            extra()
        for s in (1, 2):
            for h in (0, 1):
                self.copy(s, h, s).wait_recv()

    def total(self, at):
        value = self.mine[0, at, :].astype(F32)
        for s in (1, 2) if self.square else range(1, self.plane.chips):
            value = value + self.landed[s, at, :].astype(F32)
        return value

    def finish(self):
        for copy in self.sent:
            copy.wait_send()


class Scatter:
    def __init__(self, plane, part, mine, other, landed, send, recv, send2, recv2, local):
        self.plane, self.mine, self.other = plane, mine, other
        self.spread = Spread(plane, mine, landed, send2, recv2)
        self.order = self.spread.order
        self.loads, self.across = {}, {}
        for s in self.order:
            block = plane.same(s)
            self.loads[s] = pltpu.make_async_copy(part.at[block], mine.at[s], local.at[s])
            self.across[s] = push(
                part.at[block + 1 - 2 * plane.core],
                other.at[s],
                send.at[s],
                recv.at[s],
                "ctx",
                plane.mate,
            )

    def start(self):
        for s in self.order:
            self.across[s].start()
            self.loads[s].start()

    def run(self, extra=None):
        mine, other = self.mine, self.other
        for s in self.order:
            self.loads[s].wait()
            self.across[s].wait_recv()

            def add(at, s=s):
                total = mine[s, at, :].astype(F32) + other[s, at, :].astype(F32)
                mine[s, at, :] = total.astype(BF16)

            by_rows(mine.shape[1], add)
            self.spread.ready(s)
        if extra is not None:
            extra()
        self.spread.settle()

    def total(self, at):
        return self.spread.total(at)

    def finish(self):
        for s in self.order:
            self.across[s].wait_send()
        self.spread.finish()


class Product:
    def __init__(self, plane, value, mine, other, landed, given, send, recv, send2, recv2):
        self.plane, self.value = plane, value
        self.mine, self.other, self.given = mine, other, given
        self.spread = Spread(plane, mine, landed, send2, recv2)
        self.order = self.spread.order
        self.across = {
            s: push(given.at[s], other.at[s], send.at[s], recv.at[s], "ctx", plane.mate)
            for s in self.order
        }

    def start(self):
        plane = self.plane
        for s in self.order:
            block = plane.same(s) + 1 - 2 * plane.core

            def fill(at, s=s, block=block):
                self.given[s, :, at] = self.value(block, at).astype(BF16)

            by_cols(self.mine.shape[2], fill)
            self.across[s].start()

    def run(self, extra=None):
        plane, mine, other = self.plane, self.mine, self.other
        for s in self.order:
            block = plane.same(s)
            self.across[s].wait_recv()

            def fill(at, s=s, block=block):
                total = self.value(block, at) + other[s, :, at].astype(F32)
                mine[s, :, at] = total.astype(BF16)

            by_cols(mine.shape[2], fill)
            self.spread.ready(s)
        self.spread.settle(extra)

    total = Scatter.total
    finish = Scatter.finish


def by_cols(width, body):
    span = 512

    def one(index, carry):
        body(pl.ds(pl.multiple_of(index * span, span), span))
        return carry

    lax.fori_loop(0, width // span, one, 0)


def gather_sems(n):
    return [DMA((12 if n == 8 else n,)), DMA((12 if n == 8 else n,)), DMA(())]


def scatter_scratch(n, rows, width):
    chips = n // 2
    return (
        [pltpu.VMEM((chips, rows, width), BF16)] * 3
        + [DMA((chips,)), DMA((chips,)), DMA((n,)), DMA((n,))]
        + [DMA((chips,))]
    )


def product_scratch(n, rows, width):
    chips = n // 2
    return [pltpu.VMEM((chips, rows, width), BF16)] * 4 + [
        DMA((chips,)),
        DMA((chips,)),
        DMA((n,)),
        DMA((n,)),
    ]


def comm_call(kernel, ident, outs, out_specs, in_specs, scratch, micros, *args):
    return pl.pallas_call(
        kernel,
        out_shape=outs,
        in_specs=in_specs,
        out_specs=out_specs,
        scratch_shapes=scratch,
        compiler_params=pltpu.CompilerParams(
            collective_id=ident, has_side_effects=True, vmem_limit_bytes=VMEM_LIMIT
        ),
        cost_estimate=pl.CostEstimate(
            flops=0, transcendentals=0, bytes_accessed=int(micros * 3.0e6)
        ),
    )(*args)


def swap_all(n, src, out, send, recv, local):
    me = lax.axis_index("ctx")
    own = pltpu.make_async_copy(src.at[me], out.at[me], local)
    own.start()
    copies = []
    for s in range(n - 1, 0, -1):
        peer = flip(me, s, n)
        copies.append(push(src.at[peer], out.at[me], send.at[s], recv.at[s], "ctx", peer))
        copies[-1].start()
    return own, copies


class RowSwap:
    def __init__(self, n, n_dp, src, dst, send, recv, spread):
        self.me = lax.axis_index("ctx")
        self.dst, self.send, self.recv, self.n_dp = dst, send, recv, n_dp
        self.entries = []
        for k in range(n_dp):
            flat = self.me * n_dp + k if spread else k * n + self.me
            peer = flat % n if spread else flat // n_dp
            slot = flat // n if spread else flat % n_dp
            far = push(src.at[k], dst.at[slot], send.at[k], recv.at[slot], "ctx", peer)
            near = pltpu.make_async_copy(src.at[k], dst.at[slot], recv.at[slot])
            self.entries.append((peer, far, near))

    def start(self):
        for peer, far, near in self.entries:
            pl.when(peer != self.me)(far.start)
            pl.when(peer == self.me)(near.start)

    def arrive(self):
        for slot in range(self.n_dp):
            block = self.dst.at[slot]
            pltpu.make_async_copy(block, block, self.recv.at[slot]).wait()

    def finish(self):
        for peer, far, near in self.entries:
            pl.when(peer != self.me)(far.wait_send)


def meet_all(n):
    me = lax.axis_index("ctx")
    meet([("ctx", flip(me, s, n)) for s in range(1, n)])


def prep_kernel(n, n_dp, cols_ref, small_ref, out_ref, all_ref, *sems):
    send, recv, local, gsend, grecv, zsend, zrecv = sems
    me, row = lax.axis_index("ctx"), lax.axis_index("dp")
    meet(
        [("ctx", flip(me, s, n)) for s in range(1, n)]
        + [("dp", flip(row, s, n_dp)) for s in range(1, n_dp)]
    )
    all_ref[row, me] = small_ref[...]
    smalls = []
    for s in range(1, n):
        peer = flip(me, s, n)
        smalls.append(push(small_ref, all_ref.at[row, me], gsend.at[s], grecv.at[s], "ctx", peer))
        smalls[-1].start()
    own, copies = swap_all(n, cols_ref, out_ref, send, recv, local)
    for copy in smalls:
        copy.wait_recv()
    planes = []
    for s in range(1, n_dp):
        peer = flip(row, s, n_dp)
        planes.append(push(all_ref.at[row], all_ref.at[row], zsend.at[s], zrecv.at[s], "dp", peer))
        planes[-1].start()
    for copy in copies + planes:
        copy.wait_recv()
    for copy in copies + planes + smalls:
        copy.wait_send()
    own.wait()


class Gains:
    def __init__(self, n, n_dp, small, landed, mid, second, gsend, grecv, zsend, zrecv):
        self.me, self.row = lax.axis_index("ctx"), lax.axis_index("dp")
        self.small, self.landed, self.mid, self.second = small, landed, mid, second
        self.near, self.far = [], []
        for s in range(1, n):
            peer = flip(self.me, s, n)
            self.near.append(push(small.at[peer], landed.at[s], gsend.at[s], grecv.at[s], "ctx", peer))
        for s in range(1, n_dp):
            peer = flip(self.row, s, n_dp)
            self.far.append(push(mid.at[peer], second.at[s], zsend.at[s], zrecv.at[s], "dp", peer))

    def start(self):
        for copy in self.near:
            copy.start()

    def middle(self):
        value = self.small[self.me]
        for s, copy in enumerate(self.near, 1):
            copy.wait_recv()
            value = value + self.landed[s]
        self.mid[...] = value
        for copy in self.far:
            copy.start()

    def finish(self):
        value = self.mid[self.row]
        for s, copy in enumerate(self.far, 1):
            copy.wait_recv()
            value = value + self.second[s]
        for copy in self.near + self.far:
            copy.wait_send()
        return value


def post_kernel(n, src_ref, query_ref, key_ref, value_ref, blocks, send, recv, local):
    me = lax.axis_index("ctx")
    meet([("ctx", flip(me, s, n)) for s in range(1, n)])
    own, copies = swap_all(n, src_ref, blocks, send, recv, local)
    for copy in copies:
        copy.wait_recv()
    own.wait()
    share = n // KV
    qw = HQ * HD // n
    for c in range(n):
        query_ref[:, c * qw : (c + 1) * qw] = blocks[c, :, :qw].astype(F32)
    for g in range(KV):
        for out, at in ((key_ref, qw), (value_ref, qw + HD)):
            total = blocks[g * share, :, at : at + HD].astype(F32)
            for c in range(1, share):
                total = total + blocks[g * share + c, :, at : at + HD].astype(F32)
            out[:, g * HD : (g + 1) * HD] = total
    for copy in copies:
        copy.wait_send()


def swap_sems(n, n_dp):
    return [DMA((n,)), DMA((n,)), DMA(()), DMA((n,)), DMA((n,)), DMA((n_dp,)), DMA((n_dp,))]


def prep(n, n_dp, cols, small):
    shape = jax.ShapeDtypeStruct
    return comm_call(
        functools.partial(prep_kernel, n, n_dp),
        0,
        [shape(cols.shape, cols.dtype), shape((n_dp, n) + small.shape, F32)],
        [ANY, VM],
        [ANY, VM],
        swap_sems(n, n_dp),
        8,
        cols,
        small,
    )


def post(n, cols):
    shape = jax.ShapeDtypeStruct
    depth = cols.shape[1]
    return comm_call(
        functools.partial(post_kernel, n),
        1,
        [
            shape((depth, HQ * HD), F32),
            shape((depth, KV * HD), F32),
            shape((depth, KV * HD), F32),
        ],
        [VM] * 3,
        [VM],
        [pltpu.VMEM(cols.shape, BF16), DMA((n,)), DMA((n,)), DMA(())],
        10,
        cols,
    )


def first_kernel(
    n, x_ref, gain_ref, info_ref, grad_ref, nall_ref, iall_ref, gall_ref, low, *sems
):
    plane = Plane(n)
    plane.meet()
    infos = Gather(plane, info_ref, iall_ref, *sems[0:3])
    infos.start()

    def norm(at):
        value = x_ref[at, :].astype(F32)
        low[at, :] = (value * rms_parts(value) * gain_ref[...]).astype(BF16)

    by_rows(x_ref.shape[0], norm)
    normed = gather_of(plane, low, nall_ref, *sems[3:6])
    normed.start()
    grads = gather_of(plane, grad_ref, gall_ref, *sems[6:9])
    grads.start()
    infos.forward()
    normed.forward()
    grads.forward()
    infos.finish()
    normed.finish()
    grads.finish()


def first(n, x, gain, info, grad):
    shape = jax.ShapeDtypeStruct
    many = lambda array, kind: shape((n,) + array.shape, kind)
    return comm_call(
        functools.partial(first_kernel, n),
        2,
        [many(x, BF16), many(info, F32), many(grad, BF16)],
        [ANY] * 3,
        [VM] * 4,
        [pltpu.VMEM(x.shape, BF16)]
        + [DMA((n,)), DMA((n,)), DMA(())]
        + gather_sems(n)
        + gather_sems(n),
        90,
        x,
        gain,
        info,
        grad,
    )


def middle_kernel(
    n, attn_ref, wout_ref, x_ref, gain_ref, after_ref, all_ref, low, *scratch
):
    plane = Plane(n)
    plane.meet()
    rows = x_ref.shape[0]

    def value(block, at):
        left = attn_ref[pl.ds(pl.multiple_of(block * rows, rows), rows), :]
        return dot(left, wout_ref[:, at])

    sums = Product(plane, value, *scratch[:8])
    sums.start()
    sums.run()

    def norm(at):
        value = x_ref[at, :].astype(F32) + sums.total(at)
        after_ref[at, :] = value
        low[at, :] = (value * rms_parts(value) * gain_ref[...]).astype(BF16)

    by_rows(rows, norm)
    normed = gather_of(plane, low, all_ref, *scratch[8:])
    normed.start()
    normed.forward()
    sums.finish()
    normed.finish()


def middle(n, attn, wout, x, gain):
    shape = jax.ShapeDtypeStruct
    return comm_call(
        functools.partial(middle_kernel, n),
        3,
        [shape(x.shape, F32), shape((n,) + x.shape, BF16)],
        [VM, ANY],
        [VM, VM, VM, VM],
        [pltpu.VMEM(x.shape, BF16)]
        + product_scratch(n, *x.shape)
        + gather_sems(n),
        105,
        attn,
        wout,
        x,
        gain,
    )


def turn_kernel(
    n, part_ref, after_ref, grad_ref, gain_ref, mid_ref, fpart_ref, all_ref, low, *scratch
):
    plane = Plane(n)
    plane.meet()
    sums = Scatter(plane, part_ref, *scratch[:8])
    sums.start()
    fpart_ref[...] = jnp.zeros_like(fpart_ref)
    sums.run()

    def norm(at):
        value = after_ref[at, :]
        inv = rms_parts(value)
        unit = value * inv
        grad = sums.total(at)
        fpart_ref[0:1, :] += jnp.sum(grad * unit, axis=0, keepdims=True)
        mid = grad_ref[at, :].astype(F32) + rms_back(grad, unit, inv, gain_ref[...])
        mid_ref[at, :] = mid
        low[at, :] = mid.astype(BF16)

    by_rows(after_ref.shape[0], norm)
    branch = gather_of(plane, low, all_ref, *scratch[8:])
    branch.start()
    branch.forward()
    sums.finish()
    branch.finish()


def turn(n, part, after, grad, gain):
    shape = jax.ShapeDtypeStruct
    return comm_call(
        functools.partial(turn_kernel, n),
        4,
        [
            shape(after.shape, F32),
            shape((8, after.shape[1]), F32),
            shape((n,) + after.shape, BF16),
        ],
        [VM, VM, ANY],
        [ANY, VM, VM, VM],
        [pltpu.VMEM(after.shape, BF16)] + scatter_scratch(n, *after.shape) + gather_sems(n),
        95,
        part,
        after,
        grad,
        gain,
    )


def last_kernel(
    n,
    grad_ref,
    wqkv_ref,
    x_ref,
    mid_ref,
    gain_ref,
    *rest,
):
    fused = n == 8
    normed_ref, rest = (rest[0], rest[1:]) if fused else (None, rest)
    out_ref, apart_ref, rest = rest[0], rest[1], rest[2:]
    wgrad_ref, scratch = (rest[0], rest[1:]) if fused else (None, rest)
    plane = Plane(n)
    plane.meet()
    apart_ref[...] = jnp.zeros_like(apart_ref)
    rows = x_ref.shape[0]

    def value(block, at):
        left = grad_ref[pl.ds(pl.multiple_of(block * rows, rows), rows), :]
        return dot(left, wqkv_ref[at, :], NT)

    sums = Product(plane, value, *scratch[:8])
    sums.start()

    def weights():
        def fill(at):
            wgrad_ref[at, :] = dot(normed_ref[:, at], grad_ref[...], TN).astype(BF16)

        by_cols(normed_ref.shape[1], fill)

    sums.run(weights if fused else None)

    def norm(at):
        value = x_ref[at, :].astype(F32)
        inv = rms_parts(value)
        unit = value * inv
        grad = sums.total(at)
        apart_ref[0:1, :] += jnp.sum(grad * unit, axis=0, keepdims=True)
        out_ref[at, :] = mid_ref[at, :] + rms_back(grad, unit, inv, gain_ref[...])

    by_rows(rows, norm)
    sums.finish()


def last(n, grad, wqkv, x, mid, gain, normed):
    shape = jax.ShapeDtypeStruct
    outs = [shape(mid.shape, F32), shape((8, mid.shape[1]), F32)]
    more = [normed] if n == 8 else []
    outs += [shape(wqkv.shape, BF16) for _ in more]
    got = comm_call(
        functools.partial(last_kernel, n),
        5,
        outs,
        [VM] * len(outs),
        [VM] * (5 + len(more)),
        product_scratch(n, *mid.shape),
        60,
        grad,
        wqkv,
        x,
        mid,
        gain,
        *more,
    )
    return got if more else (*got, dot(normed, grad, TN).astype(BF16))


def close_kernel(n, n_dp, part_ref, after_ref, small_ref, out_ref, sum_ref, *scratch):
    meet(
        [("ctx", flip(lax.axis_index("ctx"), s, n)) for s in range(1, n)]
        + [("dp", flip(lax.axis_index("dp"), s, n_dp)) for s in range(1, n_dp)]
    )
    plane = Plane(n)
    sums = Scatter(plane, part_ref, *scratch[:8])
    sums.start()
    gains = Gains(n, n_dp, small_ref, *scratch[8:])
    gains.start()
    sums.run(gains.middle)

    def add(at):
        out_ref[at, :] = (after_ref[at, :] + sums.total(at)).astype(BF16)

    by_rows(after_ref.shape[0], add)
    sums.finish()
    sum_ref[...] = gains.finish()


def close(n, n_dp, part, after, small):
    shape = jax.ShapeDtypeStruct
    tile = small.shape[2:]
    return comm_call(
        functools.partial(close_kernel, n, n_dp),
        6,
        [shape(after.shape, BF16), shape(tile, F32)],
        [VM, VM],
        [ANY, VM, VM],
        scatter_scratch(n, *after.shape)
        + [
            pltpu.VMEM((n, n_dp) + tile, F32),
            pltpu.VMEM((n_dp,) + tile, F32),
            pltpu.VMEM((n_dp,) + tile, F32),
            DMA((n,)),
            DMA((n,)),
            DMA((n_dp,)),
            DMA((n_dp,)),
        ],
        50,
        part,
        after,
        small,
    )


def attn_forward_kernel(
    n,
    n_dp,
    heads,
    back,
    normed_ref,
    wqkv_ref,
    cos_ref,
    sin_ref,
    qgain_ref,
    kgain_ref,
    docc_ref,
    docr_ref,
    rows_ref,
    qlin_ref,
    klin_ref,
    q_ref,
    k_ref,
    v_ref,
    attn_ref,
    total_ref,
    wout_ref,
    acc_ref,
    sum_ref,
    *sems,
):
    step = pl.program_id(0)

    @pl.when(step == 0)
    def _():
        meet_all(n)
        RowSwap(n, n_dp, rows_ref, wout_ref, *sems, False).start()

    rows = normed_ref.shape[0]
    lin = dot(normed_ref[...], wqkv_ref[...])
    here = pl.ds(step * rows, rows)
    cosine = cos_ref[...]
    sine = sin_ref[...]
    qw = heads * HD
    for head in range(heads):
        cols = slice(head * HD, (head + 1) * HD)
        part = lin[:, cols]
        qlin_ref[:, cols] = part
        q_ref[:, cols] = head_forward(part, qgain_ref[...], cosine, sine).astype(BF16)
    key_lin = lin[:, qw : qw + HD]
    klin_ref[...] = key_lin
    k_ref[here, :] = head_forward(key_lin, kgain_ref[...], cosine, sine).astype(BF16)
    v_ref[here, :] = lin[:, qw + HD :].astype(BF16)
    acc_ref[...] = jnp.zeros_like(acc_ref)
    sum_ref[...] = jnp.zeros_like(sum_ref)
    row_pos = step * rows + lax.broadcasted_iota(jnp.int32, (rows, rows), 0)
    col_off = lax.broadcasted_iota(jnp.int32, (rows, rows), 1)

    def one(block, carry):
        at = pl.ds(pl.multiple_of(block * rows, rows), rows)
        key = k_ref[at, :]
        val = v_ref[at, :]
        allowed = (docc_ref[...] == docr_ref[:, at]) & (block * rows + col_off <= row_pos)
        for head in range(heads):
            cols = slice(head * HD, (head + 1) * HD)
            score = dot(q_ref[:, cols], key, NT) * SCALE2
            expo = jnp.where(allowed, jnp.exp2(score), 0.0)
            folded = expo[:, :HD]
            for piece in range(1, rows // HD):
                folded = folded + expo[:, piece * HD : (piece + 1) * HD]
            sum_ref[:, cols] += folded
            acc_ref[:, cols] += dot(expo.astype(BF16), val)
        return carry

    lax.fori_loop(jnp.maximum(step - back, 0), step + 1, one, 0)
    lane = lax.broadcasted_iota(jnp.int32, (rows, HD), 1)
    totals = jnp.ones((rows, HD), F32)
    for head in range(heads):
        cols = slice(head * HD, (head + 1) * HD)
        total = jnp.sum(sum_ref[:, cols], axis=-1, keepdims=True)
        totals = jnp.where(lane == head, total, totals)
        attn_ref[:, cols] = (acc_ref[:, cols] / total).astype(BF16)
    total_ref[...] = totals

    @pl.when(step == pl.num_programs(0) - 1)
    def _():
        swap = RowSwap(n, n_dp, rows_ref, wout_ref, *sems, False)
        swap.arrive()
        swap.finish()


def attn_forward(n, n_dp, normed, wqkv, cosine, sine, qgain, kgain, doc, wrows, rows):
    length, width = normed.shape
    qw = wqkv.shape[1] - 2 * HD
    heads = qw // HD
    blk = lambda cols: pl.BlockSpec((rows, cols), lambda i: (i, 0))
    whole = lambda shape: pl.BlockSpec(shape, lambda i: (0, 0))
    shape = jax.ShapeDtypeStruct
    return pl.pallas_call(
        functools.partial(attn_forward_kernel, n, n_dp, heads, MOST // rows),
        grid=(length // rows,),
        in_specs=[
            blk(width),
            whole(wqkv.shape),
            blk(HD),
            blk(HD),
            whole((1, HD)),
            whole((1, HD)),
            blk(1),
            whole((1, length)),
            ANY,
        ],
        out_specs=[
            blk(qw),
            blk(HD),
            blk(qw),
            whole((length, HD)),
            whole((length, HD)),
            blk(qw),
            blk(HD),
            ANY,
        ],
        out_shape=[
            shape((length, qw), F32),
            shape((length, HD), F32),
            shape((length, qw), BF16),
            shape((length, HD), BF16),
            shape((length, HD), BF16),
            shape((length, qw), BF16),
            shape((length, HD), F32),
            shape(wrows.shape, BF16),
        ],
        scratch_shapes=[pltpu.VMEM((rows, qw), F32), pltpu.VMEM((rows, qw), F32)]
        + [DMA((n_dp,)), DMA((n_dp,))],
        compiler_params=pltpu.CompilerParams(
            collective_id=7, has_side_effects=True, vmem_limit_bytes=VMEM_LIMIT
        ),
        cost_estimate=pl.CostEstimate(
            flops=35 * 10**9, transcendentals=0, bytes_accessed=30 * 2**20
        ),
        name="attn_forward",
    )(normed, wqkv, cosine, sine, qgain, kgain, doc[:, None], doc[None, :], wrows)


def attn_backward_kernel(
    n,
    n_dp,
    heads,
    back,
    branch_ref,
    wout_ref,
    attn_ref,
    total_ref,
    q_ref,
    k_ref,
    v_ref,
    qlin_ref,
    klin_ref,
    cos_ref,
    sin_ref,
    qgain_ref,
    kgain_ref,
    docc_ref,
    docr_ref,
    wgrad_ref,
    dqkv_ref,
    gains_ref,
    swapped_ref,
    dk_ref,
    dv_ref,
    dqa_ref,
    *sems,
):
    step = pl.program_id(0)

    @pl.when(step == 0)
    def _():
        meet_all(n)
        RowSwap(n, n_dp, wgrad_ref, swapped_ref, *sems, True).start()

    @pl.when(step == pl.num_programs(0) - 1)
    def _():
        swap = RowSwap(n, n_dp, wgrad_ref, swapped_ref, *sems, True)
        swap.arrive()
        swap.finish()

    rows = branch_ref.shape[0]
    here = pl.ds(pl.multiple_of(step * rows, rows), rows)

    @pl.when(step == 0)
    def _():
        gains_ref[...] = jnp.zeros_like(gains_ref)

    dk_ref[here, :] = jnp.zeros((rows, HD), F32)
    dv_ref[here, :] = jnp.zeros((rows, HD), F32)
    dqa_ref[...] = jnp.zeros_like(dqa_ref)
    attn_grad = dot(branch_ref[...], wout_ref[...], NT)
    grads = []
    shifts = []
    for head in range(heads):
        cols = slice(head * HD, (head + 1) * HD)
        part = attn_grad[:, cols]
        inv_total = 1.0 / total_ref[:, head : head + 1]
        delta = jnp.sum(part * attn_ref[:, cols].astype(F32), axis=-1, keepdims=True)
        grads.append((part * inv_total).astype(BF16))
        shifts.append(delta * inv_total)
    row_pos = step * rows + lax.broadcasted_iota(jnp.int32, (rows, rows), 0)
    col_off = lax.broadcasted_iota(jnp.int32, (rows, rows), 1)

    def one(block, carry):
        at = pl.ds(pl.multiple_of(block * rows, rows), rows)
        key = k_ref[at, :]
        val = v_ref[at, :]
        allowed = (docc_ref[...] == docr_ref[:, at]) & (block * rows + col_off <= row_pos)
        dk = jnp.zeros((rows, HD), F32)
        dv = jnp.zeros((rows, HD), F32)
        for head in range(heads):
            cols = slice(head * HD, (head + 1) * HD)
            query = q_ref[:, cols]
            score = dot(query, key, NT) * SCALE2
            expo = jnp.where(allowed, jnp.exp2(score), 0.0)
            prod = dot(grads[head], val, NT)
            score_grad = (expo * (prod - shifts[head])).astype(BF16)
            dv += dot(expo.astype(BF16), grads[head], TN)
            dk += dot(score_grad, query, TN)
            dqa_ref[:, cols] += dot(score_grad, key)
        dk_ref[at, :] += dk
        dv_ref[at, :] += dv
        return carry

    lax.fori_loop(jnp.maximum(step - back, 0), step + 1, one, 0)
    cosine = cos_ref[here, :]
    sine = sin_ref[here, :]
    for head in range(heads):
        cols = slice(head * HD, (head + 1) * HD)
        grad, gain_part = head_backward(
            qlin_ref[:, cols], qgain_ref[...], cosine, sine, dqa_ref[:, cols] * SCALE
        )
        dqkv_ref[here, cols] = grad.astype(BF16)
        gains_ref[0:1, :] += gain_part

    @pl.when(step == pl.num_programs(0) - 1)
    def _():
        def finish(block, carry):
            at = pl.ds(pl.multiple_of(block * rows, rows), rows)
            grad, gain_part = head_backward(
                klin_ref[at, :], kgain_ref[...], cos_ref[at, :], sin_ref[at, :], dk_ref[at, :] * SCALE
            )
            qw = heads * HD
            dqkv_ref[at, qw : qw + HD] = grad.astype(BF16)
            dqkv_ref[at, qw + HD :] = dv_ref[at, :].astype(BF16)
            gains_ref[1:2, :] += gain_part
            return carry

        lax.fori_loop(0, pl.num_programs(0), finish, 0)


def attn_backward(n, n_dp, wgrad, branch, wout, attn, total, q, k, v, qlin, klin, cosine, sine, qgain, kgain, doc, rows):
    length, width = branch.shape
    qw = wout.shape[0]
    heads = qw // HD
    blk = lambda cols: pl.BlockSpec((rows, cols), lambda i: (i, 0))
    whole = lambda shape: pl.BlockSpec(shape, lambda i: (0, 0))
    shape = jax.ShapeDtypeStruct
    full = whole((length, HD))
    return pl.pallas_call(
        functools.partial(attn_backward_kernel, n, n_dp, heads, MOST // rows),
        grid=(length // rows,),
        in_specs=[
            blk(width),
            whole(wout.shape),
            blk(qw),
            blk(HD),
            blk(qw),
            full,
            full,
            blk(qw),
            full,
            full,
            full,
            whole((1, HD)),
            whole((1, HD)),
            blk(1),
            whole((1, length)),
            ANY,
        ],
        out_specs=[whole((length, qw + 2 * HD)), whole((8, HD)), ANY],
        out_shape=[
            shape((length, qw + 2 * HD), BF16),
            shape((8, HD), F32),
            shape(wgrad.shape, BF16),
        ],
        scratch_shapes=[
            pltpu.VMEM((length, HD), F32),
            pltpu.VMEM((length, HD), F32),
            pltpu.VMEM((rows, qw), F32),
            DMA((n_dp,)),
            DMA((n_dp,)),
        ],
        compiler_params=pltpu.CompilerParams(
            collective_id=9, has_side_effects=True, vmem_limit_bytes=VMEM_LIMIT
        ),
        cost_estimate=pl.CostEstimate(
            flops=60 * 10**9, transcendentals=0, bytes_accessed=30 * 2**20
        ),
        name="attn_backward",
    )(branch, wout, attn, total, q, k, v, qlin, klin, cosine, sine, qgain, kgain, doc[:, None], doc[None, :], wgrad)


def expert_kernel(chained, low, aliased, plan, z_ref, n2_ref, top_ref, prob_ref, *rest):
    if aliased:
        rest = rest[1:]
    if chained:
        moe_in, row_in = rest[:2]
        rest = rest[2:]
    sources, rest = rest[: len(plan)], rest[len(plan) :]
    moe_ref, row_ref, grads_ref, wg_ref, wu_ref, wd_ref = rest[:6]
    ag_ref, au_ref, ad_ref, stage, wsem, sem = rest[6:]
    step = pl.program_id(0)
    rows, width = n2_ref.shape
    parts, cut, hidden = wd_ref.shape
    weights = (wg_ref, wu_ref, wd_ref)

    @pl.when(step == 0)
    def _():
        z = z_ref[0]
        for source, (kind, amount, start) in zip(sources, plan):
            count = source.shape[-2] // cut
            for k in range(parts) if kind == "all" else [amount]:
                if kind == "all":
                    src, owner, wanted = source.at[k], k, None
                elif kind == "up":
                    src, owner, wanted = source, z - k, z >= k
                else:
                    src, owner, wanted = source, z + k, z + k < parts

                def load(src=src, owner=owner, start=start, count=count):
                    for piece in range(count):
                        pltpu.make_async_copy(
                            src.at[pl.ds(piece * cut, cut), :],
                            weights[start + piece].at[owner],
                            wsem.at[start + piece, owner],
                        ).start()

                if wanted is None:
                    load()
                else:
                    pl.when(wanted)(load)
        ag_ref[...] = jnp.zeros_like(ag_ref)
        au_ref[...] = jnp.zeros_like(au_ref)
        ad_ref[...] = jnp.zeros_like(ad_ref)
        for index in range(3):
            for owner in range(parts):
                block = weights[index].at[owner]
                pltpu.make_async_copy(block, block, wsem.at[index, owner]).wait()

    n2 = n2_ref[...]
    prob = prob_ref[...]
    wg = wg_ref[...].reshape(width, hidden)
    wu = wu_ref[...].reshape(width, hidden)
    gate = dot(n2, wg)
    up = dot(n2, wu)
    sig = 1.0 / (1.0 + jnp.exp(-gate))
    silu = gate * sig
    act = (silu * up).astype(BF16)
    act_grad = jnp.zeros((rows, hidden), F32)
    for z in range(parts):
        cols = slice(z * cut, (z + 1) * cut)
        out = dot(act, wd_ref[z], NT).astype(BF16).astype(F32) * prob
        if chained:
            out = out + moe_in[:, cols].astype(F32)
        moe_ref[:, cols] = out.astype(BF16)
        route = (top_ref[:, cols].astype(F32) * prob).astype(BF16)
        act_grad += dot(route, wd_ref[z])
        ad_ref[z] += dot(route, act, TN)
    gate_grad = (act_grad * up * sig * (1.0 + gate * (1.0 - sig))).astype(BF16)
    up_grad = (act_grad * silu).astype(BF16)
    row = dot(gate_grad, wg, NT) + dot(up_grad, wu, NT)
    if chained:
        row = row + row_in[...].astype(F32)
    row_ref[...] = row.astype(BF16)
    ag_ref[...] += dot(n2, gate_grad, TN).reshape(parts, cut, hidden)
    au_ref[...] += dot(n2, up_grad, TN).reshape(parts, cut, hidden)

    @pl.when(step == pl.num_programs(0) - 1)
    def _():
        copies = []
        pieces = [
            (acc, place, z) for z in range(parts) for place, acc in enumerate((ag_ref, au_ref, ad_ref))
        ]
        for index, (acc, place, z) in enumerate(pieces):
            slot = index % 2
            if index >= 2:
                copies[index - 2].wait()
            stage[slot] = acc[z].astype(BF16)
            copies.append(
                pltpu.make_async_copy(
                    stage.at[slot],
                    grads_ref.at[z, pl.ds(place * cut, cut), pl.ds(low, acc.shape[2])],
                    sem.at[slot],
                )
            )
            copies[-1].start()
        copies[-2].wait()
        copies[-1].wait()


def expert(z, n2, top, prob, n_dp, sources, before, rows, low, full, grads):
    length, width = n2.shape
    cut = width // n_dp
    hidden = sources[0][0].shape[-1]
    blk = pl.BlockSpec((rows, width), lambda i: (i, 0))
    col = pl.BlockSpec((rows, 1), lambda i: (i, 0))
    shape = jax.ShapeDtypeStruct
    plan = tuple(entry[1:] for entry in sources)
    weight = pltpu.VMEM((n_dp, cut, hidden), BF16)
    total = pltpu.VMEM((n_dp, cut, hidden), F32)
    return pl.pallas_call(
        functools.partial(expert_kernel, len(before) > 0, low, len(grads) > 0, plan),
        grid=(length // rows,),
        in_specs=[pl.BlockSpec(memory_space=pltpu.SMEM), blk, blk, col]
        + [ANY] * len(grads)
        + [blk] * len(before)
        + [ANY] * len(sources),
        out_specs=[blk, blk, ANY],
        out_shape=[
            shape((length, width), BF16),
            shape((length, width), BF16),
            shape((n_dp, 3 * cut, full), BF16),
        ],
        input_output_aliases={4: 2} if grads else {},
        scratch_shapes=[weight] * 3
        + [total] * 3
        + [pltpu.VMEM((2, cut, hidden), BF16), DMA((3, n_dp)), DMA((2,))],
        compiler_params=pltpu.CompilerParams(vmem_limit_bytes=VMEM_LIMIT),
        cost_estimate=pl.CostEstimate(
            flops=18 * length * width * hidden,
            transcendentals=length * hidden,
            bytes_accessed=5 * length * width * 2,
        ),
        name="expert",
    )(z, n2, top, prob, *grads, *before, *[entry[0] for entry in sources])


def pack_kernel(cuts, gate_ref, up_ref, down_ref, *outs):
    cut = gate_ref.shape[0]
    for (low, high), out in zip(cuts, outs):
        out[:cut, :] = gate_ref[:, low:high]
        out[cut : 2 * cut, :] = up_ref[:, low:high]
        out[2 * cut :, :] = jnp.transpose(down_ref[low:high, :].astype(F32)).astype(BF16)


def pack(cuts, w_gate, w_up, w_down):
    cut = w_gate.shape[0]
    return pl.pallas_call(
        functools.partial(pack_kernel, cuts),
        in_specs=[VM] * 3,
        out_specs=[VM] * len(cuts),
        out_shape=[jax.ShapeDtypeStruct((3 * cut, high - low), BF16) for low, high in cuts],
        name="pack",
    )(w_gate, w_up, w_down)


def unpack_kernel(z_ref, one_ref, all_ref, up_ref, down_ref, dg_ref, du_ref, dd_ref, own, sem):
    copy = pltpu.make_async_copy(all_ref.at[z_ref[0]], own, sem)
    copy.start()
    cut = dg_ref.shape[1]
    piece = [slice(k * cut, (k + 1) * cut) for k in range(3)]
    dg_ref[1] = one_ref[piece[0], :].astype(F32)
    du_ref[1] = one_ref[piece[1], :].astype(F32)
    dd_ref[1] = jnp.transpose(one_ref[piece[2], :].astype(F32))
    copy.wait()

    def total(at):
        return own[at, :].astype(F32) + up_ref[at, :].astype(F32) + down_ref[at, :].astype(F32)

    dg_ref[0] = total(piece[0])
    du_ref[0] = total(piece[1])
    dd_ref[0] = jnp.transpose(total(piece[2]))


def unpack(z, one, grads, got):
    rows, hidden = one.shape
    cut = rows // 3
    shape = jax.ShapeDtypeStruct
    return pl.pallas_call(
        unpack_kernel,
        in_specs=[pl.BlockSpec(memory_space=pltpu.SMEM), VM, ANY, VM, VM],
        out_specs=[VM] * 3,
        out_shape=[
            shape((2, cut, hidden), F32),
            shape((2, cut, hidden), F32),
            shape((2, hidden, cut), F32),
        ],
        scratch_shapes=[pltpu.VMEM((rows, hidden), BF16), DMA(())],
        compiler_params=pltpu.CompilerParams(vmem_limit_bytes=VMEM_LIMIT),
        name="unpack",
    )(z, one, grads, *got)


def line_hop(block_up, block_down, n_dp, hop):
    up = [(i, i + 1) for i in range(hop - 1, n_dp - 1)]
    down = [(i + 1, i) for i in range(n_dp - hop)]
    return lax.ppermute(block_up, "dp", up), lax.ppermute(block_down, "dp", down)


def reduce_hop(grads, got, n_dp, hop):
    place = lax.axis_index("dp")
    reach = n_dp - hop
    spots = (jnp.minimum(place + reach, n_dp - 1), jnp.maximum(place - reach, 0))
    if got is not None:
        got = lax.optimization_barrier(got)
    blocks = [lax.dynamic_index_in_dim(grads, spot, 0, False) for spot in spots]
    if got is not None:
        blocks = [(b.astype(F32) + g.astype(F32)).astype(BF16) for b, g in zip(blocks, got)]
    up = [(i, i + 1) for i in range(hop)]
    down = [(i, i - 1) for i in range(n_dp - hop, n_dp)]
    return lax.ppermute(blocks[0], "dp", up), lax.ppermute(blocks[1], "dp", down)


def after_of(value, *others):
    return lax.optimization_barrier((value,) + others)[0]


def per_device(
    layer_input,
    doc_ids,
    route_ids,
    route_probs,
    attn_gain,
    ffn_gain,
    query_gain,
    key_gain,
    w_query,
    w_key,
    w_value,
    w_out,
    w_gate,
    w_up,
    w_down,
    out_grad,
):
    tokens, width = layer_input.shape[1:]
    n_dp = lax.axis_size("dp")
    n_ctx = lax.axis_size("ctx")
    ctx_index = lax.axis_index("ctx")
    length = tokens * n_ctx
    heads = HQ // n_ctx
    share = n_ctx // KV
    qw = heads * HD
    depth = w_query.shape[0]
    own_e = w_gate.shape[0]

    cut = attn_gain.shape[0]
    hcut = query_gain.shape[0]
    kinds = 2 * (cut + hcut)
    small = jnp.concatenate([attn_gain, ffn_gain, query_gain, key_gain]).astype(F32)
    small = jnp.pad(small, (0, 1024 - kinds)).reshape(8, HD)
    cols = jnp.concatenate(
        [
            w_query.reshape(depth, n_ctx, qw),
            jnp.repeat(w_key.reshape(depth, KV, HD), share, axis=1),
            jnp.repeat(w_value.reshape(depth, KV, HD), share, axis=1),
        ],
        axis=2,
    ).transpose(1, 0, 2)
    cols, small = prep(n_ctx, n_dp, cols, small)
    small = small.reshape(n_dp * n_ctx, 1024)
    gain_attn = small[:, :cut].reshape(1, width)
    gain_ffn = small[:, cut : 2 * cut].reshape(1, width)
    gain_query = small[:, 2 * cut : 2 * cut + hcut].reshape(1, HD)
    gain_key = small[:, 2 * cut + hcut : kinds].reshape(1, HD)
    wqkv = lax.all_gather(cols.reshape(n_ctx * depth, qw + 2 * HD), "dp", axis=0, tiled=True)
    wrows = lax.all_gather(w_out, "dp", axis=0, tiled=False)

    inputs = layer_input.reshape(tokens, width)
    top_own = out_grad.reshape(tokens, width)
    n_experts = own_e * n_ctx
    match = route_ids.reshape(1, tokens, TOP) == jnp.arange(n_experts, dtype=jnp.int32)[:, None, None]
    probs = jnp.sum(jnp.where(match, route_probs.reshape(1, tokens, TOP), 0.0), axis=2)
    info = jnp.concatenate(
        [probs, doc_ids.reshape(1, tokens).astype(F32), jnp.zeros((7, tokens), F32)], axis=0
    )
    normed, info, top_all = first(n_ctx, inputs, gain_attn, info, top_own)
    normed = normed.reshape(length, width)
    doc = info[:, n_experts].reshape(length).astype(jnp.int32)
    my_probs = lax.dynamic_slice_in_dim(info, ctx_index * own_e, own_e, 1)
    my_probs = my_probs.transpose(0, 2, 1).reshape(length, own_e)

    inverse = 1.0 / ROPE_BASE ** (jnp.arange(HD // 2, dtype=F32) * 2.0 / HD)
    angles = jnp.arange(length, dtype=F32)[:, None] * inverse[None, :]
    cosine = jnp.cos(angles)
    sine = jnp.sin(angles)
    cosine = jnp.concatenate([cosine, cosine], axis=1)
    sine = jnp.concatenate([-sine, sine], axis=1)
    qlin, klin, q, k, v, attn, total, wout = attn_forward(
        n_ctx, n_dp, normed, wqkv, cosine, sine, gain_query, gain_key, doc, wrows, tokens
    )
    wout = wout.reshape(qw, width)
    top_all = top_all.reshape(length, width)
    blocks = (n_ctx, tokens, width)
    after, normed2 = middle(n_ctx, attn, wout, inputs, gain_ffn)
    normed2 = normed2.reshape(length, width)

    z = lax.axis_index("dp").astype(jnp.int32).reshape(1)
    hidden = w_gate.shape[2]

    def run(e, sources, carried, low, grads):
        moe, rows_grad, grads = expert(
            z,
            normed2,
            top_all,
            my_probs[:, e : e + 1],
            n_dp,
            sources,
            carried,
            tokens,
            low,
            hidden,
            grads,
        )
        return (moe, rows_grad), grads

    cuts = [(0, 256), (256, hidden)]
    blocks0 = pack(cuts, w_gate[0], w_up[0], w_down[0])
    carried, grads0 = (), ()
    for index, (low, high) in enumerate(cuts):
        full = lax.all_gather(blocks0[index], "dp", axis=0, tiled=False)
        if index == 1:
            (block1,) = pack([(0, hidden)], w_gate[1], w_up[1], w_down[1])
            sources1 = [(block1, "up", 0, 0)]
            up = down = after_of(block1, full)
            up, down = line_hop(up, down, n_dp, 1)
            sources1 += [(up, "up", 1, 0), (down, "down", 1, 0)]
        carried, grads = run(0, [(full, "all", 0, 0)], carried, low, grads0)
        grads0 = (grads,)
    got = None
    for hop in range(2, n_dp + 1):
        if hop < n_dp:
            up, down = line_hop(up, down, n_dp, hop)
            sources1 += [(up, "up", hop, 0), (down, "down", hop, 0)]
        got = reduce_hop(grads, got, n_dp, hop - 1)
    (moe, rows_grad), grads1 = run(1, sources1, carried, 0, ())
    done1 = lax.psum_scatter(
        grads1.reshape(3 * width, hidden), "dp", scatter_dimension=0, tiled=True
    )
    mid, ffn_part, branch = turn(
        n_ctx, rows_grad.reshape(blocks), after, top_own, gain_ffn
    )
    branch = branch.reshape(length, width)

    out_w = dot(attn, branch, TN).astype(BF16).reshape(n_dp, qw // n_dp, width)
    dqkv, gains, out_w = attn_backward(
        n_ctx,
        n_dp,
        out_w,
        branch,
        wout,
        attn,
        total,
        q,
        k,
        v,
        qlin,
        klin,
        cosine,
        sine,
        gain_query,
        gain_key,
        doc,
        tokens,
    )
    out_w = lax.psum_scatter(out_w.reshape(qw, width), "dp", scatter_dimension=0, tiled=True)
    out_w = out_w.astype(F32)
    input_grad, attn_part, qkv_w = last(n_ctx, dqkv, wqkv, inputs, mid, gain_attn, normed)
    qkv_w = lax.psum_scatter(qkv_w, "dp", scatter_dimension=0, tiled=True)
    n_all = n_dp * n_ctx
    packed = jnp.concatenate(
        [
            attn_part[0].reshape(n_all, cut),
            ffn_part[0].reshape(n_all, cut),
            gains[0].reshape(n_all, hcut),
            gains[1].reshape(n_all, hcut),
            jnp.zeros((n_all, 1024 - kinds), F32),
        ],
        axis=1,
    )
    packed = packed.reshape(n_dp, n_ctx, 8, HD).transpose(1, 0, 2, 3)
    layer_output, packed = close(n_ctx, n_dp, moe.reshape(blocks), after, packed)
    packed = packed.reshape(1024)
    query_w, key_w, value_w = post(n_ctx, qkv_w.reshape(n_ctx, depth, qw + 2 * HD))
    gate_w, up_w, down_w = unpack(z, done1, grads, got)
    return (
        layer_output.reshape(1, tokens, width),
        input_grad.reshape(1, tokens, width),
        packed[:cut],
        packed[cut : 2 * cut],
        packed[2 * cut : 2 * cut + hcut],
        packed[2 * cut + hcut : kinds],
        query_w,
        key_w,
        value_w,
        out_w,
        gate_w,
        up_w,
        down_w,
    )


def solution(mesh):
    both = ("dp", "ctx")
    seq = P("dp", "ctx", None)
    in_specs = (
        seq,
        P("dp", "ctx"),
        seq,
        seq,
        P(both),
        P(both),
        P(both),
        P(both),
        P(both, None),
        P(both, None),
        P(both, None),
        P(both, None),
        P("ctx", "dp", None),
        P("ctx", "dp", None),
        P("ctx", None, "dp"),
        seq,
    )
    out_specs = (
        seq,
        seq,
        P(both),
        P(both),
        P(both),
        P(both),
        P(both, None),
        P(both, None),
        P(both, None),
        P(both, None),
        P("ctx", "dp", None),
        P("ctx", "dp", None),
        P("ctx", None, "dp"),
    )

    return jax.shard_map(
        per_device, mesh=mesh, in_specs=in_specs, out_specs=out_specs, check_vma=False
    )
```

```python
import functools
import math

import jax
import jax.numpy as jnp
from jax import lax
from jax.experimental import pallas as pl
from jax.experimental.pallas import tpu as pltpu
from jax.sharding import PartitionSpec as P


HQ = 32
KV = 4
HD = 128
TOP = 8
MOST = 1024
EPS = 1e-06
ROPE_BASE = 1000000.0
F32 = jnp.float32
BF16 = jnp.bfloat16
SCALE = 1.0 / math.sqrt(HD)
SCALE2 = SCALE / math.log(2.0)
VMEM_LIMIT = 60 * 1024 * 1024


def dot(left, right, dims=((1,), (0,))):
    return lax.dot_general(left, right, (dims, ((), ())), preferred_element_type=F32)


NT = ((1,), (1,))
TN = ((0,), (0,))


def rms_parts(values):
    return lax.rsqrt(jnp.mean(values * values, axis=-1, keepdims=True) + EPS)


def rms_back(grad, unit, inv, gain):
    scaled = grad * gain
    return inv * (scaled - unit * jnp.mean(scaled * unit, axis=-1, keepdims=True))


def head_forward(lin, gain, cosine, sine):
    unit = lin * rms_parts(lin) * gain
    return unit * cosine + pltpu.roll(unit, HD // 2, 1) * sine


def head_backward(lin, gain, cosine, sine, rot_grad):
    grad = rot_grad * cosine + pltpu.roll(rot_grad * sine, HD // 2, 1)
    inv = rms_parts(lin)
    unit = lin * inv
    return rms_back(grad, unit, inv, gain), jnp.sum(grad * unit, axis=0, keepdims=True)


MESH = pl.DeviceIdType.MESH
ANY = pl.BlockSpec(memory_space=pl.ANY)
VM = pl.BlockSpec(memory_space=pltpu.VMEM)
DMA = pltpu.SemaphoreType.DMA
CHUNK = 32


def flip(index, mask, count):
    result, bit = 0, 1
    while bit < count:
        digit = (index // bit) % 2
        result = result + bit * ((1 - digit) if mask & bit else digit)
        bit *= 2
    return result


def push(src, dst, send, recv, axis, peer):
    return pltpu.make_async_remote_copy(
        src_ref=src,
        dst_ref=dst,
        send_sem=send,
        recv_sem=recv,
        device_id={axis: peer},
        device_id_type=MESH,
    )


def meet(peers):
    barrier = pltpu.get_barrier_semaphore()
    for axis, peer in peers:
        pl.semaphore_signal(barrier, inc=1, device_id={axis: peer}, device_id_type=MESH)
    pl.semaphore_wait(barrier, len(peers))


class Plane:
    def __init__(self, n):
        self.chips = n // 2
        self.me = lax.axis_index("ctx")
        self.core = self.me % 2
        self.chip = self.me // 2
        self.mate = self.me + 1 - 2 * self.core

    def same(self, s):
        return 2 * flip(self.chip, s, self.chips) + self.core

    def meet(self):
        meet([("ctx", self.same(s)) for s in range(1, self.chips)] + [("ctx", self.mate)])


def far_first(chips):
    return sorted(range(1, chips), key=lambda s: -bin(s).count("1"))


class Gather:
    def __init__(self, plane, src, out, send, recv, local):
        self.plane, self.out, self.send, self.recv = plane, out, send, recv
        self.own = pltpu.make_async_copy(src, out.at[plane.me], local)
        self.far = [
            push(src, out.at[plane.me], send.at[s], recv.at[s], "ctx", plane.same(s))
            for s in far_first(plane.chips)
        ]
        self.near = push(src, out.at[plane.me], send.at[0], recv.at[0], "ctx", plane.mate)

    def start(self):
        for copy in self.far:
            copy.start()
        self.near.start()
        self.own.start()

    def forward(self):
        plane, out = self.plane, self.out
        self.passed = []
        for s in sorted(range(1, plane.chips), key=lambda s: bin(s).count("1")):
            block = out.at[plane.same(s)]
            push(block, block, self.send.at[s], self.recv.at[s], "ctx", plane.mate).wait_recv()
            slot = plane.chips + s
            copy = push(block, block, self.send.at[slot], self.recv.at[slot], "ctx", plane.mate)
            copy.start()
            self.passed.append(copy)

    def finish(self):
        for copy in self.far:
            copy.wait_send()
        self.near.wait_send()
        self.near.wait_recv()
        for copy in self.passed:
            copy.wait_send()
            copy.wait_recv()
        self.own.wait()


def by_rows(rows, body):
    def one(index, carry):
        body(pl.ds(pl.multiple_of(index * CHUNK, CHUNK), CHUNK))
        return carry

    lax.fori_loop(0, rows // CHUNK, one, 0)


class SquareGather:
    def __init__(self, plane, src, out, send, recv, local):
        self.plane, self.out, self.send, self.recv = plane, out, send, recv
        half = src.shape[0] // 2
        self.halves = [pl.ds(0, half), pl.ds(half, half)]
        mine = out.at[plane.me]
        self.own = pltpu.make_async_copy(src, mine, local)
        self.near = push(src, mine, send.at[0], recv.at[0], "ctx", plane.mate)
        self.far = []
        for s, h in ((1, 0), (2, 1), (1, 1), (2, 0)):
            part, slot = self.halves[h], 2 * s + h
            self.far.append(
                push(
                    src.at[part, :],
                    mine.at[part, :],
                    send.at[slot],
                    recv.at[slot],
                    "ctx",
                    plane.same(s),
                )
            )

    def start(self):
        for copy in self.far:
            copy.start()
        self.near.start()
        self.own.start()

    def arrived(self, s, h):
        block = self.out.at[self.plane.same(s)].at[self.halves[h], :]
        slot = 2 * s + h
        push(block, block, self.send.at[slot], self.recv.at[slot], "ctx", self.plane.mate).wait_recv()
        return block

    def forward(self):
        plane = self.plane
        self.passed = []
        for s, h in ((1, 0), (2, 1)):
            block = self.arrived(s, h)
            slot = 6 + h
            copy = push(block, block, self.send.at[slot], self.recv.at[slot], "ctx", plane.same(3 - s))
            copy.start()
            self.far.append(copy)
        for s in (1, 2, 3):
            if s < 3:
                self.arrived(s, 2 - s)
            else:
                self.arrived(3, 0)
                self.arrived(3, 1)
            block, slot = self.out.at[plane.same(s)], 7 + s
            copy = push(block, block, self.send.at[slot], self.recv.at[slot], "ctx", plane.mate)
            copy.start()
            self.passed.append(copy)

    def finish(self):
        for copy in self.far:
            copy.wait_send()
        self.near.wait_send()
        self.near.wait_recv()
        for copy in self.passed:
            copy.wait_send()
            copy.wait_recv()
        self.own.wait()


def gather_of(plane, src, out, send, recv, local):
    kind = SquareGather if plane.chips == 4 else Gather
    return kind(plane, src, out, send, recv, local)


class Spread:
    def __init__(self, plane, mine, landed, send, recv):
        self.plane, self.mine, self.landed = plane, mine, landed
        self.square = plane.chips == 4
        self.order = [3, 1, 2, 0] if self.square else far_first(plane.chips) + [0]
        self.send, self.recv = send, recv
        self.sent = []
        half = mine.shape[1] // 2
        self.halves = [pl.ds(0, half), pl.ds(half, half)]

    def copy(self, s, h, to):
        part, slot = self.halves[h], 2 * s + h
        return push(
            self.mine.at[s].at[part, :],
            self.landed.at[s].at[part, :],
            self.send.at[slot],
            self.recv.at[slot],
            "ctx",
            self.plane.same(to),
        )

    def go(self, s, h, to):
        copy = self.copy(s, h, to)
        copy.start()
        self.sent.append(copy)

    def ready(self, s):
        if self.square:
            if s == 3:
                self.go(3, 0, 1)
                self.go(3, 1, 2)
            elif s == 1:
                self.go(1, 0, 1)
            elif s == 2:
                self.go(2, 1, 2)
        elif s:
            copy = push(
                self.mine.at[s],
                self.landed.at[s],
                self.send.at[s],
                self.recv.at[s],
                "ctx",
                self.plane.same(s),
            )
            copy.start()
            self.sent.append(copy)

    def settle(self, extra=None):
        mine, landed = self.mine, self.landed
        half = mine.shape[1] // 2
        if not self.square:
            if extra is not None:
                extra()
            for copy in self.sent:
                copy.wait_recv()
            return
        for s, h in ((2, 0), (1, 1)):
            self.copy(3, h, 1).wait_recv()

            def add(at, s=s, h=h):
                rows = pl.ds(h * half + at.start, CHUNK)
                total = mine[s, rows, :].astype(F32) + landed[3, rows, :].astype(F32)
                mine[s, rows, :] = total.astype(BF16)

            by_rows(half, add)
            self.go(s, h, s)
        if extra is not None:
            extra()
        for s in (1, 2):
            for h in (0, 1):
                self.copy(s, h, s).wait_recv()

    def total(self, at):
        value = self.mine[0, at, :].astype(F32)
        for s in (1, 2) if self.square else range(1, self.plane.chips):
            value = value + self.landed[s, at, :].astype(F32)
        return value

    def finish(self):
        for copy in self.sent:
            copy.wait_send()


class Scatter:
    def __init__(self, plane, part, mine, other, landed, send, recv, send2, recv2, local):
        self.plane, self.mine, self.other = plane, mine, other
        self.spread = Spread(plane, mine, landed, send2, recv2)
        self.order = self.spread.order
        self.loads, self.across = {}, {}
        for s in self.order:
            block = plane.same(s)
            self.loads[s] = pltpu.make_async_copy(part.at[block], mine.at[s], local.at[s])
            self.across[s] = push(
                part.at[block + 1 - 2 * plane.core],
                other.at[s],
                send.at[s],
                recv.at[s],
                "ctx",
                plane.mate,
            )

    def start(self):
        for s in self.order:
            self.across[s].start()
            self.loads[s].start()

    def run(self, extra=None):
        mine, other = self.mine, self.other
        for s in self.order:
            self.loads[s].wait()
            self.across[s].wait_recv()

            def add(at, s=s):
                total = mine[s, at, :].astype(F32) + other[s, at, :].astype(F32)
                mine[s, at, :] = total.astype(BF16)

            by_rows(mine.shape[1], add)
            self.spread.ready(s)
        if extra is not None:
            extra()
        self.spread.settle()

    def total(self, at):
        return self.spread.total(at)

    def finish(self):
        for s in self.order:
            self.across[s].wait_send()
        self.spread.finish()


class Product:
    def __init__(self, plane, value, mine, other, landed, given, send, recv, send2, recv2):
        self.plane, self.value = plane, value
        self.mine, self.other, self.given = mine, other, given
        self.spread = Spread(plane, mine, landed, send2, recv2)
        self.order = self.spread.order
        self.across = {
            s: push(given.at[s], other.at[s], send.at[s], recv.at[s], "ctx", plane.mate)
            for s in self.order
        }

    def start(self):
        plane = self.plane
        for s in self.order:
            block = plane.same(s) + 1 - 2 * plane.core

            def fill(at, s=s, block=block):
                self.given[s, :, at] = self.value(block, at).astype(BF16)

            by_cols(self.mine.shape[2], fill)
            self.across[s].start()

    def run(self, extra=None):
        plane, mine, other = self.plane, self.mine, self.other
        for s in self.order:
            block = plane.same(s)
            self.across[s].wait_recv()

            def fill(at, s=s, block=block):
                total = self.value(block, at) + other[s, :, at].astype(F32)
                mine[s, :, at] = total.astype(BF16)

            by_cols(mine.shape[2], fill)
            self.spread.ready(s)
        self.spread.settle(extra)

    total = Scatter.total
    finish = Scatter.finish


def by_cols(width, body):
    span = 512

    def one(index, carry):
        body(pl.ds(pl.multiple_of(index * span, span), span))
        return carry

    lax.fori_loop(0, width // span, one, 0)


def gather_sems(n):
    return [DMA((12 if n == 8 else n,)), DMA((12 if n == 8 else n,)), DMA(())]


def scatter_scratch(n, rows, width):
    chips = n // 2
    return (
        [pltpu.VMEM((chips, rows, width), BF16)] * 3
        + [DMA((chips,)), DMA((chips,)), DMA((n,)), DMA((n,))]
        + [DMA((chips,))]
    )


def product_scratch(n, rows, width):
    chips = n // 2
    return [pltpu.VMEM((chips, rows, width), BF16)] * 4 + [
        DMA((chips,)),
        DMA((chips,)),
        DMA((n,)),
        DMA((n,)),
    ]


def comm_call(kernel, ident, outs, out_specs, in_specs, scratch, micros, *args):
    return pl.pallas_call(
        kernel,
        out_shape=outs,
        in_specs=in_specs,
        out_specs=out_specs,
        scratch_shapes=scratch,
        compiler_params=pltpu.CompilerParams(
            collective_id=ident, has_side_effects=True, vmem_limit_bytes=VMEM_LIMIT
        ),
        cost_estimate=pl.CostEstimate(
            flops=0, transcendentals=0, bytes_accessed=int(micros * 3.0e6)
        ),
    )(*args)


def swap_all(n, src, out, send, recv, local):
    me = lax.axis_index("ctx")
    own = pltpu.make_async_copy(src.at[me], out.at[me], local)
    own.start()
    copies = []
    for s in range(n - 1, 0, -1):
        peer = flip(me, s, n)
        copies.append(push(src.at[peer], out.at[me], send.at[s], recv.at[s], "ctx", peer))
        copies[-1].start()
    return own, copies


class RowSwap:
    def __init__(self, n, n_dp, src, dst, send, recv, spread):
        self.me = lax.axis_index("ctx")
        self.dst, self.send, self.recv, self.n_dp = dst, send, recv, n_dp
        self.entries = []
        for k in range(n_dp):
            flat = self.me * n_dp + k if spread else k * n + self.me
            peer = flat % n if spread else flat // n_dp
            slot = flat // n if spread else flat % n_dp
            far = push(src.at[k], dst.at[slot], send.at[k], recv.at[slot], "ctx", peer)
            near = pltpu.make_async_copy(src.at[k], dst.at[slot], recv.at[slot])
            self.entries.append((peer, far, near))

    def start(self):
        for peer, far, near in self.entries:
            pl.when(peer != self.me)(far.start)
            pl.when(peer == self.me)(near.start)

    def arrive(self):
        for slot in range(self.n_dp):
            block = self.dst.at[slot]
            pltpu.make_async_copy(block, block, self.recv.at[slot]).wait()

    def finish(self):
        for peer, far, near in self.entries:
            pl.when(peer != self.me)(far.wait_send)


def meet_all(n):
    me = lax.axis_index("ctx")
    meet([("ctx", flip(me, s, n)) for s in range(1, n)])


def prep_kernel(n, n_dp, cols_ref, small_ref, out_ref, all_ref, *sems):
    send, recv, local, gsend, grecv, zsend, zrecv = sems
    me, row = lax.axis_index("ctx"), lax.axis_index("dp")
    meet(
        [("ctx", flip(me, s, n)) for s in range(1, n)]
        + [("dp", flip(row, s, n_dp)) for s in range(1, n_dp)]
    )
    all_ref[row, me] = small_ref[...]
    smalls = []
    for s in range(1, n):
        peer = flip(me, s, n)
        smalls.append(push(small_ref, all_ref.at[row, me], gsend.at[s], grecv.at[s], "ctx", peer))
        smalls[-1].start()
    own, copies = swap_all(n, cols_ref, out_ref, send, recv, local)
    for copy in smalls:
        copy.wait_recv()
    planes = []
    for s in range(1, n_dp):
        peer = flip(row, s, n_dp)
        planes.append(push(all_ref.at[row], all_ref.at[row], zsend.at[s], zrecv.at[s], "dp", peer))
        planes[-1].start()
    for copy in copies + planes:
        copy.wait_recv()
    for copy in copies + planes + smalls:
        copy.wait_send()
    own.wait()


class Gains:
    def __init__(self, n, n_dp, small, landed, mid, second, gsend, grecv, zsend, zrecv):
        self.me, self.row = lax.axis_index("ctx"), lax.axis_index("dp")
        self.small, self.landed, self.mid, self.second = small, landed, mid, second
        self.near, self.far = [], []
        for s in range(1, n):
            peer = flip(self.me, s, n)
            self.near.append(push(small.at[peer], landed.at[s], gsend.at[s], grecv.at[s], "ctx", peer))
        for s in range(1, n_dp):
            peer = flip(self.row, s, n_dp)
            self.far.append(push(mid.at[peer], second.at[s], zsend.at[s], zrecv.at[s], "dp", peer))

    def start(self):
        for copy in self.near:
            copy.start()

    def middle(self):
        value = self.small[self.me]
        for s, copy in enumerate(self.near, 1):
            copy.wait_recv()
            value = value + self.landed[s]
        self.mid[...] = value
        for copy in self.far:
            copy.start()

    def finish(self):
        value = self.mid[self.row]
        for s, copy in enumerate(self.far, 1):
            copy.wait_recv()
            value = value + self.second[s]
        for copy in self.near + self.far:
            copy.wait_send()
        return value


def post_kernel(n, src_ref, query_ref, key_ref, value_ref, blocks, send, recv, local):
    me = lax.axis_index("ctx")
    meet([("ctx", flip(me, s, n)) for s in range(1, n)])
    own, copies = swap_all(n, src_ref, blocks, send, recv, local)
    for copy in copies:
        copy.wait_recv()
    own.wait()
    share = n // KV
    qw = HQ * HD // n
    for c in range(n):
        query_ref[:, c * qw : (c + 1) * qw] = blocks[c, :, :qw].astype(F32)
    for g in range(KV):
        for out, at in ((key_ref, qw), (value_ref, qw + HD)):
            total = blocks[g * share, :, at : at + HD].astype(F32)
            for c in range(1, share):
                total = total + blocks[g * share + c, :, at : at + HD].astype(F32)
            out[:, g * HD : (g + 1) * HD] = total
    for copy in copies:
        copy.wait_send()


def swap_sems(n, n_dp):
    return [DMA((n,)), DMA((n,)), DMA(()), DMA((n,)), DMA((n,)), DMA((n_dp,)), DMA((n_dp,))]


def prep(n, n_dp, cols, small):
    shape = jax.ShapeDtypeStruct
    return comm_call(
        functools.partial(prep_kernel, n, n_dp),
        0,
        [shape(cols.shape, cols.dtype), shape((n_dp, n) + small.shape, F32)],
        [ANY, VM],
        [ANY, VM],
        swap_sems(n, n_dp),
        8,
        cols,
        small,
    )


def post(n, cols):
    shape = jax.ShapeDtypeStruct
    depth = cols.shape[1]
    return comm_call(
        functools.partial(post_kernel, n),
        1,
        [
            shape((depth, HQ * HD), F32),
            shape((depth, KV * HD), F32),
            shape((depth, KV * HD), F32),
        ],
        [VM] * 3,
        [VM],
        [pltpu.VMEM(cols.shape, BF16), DMA((n,)), DMA((n,)), DMA(())],
        10,
        cols,
    )


def first_kernel(
    n, x_ref, gain_ref, info_ref, grad_ref, nall_ref, iall_ref, gall_ref, low, *sems
):
    plane = Plane(n)
    plane.meet()
    infos = Gather(plane, info_ref, iall_ref, *sems[0:3])
    infos.start()

    def norm(at):
        value = x_ref[at, :].astype(F32)
        low[at, :] = (value * rms_parts(value) * gain_ref[...]).astype(BF16)

    by_rows(x_ref.shape[0], norm)
    normed = gather_of(plane, low, nall_ref, *sems[3:6])
    normed.start()
    grads = gather_of(plane, grad_ref, gall_ref, *sems[6:9])
    grads.start()
    infos.forward()
    normed.forward()
    grads.forward()
    infos.finish()
    normed.finish()
    grads.finish()


def first(n, x, gain, info, grad):
    shape = jax.ShapeDtypeStruct
    many = lambda array, kind: shape((n,) + array.shape, kind)
    return comm_call(
        functools.partial(first_kernel, n),
        2,
        [many(x, BF16), many(info, F32), many(grad, BF16)],
        [ANY] * 3,
        [VM] * 4,
        [pltpu.VMEM(x.shape, BF16)]
        + [DMA((n,)), DMA((n,)), DMA(())]
        + gather_sems(n)
        + gather_sems(n),
        90,
        x,
        gain,
        info,
        grad,
    )


def middle_kernel(
    n, attn_ref, wout_ref, x_ref, gain_ref, after_ref, all_ref, low, *scratch
):
    plane = Plane(n)
    plane.meet()
    rows = x_ref.shape[0]

    def value(block, at):
        left = attn_ref[pl.ds(pl.multiple_of(block * rows, rows), rows), :]
        return dot(left, wout_ref[:, at])

    sums = Product(plane, value, *scratch[:8])
    sums.start()
    sums.run()

    def norm(at):
        value = x_ref[at, :].astype(F32) + sums.total(at)
        after_ref[at, :] = value
        low[at, :] = (value * rms_parts(value) * gain_ref[...]).astype(BF16)

    by_rows(rows, norm)
    normed = gather_of(plane, low, all_ref, *scratch[8:])
    normed.start()
    normed.forward()
    sums.finish()
    normed.finish()


def middle(n, attn, wout, x, gain):
    shape = jax.ShapeDtypeStruct
    return comm_call(
        functools.partial(middle_kernel, n),
        3,
        [shape(x.shape, F32), shape((n,) + x.shape, BF16)],
        [VM, ANY],
        [VM, VM, VM, VM],
        [pltpu.VMEM(x.shape, BF16)]
        + product_scratch(n, *x.shape)
        + gather_sems(n),
        105,
        attn,
        wout,
        x,
        gain,
    )


def turn_kernel(
    n, part_ref, after_ref, grad_ref, gain_ref, mid_ref, fpart_ref, all_ref, low, *scratch
):
    plane = Plane(n)
    plane.meet()
    sums = Scatter(plane, part_ref, *scratch[:8])
    sums.start()
    fpart_ref[...] = jnp.zeros_like(fpart_ref)
    sums.run()

    def norm(at):
        value = after_ref[at, :]
        inv = rms_parts(value)
        unit = value * inv
        grad = sums.total(at)
        fpart_ref[0:1, :] += jnp.sum(grad * unit, axis=0, keepdims=True)
        mid = grad_ref[at, :].astype(F32) + rms_back(grad, unit, inv, gain_ref[...])
        mid_ref[at, :] = mid
        low[at, :] = mid.astype(BF16)

    by_rows(after_ref.shape[0], norm)
    branch = gather_of(plane, low, all_ref, *scratch[8:])
    branch.start()
    branch.forward()
    sums.finish()
    branch.finish()


def turn(n, part, after, grad, gain):
    shape = jax.ShapeDtypeStruct
    return comm_call(
        functools.partial(turn_kernel, n),
        4,
        [
            shape(after.shape, F32),
            shape((8, after.shape[1]), F32),
            shape((n,) + after.shape, BF16),
        ],
        [VM, VM, ANY],
        [ANY, VM, VM, VM],
        [pltpu.VMEM(after.shape, BF16)] + scatter_scratch(n, *after.shape) + gather_sems(n),
        95,
        part,
        after,
        grad,
        gain,
    )


def last_kernel(
    n,
    grad_ref,
    wqkv_ref,
    x_ref,
    mid_ref,
    gain_ref,
    *rest,
):
    fused = n == 8
    normed_ref, rest = (rest[0], rest[1:]) if fused else (None, rest)
    out_ref, apart_ref, rest = rest[0], rest[1], rest[2:]
    wgrad_ref, scratch = (rest[0], rest[1:]) if fused else (None, rest)
    plane = Plane(n)
    plane.meet()
    apart_ref[...] = jnp.zeros_like(apart_ref)
    rows = x_ref.shape[0]

    def value(block, at):
        left = grad_ref[pl.ds(pl.multiple_of(block * rows, rows), rows), :]
        return dot(left, wqkv_ref[at, :], NT)

    sums = Product(plane, value, *scratch[:8])
    sums.start()

    def weights():
        def fill(at):
            wgrad_ref[at, :] = dot(normed_ref[:, at], grad_ref[...], TN).astype(BF16)

        by_cols(normed_ref.shape[1], fill)

    sums.run(weights if fused else None)

    def norm(at):
        value = x_ref[at, :].astype(F32)
        inv = rms_parts(value)
        unit = value * inv
        grad = sums.total(at)
        apart_ref[0:1, :] += jnp.sum(grad * unit, axis=0, keepdims=True)
        out_ref[at, :] = mid_ref[at, :] + rms_back(grad, unit, inv, gain_ref[...])

    by_rows(rows, norm)
    sums.finish()


def last(n, grad, wqkv, x, mid, gain, normed):
    shape = jax.ShapeDtypeStruct
    outs = [shape(mid.shape, F32), shape((8, mid.shape[1]), F32)]
    more = [normed] if n == 8 else []
    outs += [shape(wqkv.shape, BF16) for _ in more]
    got = comm_call(
        functools.partial(last_kernel, n),
        5,
        outs,
        [VM] * len(outs),
        [VM] * (5 + len(more)),
        product_scratch(n, *mid.shape),
        60,
        grad,
        wqkv,
        x,
        mid,
        gain,
        *more,
    )
    return got if more else (*got, dot(normed, grad, TN).astype(BF16))


def close_kernel(n, n_dp, part_ref, after_ref, small_ref, out_ref, sum_ref, *scratch):
    meet(
        [("ctx", flip(lax.axis_index("ctx"), s, n)) for s in range(1, n)]
        + [("dp", flip(lax.axis_index("dp"), s, n_dp)) for s in range(1, n_dp)]
    )
    plane = Plane(n)
    sums = Scatter(plane, part_ref, *scratch[:8])
    sums.start()
    gains = Gains(n, n_dp, small_ref, *scratch[8:])
    gains.start()
    sums.run(gains.middle)

    def add(at):
        out_ref[at, :] = (after_ref[at, :] + sums.total(at)).astype(BF16)

    by_rows(after_ref.shape[0], add)
    sums.finish()
    sum_ref[...] = gains.finish()


def close(n, n_dp, part, after, small):
    shape = jax.ShapeDtypeStruct
    tile = small.shape[2:]
    return comm_call(
        functools.partial(close_kernel, n, n_dp),
        6,
        [shape(after.shape, BF16), shape(tile, F32)],
        [VM, VM],
        [ANY, VM, VM],
        scatter_scratch(n, *after.shape)
        + [
            pltpu.VMEM((n, n_dp) + tile, F32),
            pltpu.VMEM((n_dp,) + tile, F32),
            pltpu.VMEM((n_dp,) + tile, F32),
            DMA((n,)),
            DMA((n,)),
            DMA((n_dp,)),
            DMA((n_dp,)),
        ],
        50,
        part,
        after,
        small,
    )


def attn_forward_kernel(
    n,
    n_dp,
    heads,
    back,
    normed_ref,
    wqkv_ref,
    cos_ref,
    sin_ref,
    qgain_ref,
    kgain_ref,
    docc_ref,
    docr_ref,
    rows_ref,
    qlin_ref,
    klin_ref,
    q_ref,
    k_ref,
    v_ref,
    attn_ref,
    total_ref,
    wout_ref,
    acc_ref,
    sum_ref,
    *sems,
):
    step = pl.program_id(0)

    @pl.when(step == 0)
    def _():
        meet_all(n)
        RowSwap(n, n_dp, rows_ref, wout_ref, *sems, False).start()

    rows = normed_ref.shape[0]
    lin = dot(normed_ref[...], wqkv_ref[...])
    here = pl.ds(step * rows, rows)
    cosine = cos_ref[...]
    sine = sin_ref[...]
    qw = heads * HD
    for head in range(heads):
        cols = slice(head * HD, (head + 1) * HD)
        part = lin[:, cols]
        qlin_ref[:, cols] = part
        q_ref[:, cols] = head_forward(part, qgain_ref[...], cosine, sine).astype(BF16)
    key_lin = lin[:, qw : qw + HD]
    klin_ref[...] = key_lin
    k_ref[here, :] = head_forward(key_lin, kgain_ref[...], cosine, sine).astype(BF16)
    v_ref[here, :] = lin[:, qw + HD :].astype(BF16)
    acc_ref[...] = jnp.zeros_like(acc_ref)
    sum_ref[...] = jnp.zeros_like(sum_ref)
    row_pos = step * rows + lax.broadcasted_iota(jnp.int32, (rows, rows), 0)
    col_off = lax.broadcasted_iota(jnp.int32, (rows, rows), 1)

    def one(block, carry):
        at = pl.ds(pl.multiple_of(block * rows, rows), rows)
        key = k_ref[at, :]
        val = v_ref[at, :]
        allowed = (docc_ref[...] == docr_ref[:, at]) & (block * rows + col_off <= row_pos)
        for head in range(heads):
            cols = slice(head * HD, (head + 1) * HD)
            score = dot(q_ref[:, cols], key, NT) * SCALE2
            expo = jnp.where(allowed, jnp.exp2(score), 0.0)
            folded = expo[:, :HD]
            for piece in range(1, rows // HD):
                folded = folded + expo[:, piece * HD : (piece + 1) * HD]
            sum_ref[:, cols] += folded
            acc_ref[:, cols] += dot(expo.astype(BF16), val)
        return carry

    lax.fori_loop(jnp.maximum(step - back, 0), step + 1, one, 0)
    lane = lax.broadcasted_iota(jnp.int32, (rows, HD), 1)
    totals = jnp.ones((rows, HD), F32)
    for head in range(heads):
        cols = slice(head * HD, (head + 1) * HD)
        total = jnp.sum(sum_ref[:, cols], axis=-1, keepdims=True)
        totals = jnp.where(lane == head, total, totals)
        attn_ref[:, cols] = (acc_ref[:, cols] / total).astype(BF16)
    total_ref[...] = totals

    @pl.when(step == pl.num_programs(0) - 1)
    def _():
        swap = RowSwap(n, n_dp, rows_ref, wout_ref, *sems, False)
        swap.arrive()
        swap.finish()


def attn_forward(n, n_dp, normed, wqkv, cosine, sine, qgain, kgain, doc, wrows, rows):
    length, width = normed.shape
    qw = wqkv.shape[1] - 2 * HD
    heads = qw // HD
    blk = lambda cols: pl.BlockSpec((rows, cols), lambda i: (i, 0))
    whole = lambda shape: pl.BlockSpec(shape, lambda i: (0, 0))
    shape = jax.ShapeDtypeStruct
    return pl.pallas_call(
        functools.partial(attn_forward_kernel, n, n_dp, heads, MOST // rows),
        grid=(length // rows,),
        in_specs=[
            blk(width),
            whole(wqkv.shape),
            blk(HD),
            blk(HD),
            whole((1, HD)),
            whole((1, HD)),
            blk(1),
            whole((1, length)),
            ANY,
        ],
        out_specs=[
            blk(qw),
            blk(HD),
            blk(qw),
            whole((length, HD)),
            whole((length, HD)),
            blk(qw),
            blk(HD),
            ANY,
        ],
        out_shape=[
            shape((length, qw), F32),
            shape((length, HD), F32),
            shape((length, qw), BF16),
            shape((length, HD), BF16),
            shape((length, HD), BF16),
            shape((length, qw), BF16),
            shape((length, HD), F32),
            shape(wrows.shape, BF16),
        ],
        scratch_shapes=[pltpu.VMEM((rows, qw), F32), pltpu.VMEM((rows, qw), F32)]
        + [DMA((n_dp,)), DMA((n_dp,))],
        compiler_params=pltpu.CompilerParams(
            collective_id=7, has_side_effects=True, vmem_limit_bytes=VMEM_LIMIT
        ),
        cost_estimate=pl.CostEstimate(
            flops=35 * 10**9, transcendentals=0, bytes_accessed=30 * 2**20
        ),
        name="attn_forward",
    )(normed, wqkv, cosine, sine, qgain, kgain, doc[:, None], doc[None, :], wrows)


def attn_backward_kernel(
    n,
    n_dp,
    heads,
    back,
    branch_ref,
    wout_ref,
    attn_ref,
    total_ref,
    q_ref,
    k_ref,
    v_ref,
    qlin_ref,
    klin_ref,
    cos_ref,
    sin_ref,
    qgain_ref,
    kgain_ref,
    docc_ref,
    docr_ref,
    wgrad_ref,
    dqkv_ref,
    gains_ref,
    swapped_ref,
    dk_ref,
    dv_ref,
    dqa_ref,
    *sems,
):
    step = pl.program_id(0)

    @pl.when(step == 0)
    def _():
        meet_all(n)
        RowSwap(n, n_dp, wgrad_ref, swapped_ref, *sems, True).start()

    @pl.when(step == pl.num_programs(0) - 1)
    def _():
        swap = RowSwap(n, n_dp, wgrad_ref, swapped_ref, *sems, True)
        swap.arrive()
        swap.finish()

    rows = branch_ref.shape[0]
    here = pl.ds(pl.multiple_of(step * rows, rows), rows)

    @pl.when(step == 0)
    def _():
        gains_ref[...] = jnp.zeros_like(gains_ref)

    dk_ref[here, :] = jnp.zeros((rows, HD), F32)
    dv_ref[here, :] = jnp.zeros((rows, HD), F32)
    dqa_ref[...] = jnp.zeros_like(dqa_ref)
    attn_grad = dot(branch_ref[...], wout_ref[...], NT)
    grads = []
    shifts = []
    for head in range(heads):
        cols = slice(head * HD, (head + 1) * HD)
        part = attn_grad[:, cols]
        inv_total = 1.0 / total_ref[:, head : head + 1]
        delta = jnp.sum(part * attn_ref[:, cols].astype(F32), axis=-1, keepdims=True)
        grads.append((part * inv_total).astype(BF16))
        shifts.append(delta * inv_total)
    row_pos = step * rows + lax.broadcasted_iota(jnp.int32, (rows, rows), 0)
    col_off = lax.broadcasted_iota(jnp.int32, (rows, rows), 1)

    def one(block, carry):
        at = pl.ds(pl.multiple_of(block * rows, rows), rows)
        key = k_ref[at, :]
        val = v_ref[at, :]
        allowed = (docc_ref[...] == docr_ref[:, at]) & (block * rows + col_off <= row_pos)
        dk = jnp.zeros((rows, HD), F32)
        dv = jnp.zeros((rows, HD), F32)
        for head in range(heads):
            cols = slice(head * HD, (head + 1) * HD)
            query = q_ref[:, cols]
            score = dot(query, key, NT) * SCALE2
            expo = jnp.where(allowed, jnp.exp2(score), 0.0)
            prod = dot(grads[head], val, NT)
            score_grad = (expo * (prod - shifts[head])).astype(BF16)
            dv += dot(expo.astype(BF16), grads[head], TN)
            dk += dot(score_grad, query, TN)
            dqa_ref[:, cols] += dot(score_grad, key)
        dk_ref[at, :] += dk
        dv_ref[at, :] += dv
        return carry

    lax.fori_loop(jnp.maximum(step - back, 0), step + 1, one, 0)
    cosine = cos_ref[here, :]
    sine = sin_ref[here, :]
    for head in range(heads):
        cols = slice(head * HD, (head + 1) * HD)
        grad, gain_part = head_backward(
            qlin_ref[:, cols], qgain_ref[...], cosine, sine, dqa_ref[:, cols] * SCALE
        )
        dqkv_ref[here, cols] = grad.astype(BF16)
        gains_ref[0:1, :] += gain_part

    @pl.when(step == pl.num_programs(0) - 1)
    def _():
        def finish(block, carry):
            at = pl.ds(pl.multiple_of(block * rows, rows), rows)
            grad, gain_part = head_backward(
                klin_ref[at, :], kgain_ref[...], cos_ref[at, :], sin_ref[at, :], dk_ref[at, :] * SCALE
            )
            qw = heads * HD
            dqkv_ref[at, qw : qw + HD] = grad.astype(BF16)
            dqkv_ref[at, qw + HD :] = dv_ref[at, :].astype(BF16)
            gains_ref[1:2, :] += gain_part
            return carry

        lax.fori_loop(0, pl.num_programs(0), finish, 0)


def attn_backward(n, n_dp, wgrad, branch, wout, attn, total, q, k, v, qlin, klin, cosine, sine, qgain, kgain, doc, rows):
    length, width = branch.shape
    qw = wout.shape[0]
    heads = qw // HD
    blk = lambda cols: pl.BlockSpec((rows, cols), lambda i: (i, 0))
    whole = lambda shape: pl.BlockSpec(shape, lambda i: (0, 0))
    shape = jax.ShapeDtypeStruct
    full = whole((length, HD))
    return pl.pallas_call(
        functools.partial(attn_backward_kernel, n, n_dp, heads, MOST // rows),
        grid=(length // rows,),
        in_specs=[
            blk(width),
            whole(wout.shape),
            blk(qw),
            blk(HD),
            blk(qw),
            full,
            full,
            blk(qw),
            full,
            full,
            full,
            whole((1, HD)),
            whole((1, HD)),
            blk(1),
            whole((1, length)),
            ANY,
        ],
        out_specs=[whole((length, qw + 2 * HD)), whole((8, HD)), ANY],
        out_shape=[
            shape((length, qw + 2 * HD), BF16),
            shape((8, HD), F32),
            shape(wgrad.shape, BF16),
        ],
        scratch_shapes=[
            pltpu.VMEM((length, HD), F32),
            pltpu.VMEM((length, HD), F32),
            pltpu.VMEM((rows, qw), F32),
            DMA((n_dp,)),
            DMA((n_dp,)),
        ],
        compiler_params=pltpu.CompilerParams(
            collective_id=9, has_side_effects=True, vmem_limit_bytes=VMEM_LIMIT
        ),
        cost_estimate=pl.CostEstimate(
            flops=60 * 10**9, transcendentals=0, bytes_accessed=30 * 2**20
        ),
        name="attn_backward",
    )(branch, wout, attn, total, q, k, v, qlin, klin, cosine, sine, qgain, kgain, doc[:, None], doc[None, :], wgrad)


def expert_kernel(chained, low, aliased, plan, z_ref, n2_ref, top_ref, prob_ref, *rest):
    if aliased:
        rest = rest[1:]
    if chained:
        moe_in, row_in = rest[:2]
        rest = rest[2:]
    sources, rest = rest[: len(plan)], rest[len(plan) :]
    moe_ref, row_ref, grads_ref, wg_ref, wu_ref, wd_ref = rest[:6]
    ag_ref, au_ref, ad_ref, stage, wsem, sem = rest[6:]
    step = pl.program_id(0)
    rows, width = n2_ref.shape
    parts, cut, hidden = wd_ref.shape
    weights = (wg_ref, wu_ref, wd_ref)

    @pl.when(step == 0)
    def _():
        z = z_ref[0]
        for source, (kind, amount, start) in zip(sources, plan):
            count = source.shape[-2] // cut
            for k in range(parts) if kind == "all" else [amount]:
                if kind == "all":
                    src, owner, wanted = source.at[k], k, None
                elif kind == "up":
                    src, owner, wanted = source, z - k, z >= k
                else:
                    src, owner, wanted = source, z + k, z + k < parts

                def load(src=src, owner=owner, start=start, count=count):
                    for piece in range(count):
                        pltpu.make_async_copy(
                            src.at[pl.ds(piece * cut, cut), :],
                            weights[start + piece].at[owner],
                            wsem.at[start + piece, owner],
                        ).start()

                if wanted is None:
                    load()
                else:
                    pl.when(wanted)(load)
        ag_ref[...] = jnp.zeros_like(ag_ref)
        au_ref[...] = jnp.zeros_like(au_ref)
        ad_ref[...] = jnp.zeros_like(ad_ref)
        for index in range(3):
            for owner in range(parts):
                block = weights[index].at[owner]
                pltpu.make_async_copy(block, block, wsem.at[index, owner]).wait()

    n2 = n2_ref[...]
    prob = prob_ref[...]
    wg = wg_ref[...].reshape(width, hidden)
    wu = wu_ref[...].reshape(width, hidden)
    gate = dot(n2, wg)
    up = dot(n2, wu)
    sig = 1.0 / (1.0 + jnp.exp(-gate))
    silu = gate * sig
    act = (silu * up).astype(BF16)
    act_grad = jnp.zeros((rows, hidden), F32)
    for z in range(parts):
        cols = slice(z * cut, (z + 1) * cut)
        out = dot(act, wd_ref[z], NT).astype(BF16).astype(F32) * prob
        if chained:
            out = out + moe_in[:, cols].astype(F32)
        moe_ref[:, cols] = out.astype(BF16)
        route = (top_ref[:, cols].astype(F32) * prob).astype(BF16)
        act_grad += dot(route, wd_ref[z])
        ad_ref[z] += dot(route, act, TN)
    gate_grad = (act_grad * up * sig * (1.0 + gate * (1.0 - sig))).astype(BF16)
    up_grad = (act_grad * silu).astype(BF16)
    row = dot(gate_grad, wg, NT) + dot(up_grad, wu, NT)
    if chained:
        row = row + row_in[...].astype(F32)
    row_ref[...] = row.astype(BF16)
    ag_ref[...] += dot(n2, gate_grad, TN).reshape(parts, cut, hidden)
    au_ref[...] += dot(n2, up_grad, TN).reshape(parts, cut, hidden)

    @pl.when(step == pl.num_programs(0) - 1)
    def _():
        copies = []
        pieces = [
            (acc, place, z) for z in range(parts) for place, acc in enumerate((ag_ref, au_ref, ad_ref))
        ]
        for index, (acc, place, z) in enumerate(pieces):
            slot = index % 2
            if index >= 2:
                copies[index - 2].wait()
            stage[slot] = acc[z].astype(BF16)
            copies.append(
                pltpu.make_async_copy(
                    stage.at[slot],
                    grads_ref.at[z, pl.ds(place * cut, cut), pl.ds(low, acc.shape[2])],
                    sem.at[slot],
                )
            )
            copies[-1].start()
        copies[-2].wait()
        copies[-1].wait()


def expert(z, n2, top, prob, n_dp, sources, before, rows, low, full, grads):
    length, width = n2.shape
    cut = width // n_dp
    hidden = sources[0][0].shape[-1]
    blk = pl.BlockSpec((rows, width), lambda i: (i, 0))
    col = pl.BlockSpec((rows, 1), lambda i: (i, 0))
    shape = jax.ShapeDtypeStruct
    plan = tuple(entry[1:] for entry in sources)
    weight = pltpu.VMEM((n_dp, cut, hidden), BF16)
    total = pltpu.VMEM((n_dp, cut, hidden), F32)
    return pl.pallas_call(
        functools.partial(expert_kernel, len(before) > 0, low, len(grads) > 0, plan),
        grid=(length // rows,),
        in_specs=[pl.BlockSpec(memory_space=pltpu.SMEM), blk, blk, col]
        + [ANY] * len(grads)
        + [blk] * len(before)
        + [ANY] * len(sources),
        out_specs=[blk, blk, ANY],
        out_shape=[
            shape((length, width), BF16),
            shape((length, width), BF16),
            shape((n_dp, 3 * cut, full), BF16),
        ],
        input_output_aliases={4: 2} if grads else {},
        scratch_shapes=[weight] * 3
        + [total] * 3
        + [pltpu.VMEM((2, cut, hidden), BF16), DMA((3, n_dp)), DMA((2,))],
        compiler_params=pltpu.CompilerParams(vmem_limit_bytes=VMEM_LIMIT),
        cost_estimate=pl.CostEstimate(
            flops=18 * length * width * hidden,
            transcendentals=length * hidden,
            bytes_accessed=5 * length * width * 2,
        ),
        name="expert",
    )(z, n2, top, prob, *grads, *before, *[entry[0] for entry in sources])


def pack_kernel(cuts, gate_ref, up_ref, down_ref, *outs):
    cut = gate_ref.shape[0]
    for (low, high), out in zip(cuts, outs):
        out[:cut, :] = gate_ref[:, low:high]
        out[cut : 2 * cut, :] = up_ref[:, low:high]
        out[2 * cut :, :] = jnp.transpose(down_ref[low:high, :].astype(F32)).astype(BF16)


def pack(cuts, w_gate, w_up, w_down):
    cut = w_gate.shape[0]
    return pl.pallas_call(
        functools.partial(pack_kernel, cuts),
        in_specs=[VM] * 3,
        out_specs=[VM] * len(cuts),
        out_shape=[jax.ShapeDtypeStruct((3 * cut, high - low), BF16) for low, high in cuts],
        name="pack",
    )(w_gate, w_up, w_down)


def unpack_kernel(
    z_ref, one_ref, all_ref, up0_ref, down0_ref, up1_ref, down1_ref, dg_ref, du_ref, dd_ref, own, sem
):
    copy = pltpu.make_async_copy(all_ref.at[z_ref[0]], own, sem)
    copy.start()
    cut = dg_ref.shape[1]
    half = up0_ref.shape[0]
    piece = [slice(k * cut, (k + 1) * cut) for k in range(3)]
    dg_ref[1] = one_ref[piece[0], :].astype(F32)
    du_ref[1] = one_ref[piece[1], :].astype(F32)
    dd_ref[1] = jnp.transpose(one_ref[piece[2], :].astype(F32))
    copy.wait()

    def total(low, high):
        shift, up, down = (0, up0_ref, down0_ref) if high <= half else (half, up1_ref, down1_ref)
        there = slice(low - shift, high - shift)
        value = own[low:high, :].astype(F32)
        return value + up[there, :].astype(F32) + down[there, :].astype(F32)

    dg_ref[0] = total(0, cut)
    du_ref[0, : half - cut] = total(cut, half)
    du_ref[0, half - cut :] = total(half, 2 * cut)
    dd_ref[0] = jnp.transpose(total(2 * cut, 3 * cut))


def unpack(z, one, grads, got):
    rows, hidden = one.shape
    cut = rows // 3
    shape = jax.ShapeDtypeStruct
    return pl.pallas_call(
        unpack_kernel,
        in_specs=[pl.BlockSpec(memory_space=pltpu.SMEM), VM, ANY, VM, VM, VM, VM],
        out_specs=[VM] * 3,
        out_shape=[
            shape((2, cut, hidden), F32),
            shape((2, cut, hidden), F32),
            shape((2, hidden, cut), F32),
        ],
        scratch_shapes=[pltpu.VMEM((rows, hidden), BF16), DMA(())],
        compiler_params=pltpu.CompilerParams(vmem_limit_bytes=VMEM_LIMIT),
        name="unpack",
    )(z, one, grads, *got)


def line_hop(block_up, block_down, n_dp, hop):
    up = [(i, i + 1) for i in range(hop - 1, n_dp - 1)]
    down = [(i + 1, i) for i in range(n_dp - hop)]
    return lax.ppermute(block_up, "dp", up), lax.ppermute(block_down, "dp", down)


def reduce_hop(grads, got, n_dp, hop, rows, before):
    place = lax.axis_index("dp")
    reach = n_dp - hop
    zero = jnp.int32(0)
    size = (1, rows[1] - rows[0], grads.shape[2])
    spots = (jnp.minimum(place + reach, n_dp - 1), jnp.maximum(place - reach, 0))
    if got is not None:
        got = lax.optimization_barrier((*got, *before))[:2]
    elif before:
        grads = after_of(grads, *before)
    blocks = [
        lax.dynamic_slice(grads, (spot.astype(jnp.int32), jnp.int32(rows[0]), zero), size)[0]
        for spot in spots
    ]
    if got is not None:
        blocks = [(b.astype(F32) + g.astype(F32)).astype(BF16) for b, g in zip(blocks, got)]
    up = [(i, i + 1) for i in range(hop)]
    down = [(i, i - 1) for i in range(n_dp - hop, n_dp)]
    sent = lax.ppermute(blocks[0], "dp", up), lax.ppermute(blocks[1], "dp", down)
    return sent, tuple(blocks)


def after_of(value, *others):
    return lax.optimization_barrier((value,) + others)[0]


def per_device(
    layer_input,
    doc_ids,
    route_ids,
    route_probs,
    attn_gain,
    ffn_gain,
    query_gain,
    key_gain,
    w_query,
    w_key,
    w_value,
    w_out,
    w_gate,
    w_up,
    w_down,
    out_grad,
):
    tokens, width = layer_input.shape[1:]
    n_dp = lax.axis_size("dp")
    n_ctx = lax.axis_size("ctx")
    ctx_index = lax.axis_index("ctx")
    length = tokens * n_ctx
    heads = HQ // n_ctx
    share = n_ctx // KV
    qw = heads * HD
    depth = w_query.shape[0]
    own_e = w_gate.shape[0]

    cut = attn_gain.shape[0]
    hcut = query_gain.shape[0]
    kinds = 2 * (cut + hcut)
    small = jnp.concatenate([attn_gain, ffn_gain, query_gain, key_gain]).astype(F32)
    small = jnp.pad(small, (0, 1024 - kinds)).reshape(8, HD)
    cols = jnp.concatenate(
        [
            w_query.reshape(depth, n_ctx, qw),
            jnp.repeat(w_key.reshape(depth, KV, HD), share, axis=1),
            jnp.repeat(w_value.reshape(depth, KV, HD), share, axis=1),
        ],
        axis=2,
    ).transpose(1, 0, 2)
    cols, small = prep(n_ctx, n_dp, cols, small)
    small = small.reshape(n_dp * n_ctx, 1024)
    gain_attn = small[:, :cut].reshape(1, width)
    gain_ffn = small[:, cut : 2 * cut].reshape(1, width)
    gain_query = small[:, 2 * cut : 2 * cut + hcut].reshape(1, HD)
    gain_key = small[:, 2 * cut + hcut : kinds].reshape(1, HD)
    wqkv = lax.all_gather(cols.reshape(n_ctx * depth, qw + 2 * HD), "dp", axis=0, tiled=True)
    wrows = lax.all_gather(w_out, "dp", axis=0, tiled=False)

    inputs = layer_input.reshape(tokens, width)
    top_own = out_grad.reshape(tokens, width)
    n_experts = own_e * n_ctx
    match = route_ids.reshape(1, tokens, TOP) == jnp.arange(n_experts, dtype=jnp.int32)[:, None, None]
    probs = jnp.sum(jnp.where(match, route_probs.reshape(1, tokens, TOP), 0.0), axis=2)
    info = jnp.concatenate(
        [probs, doc_ids.reshape(1, tokens).astype(F32), jnp.zeros((7, tokens), F32)], axis=0
    )
    normed, info, top_all = first(n_ctx, inputs, gain_attn, info, top_own)
    normed = normed.reshape(length, width)
    doc = info[:, n_experts].reshape(length).astype(jnp.int32)
    my_probs = lax.dynamic_slice_in_dim(info, ctx_index * own_e, own_e, 1)
    my_probs = my_probs.transpose(0, 2, 1).reshape(length, own_e)

    inverse = 1.0 / ROPE_BASE ** (jnp.arange(HD // 2, dtype=F32) * 2.0 / HD)
    angles = jnp.arange(length, dtype=F32)[:, None] * inverse[None, :]
    cosine = jnp.cos(angles)
    sine = jnp.sin(angles)
    cosine = jnp.concatenate([cosine, cosine], axis=1)
    sine = jnp.concatenate([-sine, sine], axis=1)
    qlin, klin, q, k, v, attn, total, wout = attn_forward(
        n_ctx, n_dp, normed, wqkv, cosine, sine, gain_query, gain_key, doc, wrows, tokens
    )
    wout = wout.reshape(qw, width)
    top_all = top_all.reshape(length, width)
    blocks = (n_ctx, tokens, width)
    after, normed2 = middle(n_ctx, attn, wout, inputs, gain_ffn)
    normed2 = normed2.reshape(length, width)

    z = lax.axis_index("dp").astype(jnp.int32).reshape(1)
    hidden = w_gate.shape[2]

    def run(e, sources, carried, low, grads):
        moe, rows_grad, grads = expert(
            z,
            normed2,
            top_all,
            my_probs[:, e : e + 1],
            n_dp,
            sources,
            carried,
            tokens,
            low,
            hidden,
            grads,
        )
        return (moe, rows_grad), grads

    cuts = [(0, 256), (256, hidden)]
    blocks0 = pack(cuts, w_gate[0], w_up[0], w_down[0])
    carried, grads0 = (), ()
    for index, (low, high) in enumerate(cuts):
        full = lax.all_gather(blocks0[index], "dp", axis=0, tiled=False)
        if index == 1:
            (block1,) = pack([(0, hidden)], w_gate[1], w_up[1], w_down[1])
            sources1 = [(block1, "up", 0, 0)]
            up = down = after_of(block1, full)
            up, down = line_hop(up, down, n_dp, 1)
            sources1 += [(up, "up", 1, 0), (down, "down", 1, 0)]
        carried, grads = run(0, [(full, "all", 0, 0)], carried, low, grads0)
        grads0 = (grads,)
    rows_all = 3 * (width // n_dp)
    spans = {"a": (0, rows_all // 2), "b": (rows_all // 2, rows_all)}
    got, before = {tag: None for tag in spans}, ()
    for hop in range(2, n_dp + 1):
        if hop < n_dp:
            up, down = line_hop(up, down, n_dp, hop)
            sources1 += [(up, "up", hop, 0), (down, "down", hop, 0)]
        for tag, rows in spans.items():
            got[tag], before = reduce_hop(grads, got[tag], n_dp, hop - 1, rows, before)
    (moe, rows_grad), grads1 = run(1, sources1, carried, 0, ())
    done1 = lax.psum_scatter(
        grads1.reshape(3 * width, hidden), "dp", scatter_dimension=0, tiled=True
    )
    mid, ffn_part, branch = turn(
        n_ctx, rows_grad.reshape(blocks), after, top_own, gain_ffn
    )
    branch = branch.reshape(length, width)

    out_w = dot(attn, branch, TN).astype(BF16).reshape(n_dp, qw // n_dp, width)
    dqkv, gains, out_w = attn_backward(
        n_ctx,
        n_dp,
        out_w,
        branch,
        wout,
        attn,
        total,
        q,
        k,
        v,
        qlin,
        klin,
        cosine,
        sine,
        gain_query,
        gain_key,
        doc,
        tokens,
    )
    out_w = lax.psum_scatter(out_w.reshape(qw, width), "dp", scatter_dimension=0, tiled=True)
    out_w = out_w.astype(F32)
    input_grad, attn_part, qkv_w = last(n_ctx, dqkv, wqkv, inputs, mid, gain_attn, normed)
    qkv_w = lax.psum_scatter(qkv_w, "dp", scatter_dimension=0, tiled=True)
    n_all = n_dp * n_ctx
    packed = jnp.concatenate(
        [
            attn_part[0].reshape(n_all, cut),
            ffn_part[0].reshape(n_all, cut),
            gains[0].reshape(n_all, hcut),
            gains[1].reshape(n_all, hcut),
            jnp.zeros((n_all, 1024 - kinds), F32),
        ],
        axis=1,
    )
    packed = packed.reshape(n_dp, n_ctx, 8, HD).transpose(1, 0, 2, 3)
    layer_output, packed = close(n_ctx, n_dp, moe.reshape(blocks), after, packed)
    packed = packed.reshape(1024)
    query_w, key_w, value_w = post(n_ctx, qkv_w.reshape(n_ctx, depth, qw + 2 * HD))
    gate_w, up_w, down_w = unpack(z, done1, grads, got["a"] + got["b"])
    return (
        layer_output.reshape(1, tokens, width),
        input_grad.reshape(1, tokens, width),
        packed[:cut],
        packed[cut : 2 * cut],
        packed[2 * cut : 2 * cut + hcut],
        packed[2 * cut + hcut : kinds],
        query_w,
        key_w,
        value_w,
        out_w,
        gate_w,
        up_w,
        down_w,
    )


def solution(mesh):
    both = ("dp", "ctx")
    seq = P("dp", "ctx", None)
    in_specs = (
        seq,
        P("dp", "ctx"),
        seq,
        seq,
        P(both),
        P(both),
        P(both),
        P(both),
        P(both, None),
        P(both, None),
        P(both, None),
        P(both, None),
        P("ctx", "dp", None),
        P("ctx", "dp", None),
        P("ctx", None, "dp"),
        seq,
    )
    out_specs = (
        seq,
        seq,
        P(both),
        P(both),
        P(both),
        P(both),
        P(both, None),
        P(both, None),
        P(both, None),
        P(both, None),
        P("ctx", "dp", None),
        P("ctx", "dp", None),
        P("ctx", None, "dp"),
    )

    return jax.shard_map(
        per_device, mesh=mesh, in_specs=in_specs, out_specs=out_specs, check_vma=False
    )
```

```python
import functools
import math

import jax
import jax.numpy as jnp
from jax import lax
from jax.experimental import pallas as pl
from jax.experimental.pallas import tpu as pltpu
from jax.sharding import PartitionSpec as P


HQ = 32
KV = 4
HD = 128
TOP = 8
MOST = 1024
EPS = 1e-06
ROPE_BASE = 1000000.0
F32 = jnp.float32
BF16 = jnp.bfloat16
SCALE = 1.0 / math.sqrt(HD)
SCALE2 = SCALE / math.log(2.0)
VMEM_LIMIT = 60 * 1024 * 1024


def dot(left, right, dims=((1,), (0,))):
    return lax.dot_general(left, right, (dims, ((), ())), preferred_element_type=F32)


NT = ((1,), (1,))
TN = ((0,), (0,))


def rms_parts(values):
    return lax.rsqrt(jnp.mean(values * values, axis=-1, keepdims=True) + EPS)


def rms_back(grad, unit, inv, gain):
    scaled = grad * gain
    return inv * (scaled - unit * jnp.mean(scaled * unit, axis=-1, keepdims=True))


def head_forward(lin, gain, cosine, sine):
    unit = lin * rms_parts(lin) * gain
    return unit * cosine + pltpu.roll(unit, HD // 2, 1) * sine


def head_backward(lin, gain, cosine, sine, rot_grad):
    grad = rot_grad * cosine + pltpu.roll(rot_grad * sine, HD // 2, 1)
    inv = rms_parts(lin)
    unit = lin * inv
    return rms_back(grad, unit, inv, gain), jnp.sum(grad * unit, axis=0, keepdims=True)


MESH = pl.DeviceIdType.MESH
ANY = pl.BlockSpec(memory_space=pl.ANY)
VM = pl.BlockSpec(memory_space=pltpu.VMEM)
DMA = pltpu.SemaphoreType.DMA
CHUNK = 32


def flip(index, mask, count):
    result, bit = 0, 1
    while bit < count:
        digit = (index // bit) % 2
        result = result + bit * ((1 - digit) if mask & bit else digit)
        bit *= 2
    return result


def push(src, dst, send, recv, axis, peer):
    return pltpu.make_async_remote_copy(
        src_ref=src,
        dst_ref=dst,
        send_sem=send,
        recv_sem=recv,
        device_id={axis: peer},
        device_id_type=MESH,
    )


def meet(peers):
    barrier = pltpu.get_barrier_semaphore()
    for axis, peer in peers:
        pl.semaphore_signal(barrier, inc=1, device_id={axis: peer}, device_id_type=MESH)
    pl.semaphore_wait(barrier, len(peers))


class Plane:
    def __init__(self, n):
        self.chips = n // 2
        self.me = lax.axis_index("ctx")
        self.core = self.me % 2
        self.chip = self.me // 2
        self.mate = self.me + 1 - 2 * self.core

    def same(self, s):
        return 2 * flip(self.chip, s, self.chips) + self.core

    def meet(self):
        meet([("ctx", self.same(s)) for s in range(1, self.chips)] + [("ctx", self.mate)])


def far_first(chips):
    return sorted(range(1, chips), key=lambda s: -bin(s).count("1"))


class Gather:
    def __init__(self, plane, src, out, send, recv, local):
        self.plane, self.out, self.send, self.recv = plane, out, send, recv
        self.own = pltpu.make_async_copy(src, out.at[plane.me], local)
        self.far = [
            push(src, out.at[plane.me], send.at[s], recv.at[s], "ctx", plane.same(s))
            for s in far_first(plane.chips)
        ]
        self.near = push(src, out.at[plane.me], send.at[0], recv.at[0], "ctx", plane.mate)

    def start(self):
        for copy in self.far:
            copy.start()
        self.near.start()
        self.own.start()

    def forward(self):
        plane, out = self.plane, self.out
        self.passed = []
        for s in sorted(range(1, plane.chips), key=lambda s: bin(s).count("1")):
            block = out.at[plane.same(s)]
            push(block, block, self.send.at[s], self.recv.at[s], "ctx", plane.mate).wait_recv()
            slot = plane.chips + s
            copy = push(block, block, self.send.at[slot], self.recv.at[slot], "ctx", plane.mate)
            copy.start()
            self.passed.append(copy)

    def finish(self):
        for copy in self.far:
            copy.wait_send()
        self.near.wait_send()
        self.near.wait_recv()
        for copy in self.passed:
            copy.wait_send()
            copy.wait_recv()
        self.own.wait()


def by_rows(rows, body):
    def one(index, carry):
        body(pl.ds(pl.multiple_of(index * CHUNK, CHUNK), CHUNK))
        return carry

    lax.fori_loop(0, rows // CHUNK, one, 0)


class SquareGather:
    def __init__(self, plane, src, out, send, recv, local):
        self.plane, self.out, self.send, self.recv = plane, out, send, recv
        half = src.shape[0] // 2
        self.halves = [pl.ds(0, half), pl.ds(half, half)]
        mine = out.at[plane.me]
        self.own = pltpu.make_async_copy(src, mine, local)
        self.near = push(src, mine, send.at[0], recv.at[0], "ctx", plane.mate)
        self.far = []
        for s, h in ((1, 0), (2, 1), (1, 1), (2, 0)):
            part, slot = self.halves[h], 2 * s + h
            self.far.append(
                push(
                    src.at[part, :],
                    mine.at[part, :],
                    send.at[slot],
                    recv.at[slot],
                    "ctx",
                    plane.same(s),
                )
            )

    def start(self):
        for copy in self.far:
            copy.start()
        self.near.start()
        self.own.start()

    def arrived(self, s, h):
        block = self.out.at[self.plane.same(s)].at[self.halves[h], :]
        slot = 2 * s + h
        push(block, block, self.send.at[slot], self.recv.at[slot], "ctx", self.plane.mate).wait_recv()
        return block

    def forward(self):
        plane = self.plane
        self.passed = []
        for s, h in ((1, 0), (2, 1)):
            block = self.arrived(s, h)
            slot = 6 + h
            copy = push(block, block, self.send.at[slot], self.recv.at[slot], "ctx", plane.same(3 - s))
            copy.start()
            self.far.append(copy)
        for s in (1, 2, 3):
            if s < 3:
                self.arrived(s, 2 - s)
            else:
                self.arrived(3, 0)
                self.arrived(3, 1)
            block, slot = self.out.at[plane.same(s)], 7 + s
            copy = push(block, block, self.send.at[slot], self.recv.at[slot], "ctx", plane.mate)
            copy.start()
            self.passed.append(copy)

    def finish(self):
        for copy in self.far:
            copy.wait_send()
        self.near.wait_send()
        self.near.wait_recv()
        for copy in self.passed:
            copy.wait_send()
            copy.wait_recv()
        self.own.wait()


def gather_of(plane, src, out, send, recv, local):
    kind = SquareGather if plane.chips == 4 else Gather
    return kind(plane, src, out, send, recv, local)


class Spread:
    def __init__(self, plane, mine, landed, send, recv):
        self.plane, self.mine, self.landed = plane, mine, landed
        self.square = plane.chips == 4
        self.order = [3, 1, 2, 0] if self.square else far_first(plane.chips) + [0]
        self.send, self.recv = send, recv
        half = mine.shape[1] // 2
        self.halves = [pl.ds(0, half), pl.ds(half, half)]

    def copy(self, s, h, to):
        part, slot = self.halves[h], 2 * s + h
        return push(
            self.mine.at[s].at[part, :],
            self.landed.at[s].at[part, :],
            self.send.at[slot],
            self.recv.at[slot],
            "ctx",
            self.plane.same(to),
        )

    def go(self, s, h, to):
        self.copy(s, h, to).start()

    def ready(self, s):
        if self.square:
            if s == 3:
                self.go(3, 0, 1)
                self.go(3, 1, 2)
            elif s == 1:
                self.go(1, 0, 1)
            elif s == 2:
                self.go(2, 1, 2)
        elif s:
            push(
                self.mine.at[s],
                self.landed.at[s],
                self.send.at[s],
                self.recv.at[s],
                "ctx",
                self.plane.same(s),
            ).start()

    def sends(self):
        if self.square:
            hops = ((3, 0, 1), (3, 1, 2), (1, 0, 1), (2, 1, 2), (2, 0, 2), (1, 1, 1))
            return [self.copy(*hop) for hop in hops]
        return [
            push(
                self.mine.at[s],
                self.landed.at[s],
                self.send.at[s],
                self.recv.at[s],
                "ctx",
                self.plane.same(s),
            )
            for s in self.order
            if s
        ]

    def relay(self):
        mine, landed = self.mine, self.landed
        half = mine.shape[1] // 2
        if not self.square:
            return
        for s, h in ((2, 0), (1, 1)):
            self.copy(3, h, 1).wait_recv()

            def add(at, s=s, h=h):
                rows = pl.ds(h * half + at.start, CHUNK)
                total = mine[s, rows, :].astype(F32) + landed[3, rows, :].astype(F32)
                mine[s, rows, :] = total.astype(BF16)

            by_rows(half, add)
            self.copy(s, h, s).start()

    def gathered(self):
        if not self.square:
            for copy in self.sends():
                copy.wait_recv()
            return
        for s in (1, 2):
            for h in (0, 1):
                self.copy(s, h, s).wait_recv()

    def settle(self, extra=None):
        self.relay()
        if extra is not None:
            extra()
        self.gathered()

    def total(self, at):
        value = self.mine[0, at, :].astype(F32)
        for s in (1, 2) if self.square else range(1, self.plane.chips):
            value = value + self.landed[s, at, :].astype(F32)
        return value

    def finish(self):
        for copy in self.sends():
            copy.wait_send()


class Scatter:
    def __init__(self, plane, part, mine, other, landed, send, recv, send2, recv2, local):
        self.plane, self.mine, self.other = plane, mine, other
        self.spread = Spread(plane, mine, landed, send2, recv2)
        self.order = self.spread.order
        self.loads, self.across = {}, {}
        for s in self.order:
            block = plane.same(s)
            self.loads[s] = pltpu.make_async_copy(part.at[block], mine.at[s], local.at[s])
            self.across[s] = push(
                part.at[block + 1 - 2 * plane.core],
                other.at[s],
                send.at[s],
                recv.at[s],
                "ctx",
                plane.mate,
            )

    def start(self):
        for s in self.order:
            self.across[s].start()
            self.loads[s].start()

    def pairs(self):
        mine, other = self.mine, self.other
        for s in self.order:
            self.loads[s].wait()
            self.across[s].wait_recv()

            def add(at, s=s):
                total = mine[s, at, :].astype(F32) + other[s, at, :].astype(F32)
                mine[s, at, :] = total.astype(BF16)

            by_rows(mine.shape[1], add)
            self.spread.ready(s)

    def run(self):
        self.pairs()
        self.spread.settle()

    def total(self, at):
        return self.spread.total(at)

    def finish(self):
        for s in self.order:
            self.across[s].wait_send()
        self.spread.finish()


class Product:
    def __init__(self, plane, value, mine, other, landed, given, send, recv, send2, recv2):
        self.plane, self.value = plane, value
        self.mine, self.other, self.given = mine, other, given
        self.spread = Spread(plane, mine, landed, send2, recv2)
        self.order = self.spread.order
        self.across = {
            s: push(given.at[s], other.at[s], send.at[s], recv.at[s], "ctx", plane.mate)
            for s in self.order
        }

    def start(self):
        plane = self.plane
        for s in self.order:
            block = plane.same(s) + 1 - 2 * plane.core

            def fill(at, s=s, block=block):
                self.given[s, :, at] = self.value(block, at).astype(BF16)

            by_cols(self.mine.shape[2], fill)
            self.across[s].start()

    def run(self, extra=None):
        plane, mine, other = self.plane, self.mine, self.other
        for s in self.order:
            block = plane.same(s)
            self.across[s].wait_recv()

            def fill(at, s=s, block=block):
                total = self.value(block, at) + other[s, :, at].astype(F32)
                mine[s, :, at] = total.astype(BF16)

            by_cols(mine.shape[2], fill)
            self.spread.ready(s)
        self.spread.settle(extra)

    total = Scatter.total
    finish = Scatter.finish


def by_cols(width, body):
    span = 512

    def one(index, carry):
        body(pl.ds(pl.multiple_of(index * span, span), span))
        return carry

    lax.fori_loop(0, width // span, one, 0)


def gather_sems(n):
    return [DMA((12 if n == 8 else n,)), DMA((12 if n == 8 else n,)), DMA(())]


def scatter_scratch(n, rows, width):
    chips = n // 2
    return (
        [pltpu.VMEM((chips, rows, width), BF16)] * 3
        + [DMA((chips,)), DMA((chips,)), DMA((n,)), DMA((n,))]
        + [DMA((chips,))]
    )


def product_scratch(n, rows, width):
    chips = n // 2
    return [pltpu.VMEM((chips, rows, width), BF16)] * 4 + [
        DMA((chips,)),
        DMA((chips,)),
        DMA((n,)),
        DMA((n,)),
    ]


def comm_call(kernel, ident, outs, out_specs, in_specs, scratch, micros, *args):
    return pl.pallas_call(
        kernel,
        out_shape=outs,
        in_specs=in_specs,
        out_specs=out_specs,
        scratch_shapes=scratch,
        compiler_params=pltpu.CompilerParams(
            collective_id=ident, has_side_effects=True, vmem_limit_bytes=VMEM_LIMIT
        ),
        cost_estimate=pl.CostEstimate(
            flops=0, transcendentals=0, bytes_accessed=int(micros * 3.0e6)
        ),
    )(*args)


def swap_all(n, src, out, send, recv, local):
    me = lax.axis_index("ctx")
    own = pltpu.make_async_copy(src.at[me], out.at[me], local)
    own.start()
    copies = []
    for s in range(n - 1, 0, -1):
        peer = flip(me, s, n)
        copies.append(push(src.at[peer], out.at[me], send.at[s], recv.at[s], "ctx", peer))
        copies[-1].start()
    return own, copies


class RowSwap:
    def __init__(self, n, n_dp, src, dst, send, recv, spread):
        self.me = lax.axis_index("ctx")
        self.dst, self.send, self.recv, self.n_dp = dst, send, recv, n_dp
        self.entries = []
        for k in range(n_dp):
            flat = self.me * n_dp + k if spread else k * n + self.me
            peer = flat % n if spread else flat // n_dp
            slot = flat // n if spread else flat % n_dp
            far = push(src.at[k], dst.at[slot], send.at[k], recv.at[slot], "ctx", peer)
            near = pltpu.make_async_copy(src.at[k], dst.at[slot], recv.at[slot])
            self.entries.append((peer, far, near))

    def start(self):
        for peer, far, near in self.entries:
            pl.when(peer != self.me)(far.start)
            pl.when(peer == self.me)(near.start)

    def arrive(self):
        for slot in range(self.n_dp):
            block = self.dst.at[slot]
            pltpu.make_async_copy(block, block, self.recv.at[slot]).wait()

    def finish(self):
        for peer, far, near in self.entries:
            pl.when(peer != self.me)(far.wait_send)


def meet_all(n):
    me = lax.axis_index("ctx")
    meet([("ctx", flip(me, s, n)) for s in range(1, n)])


def prep_kernel(n, n_dp, cols_ref, small_ref, out_ref, all_ref, *sems):
    send, recv, local, gsend, grecv, zsend, zrecv = sems
    me, row = lax.axis_index("ctx"), lax.axis_index("dp")
    meet(
        [("ctx", flip(me, s, n)) for s in range(1, n)]
        + [("dp", flip(row, s, n_dp)) for s in range(1, n_dp)]
    )
    all_ref[row, me] = small_ref[...]
    smalls = []
    for s in range(1, n):
        peer = flip(me, s, n)
        smalls.append(push(small_ref, all_ref.at[row, me], gsend.at[s], grecv.at[s], "ctx", peer))
        smalls[-1].start()
    own, copies = swap_all(n, cols_ref, out_ref, send, recv, local)
    for copy in smalls:
        copy.wait_recv()
    planes = []
    for s in range(1, n_dp):
        peer = flip(row, s, n_dp)
        planes.append(push(all_ref.at[row], all_ref.at[row], zsend.at[s], zrecv.at[s], "dp", peer))
        planes[-1].start()
    for copy in copies + planes:
        copy.wait_recv()
    for copy in copies + planes + smalls:
        copy.wait_send()
    own.wait()


class Gains:
    def __init__(self, n, n_dp, small, landed, mid, second, gsend, grecv, zsend, zrecv):
        self.me, self.row = lax.axis_index("ctx"), lax.axis_index("dp")
        self.small, self.landed, self.mid, self.second = small, landed, mid, second
        self.near, self.far = [], []
        for s in range(1, n):
            peer = flip(self.me, s, n)
            self.near.append(push(small.at[peer], landed.at[s], gsend.at[s], grecv.at[s], "ctx", peer))
        for s in range(1, n_dp):
            peer = flip(self.row, s, n_dp)
            self.far.append(push(mid.at[peer], second.at[s], zsend.at[s], zrecv.at[s], "dp", peer))

    def start(self):
        for copy in self.near:
            copy.start()

    def middle(self):
        value = self.small[self.me]
        for s, copy in enumerate(self.near, 1):
            copy.wait_recv()
            value = value + self.landed[s]
        self.mid[...] = value
        for copy in self.far:
            copy.start()

    def finish(self):
        value = self.mid[self.row]
        for s, copy in enumerate(self.far, 1):
            copy.wait_recv()
            value = value + self.second[s]
        for copy in self.near + self.far:
            copy.wait_send()
        return value


def post_kernel(n, src_ref, query_ref, key_ref, value_ref, blocks, send, recv, local):
    me = lax.axis_index("ctx")
    meet([("ctx", flip(me, s, n)) for s in range(1, n)])
    own, copies = swap_all(n, src_ref, blocks, send, recv, local)
    for copy in copies:
        copy.wait_recv()
    own.wait()
    share = n // KV
    qw = HQ * HD // n
    for c in range(n):
        query_ref[:, c * qw : (c + 1) * qw] = blocks[c, :, :qw].astype(F32)
    for g in range(KV):
        for out, at in ((key_ref, qw), (value_ref, qw + HD)):
            total = blocks[g * share, :, at : at + HD].astype(F32)
            for c in range(1, share):
                total = total + blocks[g * share + c, :, at : at + HD].astype(F32)
            out[:, g * HD : (g + 1) * HD] = total
    for copy in copies:
        copy.wait_send()


def swap_sems(n, n_dp):
    return [DMA((n,)), DMA((n,)), DMA(()), DMA((n,)), DMA((n,)), DMA((n_dp,)), DMA((n_dp,))]


def prep(n, n_dp, cols, small):
    shape = jax.ShapeDtypeStruct
    return comm_call(
        functools.partial(prep_kernel, n, n_dp),
        0,
        [shape(cols.shape, cols.dtype), shape((n_dp, n) + small.shape, F32)],
        [ANY, VM],
        [ANY, VM],
        swap_sems(n, n_dp),
        8,
        cols,
        small,
    )


def post(n, cols):
    shape = jax.ShapeDtypeStruct
    depth = cols.shape[1]
    return comm_call(
        functools.partial(post_kernel, n),
        1,
        [
            shape((depth, HQ * HD), F32),
            shape((depth, KV * HD), F32),
            shape((depth, KV * HD), F32),
        ],
        [VM] * 3,
        [VM],
        [pltpu.VMEM(cols.shape, BF16), DMA((n,)), DMA((n,)), DMA(())],
        10,
        cols,
    )


def first_kernel(
    n, x_ref, gain_ref, info_ref, grad_ref, nall_ref, iall_ref, gall_ref, low, *sems
):
    plane = Plane(n)
    plane.meet()
    infos = Gather(plane, info_ref, iall_ref, *sems[0:3])
    infos.start()

    def norm(at):
        value = x_ref[at, :].astype(F32)
        low[at, :] = (value * rms_parts(value) * gain_ref[...]).astype(BF16)

    by_rows(x_ref.shape[0], norm)
    normed = gather_of(plane, low, nall_ref, *sems[3:6])
    normed.start()
    grads = gather_of(plane, grad_ref, gall_ref, *sems[6:9])
    grads.start()
    infos.forward()
    normed.forward()
    grads.forward()
    infos.finish()
    normed.finish()
    grads.finish()


def first(n, x, gain, info, grad):
    shape = jax.ShapeDtypeStruct
    many = lambda array, kind: shape((n,) + array.shape, kind)
    return comm_call(
        functools.partial(first_kernel, n),
        2,
        [many(x, BF16), many(info, F32), many(grad, BF16)],
        [ANY] * 3,
        [VM] * 4,
        [pltpu.VMEM(x.shape, BF16)]
        + [DMA((n,)), DMA((n,)), DMA(())]
        + gather_sems(n)
        + gather_sems(n),
        90,
        x,
        gain,
        info,
        grad,
    )


def middle_kernel(
    n, attn_ref, wout_ref, x_ref, gain_ref, after_ref, all_ref, low, *scratch
):
    plane = Plane(n)
    plane.meet()
    rows = x_ref.shape[0]

    def value(block, at):
        left = attn_ref[pl.ds(pl.multiple_of(block * rows, rows), rows), :]
        return dot(left, wout_ref[:, at])

    sums = Product(plane, value, *scratch[:8])
    sums.start()
    sums.run()

    def norm(at):
        value = x_ref[at, :].astype(F32) + sums.total(at)
        after_ref[at, :] = value
        low[at, :] = (value * rms_parts(value) * gain_ref[...]).astype(BF16)

    by_rows(rows, norm)
    normed = gather_of(plane, low, all_ref, *scratch[8:])
    normed.start()
    normed.forward()
    sums.finish()
    normed.finish()


def middle(n, attn, wout, x, gain):
    shape = jax.ShapeDtypeStruct
    return comm_call(
        functools.partial(middle_kernel, n),
        3,
        [shape(x.shape, F32), shape((n,) + x.shape, BF16)],
        [VM, ANY],
        [VM, VM, VM, VM],
        [pltpu.VMEM(x.shape, BF16)]
        + product_scratch(n, *x.shape)
        + gather_sems(n),
        105,
        attn,
        wout,
        x,
        gain,
    )


def turn_kernel(
    n, part_ref, after_ref, grad_ref, gain_ref, mid_ref, fpart_ref, all_ref, low, *scratch
):
    plane = Plane(n)
    plane.meet()
    sums = Scatter(plane, part_ref, *scratch[:8])
    sums.start()
    fpart_ref[...] = jnp.zeros_like(fpart_ref)
    sums.run()

    def norm(at):
        value = after_ref[at, :]
        inv = rms_parts(value)
        unit = value * inv
        grad = sums.total(at)
        fpart_ref[0:1, :] += jnp.sum(grad * unit, axis=0, keepdims=True)
        mid = grad_ref[at, :].astype(F32) + rms_back(grad, unit, inv, gain_ref[...])
        mid_ref[at, :] = mid
        low[at, :] = mid.astype(BF16)

    by_rows(after_ref.shape[0], norm)
    branch = gather_of(plane, low, all_ref, *scratch[8:])
    branch.start()
    branch.forward()
    sums.finish()
    branch.finish()


def turn(n, part, after, grad, gain):
    shape = jax.ShapeDtypeStruct
    return comm_call(
        functools.partial(turn_kernel, n),
        4,
        [
            shape(after.shape, F32),
            shape((8, after.shape[1]), F32),
            shape((n,) + after.shape, BF16),
        ],
        [VM, VM, ANY],
        [ANY, VM, VM, VM],
        [pltpu.VMEM(after.shape, BF16)] + scatter_scratch(n, *after.shape) + gather_sems(n),
        95,
        part,
        after,
        grad,
        gain,
    )


def last_kernel(n, grad_ref, wqkv_ref, x_ref, mid_ref, gain_ref, out_ref, apart_ref, *scratch):
    plane = Plane(n)
    plane.meet()
    apart_ref[...] = jnp.zeros_like(apart_ref)
    rows = x_ref.shape[0]

    def value(block, at):
        left = grad_ref[pl.ds(pl.multiple_of(block * rows, rows), rows), :]
        return dot(left, wqkv_ref[at, :], NT)

    sums = Product(plane, value, *scratch[:8])
    sums.start()
    sums.run()

    def norm(at):
        value = x_ref[at, :].astype(F32)
        inv = rms_parts(value)
        unit = value * inv
        grad = sums.total(at)
        apart_ref[0:1, :] += jnp.sum(grad * unit, axis=0, keepdims=True)
        out_ref[at, :] = mid_ref[at, :] + rms_back(grad, unit, inv, gain_ref[...])

    by_rows(rows, norm)
    sums.finish()


def last(n, grad, wqkv, x, mid, gain):
    shape = jax.ShapeDtypeStruct
    return comm_call(
        functools.partial(last_kernel, n),
        5,
        [shape(mid.shape, F32), shape((8, mid.shape[1]), F32)],
        [VM, VM],
        [VM] * 5,
        product_scratch(n, *mid.shape),
        60,
        grad,
        wqkv,
        x,
        mid,
        gain,
    )


def gains_kernel(n, n_dp, small_ref, sum_ref, *scratch):
    meet(
        [("ctx", flip(lax.axis_index("ctx"), s, n)) for s in range(1, n)]
        + [("dp", flip(lax.axis_index("dp"), s, n_dp)) for s in range(1, n_dp)]
    )
    gains = Gains(n, n_dp, small_ref, *scratch)
    gains.start()
    gains.middle()
    sum_ref[...] = gains.finish()


def gains_sum(n, n_dp, small):
    tile = small.shape[2:]
    return comm_call(
        functools.partial(gains_kernel, n, n_dp),
        8,
        jax.ShapeDtypeStruct(tile, F32),
        VM,
        [VM],
        [
            pltpu.VMEM((n, n_dp) + tile, F32),
            pltpu.VMEM((n_dp,) + tile, F32),
            pltpu.VMEM((n_dp,) + tile, F32),
            DMA((n,)),
            DMA((n,)),
            DMA((n_dp,)),
            DMA((n_dp,)),
        ],
        10,
        small,
    )


def attn_forward_kernel(
    n,
    n_dp,
    heads,
    back,
    normed_ref,
    wqkv_ref,
    cos_ref,
    sin_ref,
    qgain_ref,
    kgain_ref,
    docc_ref,
    docr_ref,
    rows_ref,
    qlin_ref,
    klin_ref,
    q_ref,
    k_ref,
    v_ref,
    attn_ref,
    total_ref,
    wout_ref,
    acc_ref,
    sum_ref,
    *sems,
):
    step = pl.program_id(0)

    @pl.when(step == 0)
    def _():
        meet_all(n)
        RowSwap(n, n_dp, rows_ref, wout_ref, *sems, False).start()

    rows = normed_ref.shape[0]
    lin = dot(normed_ref[...], wqkv_ref[...])
    here = pl.ds(step * rows, rows)
    cosine = cos_ref[...]
    sine = sin_ref[...]
    qw = heads * HD
    for head in range(heads):
        cols = slice(head * HD, (head + 1) * HD)
        part = lin[:, cols]
        qlin_ref[:, cols] = part
        q_ref[:, cols] = head_forward(part, qgain_ref[...], cosine, sine).astype(BF16)
    key_lin = lin[:, qw : qw + HD]
    klin_ref[...] = key_lin
    k_ref[here, :] = head_forward(key_lin, kgain_ref[...], cosine, sine).astype(BF16)
    v_ref[here, :] = lin[:, qw + HD :].astype(BF16)
    acc_ref[...] = jnp.zeros_like(acc_ref)
    sum_ref[...] = jnp.zeros_like(sum_ref)
    row_pos = step * rows + lax.broadcasted_iota(jnp.int32, (rows, rows), 0)
    col_off = lax.broadcasted_iota(jnp.int32, (rows, rows), 1)

    def one(block, carry):
        at = pl.ds(pl.multiple_of(block * rows, rows), rows)
        key = k_ref[at, :]
        val = v_ref[at, :]
        allowed = (docc_ref[...] == docr_ref[:, at]) & (block * rows + col_off <= row_pos)
        for head in range(heads):
            cols = slice(head * HD, (head + 1) * HD)
            score = dot(q_ref[:, cols], key, NT) * SCALE2
            expo = jnp.where(allowed, jnp.exp2(score), 0.0)
            folded = expo[:, :HD]
            for piece in range(1, rows // HD):
                folded = folded + expo[:, piece * HD : (piece + 1) * HD]
            sum_ref[:, cols] += folded
            acc_ref[:, cols] += dot(expo.astype(BF16), val)
        return carry

    lax.fori_loop(jnp.maximum(step - back, 0), step + 1, one, 0)
    lane = lax.broadcasted_iota(jnp.int32, (rows, HD), 1)
    totals = jnp.ones((rows, HD), F32)
    for head in range(heads):
        cols = slice(head * HD, (head + 1) * HD)
        total = jnp.sum(sum_ref[:, cols], axis=-1, keepdims=True)
        totals = jnp.where(lane == head, total, totals)
        attn_ref[:, cols] = (acc_ref[:, cols] / total).astype(BF16)
    total_ref[...] = totals

    @pl.when(step == pl.num_programs(0) - 1)
    def _():
        swap = RowSwap(n, n_dp, rows_ref, wout_ref, *sems, False)
        swap.arrive()
        swap.finish()


def attn_forward(n, n_dp, normed, wqkv, cosine, sine, qgain, kgain, doc, wrows, rows):
    length, width = normed.shape
    qw = wqkv.shape[1] - 2 * HD
    heads = qw // HD
    blk = lambda cols: pl.BlockSpec((rows, cols), lambda i: (i, 0))
    whole = lambda shape: pl.BlockSpec(shape, lambda i: (0, 0))
    shape = jax.ShapeDtypeStruct
    return pl.pallas_call(
        functools.partial(attn_forward_kernel, n, n_dp, heads, MOST // rows),
        grid=(length // rows,),
        in_specs=[
            blk(width),
            whole(wqkv.shape),
            blk(HD),
            blk(HD),
            whole((1, HD)),
            whole((1, HD)),
            blk(1),
            whole((1, length)),
            ANY,
        ],
        out_specs=[
            blk(qw),
            blk(HD),
            blk(qw),
            whole((length, HD)),
            whole((length, HD)),
            blk(qw),
            blk(HD),
            ANY,
        ],
        out_shape=[
            shape((length, qw), F32),
            shape((length, HD), F32),
            shape((length, qw), BF16),
            shape((length, HD), BF16),
            shape((length, HD), BF16),
            shape((length, qw), BF16),
            shape((length, HD), F32),
            shape(wrows.shape, BF16),
        ],
        scratch_shapes=[pltpu.VMEM((rows, qw), F32), pltpu.VMEM((rows, qw), F32)]
        + [DMA((n_dp,)), DMA((n_dp,))],
        compiler_params=pltpu.CompilerParams(
            collective_id=7, has_side_effects=True, vmem_limit_bytes=VMEM_LIMIT
        ),
        cost_estimate=pl.CostEstimate(
            flops=35 * 10**9, transcendentals=0, bytes_accessed=30 * 2**20
        ),
        name="attn_forward",
    )(normed, wqkv, cosine, sine, qgain, kgain, doc[:, None], doc[None, :], wrows)


def attn_backward_kernel(
    n,
    n_dp,
    heads,
    back,
    branch_ref,
    wout_ref,
    attn_ref,
    total_ref,
    q_ref,
    k_ref,
    v_ref,
    qlin_ref,
    klin_ref,
    cos_ref,
    sin_ref,
    qgain_ref,
    kgain_ref,
    docc_ref,
    docr_ref,
    wgrad_ref,
    moe_ref,
    after_ref,
    dqkv_ref,
    gains_ref,
    swapped_ref,
    final_ref,
    dk_ref,
    dv_ref,
    dqa_ref,
    *sems,
):
    step = pl.program_id(0)

    steps = pl.num_programs(0)

    def scatter():
        return Scatter(Plane(n), moe_ref, *sems[2:])

    @pl.when(step == 0)
    def _():
        meet_all(n)
        scatter().start()
        RowSwap(n, n_dp, wgrad_ref, swapped_ref, *sems[:2], True).start()

    @pl.when(step == 2)
    def _():
        scatter().pairs()

    @pl.when(step == steps - 2)
    def _():
        scatter().spread.relay()

    rows = branch_ref.shape[0]
    here = pl.ds(pl.multiple_of(step * rows, rows), rows)

    @pl.when(step == 0)
    def _():
        gains_ref[...] = jnp.zeros_like(gains_ref)

    dk_ref[here, :] = jnp.zeros((rows, HD), F32)
    dv_ref[here, :] = jnp.zeros((rows, HD), F32)
    dqa_ref[...] = jnp.zeros_like(dqa_ref)
    attn_grad = dot(branch_ref[...], wout_ref[...], NT)
    grads = []
    shifts = []
    for head in range(heads):
        cols = slice(head * HD, (head + 1) * HD)
        part = attn_grad[:, cols]
        inv_total = 1.0 / total_ref[:, head : head + 1]
        delta = jnp.sum(part * attn_ref[:, cols].astype(F32), axis=-1, keepdims=True)
        grads.append((part * inv_total).astype(BF16))
        shifts.append(delta * inv_total)
    row_pos = step * rows + lax.broadcasted_iota(jnp.int32, (rows, rows), 0)
    col_off = lax.broadcasted_iota(jnp.int32, (rows, rows), 1)

    def one(block, carry):
        at = pl.ds(pl.multiple_of(block * rows, rows), rows)
        key = k_ref[at, :]
        val = v_ref[at, :]
        allowed = (docc_ref[...] == docr_ref[:, at]) & (block * rows + col_off <= row_pos)
        dk = jnp.zeros((rows, HD), F32)
        dv = jnp.zeros((rows, HD), F32)
        for head in range(heads):
            cols = slice(head * HD, (head + 1) * HD)
            query = q_ref[:, cols]
            score = dot(query, key, NT) * SCALE2
            expo = jnp.where(allowed, jnp.exp2(score), 0.0)
            prod = dot(grads[head], val, NT)
            score_grad = (expo * (prod - shifts[head])).astype(BF16)
            dv += dot(expo.astype(BF16), grads[head], TN)
            dk += dot(score_grad, query, TN)
            dqa_ref[:, cols] += dot(score_grad, key)
        dk_ref[at, :] += dk
        dv_ref[at, :] += dv
        return carry

    lax.fori_loop(jnp.maximum(step - back, 0), step + 1, one, 0)
    cosine = cos_ref[here, :]
    sine = sin_ref[here, :]
    for head in range(heads):
        cols = slice(head * HD, (head + 1) * HD)
        grad, gain_part = head_backward(
            qlin_ref[:, cols], qgain_ref[...], cosine, sine, dqa_ref[:, cols] * SCALE
        )
        dqkv_ref[here, cols] = grad.astype(BF16)
        gains_ref[0:1, :] += gain_part

    @pl.when(step == pl.num_programs(0) - 1)
    def _():
        def finish(block, carry):
            at = pl.ds(pl.multiple_of(block * rows, rows), rows)
            grad, gain_part = head_backward(
                klin_ref[at, :], kgain_ref[...], cos_ref[at, :], sin_ref[at, :], dk_ref[at, :] * SCALE
            )
            qw = heads * HD
            dqkv_ref[at, qw : qw + HD] = grad.astype(BF16)
            dqkv_ref[at, qw + HD :] = dv_ref[at, :].astype(BF16)
            gains_ref[1:2, :] += gain_part
            return carry

        lax.fori_loop(0, pl.num_programs(0), finish, 0)
        sums = scatter()
        sums.spread.gathered()

        def add(at):
            final_ref[at, :] = (after_ref[at, :] + sums.total(at)).astype(BF16)

        by_rows(rows, add)
        sums.finish()
        swap = RowSwap(n, n_dp, wgrad_ref, swapped_ref, *sems[:2], True)
        swap.arrive()
        swap.finish()


def attn_backward(n, n_dp, wgrad, moe, after, branch, wout, attn, total, q, k, v, qlin, klin, cosine, sine, qgain, kgain, doc, rows):
    length, width = branch.shape
    qw = wout.shape[0]
    heads = qw // HD
    blk = lambda cols: pl.BlockSpec((rows, cols), lambda i: (i, 0))
    whole = lambda shape: pl.BlockSpec(shape, lambda i: (0, 0), pipeline_mode=pl.Buffered(1))
    shape = jax.ShapeDtypeStruct
    full = whole((length, HD))
    return pl.pallas_call(
        functools.partial(attn_backward_kernel, n, n_dp, heads, MOST // rows),
        grid=(length // rows,),
        in_specs=[
            blk(width),
            whole(wout.shape),
            blk(qw),
            blk(HD),
            blk(qw),
            full,
            full,
            blk(qw),
            full,
            full,
            full,
            whole((1, HD)),
            whole((1, HD)),
            blk(1),
            whole((1, length)),
            ANY,
            ANY,
            whole(after.shape),
        ],
        out_specs=[whole((length, qw + 2 * HD)), whole((8, HD)), ANY, whole(after.shape)],
        out_shape=[
            shape((length, qw + 2 * HD), BF16),
            shape((8, HD), F32),
            shape(wgrad.shape, BF16),
            shape(after.shape, BF16),
        ],
        scratch_shapes=[
            pltpu.VMEM((length, HD), F32),
            pltpu.VMEM((length, HD), F32),
            pltpu.VMEM((rows, qw), F32),
            DMA((n_dp,)),
            DMA((n_dp,)),
        ]
        + scatter_scratch(n, *after.shape),
        compiler_params=pltpu.CompilerParams(
            collective_id=9, has_side_effects=True, vmem_limit_bytes=VMEM_LIMIT
        ),
        cost_estimate=pl.CostEstimate(
            flops=60 * 10**9, transcendentals=0, bytes_accessed=30 * 2**20
        ),
        name="attn_backward",
    )(branch, wout, attn, total, q, k, v, qlin, klin, cosine, sine, qgain, kgain, doc[:, None], doc[None, :], wgrad, moe, after)


def expert_kernel(chained, low, aliased, plan, z_ref, n2_ref, top_ref, prob_ref, *rest):
    if aliased:
        rest = rest[1:]
    if chained:
        moe_in, row_in = rest[:2]
        rest = rest[2:]
    sources, rest = rest[: len(plan)], rest[len(plan) :]
    moe_ref, row_ref, grads_ref, wg_ref, wu_ref, wd_ref = rest[:6]
    ag_ref, au_ref, ad_ref, stage, wsem, sem = rest[6:]
    step = pl.program_id(0)
    rows, width = n2_ref.shape
    parts, cut, hidden = wd_ref.shape
    weights = (wg_ref, wu_ref, wd_ref)

    @pl.when(step == 0)
    def _():
        z = z_ref[0]
        for source, (kind, amount, start) in zip(sources, plan):
            count = source.shape[-2] // cut
            for k in range(parts) if kind == "all" else [amount]:
                if kind == "all":
                    src, owner, wanted = source.at[k], k, None
                elif kind == "up":
                    src, owner, wanted = source, z - k, z >= k
                else:
                    src, owner, wanted = source, z + k, z + k < parts

                def load(src=src, owner=owner, start=start, count=count):
                    for piece in range(count):
                        pltpu.make_async_copy(
                            src.at[pl.ds(piece * cut, cut), :],
                            weights[start + piece].at[owner],
                            wsem.at[start + piece, owner],
                        ).start()

                if wanted is None:
                    load()
                else:
                    pl.when(wanted)(load)
        ag_ref[...] = jnp.zeros_like(ag_ref)
        au_ref[...] = jnp.zeros_like(au_ref)
        ad_ref[...] = jnp.zeros_like(ad_ref)
        for index in range(3):
            for owner in range(parts):
                block = weights[index].at[owner]
                pltpu.make_async_copy(block, block, wsem.at[index, owner]).wait()

    n2 = n2_ref[...]
    prob = prob_ref[...]
    wg = wg_ref[...].reshape(width, hidden)
    wu = wu_ref[...].reshape(width, hidden)
    gate = dot(n2, wg)
    up = dot(n2, wu)
    sig = 1.0 / (1.0 + jnp.exp(-gate))
    silu = gate * sig
    act = (silu * up).astype(BF16)
    act_grad = jnp.zeros((rows, hidden), F32)
    for z in range(parts):
        cols = slice(z * cut, (z + 1) * cut)
        out = dot(act, wd_ref[z], NT).astype(BF16).astype(F32) * prob
        if chained:
            out = out + moe_in[:, cols].astype(F32)
        moe_ref[:, cols] = out.astype(BF16)
        route = (top_ref[:, cols].astype(F32) * prob).astype(BF16)
        act_grad += dot(route, wd_ref[z])
        ad_ref[z] += dot(route, act, TN)
    gate_grad = (act_grad * up * sig * (1.0 + gate * (1.0 - sig))).astype(BF16)
    up_grad = (act_grad * silu).astype(BF16)
    row = dot(gate_grad, wg, NT) + dot(up_grad, wu, NT)
    if chained:
        row = row + row_in[...].astype(F32)
    row_ref[...] = row.astype(BF16)
    ag_ref[...] += dot(n2, gate_grad, TN).reshape(parts, cut, hidden)
    au_ref[...] += dot(n2, up_grad, TN).reshape(parts, cut, hidden)

    @pl.when(step == pl.num_programs(0) - 1)
    def _():
        copies = []
        pieces = [
            (acc, place, z) for z in range(parts) for place, acc in enumerate((ag_ref, au_ref, ad_ref))
        ]
        for index, (acc, place, z) in enumerate(pieces):
            slot = index % 2
            if index >= 2:
                copies[index - 2].wait()
            stage[slot] = acc[z].astype(BF16)
            copies.append(
                pltpu.make_async_copy(
                    stage.at[slot],
                    grads_ref.at[z, pl.ds(place * cut, cut), pl.ds(low, acc.shape[2])],
                    sem.at[slot],
                )
            )
            copies[-1].start()
        copies[-2].wait()
        copies[-1].wait()


def expert(z, n2, top, prob, n_dp, sources, before, rows, low, full, grads):
    length, width = n2.shape
    cut = width // n_dp
    hidden = sources[0][0].shape[-1]
    blk = pl.BlockSpec((rows, width), lambda i: (i, 0))
    col = pl.BlockSpec((rows, 1), lambda i: (i, 0))
    shape = jax.ShapeDtypeStruct
    plan = tuple(entry[1:] for entry in sources)
    weight = pltpu.VMEM((n_dp, cut, hidden), BF16)
    total = pltpu.VMEM((n_dp, cut, hidden), F32)
    return pl.pallas_call(
        functools.partial(expert_kernel, len(before) > 0, low, len(grads) > 0, plan),
        grid=(length // rows,),
        in_specs=[pl.BlockSpec(memory_space=pltpu.SMEM), blk, blk, col]
        + [ANY] * len(grads)
        + [blk] * len(before)
        + [ANY] * len(sources),
        out_specs=[blk, blk, ANY],
        out_shape=[
            shape((length, width), BF16),
            shape((length, width), BF16),
            shape((n_dp, 3 * cut, full), BF16),
        ],
        input_output_aliases={4: 2} if grads else {},
        scratch_shapes=[weight] * 3
        + [total] * 3
        + [pltpu.VMEM((2, cut, hidden), BF16), DMA((3, n_dp)), DMA((2,))],
        compiler_params=pltpu.CompilerParams(vmem_limit_bytes=VMEM_LIMIT),
        cost_estimate=pl.CostEstimate(
            flops=18 * length * width * hidden,
            transcendentals=length * hidden,
            bytes_accessed=5 * length * width * 2,
        ),
        name="expert",
    )(z, n2, top, prob, *grads, *before, *[entry[0] for entry in sources])


def pack_kernel(cuts, gate_ref, up_ref, down_ref, *outs):
    cut = gate_ref.shape[0]
    for (low, high), out in zip(cuts, outs):
        out[:cut, :] = gate_ref[:, low:high]
        out[cut : 2 * cut, :] = up_ref[:, low:high]
        out[2 * cut :, :] = jnp.transpose(down_ref[low:high, :].astype(F32)).astype(BF16)


def pack(cuts, w_gate, w_up, w_down):
    cut = w_gate.shape[0]
    return pl.pallas_call(
        functools.partial(pack_kernel, cuts),
        in_specs=[VM] * 3,
        out_specs=[VM] * len(cuts),
        out_shape=[jax.ShapeDtypeStruct((3 * cut, high - low), BF16) for low, high in cuts],
        name="pack",
    )(w_gate, w_up, w_down)


def unpack_kernel(
    z_ref, one_ref, all_ref, up0_ref, down0_ref, up1_ref, down1_ref, dg_ref, du_ref, dd_ref, own, sem
):
    copy = pltpu.make_async_copy(all_ref.at[z_ref[0]], own, sem)
    copy.start()
    cut = dg_ref.shape[1]
    half = up0_ref.shape[0]
    piece = [slice(k * cut, (k + 1) * cut) for k in range(3)]
    dg_ref[1] = one_ref[piece[0], :].astype(F32)
    du_ref[1] = one_ref[piece[1], :].astype(F32)
    dd_ref[1] = jnp.transpose(one_ref[piece[2], :].astype(F32))
    copy.wait()

    def total(low, high):
        shift, up, down = (0, up0_ref, down0_ref) if high <= half else (half, up1_ref, down1_ref)
        there = slice(low - shift, high - shift)
        value = own[low:high, :].astype(F32)
        return value + up[there, :].astype(F32) + down[there, :].astype(F32)

    dg_ref[0] = total(0, cut)
    du_ref[0, : half - cut] = total(cut, half)
    du_ref[0, half - cut :] = total(half, 2 * cut)
    dd_ref[0] = jnp.transpose(total(2 * cut, 3 * cut))


def unpack(z, one, grads, got):
    rows, hidden = one.shape
    cut = rows // 3
    shape = jax.ShapeDtypeStruct
    return pl.pallas_call(
        unpack_kernel,
        in_specs=[pl.BlockSpec(memory_space=pltpu.SMEM), VM, ANY, VM, VM, VM, VM],
        out_specs=[VM] * 3,
        out_shape=[
            shape((2, cut, hidden), F32),
            shape((2, cut, hidden), F32),
            shape((2, hidden, cut), F32),
        ],
        scratch_shapes=[pltpu.VMEM((rows, hidden), BF16), DMA(())],
        compiler_params=pltpu.CompilerParams(vmem_limit_bytes=VMEM_LIMIT),
        name="unpack",
    )(z, one, grads, *got)


def line_hop(block_up, block_down, n_dp, hop):
    up = [(i, i + 1) for i in range(hop - 1, n_dp - 1)]
    down = [(i + 1, i) for i in range(n_dp - hop)]
    return lax.ppermute(block_up, "dp", up), lax.ppermute(block_down, "dp", down)


def reduce_hop(grads, got, n_dp, hop, rows, before):
    place = lax.axis_index("dp")
    reach = n_dp - hop
    zero = jnp.int32(0)
    size = (1, rows[1] - rows[0], grads.shape[2])
    spots = (jnp.minimum(place + reach, n_dp - 1), jnp.maximum(place - reach, 0))
    if got is not None:
        got = lax.optimization_barrier((*got, *before))[:2]
    elif before:
        grads = after_of(grads, *before)
    blocks = [
        lax.dynamic_slice(grads, (spot.astype(jnp.int32), jnp.int32(rows[0]), zero), size)[0]
        for spot in spots
    ]
    if got is not None:
        blocks = [(b.astype(F32) + g.astype(F32)).astype(BF16) for b, g in zip(blocks, got)]
    up = [(i, i + 1) for i in range(hop)]
    down = [(i, i - 1) for i in range(n_dp - hop, n_dp)]
    sent = lax.ppermute(blocks[0], "dp", up), lax.ppermute(blocks[1], "dp", down)
    return sent, tuple(blocks)


def after_of(value, *others):
    return lax.optimization_barrier((value,) + others)[0]


def per_device(
    layer_input,
    doc_ids,
    route_ids,
    route_probs,
    attn_gain,
    ffn_gain,
    query_gain,
    key_gain,
    w_query,
    w_key,
    w_value,
    w_out,
    w_gate,
    w_up,
    w_down,
    out_grad,
):
    tokens, width = layer_input.shape[1:]
    n_dp = lax.axis_size("dp")
    n_ctx = lax.axis_size("ctx")
    ctx_index = lax.axis_index("ctx")
    length = tokens * n_ctx
    heads = HQ // n_ctx
    share = n_ctx // KV
    qw = heads * HD
    depth = w_query.shape[0]
    own_e = w_gate.shape[0]

    cut = attn_gain.shape[0]
    hcut = query_gain.shape[0]
    kinds = 2 * (cut + hcut)
    small = jnp.concatenate([attn_gain, ffn_gain, query_gain, key_gain]).astype(F32)
    small = jnp.pad(small, (0, 1024 - kinds)).reshape(8, HD)
    cols = jnp.concatenate(
        [
            w_query.reshape(depth, n_ctx, qw),
            jnp.repeat(w_key.reshape(depth, KV, HD), share, axis=1),
            jnp.repeat(w_value.reshape(depth, KV, HD), share, axis=1),
        ],
        axis=2,
    ).transpose(1, 0, 2)
    cols, small = prep(n_ctx, n_dp, cols, small)
    small = small.reshape(n_dp * n_ctx, 1024)
    gain_attn = small[:, :cut].reshape(1, width)
    gain_ffn = small[:, cut : 2 * cut].reshape(1, width)
    gain_query = small[:, 2 * cut : 2 * cut + hcut].reshape(1, HD)
    gain_key = small[:, 2 * cut + hcut : kinds].reshape(1, HD)
    wqkv = lax.all_gather(cols.reshape(n_ctx * depth, qw + 2 * HD), "dp", axis=0, tiled=True)
    wrows = lax.all_gather(w_out, "dp", axis=0, tiled=False)

    inputs = layer_input.reshape(tokens, width)
    top_own = out_grad.reshape(tokens, width)
    n_experts = own_e * n_ctx
    match = route_ids.reshape(1, tokens, TOP) == jnp.arange(n_experts, dtype=jnp.int32)[:, None, None]
    probs = jnp.sum(jnp.where(match, route_probs.reshape(1, tokens, TOP), 0.0), axis=2)
    info = jnp.concatenate(
        [probs, doc_ids.reshape(1, tokens).astype(F32), jnp.zeros((7, tokens), F32)], axis=0
    )
    normed, info, top_all = first(n_ctx, inputs, gain_attn, info, top_own)
    normed = normed.reshape(length, width)
    doc = info[:, n_experts].reshape(length).astype(jnp.int32)
    my_probs = lax.dynamic_slice_in_dim(info, ctx_index * own_e, own_e, 1)
    my_probs = my_probs.transpose(0, 2, 1).reshape(length, own_e)

    inverse = 1.0 / ROPE_BASE ** (jnp.arange(HD // 2, dtype=F32) * 2.0 / HD)
    angles = jnp.arange(length, dtype=F32)[:, None] * inverse[None, :]
    cosine = jnp.cos(angles)
    sine = jnp.sin(angles)
    cosine = jnp.concatenate([cosine, cosine], axis=1)
    sine = jnp.concatenate([-sine, sine], axis=1)
    qlin, klin, q, k, v, attn, total, wout = attn_forward(
        n_ctx, n_dp, normed, wqkv, cosine, sine, gain_query, gain_key, doc, wrows, tokens
    )
    wout = wout.reshape(qw, width)
    top_all = top_all.reshape(length, width)
    blocks = (n_ctx, tokens, width)
    after, normed2 = middle(n_ctx, attn, wout, inputs, gain_ffn)
    normed2 = normed2.reshape(length, width)

    z = lax.axis_index("dp").astype(jnp.int32).reshape(1)
    hidden = w_gate.shape[2]

    def run(e, sources, carried, low, grads):
        moe, rows_grad, grads = expert(
            z,
            normed2,
            top_all,
            my_probs[:, e : e + 1],
            n_dp,
            sources,
            carried,
            tokens,
            low,
            hidden,
            grads,
        )
        return (moe, rows_grad), grads

    cuts = [(0, 256), (256, hidden)]
    blocks0 = pack(cuts, w_gate[0], w_up[0], w_down[0])
    carried, grads0 = (), ()
    for index, (low, high) in enumerate(cuts):
        full = lax.all_gather(blocks0[index], "dp", axis=0, tiled=False)
        if index == 1:
            (block1,) = pack([(0, hidden)], w_gate[1], w_up[1], w_down[1])
            sources1 = [(block1, "up", 0, 0)]
            up = down = after_of(block1, full)
            up, down = line_hop(up, down, n_dp, 1)
            sources1 += [(up, "up", 1, 0), (down, "down", 1, 0)]
        carried, grads = run(0, [(full, "all", 0, 0)], carried, low, grads0)
        grads0 = (grads,)
    rows_all = 3 * (width // n_dp)
    spans = {"a": (0, rows_all // 2), "b": (rows_all // 2, rows_all)}
    got, before = {tag: None for tag in spans}, ()
    for hop in range(2, n_dp + 1):
        if hop < n_dp:
            up, down = line_hop(up, down, n_dp, hop)
            sources1 += [(up, "up", hop, 0), (down, "down", hop, 0)]
        for tag, rows in spans.items():
            got[tag], before = reduce_hop(grads, got[tag], n_dp, hop - 1, rows, before)
    (moe, rows_grad), grads1 = run(1, sources1, carried, 0, ())
    done1 = lax.psum_scatter(
        grads1.reshape(3 * width, hidden), "dp", scatter_dimension=0, tiled=True
    )
    mid, ffn_part, branch = turn(
        n_ctx, rows_grad.reshape(blocks), after, top_own, gain_ffn
    )
    branch = branch.reshape(length, width)

    out_w = dot(attn, branch, TN).astype(BF16).reshape(n_dp, qw // n_dp, width)
    dqkv, gains, out_w, layer_output = attn_backward(
        n_ctx,
        n_dp,
        out_w,
        moe.reshape(blocks),
        after,
        branch,
        wout,
        attn,
        total,
        q,
        k,
        v,
        qlin,
        klin,
        cosine,
        sine,
        gain_query,
        gain_key,
        doc,
        tokens,
    )
    qkv_w = dot(normed, dqkv, TN).astype(BF16)
    qkv_w = lax.psum_scatter(qkv_w, "dp", scatter_dimension=0, tiled=True)
    out_w = lax.psum_scatter(out_w.reshape(qw, width), "dp", scatter_dimension=0, tiled=True)
    out_w = out_w.astype(F32)
    input_grad, attn_part = last(n_ctx, dqkv, wqkv, inputs, mid, gain_attn)
    n_all = n_dp * n_ctx
    packed = jnp.concatenate(
        [
            attn_part[0].reshape(n_all, cut),
            ffn_part[0].reshape(n_all, cut),
            gains[0].reshape(n_all, hcut),
            gains[1].reshape(n_all, hcut),
            jnp.zeros((n_all, 1024 - kinds), F32),
        ],
        axis=1,
    )
    packed = packed.reshape(n_dp, n_ctx, 8, HD).transpose(1, 0, 2, 3)
    packed = gains_sum(n_ctx, n_dp, packed)
    packed = packed.reshape(1024)
    query_w, key_w, value_w = post(n_ctx, qkv_w.reshape(n_ctx, depth, qw + 2 * HD))
    gate_w, up_w, down_w = unpack(z, done1, grads, got["a"] + got["b"])
    return (
        layer_output.reshape(1, tokens, width),
        input_grad.reshape(1, tokens, width),
        packed[:cut],
        packed[cut : 2 * cut],
        packed[2 * cut : 2 * cut + hcut],
        packed[2 * cut + hcut : kinds],
        query_w,
        key_w,
        value_w,
        out_w,
        gate_w,
        up_w,
        down_w,
    )


def solution(mesh):
    both = ("dp", "ctx")
    seq = P("dp", "ctx", None)
    in_specs = (
        seq,
        P("dp", "ctx"),
        seq,
        seq,
        P(both),
        P(both),
        P(both),
        P(both),
        P(both, None),
        P(both, None),
        P(both, None),
        P(both, None),
        P("ctx", "dp", None),
        P("ctx", "dp", None),
        P("ctx", None, "dp"),
        seq,
    )
    out_specs = (
        seq,
        seq,
        P(both),
        P(both),
        P(both),
        P(both),
        P(both, None),
        P(both, None),
        P(both, None),
        P(both, None),
        P("ctx", "dp", None),
        P("ctx", "dp", None),
        P("ctx", None, "dp"),
    )

    return jax.shard_map(
        per_device, mesh=mesh, in_specs=in_specs, out_specs=out_specs, check_vma=False
    )
```

```python
import functools
import math

import jax
import jax.numpy as jnp
from jax import lax
from jax.experimental import pallas as pl
from jax.experimental.pallas import tpu as pltpu
from jax.sharding import PartitionSpec as P


HQ = 32
KV = 4
HD = 128
TOP = 8
MOST = 1024
EPS = 1e-06
ROPE_BASE = 1000000.0
F32 = jnp.float32
BF16 = jnp.bfloat16
SCALE = 1.0 / math.sqrt(HD)
SCALE2 = SCALE / math.log(2.0)
VMEM_LIMIT = 60 * 1024 * 1024


def dot(left, right, dims=((1,), (0,))):
    return lax.dot_general(left, right, (dims, ((), ())), preferred_element_type=F32)


NT = ((1,), (1,))
TN = ((0,), (0,))


def rms_parts(values):
    return lax.rsqrt(jnp.mean(values * values, axis=-1, keepdims=True) + EPS)


def rms_back(grad, unit, inv, gain):
    scaled = grad * gain
    return inv * (scaled - unit * jnp.mean(scaled * unit, axis=-1, keepdims=True))


def head_forward(lin, gain, cosine, sine):
    unit = lin * rms_parts(lin) * gain
    return unit * cosine + pltpu.roll(unit, HD // 2, 1) * sine


def head_backward(lin, gain, cosine, sine, rot_grad):
    grad = rot_grad * cosine + pltpu.roll(rot_grad * sine, HD // 2, 1)
    inv = rms_parts(lin)
    unit = lin * inv
    return rms_back(grad, unit, inv, gain), jnp.sum(grad * unit, axis=0, keepdims=True)


MESH = pl.DeviceIdType.MESH
ANY = pl.BlockSpec(memory_space=pl.ANY)
VM = pl.BlockSpec(memory_space=pltpu.VMEM)
DMA = pltpu.SemaphoreType.DMA
CHUNK = 32


def flip(index, mask, count):
    result, bit = 0, 1
    while bit < count:
        digit = (index // bit) % 2
        result = result + bit * ((1 - digit) if mask & bit else digit)
        bit *= 2
    return result


def push(src, dst, send, recv, axis, peer):
    return pltpu.make_async_remote_copy(
        src_ref=src,
        dst_ref=dst,
        send_sem=send,
        recv_sem=recv,
        device_id={axis: peer},
        device_id_type=MESH,
    )


def meet(peers):
    barrier = pltpu.get_barrier_semaphore()
    for axis, peer in peers:
        pl.semaphore_signal(barrier, inc=1, device_id={axis: peer}, device_id_type=MESH)
    pl.semaphore_wait(barrier, len(peers))


class Plane:
    def __init__(self, n):
        self.chips = n // 2
        self.me = lax.axis_index("ctx")
        self.core = self.me % 2
        self.chip = self.me // 2
        self.mate = self.me + 1 - 2 * self.core

    def same(self, s):
        return 2 * flip(self.chip, s, self.chips) + self.core

    def meet(self):
        meet([("ctx", self.same(s)) for s in range(1, self.chips)] + [("ctx", self.mate)])


def far_first(chips):
    return sorted(range(1, chips), key=lambda s: -bin(s).count("1"))


class Gather:
    def __init__(self, plane, src, out, send, recv, local):
        self.plane, self.out, self.send, self.recv = plane, out, send, recv
        self.own = pltpu.make_async_copy(src, out.at[plane.me], local)
        self.far = [
            push(src, out.at[plane.me], send.at[s], recv.at[s], "ctx", plane.same(s))
            for s in far_first(plane.chips)
        ]
        self.near = push(src, out.at[plane.me], send.at[0], recv.at[0], "ctx", plane.mate)

    def start(self):
        for copy in self.far:
            copy.start()
        self.near.start()
        self.own.start()

    def forward(self):
        plane, out = self.plane, self.out
        self.passed = []
        for s in sorted(range(1, plane.chips), key=lambda s: bin(s).count("1")):
            block = out.at[plane.same(s)]
            push(block, block, self.send.at[s], self.recv.at[s], "ctx", plane.mate).wait_recv()
            slot = plane.chips + s
            copy = push(block, block, self.send.at[slot], self.recv.at[slot], "ctx", plane.mate)
            copy.start()
            self.passed.append(copy)

    def finish(self):
        for copy in self.far:
            copy.wait_send()
        self.near.wait_send()
        self.near.wait_recv()
        for copy in self.passed:
            copy.wait_send()
            copy.wait_recv()
        self.own.wait()


def by_rows(rows, body):
    def one(index, carry):
        body(pl.ds(pl.multiple_of(index * CHUNK, CHUNK), CHUNK))
        return carry

    lax.fori_loop(0, rows // CHUNK, one, 0)


class SquareGather:
    def __init__(self, plane, src, out, send, recv, local):
        self.plane, self.out, self.send, self.recv = plane, out, send, recv
        half = src.shape[0] // 2
        self.halves = [pl.ds(0, half), pl.ds(half, half)]
        mine = out.at[plane.me]
        self.own = pltpu.make_async_copy(src, mine, local)
        self.near = push(src, mine, send.at[0], recv.at[0], "ctx", plane.mate)
        self.far = []
        for s, h in ((1, 0), (2, 1), (1, 1), (2, 0)):
            part, slot = self.halves[h], 2 * s + h
            self.far.append(
                push(
                    src.at[part, :],
                    mine.at[part, :],
                    send.at[slot],
                    recv.at[slot],
                    "ctx",
                    plane.same(s),
                )
            )

    def start(self):
        for copy in self.far:
            copy.start()
        self.near.start()
        self.own.start()

    def arrived(self, s, h):
        block = self.out.at[self.plane.same(s)].at[self.halves[h], :]
        slot = 2 * s + h
        push(block, block, self.send.at[slot], self.recv.at[slot], "ctx", self.plane.mate).wait_recv()
        return block

    def forward(self):
        plane = self.plane
        self.passed = []
        for s, h in ((1, 0), (2, 1)):
            block = self.arrived(s, h)
            slot = 6 + h
            copy = push(block, block, self.send.at[slot], self.recv.at[slot], "ctx", plane.same(3 - s))
            copy.start()
            self.far.append(copy)
        for s in (1, 2, 3):
            if s < 3:
                self.arrived(s, 2 - s)
            else:
                self.arrived(3, 0)
                self.arrived(3, 1)
            block, slot = self.out.at[plane.same(s)], 7 + s
            copy = push(block, block, self.send.at[slot], self.recv.at[slot], "ctx", plane.mate)
            copy.start()
            self.passed.append(copy)

    def finish(self):
        for copy in self.far:
            copy.wait_send()
        self.near.wait_send()
        self.near.wait_recv()
        for copy in self.passed:
            copy.wait_send()
            copy.wait_recv()
        self.own.wait()


def gather_of(plane, src, out, send, recv, local):
    kind = SquareGather if plane.chips == 4 else Gather
    return kind(plane, src, out, send, recv, local)


class Spread:
    def __init__(self, plane, mine, landed, send, recv):
        self.plane, self.mine, self.landed = plane, mine, landed
        self.square = plane.chips == 4
        self.order = [3, 1, 2, 0] if self.square else far_first(plane.chips) + [0]
        self.send, self.recv = send, recv
        half = mine.shape[1] // 2
        self.halves = [pl.ds(0, half), pl.ds(half, half)]

    def copy(self, s, h, to):
        part, slot = self.halves[h], 2 * s + h
        return push(
            self.mine.at[s].at[part, :],
            self.landed.at[s].at[part, :],
            self.send.at[slot],
            self.recv.at[slot],
            "ctx",
            self.plane.same(to),
        )

    def go(self, s, h, to):
        self.copy(s, h, to).start()

    def ready(self, s):
        if self.square:
            if s == 3:
                self.go(3, 0, 1)
                self.go(3, 1, 2)
            elif s == 1:
                self.go(1, 0, 1)
            elif s == 2:
                self.go(2, 1, 2)
        elif s:
            push(
                self.mine.at[s],
                self.landed.at[s],
                self.send.at[s],
                self.recv.at[s],
                "ctx",
                self.plane.same(s),
            ).start()

    def sends(self):
        if self.square:
            hops = ((3, 0, 1), (3, 1, 2), (1, 0, 1), (2, 1, 2), (2, 0, 2), (1, 1, 1))
            return [self.copy(*hop) for hop in hops]
        return [
            push(
                self.mine.at[s],
                self.landed.at[s],
                self.send.at[s],
                self.recv.at[s],
                "ctx",
                self.plane.same(s),
            )
            for s in self.order
            if s
        ]

    def relay(self):
        mine, landed = self.mine, self.landed
        half = mine.shape[1] // 2
        if not self.square:
            return
        for s, h in ((2, 0), (1, 1)):
            self.copy(3, h, 1).wait_recv()

            def add(at, s=s, h=h):
                rows = pl.ds(h * half + at.start, CHUNK)
                total = mine[s, rows, :].astype(F32) + landed[3, rows, :].astype(F32)
                mine[s, rows, :] = total.astype(BF16)

            by_rows(half, add)
            self.copy(s, h, s).start()

    def gathered(self):
        if not self.square:
            for copy in self.sends():
                copy.wait_recv()
            return
        for s in (1, 2):
            for h in (0, 1):
                self.copy(s, h, s).wait_recv()

    def settle(self, extra=None):
        self.relay()
        if extra is not None:
            extra()
        self.gathered()

    def total(self, at):
        value = self.mine[0, at, :].astype(F32)
        for s in (1, 2) if self.square else range(1, self.plane.chips):
            value = value + self.landed[s, at, :].astype(F32)
        return value

    def finish(self):
        for copy in self.sends():
            copy.wait_send()


class Scatter:
    def __init__(self, plane, part, mine, other, landed, send, recv, send2, recv2, local):
        self.plane, self.mine, self.other = plane, mine, other
        self.spread = Spread(plane, mine, landed, send2, recv2)
        self.order = self.spread.order
        self.loads, self.across = {}, {}
        for s in self.order:
            block = plane.same(s)
            self.loads[s] = pltpu.make_async_copy(part.at[block], mine.at[s], local.at[s])
            self.across[s] = push(
                part.at[block + 1 - 2 * plane.core],
                other.at[s],
                send.at[s],
                recv.at[s],
                "ctx",
                plane.mate,
            )

    def start(self):
        for s in self.order:
            self.across[s].start()
            self.loads[s].start()

    def pairs(self):
        mine, other = self.mine, self.other
        for s in self.order:
            self.loads[s].wait()
            self.across[s].wait_recv()

            def add(at, s=s):
                total = mine[s, at, :].astype(F32) + other[s, at, :].astype(F32)
                mine[s, at, :] = total.astype(BF16)

            by_rows(mine.shape[1], add)
            self.spread.ready(s)

    def run(self):
        self.pairs()
        self.spread.settle()

    def total(self, at):
        return self.spread.total(at)

    def finish(self):
        for s in self.order:
            self.across[s].wait_send()
        self.spread.finish()


class Product:
    def __init__(self, plane, value, mine, other, landed, given, send, recv, send2, recv2):
        self.plane, self.value = plane, value
        self.mine, self.other, self.given = mine, other, given
        self.spread = Spread(plane, mine, landed, send2, recv2)
        self.order = self.spread.order
        self.across = {
            s: push(given.at[s], other.at[s], send.at[s], recv.at[s], "ctx", plane.mate)
            for s in self.order
        }

    def start(self):
        plane = self.plane
        for s in self.order:
            block = plane.same(s) + 1 - 2 * plane.core

            def fill(at, s=s, block=block):
                self.given[s, :, at] = self.value(block, at).astype(BF16)

            by_cols(self.mine.shape[2], fill)
            self.across[s].start()

    def run(self, extra=None):
        plane, mine, other = self.plane, self.mine, self.other
        for s in self.order:
            block = plane.same(s)
            self.across[s].wait_recv()

            def fill(at, s=s, block=block):
                total = self.value(block, at) + other[s, :, at].astype(F32)
                mine[s, :, at] = total.astype(BF16)

            by_cols(mine.shape[2], fill)
            self.spread.ready(s)
        self.spread.settle(extra)

    total = Scatter.total
    finish = Scatter.finish


def by_cols(width, body):
    span = 512

    def one(index, carry):
        body(pl.ds(pl.multiple_of(index * span, span), span))
        return carry

    lax.fori_loop(0, width // span, one, 0)


def gather_sems(n):
    return [DMA((12 if n == 8 else n,)), DMA((12 if n == 8 else n,)), DMA(())]


def scatter_scratch(n, rows, width):
    chips = n // 2
    return (
        [pltpu.VMEM((chips, rows, width), BF16)] * 3
        + [DMA((chips,)), DMA((chips,)), DMA((n,)), DMA((n,))]
        + [DMA((chips,))]
    )


def product_scratch(n, rows, width):
    chips = n // 2
    return [pltpu.VMEM((chips, rows, width), BF16)] * 4 + [
        DMA((chips,)),
        DMA((chips,)),
        DMA((n,)),
        DMA((n,)),
    ]


def comm_call(kernel, ident, outs, out_specs, in_specs, scratch, micros, *args):
    return pl.pallas_call(
        kernel,
        out_shape=outs,
        in_specs=in_specs,
        out_specs=out_specs,
        scratch_shapes=scratch,
        compiler_params=pltpu.CompilerParams(
            collective_id=ident, has_side_effects=True, vmem_limit_bytes=VMEM_LIMIT
        ),
        cost_estimate=pl.CostEstimate(
            flops=0, transcendentals=0, bytes_accessed=int(micros * 3.0e6)
        ),
    )(*args)


def swap_all(n, src, out, send, recv, local):
    me = lax.axis_index("ctx")
    own = pltpu.make_async_copy(src.at[me], out.at[me], local)
    own.start()
    copies = []
    for s in range(n - 1, 0, -1):
        peer = flip(me, s, n)
        copies.append(push(src.at[peer], out.at[me], send.at[s], recv.at[s], "ctx", peer))
        copies[-1].start()
    return own, copies


class RowSwap:
    def __init__(self, n, n_dp, src, dst, send, recv, spread):
        self.me = lax.axis_index("ctx")
        self.dst, self.send, self.recv, self.n_dp = dst, send, recv, n_dp
        self.entries = []
        for k in range(n_dp):
            flat = self.me * n_dp + k if spread else k * n + self.me
            peer = flat % n if spread else flat // n_dp
            slot = flat // n if spread else flat % n_dp
            far = push(src.at[k], dst.at[slot], send.at[k], recv.at[slot], "ctx", peer)
            near = pltpu.make_async_copy(src.at[k], dst.at[slot], recv.at[slot])
            self.entries.append((peer, far, near))

    def start(self):
        for peer, far, near in self.entries:
            pl.when(peer != self.me)(far.start)
            pl.when(peer == self.me)(near.start)

    def arrive(self):
        for slot in range(self.n_dp):
            block = self.dst.at[slot]
            pltpu.make_async_copy(block, block, self.recv.at[slot]).wait()

    def finish(self):
        for peer, far, near in self.entries:
            pl.when(peer != self.me)(far.wait_send)


def meet_all(n):
    me = lax.axis_index("ctx")
    meet([("ctx", flip(me, s, n)) for s in range(1, n)])


def prep_kernel(n, n_dp, cols_ref, small_ref, out_ref, all_ref, *sems):
    send, recv, local, gsend, grecv, zsend, zrecv = sems
    me, row = lax.axis_index("ctx"), lax.axis_index("dp")
    meet(
        [("ctx", flip(me, s, n)) for s in range(1, n)]
        + [("dp", flip(row, s, n_dp)) for s in range(1, n_dp)]
    )
    all_ref[row, me] = small_ref[...]
    smalls = []
    for s in range(1, n):
        peer = flip(me, s, n)
        smalls.append(push(small_ref, all_ref.at[row, me], gsend.at[s], grecv.at[s], "ctx", peer))
        smalls[-1].start()
    own, copies = swap_all(n, cols_ref, out_ref, send, recv, local)
    for copy in smalls:
        copy.wait_recv()
    planes = []
    for s in range(1, n_dp):
        peer = flip(row, s, n_dp)
        planes.append(push(all_ref.at[row], all_ref.at[row], zsend.at[s], zrecv.at[s], "dp", peer))
        planes[-1].start()
    for copy in copies + planes:
        copy.wait_recv()
    for copy in copies + planes + smalls:
        copy.wait_send()
    own.wait()


class Gains:
    def __init__(self, n, n_dp, small, landed, mid, second, gsend, grecv, zsend, zrecv):
        self.me, self.row = lax.axis_index("ctx"), lax.axis_index("dp")
        self.small, self.landed, self.mid, self.second = small, landed, mid, second
        self.near, self.far = [], []
        for s in range(1, n):
            peer = flip(self.me, s, n)
            self.near.append(push(small.at[peer], landed.at[s], gsend.at[s], grecv.at[s], "ctx", peer))
        for s in range(1, n_dp):
            peer = flip(self.row, s, n_dp)
            self.far.append(push(mid.at[peer], second.at[s], zsend.at[s], zrecv.at[s], "dp", peer))

    def start(self):
        for copy in self.near:
            copy.start()

    def middle(self):
        value = self.small[self.me]
        for s, copy in enumerate(self.near, 1):
            copy.wait_recv()
            value = value + self.landed[s]
        self.mid[...] = value
        for copy in self.far:
            copy.start()

    def finish(self):
        value = self.mid[self.row]
        for s, copy in enumerate(self.far, 1):
            copy.wait_recv()
            value = value + self.second[s]
        for copy in self.near + self.far:
            copy.wait_send()
        return value


def post_kernel(n, src_ref, query_ref, key_ref, value_ref, blocks, send, recv, local):
    me = lax.axis_index("ctx")
    meet([("ctx", flip(me, s, n)) for s in range(1, n)])
    own, copies = swap_all(n, src_ref, blocks, send, recv, local)
    for copy in copies:
        copy.wait_recv()
    own.wait()
    share = n // KV
    qw = HQ * HD // n
    for c in range(n):
        query_ref[:, c * qw : (c + 1) * qw] = blocks[c, :, :qw].astype(F32)
    for g in range(KV):
        for out, kind in ((key_ref, 0), (value_ref, 1)):
            total = blocks[g * share + kind, :, qw:].astype(F32)
            for c in range(2 + kind, share, 2):
                total = total + blocks[g * share + c, :, qw:].astype(F32)
            out[:, g * HD : (g + 1) * HD] = total
    for copy in copies:
        copy.wait_send()


def swap_sems(n, n_dp):
    return [DMA((n,)), DMA((n,)), DMA(()), DMA((n,)), DMA((n,)), DMA((n_dp,)), DMA((n_dp,))]


def prep(n, n_dp, cols, small):
    shape = jax.ShapeDtypeStruct
    return comm_call(
        functools.partial(prep_kernel, n, n_dp),
        0,
        [shape(cols.shape, cols.dtype), shape((n_dp, n) + small.shape, F32)],
        [ANY, VM],
        [ANY, VM],
        swap_sems(n, n_dp),
        8,
        cols,
        small,
    )


def post(n, cols):
    shape = jax.ShapeDtypeStruct
    depth = cols.shape[1]
    return comm_call(
        functools.partial(post_kernel, n),
        1,
        [
            shape((depth, HQ * HD), F32),
            shape((depth, KV * HD), F32),
            shape((depth, KV * HD), F32),
        ],
        [VM] * 3,
        [VM],
        [pltpu.VMEM(cols.shape, BF16), DMA((n,)), DMA((n,)), DMA(())],
        10,
        cols,
    )


def first_kernel(
    n, x_ref, gain_ref, info_ref, grad_ref, nall_ref, iall_ref, gall_ref, low, *sems
):
    plane = Plane(n)
    plane.meet()
    infos = Gather(plane, info_ref, iall_ref, *sems[0:3])
    infos.start()

    def norm(at):
        value = x_ref[at, :].astype(F32)
        low[at, :] = (value * rms_parts(value) * gain_ref[...]).astype(BF16)

    by_rows(x_ref.shape[0], norm)
    normed = gather_of(plane, low, nall_ref, *sems[3:6])
    normed.start()
    grads = gather_of(plane, grad_ref, gall_ref, *sems[6:9])
    grads.start()
    infos.forward()
    normed.forward()
    grads.forward()
    infos.finish()
    normed.finish()
    grads.finish()


def first(n, x, gain, info, grad):
    shape = jax.ShapeDtypeStruct
    many = lambda array, kind: shape((n,) + array.shape, kind)
    return comm_call(
        functools.partial(first_kernel, n),
        2,
        [many(x, BF16), many(info, F32), many(grad, BF16)],
        [ANY] * 3,
        [VM] * 4,
        [pltpu.VMEM(x.shape, BF16)]
        + [DMA((n,)), DMA((n,)), DMA(())]
        + gather_sems(n)
        + gather_sems(n),
        90,
        x,
        gain,
        info,
        grad,
    )


def middle_kernel(
    n, attn_ref, wout_ref, x_ref, gain_ref, after_ref, all_ref, low, *scratch
):
    plane = Plane(n)
    plane.meet()
    rows = x_ref.shape[0]

    def value(block, at):
        left = attn_ref[pl.ds(pl.multiple_of(block * rows, rows), rows), :]
        return dot(left, wout_ref[:, at])

    sums = Product(plane, value, *scratch[:8])
    sums.start()
    sums.run()

    def norm(at):
        value = x_ref[at, :].astype(F32) + sums.total(at)
        after_ref[at, :] = value
        low[at, :] = (value * rms_parts(value) * gain_ref[...]).astype(BF16)

    by_rows(rows, norm)
    normed = gather_of(plane, low, all_ref, *scratch[8:])
    normed.start()
    normed.forward()
    sums.finish()
    normed.finish()


def middle(n, attn, wout, x, gain):
    shape = jax.ShapeDtypeStruct
    return comm_call(
        functools.partial(middle_kernel, n),
        3,
        [shape(x.shape, F32), shape((n,) + x.shape, BF16)],
        [VM, ANY],
        [VM, VM, VM, VM],
        [pltpu.VMEM(x.shape, BF16)]
        + product_scratch(n, *x.shape)
        + gather_sems(n),
        105,
        attn,
        wout,
        x,
        gain,
    )


def turn_kernel(
    n, part_ref, after_ref, grad_ref, gain_ref, mid_ref, fpart_ref, all_ref, low, *scratch
):
    plane = Plane(n)
    plane.meet()
    sums = Scatter(plane, part_ref, *scratch[:8])
    sums.start()
    fpart_ref[...] = jnp.zeros_like(fpart_ref)
    sums.run()

    def norm(at):
        value = after_ref[at, :]
        inv = rms_parts(value)
        unit = value * inv
        grad = sums.total(at)
        fpart_ref[0:1, :] += jnp.sum(grad * unit, axis=0, keepdims=True)
        mid = grad_ref[at, :].astype(F32) + rms_back(grad, unit, inv, gain_ref[...])
        mid_ref[at, :] = mid
        low[at, :] = mid.astype(BF16)

    by_rows(after_ref.shape[0], norm)
    branch = gather_of(plane, low, all_ref, *scratch[8:])
    branch.start()
    branch.forward()
    sums.finish()
    branch.finish()


def turn(n, part, after, grad, gain):
    shape = jax.ShapeDtypeStruct
    return comm_call(
        functools.partial(turn_kernel, n),
        4,
        [
            shape(after.shape, F32),
            shape((8, after.shape[1]), F32),
            shape((n,) + after.shape, BF16),
        ],
        [VM, VM, ANY],
        [ANY, VM, VM, VM],
        [pltpu.VMEM(after.shape, BF16)] + scatter_scratch(n, *after.shape) + gather_sems(n),
        95,
        part,
        after,
        grad,
        gain,
    )


def last_kernel(n, grad_ref, wqkv_ref, x_ref, mid_ref, gain_ref, out_ref, apart_ref, *scratch):
    plane = Plane(n)
    plane.meet()
    apart_ref[...] = jnp.zeros_like(apart_ref)
    rows = x_ref.shape[0]

    def value(block, at):
        left = grad_ref[pl.ds(pl.multiple_of(block * rows, rows), rows), :]
        return dot(left, wqkv_ref[at, :], NT)

    sums = Product(plane, value, *scratch[:8])
    sums.start()
    sums.run()

    def norm(at):
        value = x_ref[at, :].astype(F32)
        inv = rms_parts(value)
        unit = value * inv
        grad = sums.total(at)
        apart_ref[0:1, :] += jnp.sum(grad * unit, axis=0, keepdims=True)
        out_ref[at, :] = mid_ref[at, :] + rms_back(grad, unit, inv, gain_ref[...])

    by_rows(rows, norm)
    sums.finish()


def last(n, grad, wqkv, x, mid, gain):
    shape = jax.ShapeDtypeStruct
    return comm_call(
        functools.partial(last_kernel, n),
        5,
        [shape(mid.shape, F32), shape((8, mid.shape[1]), F32)],
        [VM, VM],
        [VM] * 5,
        product_scratch(n, *mid.shape),
        60,
        grad,
        wqkv,
        x,
        mid,
        gain,
    )


def gains_kernel(n, n_dp, small_ref, sum_ref, *scratch):
    meet(
        [("ctx", flip(lax.axis_index("ctx"), s, n)) for s in range(1, n)]
        + [("dp", flip(lax.axis_index("dp"), s, n_dp)) for s in range(1, n_dp)]
    )
    gains = Gains(n, n_dp, small_ref, *scratch)
    gains.start()
    gains.middle()
    sum_ref[...] = gains.finish()


def gains_sum(n, n_dp, small):
    tile = small.shape[2:]
    return comm_call(
        functools.partial(gains_kernel, n, n_dp),
        8,
        jax.ShapeDtypeStruct(tile, F32),
        VM,
        [VM],
        [
            pltpu.VMEM((n, n_dp) + tile, F32),
            pltpu.VMEM((n_dp,) + tile, F32),
            pltpu.VMEM((n_dp,) + tile, F32),
            DMA((n,)),
            DMA((n,)),
            DMA((n_dp,)),
            DMA((n_dp,)),
        ],
        10,
        small,
    )


def attn_forward_kernel(
    n,
    n_dp,
    heads,
    back,
    normed_ref,
    wqkv_ref,
    cos_ref,
    sin_ref,
    qgain_ref,
    kgain_ref,
    docc_ref,
    docr_ref,
    rows_ref,
    qlin_ref,
    klin_ref,
    q_ref,
    k_ref,
    v_ref,
    attn_ref,
    total_ref,
    wout_ref,
    acc_ref,
    sum_ref,
    mate_ref,
    *sems,
):
    step = pl.program_id(0)

    @pl.when(step == 0)
    def _():
        meet_all(n)
        copy = push(
            wqkv_ref.at[:, pl.ds(heads * HD, HD)],
            mate_ref,
            sems[2],
            sems[3],
            "ctx",
            Plane(n).mate,
        )
        copy.start()
        RowSwap(n, n_dp, rows_ref, wout_ref, *sems[:2], False).start()
        copy.wait_recv()
        copy.wait_send()

    rows = normed_ref.shape[0]
    lin = dot(normed_ref[...], wqkv_ref[...])
    here = pl.ds(step * rows, rows)
    cosine = cos_ref[...]
    sine = sin_ref[...]
    qw = heads * HD
    for head in range(heads):
        cols = slice(head * HD, (head + 1) * HD)
        part = lin[:, cols]
        qlin_ref[:, cols] = part
        q_ref[:, cols] = head_forward(part, qgain_ref[...], cosine, sine).astype(BF16)
    own = lin[:, qw:]
    other = dot(normed_ref[...], mate_ref[...])
    first_core = lax.axis_index("ctx") % 2 == 0
    key_lin = jnp.where(first_core, own, other)
    klin_ref[...] = key_lin
    k_ref[here, :] = head_forward(key_lin, kgain_ref[...], cosine, sine).astype(BF16)
    v_ref[here, :] = jnp.where(first_core, other, own).astype(BF16)
    acc_ref[...] = jnp.zeros_like(acc_ref)
    sum_ref[...] = jnp.zeros_like(sum_ref)
    row_pos = step * rows + lax.broadcasted_iota(jnp.int32, (rows, rows), 0)
    col_off = lax.broadcasted_iota(jnp.int32, (rows, rows), 1)

    def one(block, carry):
        at = pl.ds(pl.multiple_of(block * rows, rows), rows)
        key = k_ref[at, :]
        val = v_ref[at, :]
        allowed = (docc_ref[...] == docr_ref[:, at]) & (block * rows + col_off <= row_pos)
        for head in range(heads):
            cols = slice(head * HD, (head + 1) * HD)
            score = dot(q_ref[:, cols], key, NT) * SCALE2
            expo = jnp.where(allowed, jnp.exp2(score), 0.0)
            folded = expo[:, :HD]
            for piece in range(1, rows // HD):
                folded = folded + expo[:, piece * HD : (piece + 1) * HD]
            sum_ref[:, cols] += folded
            acc_ref[:, cols] += dot(expo.astype(BF16), val)
        return carry

    lax.fori_loop(jnp.maximum(step - back, 0), step + 1, one, 0)
    lane = lax.broadcasted_iota(jnp.int32, (rows, HD), 1)
    totals = jnp.ones((rows, HD), F32)
    for head in range(heads):
        cols = slice(head * HD, (head + 1) * HD)
        total = jnp.sum(sum_ref[:, cols], axis=-1, keepdims=True)
        totals = jnp.where(lane == head, total, totals)
        attn_ref[:, cols] = (acc_ref[:, cols] / total).astype(BF16)
    total_ref[...] = totals

    @pl.when(step == pl.num_programs(0) - 1)
    def _():
        swap = RowSwap(n, n_dp, rows_ref, wout_ref, *sems[:2], False)
        swap.arrive()
        swap.finish()


def attn_forward(n, n_dp, normed, wqkv, cosine, sine, qgain, kgain, doc, wrows, rows):
    length, width = normed.shape
    qw = wqkv.shape[1] - HD
    heads = qw // HD
    blk = lambda cols: pl.BlockSpec((rows, cols), lambda i: (i, 0))
    whole = lambda shape: pl.BlockSpec(shape, lambda i: (0, 0))
    shape = jax.ShapeDtypeStruct
    return pl.pallas_call(
        functools.partial(attn_forward_kernel, n, n_dp, heads, MOST // rows),
        grid=(length // rows,),
        in_specs=[
            blk(width),
            whole(wqkv.shape),
            blk(HD),
            blk(HD),
            whole((1, HD)),
            whole((1, HD)),
            blk(1),
            whole((1, length)),
            ANY,
        ],
        out_specs=[
            blk(qw),
            blk(HD),
            blk(qw),
            whole((length, HD)),
            whole((length, HD)),
            blk(qw),
            blk(HD),
            ANY,
        ],
        out_shape=[
            shape((length, qw), F32),
            shape((length, HD), F32),
            shape((length, qw), BF16),
            shape((length, HD), BF16),
            shape((length, HD), BF16),
            shape((length, qw), BF16),
            shape((length, HD), F32),
            shape(wrows.shape, BF16),
        ],
        scratch_shapes=[
            pltpu.VMEM((rows, qw), F32),
            pltpu.VMEM((rows, qw), F32),
            pltpu.VMEM((width, HD), BF16),
        ]
        + [DMA((n_dp,)), DMA((n_dp,)), DMA(()), DMA(())],
        compiler_params=pltpu.CompilerParams(
            collective_id=7, has_side_effects=True, vmem_limit_bytes=VMEM_LIMIT
        ),
        cost_estimate=pl.CostEstimate(
            flops=35 * 10**9, transcendentals=0, bytes_accessed=30 * 2**20
        ),
        name="attn_forward",
    )(normed, wqkv, cosine, sine, qgain, kgain, doc[:, None], doc[None, :], wrows)


def attn_backward_kernel(
    n,
    n_dp,
    heads,
    back,
    branch_ref,
    wout_ref,
    attn_ref,
    total_ref,
    q_ref,
    k_ref,
    v_ref,
    qlin_ref,
    klin_ref,
    cos_ref,
    sin_ref,
    qgain_ref,
    kgain_ref,
    docc_ref,
    docr_ref,
    wgrad_ref,
    moe_ref,
    after_ref,
    dqkv_ref,
    gains_ref,
    swapped_ref,
    final_ref,
    dk_ref,
    dv_ref,
    dqa_ref,
    give_ref,
    take_ref,
    *sems,
):
    step = pl.program_id(0)

    steps = pl.num_programs(0)

    def scatter():
        return Scatter(Plane(n), moe_ref, *sems[2:10])

    @pl.when(step == 0)
    def _():
        meet_all(n)
        scatter().start()
        RowSwap(n, n_dp, wgrad_ref, swapped_ref, *sems[:2], True).start()

    @pl.when(step == 2)
    def _():
        scatter().pairs()

    @pl.when(step == steps - 2)
    def _():
        scatter().spread.relay()

    rows = branch_ref.shape[0]
    here = pl.ds(pl.multiple_of(step * rows, rows), rows)

    @pl.when(step == 0)
    def _():
        gains_ref[...] = jnp.zeros_like(gains_ref)

    dk_ref[here, :] = jnp.zeros((rows, HD), F32)
    dv_ref[here, :] = jnp.zeros((rows, HD), F32)
    dqa_ref[...] = jnp.zeros_like(dqa_ref)
    attn_grad = dot(branch_ref[...], wout_ref[...], NT)
    grads = []
    shifts = []
    for head in range(heads):
        cols = slice(head * HD, (head + 1) * HD)
        part = attn_grad[:, cols]
        inv_total = 1.0 / total_ref[:, head : head + 1]
        delta = jnp.sum(part * attn_ref[:, cols].astype(F32), axis=-1, keepdims=True)
        grads.append((part * inv_total).astype(BF16))
        shifts.append(delta * inv_total)
    row_pos = step * rows + lax.broadcasted_iota(jnp.int32, (rows, rows), 0)
    col_off = lax.broadcasted_iota(jnp.int32, (rows, rows), 1)

    def one(block, carry):
        at = pl.ds(pl.multiple_of(block * rows, rows), rows)
        key = k_ref[at, :]
        val = v_ref[at, :]
        allowed = (docc_ref[...] == docr_ref[:, at]) & (block * rows + col_off <= row_pos)
        dk = jnp.zeros((rows, HD), F32)
        dv = jnp.zeros((rows, HD), F32)
        for head in range(heads):
            cols = slice(head * HD, (head + 1) * HD)
            query = q_ref[:, cols]
            score = dot(query, key, NT) * SCALE2
            expo = jnp.where(allowed, jnp.exp2(score), 0.0)
            prod = dot(grads[head], val, NT)
            score_grad = (expo * (prod - shifts[head])).astype(BF16)
            dv += dot(expo.astype(BF16), grads[head], TN)
            dk += dot(score_grad, query, TN)
            dqa_ref[:, cols] += dot(score_grad, key)
        dk_ref[at, :] += dk
        dv_ref[at, :] += dv
        return carry

    lax.fori_loop(jnp.maximum(step - back, 0), step + 1, one, 0)
    cosine = cos_ref[here, :]
    sine = sin_ref[here, :]
    for head in range(heads):
        cols = slice(head * HD, (head + 1) * HD)
        grad, gain_part = head_backward(
            qlin_ref[:, cols], qgain_ref[...], cosine, sine, dqa_ref[:, cols] * SCALE
        )
        dqkv_ref[here, cols] = grad.astype(BF16)
        gains_ref[0:1, :] += gain_part

    @pl.when(step == pl.num_programs(0) - 1)
    def _():
        def finish(block, carry):
            at = pl.ds(pl.multiple_of(block * rows, rows), rows)
            grad, gain_part = head_backward(
                klin_ref[at, :], kgain_ref[...], cos_ref[at, :], sin_ref[at, :], dk_ref[at, :] * SCALE
            )
            first_core = lax.axis_index("ctx") % 2 == 0
            dk_ref[at, :] = jnp.where(first_core, grad, dv_ref[at, :])
            give_ref[at, :] = jnp.where(first_core, dv_ref[at, :], grad).astype(BF16)
            gains_ref[1:2, :] += gain_part
            return carry

        lax.fori_loop(0, pl.num_programs(0), finish, 0)
        trade = push(give_ref, take_ref, sems[10], sems[11], "ctx", Plane(n).mate)
        trade.start()
        sums = scatter()
        sums.spread.gathered()

        def add(at):
            final_ref[at, :] = (after_ref[at, :] + sums.total(at)).astype(BF16)

        by_rows(rows, add)
        sums.finish()
        trade.wait_recv()

        def join(block, carry):
            at = pl.ds(pl.multiple_of(block * rows, rows), rows)
            total = dk_ref[at, :] + take_ref[at, :].astype(F32)
            dqkv_ref[at, heads * HD :] = total.astype(BF16)
            return carry

        lax.fori_loop(0, pl.num_programs(0), join, 0)
        trade.wait_send()
        swap = RowSwap(n, n_dp, wgrad_ref, swapped_ref, *sems[:2], True)
        swap.arrive()
        swap.finish()


def attn_backward(n, n_dp, wgrad, moe, after, branch, wout, attn, total, q, k, v, qlin, klin, cosine, sine, qgain, kgain, doc, rows):
    length, width = branch.shape
    qw = wout.shape[0]
    heads = qw // HD
    blk = lambda cols: pl.BlockSpec((rows, cols), lambda i: (i, 0))
    whole = lambda shape: pl.BlockSpec(shape, lambda i: (0, 0), pipeline_mode=pl.Buffered(1))
    shape = jax.ShapeDtypeStruct
    full = whole((length, HD))
    return pl.pallas_call(
        functools.partial(attn_backward_kernel, n, n_dp, heads, MOST // rows),
        grid=(length // rows,),
        in_specs=[
            blk(width),
            whole(wout.shape),
            blk(qw),
            blk(HD),
            blk(qw),
            full,
            full,
            blk(qw),
            full,
            full,
            full,
            whole((1, HD)),
            whole((1, HD)),
            blk(1),
            whole((1, length)),
            ANY,
            ANY,
            whole(after.shape),
        ],
        out_specs=[whole((length, qw + HD)), whole((8, HD)), ANY, whole(after.shape)],
        out_shape=[
            shape((length, qw + HD), BF16),
            shape((8, HD), F32),
            shape(wgrad.shape, BF16),
            shape(after.shape, BF16),
        ],
        scratch_shapes=[
            pltpu.VMEM((length, HD), F32),
            pltpu.VMEM((length, HD), F32),
            pltpu.VMEM((rows, qw), F32),
            pltpu.VMEM((length, HD), BF16),
            pltpu.VMEM((length, HD), BF16),
            DMA((n_dp,)),
            DMA((n_dp,)),
        ]
        + scatter_scratch(n, *after.shape)
        + [DMA(()), DMA(())],
        compiler_params=pltpu.CompilerParams(
            collective_id=9, has_side_effects=True, vmem_limit_bytes=VMEM_LIMIT
        ),
        cost_estimate=pl.CostEstimate(
            flops=60 * 10**9, transcendentals=0, bytes_accessed=30 * 2**20
        ),
        name="attn_backward",
    )(branch, wout, attn, total, q, k, v, qlin, klin, cosine, sine, qgain, kgain, doc[:, None], doc[None, :], wgrad, moe, after)


def expert_kernel(chained, low, aliased, plan, z_ref, n2_ref, top_ref, prob_ref, *rest):
    if aliased:
        rest = rest[1:]
    if chained:
        moe_in, row_in = rest[:2]
        rest = rest[2:]
    sources, rest = rest[: len(plan)], rest[len(plan) :]
    moe_ref, row_ref, grads_ref, wg_ref, wu_ref, wd_ref = rest[:6]
    ag_ref, au_ref, ad_ref, stage, wsem, sem = rest[6:]
    step = pl.program_id(0)
    rows, width = n2_ref.shape
    parts, cut, hidden = wd_ref.shape
    weights = (wg_ref, wu_ref, wd_ref)

    @pl.when(step == 0)
    def _():
        z = z_ref[0]
        for source, (kind, amount, start) in zip(sources, plan):
            count = source.shape[-2] // cut
            for k in range(parts) if kind == "all" else [amount]:
                if kind == "all":
                    src, owner, wanted = source.at[k], k, None
                elif kind == "up":
                    src, owner, wanted = source, z - k, z >= k
                else:
                    src, owner, wanted = source, z + k, z + k < parts

                def load(src=src, owner=owner, start=start, count=count):
                    for piece in range(count):
                        pltpu.make_async_copy(
                            src.at[pl.ds(piece * cut, cut), :],
                            weights[start + piece].at[owner],
                            wsem.at[start + piece, owner],
                        ).start()

                if wanted is None:
                    load()
                else:
                    pl.when(wanted)(load)
        ag_ref[...] = jnp.zeros_like(ag_ref)
        au_ref[...] = jnp.zeros_like(au_ref)
        ad_ref[...] = jnp.zeros_like(ad_ref)
        for index in range(3):
            for owner in range(parts):
                block = weights[index].at[owner]
                pltpu.make_async_copy(block, block, wsem.at[index, owner]).wait()

    n2 = n2_ref[...]
    prob = prob_ref[...]
    wg = wg_ref[...].reshape(width, hidden)
    wu = wu_ref[...].reshape(width, hidden)
    gate = dot(n2, wg)
    up = dot(n2, wu)
    sig = 1.0 / (1.0 + jnp.exp(-gate))
    silu = gate * sig
    act = (silu * up).astype(BF16)
    act_grad = jnp.zeros((rows, hidden), F32)
    for z in range(parts):
        cols = slice(z * cut, (z + 1) * cut)
        out = dot(act, wd_ref[z], NT).astype(BF16).astype(F32) * prob
        if chained:
            out = out + moe_in[:, cols].astype(F32)
        moe_ref[:, cols] = out.astype(BF16)
        route = (top_ref[:, cols].astype(F32) * prob).astype(BF16)
        act_grad += dot(route, wd_ref[z])
        ad_ref[z] += dot(route, act, TN)
    gate_grad = (act_grad * up * sig * (1.0 + gate * (1.0 - sig))).astype(BF16)
    up_grad = (act_grad * silu).astype(BF16)
    row = dot(gate_grad, wg, NT) + dot(up_grad, wu, NT)
    if chained:
        row = row + row_in[...].astype(F32)
    row_ref[...] = row.astype(BF16)
    ag_ref[...] += dot(n2, gate_grad, TN).reshape(parts, cut, hidden)
    au_ref[...] += dot(n2, up_grad, TN).reshape(parts, cut, hidden)

    @pl.when(step == pl.num_programs(0) - 1)
    def _():
        copies = []
        pieces = [
            (acc, place, z) for z in range(parts) for place, acc in enumerate((ag_ref, au_ref, ad_ref))
        ]
        for index, (acc, place, z) in enumerate(pieces):
            slot = index % 2
            if index >= 2:
                copies[index - 2].wait()
            stage[slot] = acc[z].astype(BF16)
            copies.append(
                pltpu.make_async_copy(
                    stage.at[slot],
                    grads_ref.at[z, pl.ds(place * cut, cut), pl.ds(low, acc.shape[2])],
                    sem.at[slot],
                )
            )
            copies[-1].start()
        copies[-2].wait()
        copies[-1].wait()


def expert(z, n2, top, prob, n_dp, sources, before, rows, low, full, grads):
    length, width = n2.shape
    cut = width // n_dp
    hidden = sources[0][0].shape[-1]
    blk = pl.BlockSpec((rows, width), lambda i: (i, 0))
    col = pl.BlockSpec((rows, 1), lambda i: (i, 0))
    shape = jax.ShapeDtypeStruct
    plan = tuple(entry[1:] for entry in sources)
    weight = pltpu.VMEM((n_dp, cut, hidden), BF16)
    total = pltpu.VMEM((n_dp, cut, hidden), F32)
    return pl.pallas_call(
        functools.partial(expert_kernel, len(before) > 0, low, len(grads) > 0, plan),
        grid=(length // rows,),
        in_specs=[pl.BlockSpec(memory_space=pltpu.SMEM), blk, blk, col]
        + [ANY] * len(grads)
        + [blk] * len(before)
        + [ANY] * len(sources),
        out_specs=[blk, blk, ANY],
        out_shape=[
            shape((length, width), BF16),
            shape((length, width), BF16),
            shape((n_dp, 3 * cut, full), BF16),
        ],
        input_output_aliases={4: 2} if grads else {},
        scratch_shapes=[weight] * 3
        + [total] * 3
        + [pltpu.VMEM((2, cut, hidden), BF16), DMA((3, n_dp)), DMA((2,))],
        compiler_params=pltpu.CompilerParams(vmem_limit_bytes=VMEM_LIMIT),
        cost_estimate=pl.CostEstimate(
            flops=18 * length * width * hidden,
            transcendentals=length * hidden,
            bytes_accessed=5 * length * width * 2,
        ),
        name="expert",
    )(z, n2, top, prob, *grads, *before, *[entry[0] for entry in sources])


def pack_kernel(cuts, gate_ref, up_ref, down_ref, *outs):
    cut = gate_ref.shape[0]
    for (low, high), out in zip(cuts, outs):
        out[:cut, :] = gate_ref[:, low:high]
        out[cut : 2 * cut, :] = up_ref[:, low:high]
        out[2 * cut :, :] = jnp.transpose(down_ref[low:high, :].astype(F32)).astype(BF16)


def pack(cuts, w_gate, w_up, w_down):
    cut = w_gate.shape[0]
    return pl.pallas_call(
        functools.partial(pack_kernel, cuts),
        in_specs=[VM] * 3,
        out_specs=[VM] * len(cuts),
        out_shape=[jax.ShapeDtypeStruct((3 * cut, high - low), BF16) for low, high in cuts],
        name="pack",
    )(w_gate, w_up, w_down)


def unpack_kernel(
    z_ref, one_ref, all_ref, up0_ref, down0_ref, up1_ref, down1_ref, dg_ref, du_ref, dd_ref, own, sem
):
    copy = pltpu.make_async_copy(all_ref.at[z_ref[0]], own, sem)
    copy.start()
    cut = dg_ref.shape[1]
    half = up0_ref.shape[0]
    piece = [slice(k * cut, (k + 1) * cut) for k in range(3)]
    dg_ref[1] = one_ref[piece[0], :].astype(F32)
    du_ref[1] = one_ref[piece[1], :].astype(F32)
    dd_ref[1] = jnp.transpose(one_ref[piece[2], :].astype(F32))
    copy.wait()

    def total(low, high):
        shift, up, down = (0, up0_ref, down0_ref) if high <= half else (half, up1_ref, down1_ref)
        there = slice(low - shift, high - shift)
        value = own[low:high, :].astype(F32)
        return value + up[there, :].astype(F32) + down[there, :].astype(F32)

    dg_ref[0] = total(0, cut)
    du_ref[0, : half - cut] = total(cut, half)
    du_ref[0, half - cut :] = total(half, 2 * cut)
    dd_ref[0] = jnp.transpose(total(2 * cut, 3 * cut))


def unpack(z, one, grads, got):
    rows, hidden = one.shape
    cut = rows // 3
    shape = jax.ShapeDtypeStruct
    return pl.pallas_call(
        unpack_kernel,
        in_specs=[pl.BlockSpec(memory_space=pltpu.SMEM), VM, ANY, VM, VM, VM, VM],
        out_specs=[VM] * 3,
        out_shape=[
            shape((2, cut, hidden), F32),
            shape((2, cut, hidden), F32),
            shape((2, hidden, cut), F32),
        ],
        scratch_shapes=[pltpu.VMEM((rows, hidden), BF16), DMA(())],
        compiler_params=pltpu.CompilerParams(vmem_limit_bytes=VMEM_LIMIT),
        name="unpack",
    )(z, one, grads, *got)


def line_hop(block_up, block_down, n_dp, hop):
    up = [(i, i + 1) for i in range(hop - 1, n_dp - 1)]
    down = [(i + 1, i) for i in range(n_dp - hop)]
    return lax.ppermute(block_up, "dp", up), lax.ppermute(block_down, "dp", down)


def reduce_hop(grads, got, n_dp, hop, rows, before):
    place = lax.axis_index("dp")
    reach = n_dp - hop
    zero = jnp.int32(0)
    size = (1, rows[1] - rows[0], grads.shape[2])
    spots = (jnp.minimum(place + reach, n_dp - 1), jnp.maximum(place - reach, 0))
    if got is not None:
        got = lax.optimization_barrier((*got, *before))[:2]
    elif before:
        grads = after_of(grads, *before)
    blocks = [
        lax.dynamic_slice(grads, (spot.astype(jnp.int32), jnp.int32(rows[0]), zero), size)[0]
        for spot in spots
    ]
    if got is not None:
        blocks = [(b.astype(F32) + g.astype(F32)).astype(BF16) for b, g in zip(blocks, got)]
    up = [(i, i + 1) for i in range(hop)]
    down = [(i, i - 1) for i in range(n_dp - hop, n_dp)]
    sent = lax.ppermute(blocks[0], "dp", up), lax.ppermute(blocks[1], "dp", down)
    return sent, tuple(blocks)


def after_of(value, *others):
    return lax.optimization_barrier((value,) + others)[0]


def per_device(
    layer_input,
    doc_ids,
    route_ids,
    route_probs,
    attn_gain,
    ffn_gain,
    query_gain,
    key_gain,
    w_query,
    w_key,
    w_value,
    w_out,
    w_gate,
    w_up,
    w_down,
    out_grad,
):
    tokens, width = layer_input.shape[1:]
    n_dp = lax.axis_size("dp")
    n_ctx = lax.axis_size("ctx")
    ctx_index = lax.axis_index("ctx")
    length = tokens * n_ctx
    heads = HQ // n_ctx
    share = n_ctx // KV
    qw = heads * HD
    depth = w_query.shape[0]
    own_e = w_gate.shape[0]

    cut = attn_gain.shape[0]
    hcut = query_gain.shape[0]
    kinds = 2 * (cut + hcut)
    small = jnp.concatenate([attn_gain, ffn_gain, query_gain, key_gain]).astype(F32)
    small = jnp.pad(small, (0, 1024 - kinds)).reshape(8, HD)
    even = (jnp.arange(n_ctx) % 2 == 0)[None, :, None]
    wide = [jnp.repeat(w.reshape(depth, KV, HD), share, axis=1) for w in (w_key, w_value)]
    cols = jnp.concatenate(
        [w_query.reshape(depth, n_ctx, qw), jnp.where(even, wide[0], wide[1])], axis=2
    ).transpose(1, 0, 2)
    cols, small = prep(n_ctx, n_dp, cols, small)
    small = small.reshape(n_dp * n_ctx, 1024)
    gain_attn = small[:, :cut].reshape(1, width)
    gain_ffn = small[:, cut : 2 * cut].reshape(1, width)
    gain_query = small[:, 2 * cut : 2 * cut + hcut].reshape(1, HD)
    gain_key = small[:, 2 * cut + hcut : kinds].reshape(1, HD)
    wqkv = lax.all_gather(cols.reshape(n_ctx * depth, qw + HD), "dp", axis=0, tiled=True)
    wrows = lax.all_gather(w_out, "dp", axis=0, tiled=False)

    inputs = layer_input.reshape(tokens, width)
    top_own = out_grad.reshape(tokens, width)
    n_experts = own_e * n_ctx
    match = route_ids.reshape(1, tokens, TOP) == jnp.arange(n_experts, dtype=jnp.int32)[:, None, None]
    probs = jnp.sum(jnp.where(match, route_probs.reshape(1, tokens, TOP), 0.0), axis=2)
    info = jnp.concatenate(
        [probs, doc_ids.reshape(1, tokens).astype(F32), jnp.zeros((7, tokens), F32)], axis=0
    )
    normed, info, top_all = first(n_ctx, inputs, gain_attn, info, top_own)
    normed = normed.reshape(length, width)
    doc = info[:, n_experts].reshape(length).astype(jnp.int32)
    my_probs = lax.dynamic_slice_in_dim(info, ctx_index * own_e, own_e, 1)
    my_probs = my_probs.transpose(0, 2, 1).reshape(length, own_e)

    inverse = 1.0 / ROPE_BASE ** (jnp.arange(HD // 2, dtype=F32) * 2.0 / HD)
    angles = jnp.arange(length, dtype=F32)[:, None] * inverse[None, :]
    cosine = jnp.cos(angles)
    sine = jnp.sin(angles)
    cosine = jnp.concatenate([cosine, cosine], axis=1)
    sine = jnp.concatenate([-sine, sine], axis=1)
    qlin, klin, q, k, v, attn, total, wout = attn_forward(
        n_ctx, n_dp, normed, wqkv, cosine, sine, gain_query, gain_key, doc, wrows, tokens
    )
    wout = wout.reshape(qw, width)
    top_all = top_all.reshape(length, width)
    blocks = (n_ctx, tokens, width)
    after, normed2 = middle(n_ctx, attn, wout, inputs, gain_ffn)
    normed2 = normed2.reshape(length, width)

    z = lax.axis_index("dp").astype(jnp.int32).reshape(1)
    hidden = w_gate.shape[2]

    def run(e, sources, carried, low, grads):
        moe, rows_grad, grads = expert(
            z,
            normed2,
            top_all,
            my_probs[:, e : e + 1],
            n_dp,
            sources,
            carried,
            tokens,
            low,
            hidden,
            grads,
        )
        return (moe, rows_grad), grads

    cuts = [(0, 256), (256, hidden)]
    blocks0 = pack(cuts, w_gate[0], w_up[0], w_down[0])
    carried, grads0 = (), ()
    for index, (low, high) in enumerate(cuts):
        full = lax.all_gather(blocks0[index], "dp", axis=0, tiled=False)
        if index == 1:
            later = lax.optimization_barrier((w_gate[1], w_up[1], w_down[1], *carried))[:3]
            (block1,) = pack([(0, hidden)], *later)
            sources1 = [(block1, "up", 0, 0)]
            up = down = after_of(block1, full)
            up, down = line_hop(up, down, n_dp, 1)
            sources1 += [(up, "up", 1, 0), (down, "down", 1, 0)]
        carried, grads = run(0, [(full, "all", 0, 0)], carried, low, grads0)
        grads0 = (grads,)
    rows_all = 3 * (width // n_dp)
    spans = {"a": (0, rows_all // 2), "b": (rows_all // 2, rows_all)}
    got, before = {tag: None for tag in spans}, ()
    for hop in range(2, n_dp + 1):
        if hop < n_dp:
            up, down = line_hop(up, down, n_dp, hop)
            sources1 += [(up, "up", hop, 0), (down, "down", hop, 0)]
        for tag, rows in spans.items():
            got[tag], before = reduce_hop(grads, got[tag], n_dp, hop - 1, rows, before)
    (moe, rows_grad), grads1 = run(1, sources1, carried, 0, ())
    done1 = lax.psum_scatter(
        grads1.reshape(3 * width, hidden), "dp", scatter_dimension=0, tiled=True
    )
    mid, ffn_part, branch = turn(
        n_ctx, rows_grad.reshape(blocks), after, top_own, gain_ffn
    )
    branch = branch.reshape(length, width)

    out_w = dot(attn, branch, TN).astype(BF16).reshape(n_dp, qw // n_dp, width)
    dqkv, gains, out_w, layer_output = attn_backward(
        n_ctx,
        n_dp,
        out_w,
        moe.reshape(blocks),
        after,
        branch,
        wout,
        attn,
        total,
        q,
        k,
        v,
        qlin,
        klin,
        cosine,
        sine,
        gain_query,
        gain_key,
        doc,
        tokens,
    )
    qkv_w = dot(normed, dqkv, TN).astype(BF16)
    qkv_w = lax.psum_scatter(qkv_w, "dp", scatter_dimension=0, tiled=True)
    out_w = lax.psum_scatter(out_w.reshape(qw, width), "dp", scatter_dimension=0, tiled=True)
    out_w = out_w.astype(F32)
    input_grad, attn_part = last(n_ctx, dqkv, wqkv, inputs, mid, gain_attn)
    n_all = n_dp * n_ctx
    packed = jnp.concatenate(
        [
            attn_part[0].reshape(n_all, cut),
            ffn_part[0].reshape(n_all, cut),
            gains[0].reshape(n_all, hcut),
            gains[1].reshape(n_all, hcut),
            jnp.zeros((n_all, 1024 - kinds), F32),
        ],
        axis=1,
    )
    packed = packed.reshape(n_dp, n_ctx, 8, HD).transpose(1, 0, 2, 3)
    packed = gains_sum(n_ctx, n_dp, packed)
    packed = packed.reshape(1024)
    query_w, key_w, value_w = post(n_ctx, qkv_w.reshape(n_ctx, depth, qw + HD))
    gate_w, up_w, down_w = unpack(z, done1, grads, got["a"] + got["b"])
    return (
        layer_output.reshape(1, tokens, width),
        input_grad.reshape(1, tokens, width),
        packed[:cut],
        packed[cut : 2 * cut],
        packed[2 * cut : 2 * cut + hcut],
        packed[2 * cut + hcut : kinds],
        query_w,
        key_w,
        value_w,
        out_w,
        gate_w,
        up_w,
        down_w,
    )


def solution(mesh):
    both = ("dp", "ctx")
    seq = P("dp", "ctx", None)
    in_specs = (
        seq,
        P("dp", "ctx"),
        seq,
        seq,
        P(both),
        P(both),
        P(both),
        P(both),
        P(both, None),
        P(both, None),
        P(both, None),
        P(both, None),
        P("ctx", "dp", None),
        P("ctx", "dp", None),
        P("ctx", None, "dp"),
        seq,
    )
    out_specs = (
        seq,
        seq,
        P(both),
        P(both),
        P(both),
        P(both),
        P(both, None),
        P(both, None),
        P(both, None),
        P(both, None),
        P("ctx", "dp", None),
        P("ctx", "dp", None),
        P("ctx", None, "dp"),
    )

    return jax.shard_map(
        per_device, mesh=mesh, in_specs=in_specs, out_specs=out_specs, check_vma=False
    )
```

```python
import functools
import math

import jax
import jax.numpy as jnp
from jax import lax
from jax.experimental import pallas as pl
from jax.experimental.pallas import tpu as pltpu
from jax.sharding import PartitionSpec as P


HQ = 32
KV = 4
HD = 128
TOP = 8
MOST = 1024
EPS = 1e-06
ROPE_BASE = 1000000.0
F32 = jnp.float32
BF16 = jnp.bfloat16
SCALE = 1.0 / math.sqrt(HD)
SCALE2 = SCALE / math.log(2.0)
VMEM_LIMIT = 60 * 1024 * 1024


def dot(left, right, dims=((1,), (0,))):
    return lax.dot_general(left, right, (dims, ((), ())), preferred_element_type=F32)


NT = ((1,), (1,))
TN = ((0,), (0,))


def rms_parts(values):
    return lax.rsqrt(jnp.mean(values * values, axis=-1, keepdims=True) + EPS)


def rms_back(grad, unit, inv, gain):
    scaled = grad * gain
    return inv * (scaled - unit * jnp.mean(scaled * unit, axis=-1, keepdims=True))


def head_forward(lin, gain, cosine, sine):
    unit = lin * rms_parts(lin) * gain
    return unit * cosine + pltpu.roll(unit, HD // 2, 1) * sine


def head_backward(lin, gain, cosine, sine, rot_grad):
    grad = rot_grad * cosine + pltpu.roll(rot_grad * sine, HD // 2, 1)
    inv = rms_parts(lin)
    unit = lin * inv
    return rms_back(grad, unit, inv, gain), jnp.sum(grad * unit, axis=0, keepdims=True)


MESH = pl.DeviceIdType.MESH
ANY = pl.BlockSpec(memory_space=pl.ANY)
VM = pl.BlockSpec(memory_space=pltpu.VMEM)
DMA = pltpu.SemaphoreType.DMA
CHUNK = 32


def flip(index, mask, count):
    result, bit = 0, 1
    while bit < count:
        digit = (index // bit) % 2
        result = result + bit * ((1 - digit) if mask & bit else digit)
        bit *= 2
    return result


def push(src, dst, send, recv, axis, peer):
    return pltpu.make_async_remote_copy(
        src_ref=src,
        dst_ref=dst,
        send_sem=send,
        recv_sem=recv,
        device_id={axis: peer},
        device_id_type=MESH,
    )


def meet(peers):
    barrier = pltpu.get_barrier_semaphore()
    for axis, peer in peers:
        pl.semaphore_signal(barrier, inc=1, device_id={axis: peer}, device_id_type=MESH)
    pl.semaphore_wait(barrier, len(peers))


class Plane:
    def __init__(self, n):
        self.chips = n // 2
        self.me = lax.axis_index("ctx")
        self.core = self.me % 2
        self.chip = self.me // 2
        self.mate = self.me + 1 - 2 * self.core

    def same(self, s):
        return 2 * flip(self.chip, s, self.chips) + self.core

    def meet(self):
        meet([("ctx", self.same(s)) for s in range(1, self.chips)] + [("ctx", self.mate)])


def far_first(chips):
    return sorted(range(1, chips), key=lambda s: -bin(s).count("1"))


class Gather:
    def __init__(self, plane, src, out, send, recv, local):
        self.plane, self.out, self.send, self.recv = plane, out, send, recv
        self.own = pltpu.make_async_copy(src, out.at[plane.me], local)
        self.far = [
            push(src, out.at[plane.me], send.at[s], recv.at[s], "ctx", plane.same(s))
            for s in far_first(plane.chips)
        ]
        self.near = push(src, out.at[plane.me], send.at[0], recv.at[0], "ctx", plane.mate)

    def start(self):
        for copy in self.far:
            copy.start()
        self.near.start()
        self.own.start()

    def forward(self):
        plane, out = self.plane, self.out
        self.passed = []
        for s in sorted(range(1, plane.chips), key=lambda s: bin(s).count("1")):
            block = out.at[plane.same(s)]
            push(block, block, self.send.at[s], self.recv.at[s], "ctx", plane.mate).wait_recv()
            slot = plane.chips + s
            copy = push(block, block, self.send.at[slot], self.recv.at[slot], "ctx", plane.mate)
            copy.start()
            self.passed.append(copy)

    def finish(self):
        for copy in self.far:
            copy.wait_send()
        self.near.wait_send()
        self.near.wait_recv()
        for copy in self.passed:
            copy.wait_send()
            copy.wait_recv()
        self.own.wait()


def by_rows(rows, body):
    def one(index, carry):
        body(pl.ds(pl.multiple_of(index * CHUNK, CHUNK), CHUNK))
        return carry

    lax.fori_loop(0, rows // CHUNK, one, 0)


class SquareGather:
    def __init__(self, plane, src, out, send, recv, local):
        self.plane, self.out, self.send, self.recv = plane, out, send, recv
        half = src.shape[0] // 2
        self.halves = [pl.ds(0, half), pl.ds(half, half)]
        mine = out.at[plane.me]
        self.own = pltpu.make_async_copy(src, mine, local)
        self.near = push(src, mine, send.at[0], recv.at[0], "ctx", plane.mate)
        self.far = []
        for s, h in ((1, 0), (2, 1), (1, 1), (2, 0)):
            part, slot = self.halves[h], 2 * s + h
            self.far.append(
                push(
                    src.at[part, :],
                    mine.at[part, :],
                    send.at[slot],
                    recv.at[slot],
                    "ctx",
                    plane.same(s),
                )
            )

    def start(self):
        for copy in self.far:
            copy.start()
        self.near.start()
        self.own.start()

    def arrived(self, s, h):
        block = self.out.at[self.plane.same(s)].at[self.halves[h], :]
        slot = 2 * s + h
        push(block, block, self.send.at[slot], self.recv.at[slot], "ctx", self.plane.mate).wait_recv()
        return block

    def forward(self):
        plane = self.plane
        self.passed = []
        for s, h in ((1, 0), (2, 1)):
            block = self.arrived(s, h)
            slot = 6 + h
            copy = push(block, block, self.send.at[slot], self.recv.at[slot], "ctx", plane.same(3 - s))
            copy.start()
            self.far.append(copy)
        for s in (1, 2, 3):
            if s < 3:
                self.arrived(s, 2 - s)
            else:
                self.arrived(3, 0)
                self.arrived(3, 1)
            block, slot = self.out.at[plane.same(s)], 7 + s
            copy = push(block, block, self.send.at[slot], self.recv.at[slot], "ctx", plane.mate)
            copy.start()
            self.passed.append(copy)

    def finish(self):
        for copy in self.far:
            copy.wait_send()
        self.near.wait_send()
        self.near.wait_recv()
        for copy in self.passed:
            copy.wait_send()
            copy.wait_recv()
        self.own.wait()


def gather_of(plane, src, out, send, recv, local):
    kind = SquareGather if plane.chips == 4 else Gather
    return kind(plane, src, out, send, recv, local)


class Spread:
    def __init__(self, plane, mine, landed, send, recv):
        self.plane, self.mine, self.landed = plane, mine, landed
        self.square = plane.chips == 4
        self.order = [3, 1, 2, 0] if self.square else far_first(plane.chips) + [0]
        self.send, self.recv = send, recv
        half = mine.shape[1] // 2
        self.halves = [pl.ds(0, half), pl.ds(half, half)]

    def copy(self, s, h, to):
        part, slot = self.halves[h], 2 * s + h
        return push(
            self.mine.at[s].at[part, :],
            self.landed.at[s].at[part, :],
            self.send.at[slot],
            self.recv.at[slot],
            "ctx",
            self.plane.same(to),
        )

    def go(self, s, h, to):
        self.copy(s, h, to).start()

    def ready(self, s):
        if self.square:
            if s == 3:
                self.go(3, 0, 1)
                self.go(3, 1, 2)
            elif s == 1:
                self.go(1, 0, 1)
            elif s == 2:
                self.go(2, 1, 2)
        elif s:
            push(
                self.mine.at[s],
                self.landed.at[s],
                self.send.at[s],
                self.recv.at[s],
                "ctx",
                self.plane.same(s),
            ).start()

    def sends(self):
        if self.square:
            hops = ((3, 0, 1), (3, 1, 2), (1, 0, 1), (2, 1, 2), (2, 0, 2), (1, 1, 1))
            return [self.copy(*hop) for hop in hops]
        return [
            push(
                self.mine.at[s],
                self.landed.at[s],
                self.send.at[s],
                self.recv.at[s],
                "ctx",
                self.plane.same(s),
            )
            for s in self.order
            if s
        ]

    def relay(self):
        mine, landed = self.mine, self.landed
        half = mine.shape[1] // 2
        if not self.square:
            return
        for s, h in ((2, 0), (1, 1)):
            self.copy(3, h, 1).wait_recv()

            def add(at, s=s, h=h):
                rows = pl.ds(h * half + at.start, CHUNK)
                total = mine[s, rows, :].astype(F32) + landed[3, rows, :].astype(F32)
                mine[s, rows, :] = total.astype(BF16)

            by_rows(half, add)
            self.copy(s, h, s).start()

    def gathered(self):
        if not self.square:
            for copy in self.sends():
                copy.wait_recv()
            return
        for s in (1, 2):
            for h in (0, 1):
                self.copy(s, h, s).wait_recv()

    def settle(self, extra=None):
        self.relay()
        if extra is not None:
            extra()
        self.gathered()

    def total(self, at):
        value = self.mine[0, at, :].astype(F32)
        for s in (1, 2) if self.square else range(1, self.plane.chips):
            value = value + self.landed[s, at, :].astype(F32)
        return value

    def finish(self):
        for copy in self.sends():
            copy.wait_send()


class Scatter:
    def __init__(self, plane, part, mine, other, landed, send, recv, send2, recv2, local):
        self.plane, self.mine, self.other = plane, mine, other
        self.spread = Spread(plane, mine, landed, send2, recv2)
        self.order = self.spread.order
        self.loads, self.across = {}, {}
        for s in self.order:
            block = plane.same(s)
            self.loads[s] = pltpu.make_async_copy(part.at[block], mine.at[s], local.at[s])
            self.across[s] = push(
                part.at[block + 1 - 2 * plane.core],
                other.at[s],
                send.at[s],
                recv.at[s],
                "ctx",
                plane.mate,
            )

    def start(self):
        for s in self.order:
            self.across[s].start()
            self.loads[s].start()

    def pairs(self):
        mine, other = self.mine, self.other
        for s in self.order:
            self.loads[s].wait()
            self.across[s].wait_recv()

            def add(at, s=s):
                total = mine[s, at, :].astype(F32) + other[s, at, :].astype(F32)
                mine[s, at, :] = total.astype(BF16)

            by_rows(mine.shape[1], add)
            self.spread.ready(s)

    def run(self):
        self.pairs()
        self.spread.settle()

    def total(self, at):
        return self.spread.total(at)

    def finish(self):
        for s in self.order:
            self.across[s].wait_send()
        self.spread.finish()


class Product:
    def __init__(self, plane, value, mine, other, landed, given, send, recv, send2, recv2):
        self.plane, self.value = plane, value
        self.mine, self.other, self.given = mine, other, given
        self.spread = Spread(plane, mine, landed, send2, recv2)
        self.order = self.spread.order
        self.across = {
            s: push(given.at[s], other.at[s], send.at[s], recv.at[s], "ctx", plane.mate)
            for s in self.order
        }

    def start(self):
        plane = self.plane
        for s in self.order:
            block = plane.same(s) + 1 - 2 * plane.core

            def fill(at, s=s, block=block):
                self.given[s, :, at] = self.value(block, at).astype(BF16)

            by_cols(self.mine.shape[2], fill)
            self.across[s].start()

    def run(self, extra=None):
        plane, mine, other = self.plane, self.mine, self.other
        for s in self.order:
            block = plane.same(s)
            self.across[s].wait_recv()

            def fill(at, s=s, block=block):
                total = self.value(block, at) + other[s, :, at].astype(F32)
                mine[s, :, at] = total.astype(BF16)

            by_cols(mine.shape[2], fill)
            self.spread.ready(s)
        self.spread.settle(extra)

    total = Scatter.total
    finish = Scatter.finish


def by_cols(width, body):
    span = 512

    def one(index, carry):
        body(pl.ds(pl.multiple_of(index * span, span), span))
        return carry

    lax.fori_loop(0, width // span, one, 0)


def gather_sems(n):
    return [DMA((12 if n == 8 else n,)), DMA((12 if n == 8 else n,)), DMA(())]


def scatter_scratch(n, rows, width):
    chips = n // 2
    return (
        [pltpu.VMEM((chips, rows, width), BF16)] * 3
        + [DMA((chips,)), DMA((chips,)), DMA((n,)), DMA((n,))]
        + [DMA((chips,))]
    )


def product_scratch(n, rows, width):
    chips = n // 2
    return [pltpu.VMEM((chips, rows, width), BF16)] * 4 + [
        DMA((chips,)),
        DMA((chips,)),
        DMA((n,)),
        DMA((n,)),
    ]


def comm_call(kernel, ident, outs, out_specs, in_specs, scratch, micros, *args):
    return pl.pallas_call(
        kernel,
        out_shape=outs,
        in_specs=in_specs,
        out_specs=out_specs,
        scratch_shapes=scratch,
        compiler_params=pltpu.CompilerParams(
            collective_id=ident, has_side_effects=True, vmem_limit_bytes=VMEM_LIMIT
        ),
        cost_estimate=pl.CostEstimate(
            flops=0, transcendentals=0, bytes_accessed=int(micros * 3.0e6)
        ),
    )(*args)


def swap_all(n, src, out, send, recv, local):
    me = lax.axis_index("ctx")
    own = pltpu.make_async_copy(src.at[me], out.at[me], local)
    own.start()
    copies = []
    for s in range(n - 1, 0, -1):
        peer = flip(me, s, n)
        copies.append(push(src.at[peer], out.at[me], send.at[s], recv.at[s], "ctx", peer))
        copies[-1].start()
    return own, copies


class RowSwap:
    def __init__(self, n, n_dp, src, dst, send, recv, spread):
        self.me = lax.axis_index("ctx")
        self.dst, self.send, self.recv, self.n_dp = dst, send, recv, n_dp
        self.entries = []
        for k in range(n_dp):
            flat = self.me * n_dp + k if spread else k * n + self.me
            peer = flat % n if spread else flat // n_dp
            slot = flat // n if spread else flat % n_dp
            far = push(src.at[k], dst.at[slot], send.at[k], recv.at[slot], "ctx", peer)
            near = pltpu.make_async_copy(src.at[k], dst.at[slot], recv.at[slot])
            self.entries.append((peer, far, near))

    def start(self):
        for peer, far, near in self.entries:
            pl.when(peer != self.me)(far.start)
            pl.when(peer == self.me)(near.start)

    def arrive(self):
        for slot in range(self.n_dp):
            block = self.dst.at[slot]
            pltpu.make_async_copy(block, block, self.recv.at[slot]).wait()

    def finish(self):
        for peer, far, near in self.entries:
            pl.when(peer != self.me)(far.wait_send)


def meet_all(n):
    me = lax.axis_index("ctx")
    meet([("ctx", flip(me, s, n)) for s in range(1, n)])


class Pack:
    def __init__(self, e, sources, buffers, sems):
        self.buffers = buffers
        self.loads = [
            pltpu.make_async_copy(source.at[e], buffer, sems.at[k])
            for k, (source, buffer) in enumerate(zip(sources, buffers))
        ]

    def start(self):
        for load in self.loads:
            load.start()

    def write(self, cuts, outs):
        for load in self.loads:
            load.wait()
        gate, up, down = self.buffers
        cut = gate.shape[0]
        for (low, high), out in zip(cuts, outs):
            out[:cut, :] = gate[:, low:high]
            out[cut : 2 * cut, :] = up[:, low:high]
            out[2 * cut :, :] = jnp.transpose(down[low:high, :].astype(F32)).astype(BF16)


def pack_scratch(weights):
    return [pltpu.VMEM(w.shape[1:], BF16) for w in weights] + [DMA((3,))]


def pack_shapes(cuts, weights):
    cut = weights[0].shape[1]
    return [jax.ShapeDtypeStruct((3 * cut, high - low), BF16) for low, high in cuts]


def prep_kernel(n, n_dp, cuts, cols_ref, small_ref, *rest):
    sources, rest = rest[:3], rest[3:]
    out_ref, all_ref, rest = rest[0], rest[1], rest[2:]
    packed, rest = rest[: len(cuts)], rest[len(cuts) :]
    pack = Pack(0, sources, rest[:3], rest[3])
    pack.start()
    send, recv, local, gsend, grecv, zsend, zrecv = rest[4:]
    me, row = lax.axis_index("ctx"), lax.axis_index("dp")
    meet(
        [("ctx", flip(me, s, n)) for s in range(1, n)]
        + [("dp", flip(row, s, n_dp)) for s in range(1, n_dp)]
    )
    all_ref[row, me] = small_ref[...]
    smalls = []
    for s in range(1, n):
        peer = flip(me, s, n)
        smalls.append(push(small_ref, all_ref.at[row, me], gsend.at[s], grecv.at[s], "ctx", peer))
        smalls[-1].start()
    own, copies = swap_all(n, cols_ref, out_ref, send, recv, local)
    pack.write(cuts, packed)
    for copy in smalls:
        copy.wait_recv()
    planes = []
    for s in range(1, n_dp):
        peer = flip(row, s, n_dp)
        planes.append(push(all_ref.at[row], all_ref.at[row], zsend.at[s], zrecv.at[s], "dp", peer))
        planes[-1].start()
    for copy in copies + planes:
        copy.wait_recv()
    for copy in copies + planes + smalls:
        copy.wait_send()
    own.wait()


class Gains:
    def __init__(self, n, n_dp, small, landed, mid, second, gsend, grecv, zsend, zrecv):
        self.me, self.row = lax.axis_index("ctx"), lax.axis_index("dp")
        self.small, self.landed, self.mid, self.second = small, landed, mid, second
        self.near, self.far = [], []
        for s in range(1, n):
            peer = flip(self.me, s, n)
            self.near.append(push(small.at[peer], landed.at[s], gsend.at[s], grecv.at[s], "ctx", peer))
        for s in range(1, n_dp):
            peer = flip(self.row, s, n_dp)
            self.far.append(push(mid.at[peer], second.at[s], zsend.at[s], zrecv.at[s], "dp", peer))

    def start(self):
        for copy in self.near:
            copy.start()

    def middle(self):
        value = self.small[self.me]
        for s, copy in enumerate(self.near, 1):
            copy.wait_recv()
            value = value + self.landed[s]
        self.mid[...] = value
        for copy in self.far:
            copy.start()

    def finish(self):
        value = self.mid[self.row]
        for s, copy in enumerate(self.far, 1):
            copy.wait_recv()
            value = value + self.second[s]
        for copy in self.near + self.far:
            copy.wait_send()
        return value


def post_kernel(n, src_ref, query_ref, key_ref, value_ref, blocks, send, recv, local):
    me = lax.axis_index("ctx")
    meet([("ctx", flip(me, s, n)) for s in range(1, n)])
    own, copies = swap_all(n, src_ref, blocks, send, recv, local)
    for copy in copies:
        copy.wait_recv()
    own.wait()
    share = n // KV
    qw = HQ * HD // n
    for c in range(n):
        query_ref[:, c * qw : (c + 1) * qw] = blocks[c, :, :qw].astype(F32)
    for g in range(KV):
        for out, kind in ((key_ref, 0), (value_ref, 1)):
            total = blocks[g * share + kind, :, qw:].astype(F32)
            for c in range(2 + kind, share, 2):
                total = total + blocks[g * share + c, :, qw:].astype(F32)
            out[:, g * HD : (g + 1) * HD] = total
    for copy in copies:
        copy.wait_send()


def swap_sems(n, n_dp):
    return [DMA((n,)), DMA((n,)), DMA(()), DMA((n,)), DMA((n,)), DMA((n_dp,)), DMA((n_dp,))]


def prep(n, n_dp, cols, small, cuts, weights):
    shape = jax.ShapeDtypeStruct
    return comm_call(
        functools.partial(prep_kernel, n, n_dp, cuts),
        0,
        [shape(cols.shape, cols.dtype), shape((n_dp, n) + small.shape, F32)]
        + pack_shapes(cuts, weights),
        [ANY, VM] + [VM] * len(cuts),
        [ANY, VM, ANY, ANY, ANY],
        pack_scratch(weights) + swap_sems(n, n_dp),
        8,
        cols,
        small,
        *weights,
    )


def post(n, cols):
    shape = jax.ShapeDtypeStruct
    depth = cols.shape[1]
    return comm_call(
        functools.partial(post_kernel, n),
        1,
        [
            shape((depth, HQ * HD), F32),
            shape((depth, KV * HD), F32),
            shape((depth, KV * HD), F32),
        ],
        [VM] * 3,
        [VM],
        [pltpu.VMEM(cols.shape, BF16), DMA((n,)), DMA((n,)), DMA(())],
        10,
        cols,
    )


def first_kernel(
    n, cuts, x_ref, gain_ref, info_ref, grad_ref, *rest
):
    sources, rest = rest[:3], rest[3:]
    nall_ref, iall_ref, gall_ref, rest = rest[0], rest[1], rest[2], rest[3:]
    packed, rest = rest[: len(cuts)], rest[len(cuts) :]
    pack = Pack(1, sources, rest[:3], rest[3])
    low, sems = rest[4], rest[5:]
    pack.start()
    plane = Plane(n)
    plane.meet()
    infos = Gather(plane, info_ref, iall_ref, *sems[0:3])
    infos.start()

    def norm(at):
        value = x_ref[at, :].astype(F32)
        low[at, :] = (value * rms_parts(value) * gain_ref[...]).astype(BF16)

    by_rows(x_ref.shape[0], norm)
    normed = gather_of(plane, low, nall_ref, *sems[3:6])
    normed.start()
    grads = gather_of(plane, grad_ref, gall_ref, *sems[6:9])
    grads.start()
    pack.write(cuts, packed)
    infos.forward()
    normed.forward()
    grads.forward()
    infos.finish()
    normed.finish()
    grads.finish()


def first(n, x, gain, info, grad, cuts, weights):
    shape = jax.ShapeDtypeStruct
    many = lambda array, kind: shape((n,) + array.shape, kind)
    return comm_call(
        functools.partial(first_kernel, n, cuts),
        2,
        [many(x, BF16), many(info, F32), many(grad, BF16)] + pack_shapes(cuts, weights),
        [ANY] * 3 + [VM] * len(cuts),
        [VM] * 4 + [ANY] * 3,
        pack_scratch(weights)
        + [pltpu.VMEM(x.shape, BF16)]
        + [DMA((n,)), DMA((n,)), DMA(())]
        + gather_sems(n)
        + gather_sems(n),
        90,
        x,
        gain,
        info,
        grad,
        *weights,
    )


def middle_kernel(
    n, attn_ref, wout_ref, x_ref, gain_ref, after_ref, all_ref, low, *scratch
):
    plane = Plane(n)
    plane.meet()
    rows = x_ref.shape[0]

    def value(block, at):
        left = attn_ref[pl.ds(pl.multiple_of(block * rows, rows), rows), :]
        return dot(left, wout_ref[:, at])

    sums = Product(plane, value, *scratch[:8])
    sums.start()
    sums.run()

    def norm(at):
        value = x_ref[at, :].astype(F32) + sums.total(at)
        after_ref[at, :] = value
        low[at, :] = (value * rms_parts(value) * gain_ref[...]).astype(BF16)

    by_rows(rows, norm)
    normed = gather_of(plane, low, all_ref, *scratch[8:])
    normed.start()
    normed.forward()
    sums.finish()
    normed.finish()


def middle(n, attn, wout, x, gain):
    shape = jax.ShapeDtypeStruct
    return comm_call(
        functools.partial(middle_kernel, n),
        3,
        [shape(x.shape, F32), shape((n,) + x.shape, BF16)],
        [VM, ANY],
        [VM, VM, VM, VM],
        [pltpu.VMEM(x.shape, BF16)]
        + product_scratch(n, *x.shape)
        + gather_sems(n),
        105,
        attn,
        wout,
        x,
        gain,
    )


def turn_kernel(
    n, part_ref, after_ref, grad_ref, gain_ref, mid_ref, fpart_ref, all_ref, low, *scratch
):
    plane = Plane(n)
    plane.meet()
    sums = Scatter(plane, part_ref, *scratch[:8])
    sums.start()
    fpart_ref[...] = jnp.zeros_like(fpart_ref)
    sums.run()

    def norm(at):
        value = after_ref[at, :]
        inv = rms_parts(value)
        unit = value * inv
        grad = sums.total(at)
        fpart_ref[0:1, :] += jnp.sum(grad * unit, axis=0, keepdims=True)
        mid = grad_ref[at, :].astype(F32) + rms_back(grad, unit, inv, gain_ref[...])
        mid_ref[at, :] = mid
        low[at, :] = mid.astype(BF16)

    by_rows(after_ref.shape[0], norm)
    branch = gather_of(plane, low, all_ref, *scratch[8:])
    branch.start()
    branch.forward()
    sums.finish()
    branch.finish()


def turn(n, part, after, grad, gain):
    shape = jax.ShapeDtypeStruct
    return comm_call(
        functools.partial(turn_kernel, n),
        4,
        [
            shape(after.shape, F32),
            shape((8, after.shape[1]), F32),
            shape((n,) + after.shape, BF16),
        ],
        [VM, VM, ANY],
        [ANY, VM, VM, VM],
        [pltpu.VMEM(after.shape, BF16)] + scatter_scratch(n, *after.shape) + gather_sems(n),
        95,
        part,
        after,
        grad,
        gain,
    )


def last_kernel(n, grad_ref, wqkv_ref, x_ref, mid_ref, gain_ref, out_ref, apart_ref, *scratch):
    plane = Plane(n)
    plane.meet()
    apart_ref[...] = jnp.zeros_like(apart_ref)
    rows = x_ref.shape[0]

    def value(block, at):
        left = grad_ref[pl.ds(pl.multiple_of(block * rows, rows), rows), :]
        return dot(left, wqkv_ref[at, :], NT)

    sums = Product(plane, value, *scratch[:8])
    sums.start()
    sums.run()

    def norm(at):
        value = x_ref[at, :].astype(F32)
        inv = rms_parts(value)
        unit = value * inv
        grad = sums.total(at)
        apart_ref[0:1, :] += jnp.sum(grad * unit, axis=0, keepdims=True)
        out_ref[at, :] = mid_ref[at, :] + rms_back(grad, unit, inv, gain_ref[...])

    by_rows(rows, norm)
    sums.finish()


def last(n, grad, wqkv, x, mid, gain):
    shape = jax.ShapeDtypeStruct
    return comm_call(
        functools.partial(last_kernel, n),
        5,
        [shape(mid.shape, F32), shape((8, mid.shape[1]), F32)],
        [VM, VM],
        [VM] * 5,
        product_scratch(n, *mid.shape),
        60,
        grad,
        wqkv,
        x,
        mid,
        gain,
    )


def gains_kernel(n, n_dp, small_ref, sum_ref, *scratch):
    meet(
        [("ctx", flip(lax.axis_index("ctx"), s, n)) for s in range(1, n)]
        + [("dp", flip(lax.axis_index("dp"), s, n_dp)) for s in range(1, n_dp)]
    )
    gains = Gains(n, n_dp, small_ref, *scratch)
    gains.start()
    gains.middle()
    sum_ref[...] = gains.finish()


def gains_sum(n, n_dp, small):
    tile = small.shape[2:]
    return comm_call(
        functools.partial(gains_kernel, n, n_dp),
        8,
        jax.ShapeDtypeStruct(tile, F32),
        VM,
        [VM],
        [
            pltpu.VMEM((n, n_dp) + tile, F32),
            pltpu.VMEM((n_dp,) + tile, F32),
            pltpu.VMEM((n_dp,) + tile, F32),
            DMA((n,)),
            DMA((n,)),
            DMA((n_dp,)),
            DMA((n_dp,)),
        ],
        10,
        small,
    )


def attn_forward_kernel(
    n,
    n_dp,
    heads,
    back,
    normed_ref,
    wqkv_ref,
    cos_ref,
    sin_ref,
    qgain_ref,
    kgain_ref,
    docc_ref,
    docr_ref,
    rows_ref,
    qlin_ref,
    klin_ref,
    q_ref,
    k_ref,
    v_ref,
    attn_ref,
    total_ref,
    wout_ref,
    acc_ref,
    sum_ref,
    mate_ref,
    *sems,
):
    step = pl.program_id(0)

    @pl.when(step == 0)
    def _():
        meet_all(n)
        copy = push(
            wqkv_ref.at[:, pl.ds(heads * HD, HD)],
            mate_ref,
            sems[2],
            sems[3],
            "ctx",
            Plane(n).mate,
        )
        copy.start()
        RowSwap(n, n_dp, rows_ref, wout_ref, *sems[:2], False).start()
        copy.wait_recv()
        copy.wait_send()

    rows = normed_ref.shape[0]
    lin = dot(normed_ref[...], wqkv_ref[...])
    here = pl.ds(step * rows, rows)
    cosine = cos_ref[...]
    sine = sin_ref[...]
    qw = heads * HD
    for head in range(heads):
        cols = slice(head * HD, (head + 1) * HD)
        part = lin[:, cols]
        qlin_ref[:, cols] = part
        q_ref[:, cols] = head_forward(part, qgain_ref[...], cosine, sine).astype(BF16)
    own = lin[:, qw:]
    other = dot(normed_ref[...], mate_ref[...])
    first_core = lax.axis_index("ctx") % 2 == 0
    key_lin = jnp.where(first_core, own, other)
    klin_ref[...] = key_lin
    k_ref[here, :] = head_forward(key_lin, kgain_ref[...], cosine, sine).astype(BF16)
    v_ref[here, :] = jnp.where(first_core, other, own).astype(BF16)
    acc_ref[...] = jnp.zeros_like(acc_ref)
    sum_ref[...] = jnp.zeros_like(sum_ref)
    row_pos = step * rows + lax.broadcasted_iota(jnp.int32, (rows, rows), 0)
    col_off = lax.broadcasted_iota(jnp.int32, (rows, rows), 1)

    def one(block, carry):
        at = pl.ds(pl.multiple_of(block * rows, rows), rows)
        key = k_ref[at, :]
        val = v_ref[at, :]
        allowed = (docc_ref[...] == docr_ref[:, at]) & (block * rows + col_off <= row_pos)
        for head in range(heads):
            cols = slice(head * HD, (head + 1) * HD)
            score = dot(q_ref[:, cols], key, NT) * SCALE2
            expo = jnp.where(allowed, jnp.exp2(score), 0.0)
            folded = expo[:, :HD]
            for piece in range(1, rows // HD):
                folded = folded + expo[:, piece * HD : (piece + 1) * HD]
            sum_ref[:, cols] += folded
            acc_ref[:, cols] += dot(expo.astype(BF16), val)
        return carry

    lax.fori_loop(jnp.maximum(step - back, 0), step + 1, one, 0)
    lane = lax.broadcasted_iota(jnp.int32, (rows, HD), 1)
    totals = jnp.ones((rows, HD), F32)
    for head in range(heads):
        cols = slice(head * HD, (head + 1) * HD)
        total = jnp.sum(sum_ref[:, cols], axis=-1, keepdims=True)
        totals = jnp.where(lane == head, total, totals)
        attn_ref[:, cols] = (acc_ref[:, cols] / total).astype(BF16)
    total_ref[...] = totals

    @pl.when(step == pl.num_programs(0) - 1)
    def _():
        swap = RowSwap(n, n_dp, rows_ref, wout_ref, *sems[:2], False)
        swap.arrive()
        swap.finish()


def attn_forward(n, n_dp, normed, wqkv, cosine, sine, qgain, kgain, doc, wrows, rows):
    length, width = normed.shape
    qw = wqkv.shape[1] - HD
    heads = qw // HD
    blk = lambda cols: pl.BlockSpec((rows, cols), lambda i: (i, 0))
    whole = lambda shape: pl.BlockSpec(shape, lambda i: (0, 0))
    shape = jax.ShapeDtypeStruct
    return pl.pallas_call(
        functools.partial(attn_forward_kernel, n, n_dp, heads, MOST // rows),
        grid=(length // rows,),
        in_specs=[
            blk(width),
            whole(wqkv.shape),
            blk(HD),
            blk(HD),
            whole((1, HD)),
            whole((1, HD)),
            blk(1),
            whole((1, length)),
            ANY,
        ],
        out_specs=[
            blk(qw),
            blk(HD),
            blk(qw),
            whole((length, HD)),
            whole((length, HD)),
            blk(qw),
            blk(HD),
            ANY,
        ],
        out_shape=[
            shape((length, qw), F32),
            shape((length, HD), F32),
            shape((length, qw), BF16),
            shape((length, HD), BF16),
            shape((length, HD), BF16),
            shape((length, qw), BF16),
            shape((length, HD), F32),
            shape(wrows.shape, BF16),
        ],
        scratch_shapes=[
            pltpu.VMEM((rows, qw), F32),
            pltpu.VMEM((rows, qw), F32),
            pltpu.VMEM((width, HD), BF16),
        ]
        + [DMA((n_dp,)), DMA((n_dp,)), DMA(()), DMA(())],
        compiler_params=pltpu.CompilerParams(
            collective_id=7, has_side_effects=True, vmem_limit_bytes=VMEM_LIMIT
        ),
        cost_estimate=pl.CostEstimate(
            flops=35 * 10**9, transcendentals=0, bytes_accessed=30 * 2**20
        ),
        name="attn_forward",
    )(normed, wqkv, cosine, sine, qgain, kgain, doc[:, None], doc[None, :], wrows)


def attn_backward_kernel(
    n,
    n_dp,
    heads,
    back,
    branch_ref,
    wout_ref,
    attn_ref,
    total_ref,
    q_ref,
    k_ref,
    v_ref,
    qlin_ref,
    klin_ref,
    cos_ref,
    sin_ref,
    qgain_ref,
    kgain_ref,
    docc_ref,
    docr_ref,
    wgrad_ref,
    moe_ref,
    after_ref,
    dqkv_ref,
    gains_ref,
    swapped_ref,
    final_ref,
    dk_ref,
    dv_ref,
    dqa_ref,
    give_ref,
    take_ref,
    *sems,
):
    step = pl.program_id(0)

    steps = pl.num_programs(0)

    def scatter():
        return Scatter(Plane(n), moe_ref, *sems[2:10])

    @pl.when(step == 0)
    def _():
        meet_all(n)
        scatter().start()
        RowSwap(n, n_dp, wgrad_ref, swapped_ref, *sems[:2], True).start()

    @pl.when(step == 2)
    def _():
        scatter().pairs()

    @pl.when(step == steps - 2)
    def _():
        scatter().spread.relay()

    rows = branch_ref.shape[0]
    here = pl.ds(pl.multiple_of(step * rows, rows), rows)

    @pl.when(step == 0)
    def _():
        gains_ref[...] = jnp.zeros_like(gains_ref)

    dk_ref[here, :] = jnp.zeros((rows, HD), F32)
    dv_ref[here, :] = jnp.zeros((rows, HD), F32)
    dqa_ref[...] = jnp.zeros_like(dqa_ref)
    attn_grad = dot(branch_ref[...], wout_ref[...], NT)
    grads = []
    shifts = []
    for head in range(heads):
        cols = slice(head * HD, (head + 1) * HD)
        part = attn_grad[:, cols]
        inv_total = 1.0 / total_ref[:, head : head + 1]
        delta = jnp.sum(part * attn_ref[:, cols].astype(F32), axis=-1, keepdims=True)
        grads.append((part * inv_total).astype(BF16))
        shifts.append(delta * inv_total)
    row_pos = step * rows + lax.broadcasted_iota(jnp.int32, (rows, rows), 0)
    col_off = lax.broadcasted_iota(jnp.int32, (rows, rows), 1)

    def one(block, carry):
        at = pl.ds(pl.multiple_of(block * rows, rows), rows)
        key = k_ref[at, :]
        val = v_ref[at, :]
        allowed = (docc_ref[...] == docr_ref[:, at]) & (block * rows + col_off <= row_pos)
        dk = jnp.zeros((rows, HD), F32)
        dv = jnp.zeros((rows, HD), F32)
        for head in range(heads):
            cols = slice(head * HD, (head + 1) * HD)
            query = q_ref[:, cols]
            score = dot(query, key, NT) * SCALE2
            expo = jnp.where(allowed, jnp.exp2(score), 0.0)
            prod = dot(grads[head], val, NT)
            score_grad = (expo * (prod - shifts[head])).astype(BF16)
            dv += dot(expo.astype(BF16), grads[head], TN)
            dk += dot(score_grad, query, TN)
            dqa_ref[:, cols] += dot(score_grad, key)
        dk_ref[at, :] += dk
        dv_ref[at, :] += dv
        return carry

    lax.fori_loop(jnp.maximum(step - back, 0), step + 1, one, 0)
    cosine = cos_ref[here, :]
    sine = sin_ref[here, :]
    for head in range(heads):
        cols = slice(head * HD, (head + 1) * HD)
        grad, gain_part = head_backward(
            qlin_ref[:, cols], qgain_ref[...], cosine, sine, dqa_ref[:, cols] * SCALE
        )
        dqkv_ref[here, cols] = grad.astype(BF16)
        gains_ref[0:1, :] += gain_part

    @pl.when(step == pl.num_programs(0) - 1)
    def _():
        def finish(block, carry):
            at = pl.ds(pl.multiple_of(block * rows, rows), rows)
            grad, gain_part = head_backward(
                klin_ref[at, :], kgain_ref[...], cos_ref[at, :], sin_ref[at, :], dk_ref[at, :] * SCALE
            )
            first_core = lax.axis_index("ctx") % 2 == 0
            dk_ref[at, :] = jnp.where(first_core, grad, dv_ref[at, :])
            give_ref[at, :] = jnp.where(first_core, dv_ref[at, :], grad).astype(BF16)
            gains_ref[1:2, :] += gain_part
            return carry

        lax.fori_loop(0, pl.num_programs(0), finish, 0)
        trade = push(give_ref, take_ref, sems[10], sems[11], "ctx", Plane(n).mate)
        trade.start()
        sums = scatter()
        sums.spread.gathered()

        def add(at):
            final_ref[at, :] = (after_ref[at, :] + sums.total(at)).astype(BF16)

        by_rows(rows, add)
        sums.finish()
        trade.wait_recv()

        def join(block, carry):
            at = pl.ds(pl.multiple_of(block * rows, rows), rows)
            total = dk_ref[at, :] + take_ref[at, :].astype(F32)
            dqkv_ref[at, heads * HD :] = total.astype(BF16)
            return carry

        lax.fori_loop(0, pl.num_programs(0), join, 0)
        trade.wait_send()
        swap = RowSwap(n, n_dp, wgrad_ref, swapped_ref, *sems[:2], True)
        swap.arrive()
        swap.finish()


def attn_backward(n, n_dp, wgrad, moe, after, branch, wout, attn, total, q, k, v, qlin, klin, cosine, sine, qgain, kgain, doc, rows):
    length, width = branch.shape
    qw = wout.shape[0]
    heads = qw // HD
    blk = lambda cols: pl.BlockSpec((rows, cols), lambda i: (i, 0))
    whole = lambda shape: pl.BlockSpec(shape, lambda i: (0, 0), pipeline_mode=pl.Buffered(1))
    shape = jax.ShapeDtypeStruct
    full = whole((length, HD))
    return pl.pallas_call(
        functools.partial(attn_backward_kernel, n, n_dp, heads, MOST // rows),
        grid=(length // rows,),
        in_specs=[
            blk(width),
            whole(wout.shape),
            blk(qw),
            blk(HD),
            blk(qw),
            full,
            full,
            blk(qw),
            full,
            full,
            full,
            whole((1, HD)),
            whole((1, HD)),
            blk(1),
            whole((1, length)),
            ANY,
            ANY,
            whole(after.shape),
        ],
        out_specs=[whole((length, qw + HD)), whole((8, HD)), ANY, whole(after.shape)],
        out_shape=[
            shape((length, qw + HD), BF16),
            shape((8, HD), F32),
            shape(wgrad.shape, BF16),
            shape(after.shape, BF16),
        ],
        scratch_shapes=[
            pltpu.VMEM((length, HD), F32),
            pltpu.VMEM((length, HD), F32),
            pltpu.VMEM((rows, qw), F32),
            pltpu.VMEM((length, HD), BF16),
            pltpu.VMEM((length, HD), BF16),
            DMA((n_dp,)),
            DMA((n_dp,)),
        ]
        + scatter_scratch(n, *after.shape)
        + [DMA(()), DMA(())],
        compiler_params=pltpu.CompilerParams(
            collective_id=9, has_side_effects=True, vmem_limit_bytes=VMEM_LIMIT
        ),
        cost_estimate=pl.CostEstimate(
            flops=60 * 10**9, transcendentals=0, bytes_accessed=30 * 2**20
        ),
        name="attn_backward",
    )(branch, wout, attn, total, q, k, v, qlin, klin, cosine, sine, qgain, kgain, doc[:, None], doc[None, :], wgrad, moe, after)


def expert_kernel(chained, low, aliased, plan, z_ref, n2_ref, top_ref, prob_ref, *rest):
    if aliased:
        rest = rest[1:]
    if chained:
        moe_in, row_in = rest[:2]
        rest = rest[2:]
    sources, rest = rest[: len(plan)], rest[len(plan) :]
    moe_ref, row_ref, grads_ref, wg_ref, wu_ref, wd_ref = rest[:6]
    ag_ref, au_ref, ad_ref, stage, wsem, sem = rest[6:]
    step = pl.program_id(0)
    rows, width = n2_ref.shape
    parts, cut, hidden = wd_ref.shape
    weights = (wg_ref, wu_ref, wd_ref)

    @pl.when(step == 0)
    def _():
        z = z_ref[0]
        for source, (kind, amount, start) in zip(sources, plan):
            count = source.shape[-2] // cut
            for k in range(parts) if kind == "all" else [amount]:
                if kind == "all":
                    src, owner, wanted = source.at[k], k, None
                elif kind == "up":
                    src, owner, wanted = source, z - k, z >= k
                else:
                    src, owner, wanted = source, z + k, z + k < parts

                def load(src=src, owner=owner, start=start, count=count):
                    for piece in range(count):
                        pltpu.make_async_copy(
                            src.at[pl.ds(piece * cut, cut), :],
                            weights[start + piece].at[owner],
                            wsem.at[start + piece, owner],
                        ).start()

                if wanted is None:
                    load()
                else:
                    pl.when(wanted)(load)
        ag_ref[...] = jnp.zeros_like(ag_ref)
        au_ref[...] = jnp.zeros_like(au_ref)
        ad_ref[...] = jnp.zeros_like(ad_ref)
        for index in range(3):
            for owner in range(parts):
                block = weights[index].at[owner]
                pltpu.make_async_copy(block, block, wsem.at[index, owner]).wait()

    n2 = n2_ref[...]
    prob = prob_ref[...]
    wg = wg_ref[...].reshape(width, hidden)
    wu = wu_ref[...].reshape(width, hidden)
    gate = dot(n2, wg)
    up = dot(n2, wu)
    sig = 1.0 / (1.0 + jnp.exp(-gate))
    silu = gate * sig
    act = (silu * up).astype(BF16)
    act_grad = jnp.zeros((rows, hidden), F32)
    for z in range(parts):
        cols = slice(z * cut, (z + 1) * cut)
        out = dot(act, wd_ref[z], NT).astype(BF16).astype(F32) * prob
        if chained:
            out = out + moe_in[:, cols].astype(F32)
        moe_ref[:, cols] = out.astype(BF16)
        route = (top_ref[:, cols].astype(F32) * prob).astype(BF16)
        act_grad += dot(route, wd_ref[z])
        ad_ref[z] += dot(route, act, TN)
    gate_grad = (act_grad * up * sig * (1.0 + gate * (1.0 - sig))).astype(BF16)
    up_grad = (act_grad * silu).astype(BF16)
    row = dot(gate_grad, wg, NT) + dot(up_grad, wu, NT)
    if chained:
        row = row + row_in[...].astype(F32)
    row_ref[...] = row.astype(BF16)
    ag_ref[...] += dot(n2, gate_grad, TN).reshape(parts, cut, hidden)
    au_ref[...] += dot(n2, up_grad, TN).reshape(parts, cut, hidden)

    @pl.when(step == pl.num_programs(0) - 1)
    def _():
        copies = []
        pieces = [
            (acc, place, z) for z in range(parts) for place, acc in enumerate((ag_ref, au_ref, ad_ref))
        ]
        for index, (acc, place, z) in enumerate(pieces):
            slot = index % 2
            if index >= 2:
                copies[index - 2].wait()
            stage[slot] = acc[z].astype(BF16)
            copies.append(
                pltpu.make_async_copy(
                    stage.at[slot],
                    grads_ref.at[z, pl.ds(place * cut, cut), pl.ds(low, acc.shape[2])],
                    sem.at[slot],
                )
            )
            copies[-1].start()
        copies[-2].wait()
        copies[-1].wait()


def expert(z, n2, top, prob, n_dp, sources, before, rows, low, full, grads):
    length, width = n2.shape
    cut = width // n_dp
    hidden = sources[0][0].shape[-1]
    blk = pl.BlockSpec((rows, width), lambda i: (i, 0))
    col = pl.BlockSpec((rows, 1), lambda i: (i, 0))
    shape = jax.ShapeDtypeStruct
    plan = tuple(entry[1:] for entry in sources)
    weight = pltpu.VMEM((n_dp, cut, hidden), BF16)
    total = pltpu.VMEM((n_dp, cut, hidden), F32)
    return pl.pallas_call(
        functools.partial(expert_kernel, len(before) > 0, low, len(grads) > 0, plan),
        grid=(length // rows,),
        in_specs=[pl.BlockSpec(memory_space=pltpu.SMEM), blk, blk, col]
        + [ANY] * len(grads)
        + [blk] * len(before)
        + [ANY] * len(sources),
        out_specs=[blk, blk, ANY],
        out_shape=[
            shape((length, width), BF16),
            shape((length, width), BF16),
            shape((n_dp, 3 * cut, full), BF16),
        ],
        input_output_aliases={4: 2} if grads else {},
        scratch_shapes=[weight] * 3
        + [total] * 3
        + [pltpu.VMEM((2, cut, hidden), BF16), DMA((3, n_dp)), DMA((2,))],
        compiler_params=pltpu.CompilerParams(vmem_limit_bytes=VMEM_LIMIT),
        cost_estimate=pl.CostEstimate(
            flops=18 * length * width * hidden,
            transcendentals=length * hidden,
            bytes_accessed=5 * length * width * 2,
        ),
        name="expert",
    )(z, n2, top, prob, *grads, *before, *[entry[0] for entry in sources])


def unpack_kernel(
    z_ref, one_ref, all_ref, up0_ref, down0_ref, up1_ref, down1_ref, dg_ref, du_ref, dd_ref, own, sem
):
    copy = pltpu.make_async_copy(all_ref.at[z_ref[0]], own, sem)
    copy.start()
    cut = dg_ref.shape[1]
    half = up0_ref.shape[0]
    piece = [slice(k * cut, (k + 1) * cut) for k in range(3)]
    dg_ref[1] = one_ref[piece[0], :].astype(F32)
    du_ref[1] = one_ref[piece[1], :].astype(F32)
    dd_ref[1] = jnp.transpose(one_ref[piece[2], :].astype(F32))
    copy.wait()

    def total(low, high):
        shift, up, down = (0, up0_ref, down0_ref) if high <= half else (half, up1_ref, down1_ref)
        there = slice(low - shift, high - shift)
        value = own[low:high, :].astype(F32)
        return value + up[there, :].astype(F32) + down[there, :].astype(F32)

    dg_ref[0] = total(0, cut)
    du_ref[0, : half - cut] = total(cut, half)
    du_ref[0, half - cut :] = total(half, 2 * cut)
    dd_ref[0] = jnp.transpose(total(2 * cut, 3 * cut))


def unpack(z, one, grads, got):
    rows, hidden = one.shape
    cut = rows // 3
    shape = jax.ShapeDtypeStruct
    return pl.pallas_call(
        unpack_kernel,
        in_specs=[pl.BlockSpec(memory_space=pltpu.SMEM), VM, ANY, VM, VM, VM, VM],
        out_specs=[VM] * 3,
        out_shape=[
            shape((2, cut, hidden), F32),
            shape((2, cut, hidden), F32),
            shape((2, hidden, cut), F32),
        ],
        scratch_shapes=[pltpu.VMEM((rows, hidden), BF16), DMA(())],
        compiler_params=pltpu.CompilerParams(vmem_limit_bytes=VMEM_LIMIT),
        name="unpack",
    )(z, one, grads, *got)


def line_hop(block_up, block_down, n_dp, hop):
    up = [(i, i + 1) for i in range(hop - 1, n_dp - 1)]
    down = [(i + 1, i) for i in range(n_dp - hop)]
    return lax.ppermute(block_up, "dp", up), lax.ppermute(block_down, "dp", down)


def reduce_hop(grads, got, n_dp, hop, rows, before):
    place = lax.axis_index("dp")
    reach = n_dp - hop
    zero = jnp.int32(0)
    size = (1, rows[1] - rows[0], grads.shape[2])
    spots = (jnp.minimum(place + reach, n_dp - 1), jnp.maximum(place - reach, 0))
    if got is not None:
        got = lax.optimization_barrier((*got, *before))[:2]
    elif before:
        grads = after_of(grads, *before)
    blocks = [
        lax.dynamic_slice(grads, (spot.astype(jnp.int32), jnp.int32(rows[0]), zero), size)[0]
        for spot in spots
    ]
    if got is not None:
        blocks = [(b.astype(F32) + g.astype(F32)).astype(BF16) for b, g in zip(blocks, got)]
    up = [(i, i + 1) for i in range(hop)]
    down = [(i, i - 1) for i in range(n_dp - hop, n_dp)]
    sent = lax.ppermute(blocks[0], "dp", up), lax.ppermute(blocks[1], "dp", down)
    return sent, tuple(blocks)


def after_of(value, *others):
    return lax.optimization_barrier((value,) + others)[0]


def per_device(
    layer_input,
    doc_ids,
    route_ids,
    route_probs,
    attn_gain,
    ffn_gain,
    query_gain,
    key_gain,
    w_query,
    w_key,
    w_value,
    w_out,
    w_gate,
    w_up,
    w_down,
    out_grad,
):
    tokens, width = layer_input.shape[1:]
    n_dp = lax.axis_size("dp")
    n_ctx = lax.axis_size("ctx")
    ctx_index = lax.axis_index("ctx")
    length = tokens * n_ctx
    heads = HQ // n_ctx
    share = n_ctx // KV
    qw = heads * HD
    depth = w_query.shape[0]
    own_e = w_gate.shape[0]

    cut = attn_gain.shape[0]
    hcut = query_gain.shape[0]
    kinds = 2 * (cut + hcut)
    small = jnp.concatenate([attn_gain, ffn_gain, query_gain, key_gain]).astype(F32)
    small = jnp.pad(small, (0, 1024 - kinds)).reshape(8, HD)
    even = (jnp.arange(n_ctx) % 2 == 0)[None, :, None]
    wide = [jnp.repeat(w.reshape(depth, KV, HD), share, axis=1) for w in (w_key, w_value)]
    cols = jnp.concatenate(
        [w_query.reshape(depth, n_ctx, qw), jnp.where(even, wide[0], wide[1])], axis=2
    ).transpose(1, 0, 2)
    hidden = w_gate.shape[2]
    cuts = ((0, 256), (256, hidden))
    cols, small, *blocks0 = prep(
        n_ctx, n_dp, cols, small, cuts, (w_gate, w_up, w_down)
    )
    small = small.reshape(n_dp * n_ctx, 1024)
    gain_attn = small[:, :cut].reshape(1, width)
    gain_ffn = small[:, cut : 2 * cut].reshape(1, width)
    gain_query = small[:, 2 * cut : 2 * cut + hcut].reshape(1, HD)
    gain_key = small[:, 2 * cut + hcut : kinds].reshape(1, HD)
    wqkv = lax.all_gather(cols.reshape(n_ctx * depth, qw + HD), "dp", axis=0, tiled=True)
    wrows = lax.all_gather(w_out, "dp", axis=0, tiled=False)

    inputs = layer_input.reshape(tokens, width)
    top_own = out_grad.reshape(tokens, width)
    n_experts = own_e * n_ctx
    match = route_ids.reshape(1, tokens, TOP) == jnp.arange(n_experts, dtype=jnp.int32)[:, None, None]
    probs = jnp.sum(jnp.where(match, route_probs.reshape(1, tokens, TOP), 0.0), axis=2)
    info = jnp.concatenate(
        [probs, doc_ids.reshape(1, tokens).astype(F32), jnp.zeros((7, tokens), F32)], axis=0
    )
    normed, info, top_all, block1 = first(
        n_ctx, inputs, gain_attn, info, top_own, ((0, hidden),), (w_gate, w_up, w_down)
    )
    normed = normed.reshape(length, width)
    doc = info[:, n_experts].reshape(length).astype(jnp.int32)
    my_probs = lax.dynamic_slice_in_dim(info, ctx_index * own_e, own_e, 1)
    my_probs = my_probs.transpose(0, 2, 1).reshape(length, own_e)

    inverse = 1.0 / ROPE_BASE ** (jnp.arange(HD // 2, dtype=F32) * 2.0 / HD)
    angles = jnp.arange(length, dtype=F32)[:, None] * inverse[None, :]
    cosine = jnp.cos(angles)
    sine = jnp.sin(angles)
    cosine = jnp.concatenate([cosine, cosine], axis=1)
    sine = jnp.concatenate([-sine, sine], axis=1)
    qlin, klin, q, k, v, attn, total, wout = attn_forward(
        n_ctx, n_dp, normed, wqkv, cosine, sine, gain_query, gain_key, doc, wrows, tokens
    )
    wout = wout.reshape(qw, width)
    top_all = top_all.reshape(length, width)
    blocks = (n_ctx, tokens, width)
    after, normed2 = middle(n_ctx, attn, wout, inputs, gain_ffn)
    normed2 = normed2.reshape(length, width)

    z = lax.axis_index("dp").astype(jnp.int32).reshape(1)
    hidden = w_gate.shape[2]

    def run(e, sources, carried, low, grads):
        moe, rows_grad, grads = expert(
            z,
            normed2,
            top_all,
            my_probs[:, e : e + 1],
            n_dp,
            sources,
            carried,
            tokens,
            low,
            hidden,
            grads,
        )
        return (moe, rows_grad), grads

    carried, grads0 = (), ()
    for index, (low, high) in enumerate(cuts):
        full = lax.all_gather(blocks0[index], "dp", axis=0, tiled=False)
        if index == 1:
            sources1 = [(block1, "up", 0, 0)]
            up = down = after_of(block1, full)
            up, down = line_hop(up, down, n_dp, 1)
            sources1 += [(up, "up", 1, 0), (down, "down", 1, 0)]
        carried, grads = run(0, [(full, "all", 0, 0)], carried, low, grads0)
        grads0 = (grads,)
    rows_all = 3 * (width // n_dp)
    spans = {"a": (0, rows_all // 2), "b": (rows_all // 2, rows_all)}
    got, before = {tag: None for tag in spans}, ()
    for hop in range(2, n_dp + 1):
        if hop < n_dp:
            up, down = line_hop(up, down, n_dp, hop)
            sources1 += [(up, "up", hop, 0), (down, "down", hop, 0)]
        for tag, rows in spans.items():
            got[tag], before = reduce_hop(grads, got[tag], n_dp, hop - 1, rows, before)
    (moe, rows_grad), grads1 = run(1, sources1, carried, 0, ())
    done1 = lax.psum_scatter(
        grads1.reshape(3 * width, hidden), "dp", scatter_dimension=0, tiled=True
    )
    mid, ffn_part, branch = turn(
        n_ctx, rows_grad.reshape(blocks), after, top_own, gain_ffn
    )
    branch = branch.reshape(length, width)

    out_w = dot(attn, branch, TN).astype(BF16).reshape(n_dp, qw // n_dp, width)
    dqkv, gains, out_w, layer_output = attn_backward(
        n_ctx,
        n_dp,
        out_w,
        moe.reshape(blocks),
        after,
        branch,
        wout,
        attn,
        total,
        q,
        k,
        v,
        qlin,
        klin,
        cosine,
        sine,
        gain_query,
        gain_key,
        doc,
        tokens,
    )
    qkv_w = dot(normed, dqkv, TN).astype(BF16)
    qkv_w = lax.psum_scatter(qkv_w, "dp", scatter_dimension=0, tiled=True)
    out_w = lax.psum_scatter(out_w.reshape(qw, width), "dp", scatter_dimension=0, tiled=True)
    out_w = out_w.astype(F32)
    input_grad, attn_part = last(n_ctx, dqkv, wqkv, inputs, mid, gain_attn)
    n_all = n_dp * n_ctx
    packed = jnp.concatenate(
        [
            attn_part[0].reshape(n_all, cut),
            ffn_part[0].reshape(n_all, cut),
            gains[0].reshape(n_all, hcut),
            gains[1].reshape(n_all, hcut),
            jnp.zeros((n_all, 1024 - kinds), F32),
        ],
        axis=1,
    )
    packed = packed.reshape(n_dp, n_ctx, 8, HD).transpose(1, 0, 2, 3)
    packed = gains_sum(n_ctx, n_dp, packed)
    packed = packed.reshape(1024)
    query_w, key_w, value_w = post(n_ctx, qkv_w.reshape(n_ctx, depth, qw + HD))
    gate_w, up_w, down_w = unpack(z, done1, grads, got["a"] + got["b"])
    return (
        layer_output.reshape(1, tokens, width),
        input_grad.reshape(1, tokens, width),
        packed[:cut],
        packed[cut : 2 * cut],
        packed[2 * cut : 2 * cut + hcut],
        packed[2 * cut + hcut : kinds],
        query_w,
        key_w,
        value_w,
        out_w,
        gate_w,
        up_w,
        down_w,
    )


def solution(mesh):
    both = ("dp", "ctx")
    seq = P("dp", "ctx", None)
    in_specs = (
        seq,
        P("dp", "ctx"),
        seq,
        seq,
        P(both),
        P(both),
        P(both),
        P(both),
        P(both, None),
        P(both, None),
        P(both, None),
        P(both, None),
        P("ctx", "dp", None),
        P("ctx", "dp", None),
        P("ctx", None, "dp"),
        seq,
    )
    out_specs = (
        seq,
        seq,
        P(both),
        P(both),
        P(both),
        P(both),
        P(both, None),
        P(both, None),
        P(both, None),
        P(both, None),
        P("ctx", "dp", None),
        P("ctx", "dp", None),
        P("ctx", None, "dp"),
    )

    return jax.shard_map(
        per_device, mesh=mesh, in_specs=in_specs, out_specs=out_specs, check_vma=False
    )
```

```python
import functools
import math

import jax
import jax.numpy as jnp
from jax import lax
from jax.experimental import pallas as pl
from jax.experimental.pallas import tpu as pltpu
from jax.sharding import PartitionSpec as P


HQ = 32
KV = 4
HD = 128
TOP = 8
MOST = 1024
EPS = 1e-06
ROPE_BASE = 1000000.0
F32 = jnp.float32
BF16 = jnp.bfloat16
SCALE = 1.0 / math.sqrt(HD)
SCALE2 = SCALE / math.log(2.0)
VMEM_LIMIT = 60 * 1024 * 1024


def dot(left, right, dims=((1,), (0,))):
    return lax.dot_general(left, right, (dims, ((), ())), preferred_element_type=F32)


NT = ((1,), (1,))
TN = ((0,), (0,))


def rms_parts(values):
    return lax.rsqrt(jnp.mean(values * values, axis=-1, keepdims=True) + EPS)


def rms_back(grad, unit, inv, gain):
    scaled = grad * gain
    return inv * (scaled - unit * jnp.mean(scaled * unit, axis=-1, keepdims=True))


def head_forward(lin, gain, cosine, sine):
    unit = lin * rms_parts(lin) * gain
    return unit * cosine + pltpu.roll(unit, HD // 2, 1) * sine


def head_backward(lin, gain, cosine, sine, rot_grad):
    grad = rot_grad * cosine + pltpu.roll(rot_grad * sine, HD // 2, 1)
    inv = rms_parts(lin)
    unit = lin * inv
    return rms_back(grad, unit, inv, gain), jnp.sum(grad * unit, axis=0, keepdims=True)


MESH = pl.DeviceIdType.MESH
ANY = pl.BlockSpec(memory_space=pl.ANY)
VM = pl.BlockSpec(memory_space=pltpu.VMEM)
DMA = pltpu.SemaphoreType.DMA
CHUNK = 32


def flip(index, mask, count):
    result, bit = 0, 1
    while bit < count:
        digit = (index // bit) % 2
        result = result + bit * ((1 - digit) if mask & bit else digit)
        bit *= 2
    return result


def push(src, dst, send, recv, axis, peer):
    return pltpu.make_async_remote_copy(
        src_ref=src,
        dst_ref=dst,
        send_sem=send,
        recv_sem=recv,
        device_id={axis: peer},
        device_id_type=MESH,
    )


def meet(peers):
    barrier = pltpu.get_barrier_semaphore()
    for axis, peer in peers:
        pl.semaphore_signal(barrier, inc=1, device_id={axis: peer}, device_id_type=MESH)
    pl.semaphore_wait(barrier, len(peers))


class Plane:
    def __init__(self, n):
        self.chips = n // 2
        self.me = lax.axis_index("ctx")
        self.core = self.me % 2
        self.chip = self.me // 2
        self.mate = self.me + 1 - 2 * self.core

    def same(self, s):
        return 2 * flip(self.chip, s, self.chips) + self.core

    def meet(self):
        meet([("ctx", self.same(s)) for s in range(1, self.chips)] + [("ctx", self.mate)])


def far_first(chips):
    return sorted(range(1, chips), key=lambda s: -bin(s).count("1"))


class Gather:
    def __init__(self, plane, src, out, send, recv, local):
        self.plane, self.out, self.send, self.recv = plane, out, send, recv
        self.own = pltpu.make_async_copy(src, out.at[plane.me], local)
        self.far = [
            push(src, out.at[plane.me], send.at[s], recv.at[s], "ctx", plane.same(s))
            for s in far_first(plane.chips)
        ]
        self.near = push(src, out.at[plane.me], send.at[0], recv.at[0], "ctx", plane.mate)

    def start(self):
        for copy in self.far:
            copy.start()
        self.near.start()
        self.own.start()

    def forward(self):
        plane, out = self.plane, self.out
        self.passed = []
        for s in sorted(range(1, plane.chips), key=lambda s: bin(s).count("1")):
            block = out.at[plane.same(s)]
            push(block, block, self.send.at[s], self.recv.at[s], "ctx", plane.mate).wait_recv()
            slot = plane.chips + s
            copy = push(block, block, self.send.at[slot], self.recv.at[slot], "ctx", plane.mate)
            copy.start()
            self.passed.append(copy)

    def finish(self):
        for copy in self.far:
            copy.wait_send()
        self.near.wait_send()
        self.near.wait_recv()
        for copy in self.passed:
            copy.wait_send()
            copy.wait_recv()
        self.own.wait()


def by_rows(rows, body):
    def one(index, carry):
        body(pl.ds(pl.multiple_of(index * CHUNK, CHUNK), CHUNK))
        return carry

    lax.fori_loop(0, rows // CHUNK, one, 0)


class SquareGather:
    def __init__(self, plane, src, out, send, recv, local):
        self.plane, self.out, self.send, self.recv = plane, out, send, recv
        half = src.shape[0] // 2
        self.halves = [pl.ds(0, half), pl.ds(half, half)]
        mine = out.at[plane.me]
        self.own = pltpu.make_async_copy(src, mine, local)
        self.near = push(src, mine, send.at[0], recv.at[0], "ctx", plane.mate)
        self.far = []
        for s, h in ((1, 0), (2, 1), (1, 1), (2, 0)):
            part, slot = self.halves[h], 2 * s + h
            self.far.append(
                push(
                    src.at[part, :],
                    mine.at[part, :],
                    send.at[slot],
                    recv.at[slot],
                    "ctx",
                    plane.same(s),
                )
            )

    def start(self):
        for copy in self.far:
            copy.start()
        self.near.start()
        self.own.start()

    def arrived(self, s, h):
        block = self.out.at[self.plane.same(s)].at[self.halves[h], :]
        slot = 2 * s + h
        push(block, block, self.send.at[slot], self.recv.at[slot], "ctx", self.plane.mate).wait_recv()
        return block

    def forward(self):
        plane = self.plane
        self.passed = []
        for s, h in ((1, 0), (2, 1)):
            block = self.arrived(s, h)
            slot = 6 + h
            copy = push(block, block, self.send.at[slot], self.recv.at[slot], "ctx", plane.same(3 - s))
            copy.start()
            self.far.append(copy)
        for s in (1, 2, 3):
            if s < 3:
                self.arrived(s, 2 - s)
            else:
                self.arrived(3, 0)
                self.arrived(3, 1)
            block, slot = self.out.at[plane.same(s)], 7 + s
            copy = push(block, block, self.send.at[slot], self.recv.at[slot], "ctx", plane.mate)
            copy.start()
            self.passed.append(copy)

    def finish(self):
        for copy in self.far:
            copy.wait_send()
        self.near.wait_send()
        self.near.wait_recv()
        for copy in self.passed:
            copy.wait_send()
            copy.wait_recv()
        self.own.wait()


def gather_of(plane, src, out, send, recv, local):
    kind = SquareGather if plane.chips == 4 else Gather
    return kind(plane, src, out, send, recv, local)


class Spread:
    def __init__(self, plane, mine, landed, send, recv):
        self.plane, self.mine, self.landed = plane, mine, landed
        self.square = plane.chips == 4
        self.order = [3, 1, 2, 0] if self.square else far_first(plane.chips) + [0]
        self.send, self.recv = send, recv
        half = mine.shape[1] // 2
        self.halves = [pl.ds(0, half), pl.ds(half, half)]

    def copy(self, s, h, to):
        part, slot = self.halves[h], 2 * s + h
        return push(
            self.mine.at[s].at[part, :],
            self.landed.at[s].at[part, :],
            self.send.at[slot],
            self.recv.at[slot],
            "ctx",
            self.plane.same(to),
        )

    def go(self, s, h, to):
        self.copy(s, h, to).start()

    def ready(self, s):
        if self.square:
            if s == 3:
                self.go(3, 0, 1)
                self.go(3, 1, 2)
            elif s == 1:
                self.go(1, 0, 1)
            elif s == 2:
                self.go(2, 1, 2)
        elif s:
            push(
                self.mine.at[s],
                self.landed.at[s],
                self.send.at[s],
                self.recv.at[s],
                "ctx",
                self.plane.same(s),
            ).start()

    def sends(self):
        if self.square:
            hops = ((3, 0, 1), (3, 1, 2), (1, 0, 1), (2, 1, 2), (2, 0, 2), (1, 1, 1))
            return [self.copy(*hop) for hop in hops]
        return [
            push(
                self.mine.at[s],
                self.landed.at[s],
                self.send.at[s],
                self.recv.at[s],
                "ctx",
                self.plane.same(s),
            )
            for s in self.order
            if s
        ]

    def relay(self):
        mine, landed = self.mine, self.landed
        half = mine.shape[1] // 2
        if not self.square:
            return
        for s, h in ((2, 0), (1, 1)):
            self.copy(3, h, 1).wait_recv()

            def add(at, s=s, h=h):
                rows = pl.ds(h * half + at.start, CHUNK)
                total = mine[s, rows, :].astype(F32) + landed[3, rows, :].astype(F32)
                mine[s, rows, :] = total.astype(BF16)

            by_rows(half, add)
            self.copy(s, h, s).start()

    def gathered(self):
        if not self.square:
            for copy in self.sends():
                copy.wait_recv()
            return
        for s in (1, 2):
            for h in (0, 1):
                self.copy(s, h, s).wait_recv()

    def settle(self, extra=None):
        self.relay()
        if extra is not None:
            extra()
        self.gathered()

    def total(self, at):
        value = self.mine[0, at, :].astype(F32)
        for s in (1, 2) if self.square else range(1, self.plane.chips):
            value = value + self.landed[s, at, :].astype(F32)
        return value

    def finish(self):
        for copy in self.sends():
            copy.wait_send()


class Scatter:
    def __init__(self, plane, part, mine, other, landed, send, recv, send2, recv2, local):
        self.plane, self.mine, self.other = plane, mine, other
        self.spread = Spread(plane, mine, landed, send2, recv2)
        self.order = self.spread.order
        self.loads, self.across = {}, {}
        for s in self.order:
            block = plane.same(s)
            self.loads[s] = pltpu.make_async_copy(part.at[block], mine.at[s], local.at[s])
            self.across[s] = push(
                part.at[block + 1 - 2 * plane.core],
                other.at[s],
                send.at[s],
                recv.at[s],
                "ctx",
                plane.mate,
            )

    def start(self):
        for s in self.order:
            self.across[s].start()
            self.loads[s].start()

    def pairs(self):
        mine, other = self.mine, self.other
        for s in self.order:
            self.loads[s].wait()
            self.across[s].wait_recv()

            def add(at, s=s):
                total = mine[s, at, :].astype(F32) + other[s, at, :].astype(F32)
                mine[s, at, :] = total.astype(BF16)

            by_rows(mine.shape[1], add)
            self.spread.ready(s)

    def run(self):
        self.pairs()
        self.spread.settle()

    def total(self, at):
        return self.spread.total(at)

    def finish(self):
        for s in self.order:
            self.across[s].wait_send()
        self.spread.finish()


class Product:
    def __init__(self, plane, value, mine, other, landed, given, send, recv, send2, recv2):
        self.plane, self.value = plane, value
        self.mine, self.other, self.given = mine, other, given
        self.spread = Spread(plane, mine, landed, send2, recv2)
        self.order = self.spread.order
        self.across = {
            s: push(given.at[s], other.at[s], send.at[s], recv.at[s], "ctx", plane.mate)
            for s in self.order
        }

    def start(self):
        plane = self.plane
        for s in self.order:
            block = plane.same(s) + 1 - 2 * plane.core

            def fill(at, s=s, block=block):
                self.given[s, :, at] = self.value(block, at).astype(BF16)

            by_cols(self.mine.shape[2], fill)
            self.across[s].start()

    def run(self, extra=None):
        plane, mine, other = self.plane, self.mine, self.other
        for s in self.order:
            block = plane.same(s)
            self.across[s].wait_recv()

            def fill(at, s=s, block=block):
                total = self.value(block, at) + other[s, :, at].astype(F32)
                mine[s, :, at] = total.astype(BF16)

            by_cols(mine.shape[2], fill)
            self.spread.ready(s)
        self.spread.settle(extra)

    total = Scatter.total
    finish = Scatter.finish


def by_cols(width, body):
    span = 512

    def one(index, carry):
        body(pl.ds(pl.multiple_of(index * span, span), span))
        return carry

    lax.fori_loop(0, width // span, one, 0)


def gather_sems(n):
    return [DMA((12 if n == 8 else n,)), DMA((12 if n == 8 else n,)), DMA(())]


def scatter_scratch(n, rows, width):
    chips = n // 2
    return (
        [pltpu.VMEM((chips, rows, width), BF16)] * 3
        + [DMA((chips,)), DMA((chips,)), DMA((n,)), DMA((n,))]
        + [DMA((chips,))]
    )


def product_scratch(n, rows, width):
    chips = n // 2
    return [pltpu.VMEM((chips, rows, width), BF16)] * 4 + [
        DMA((chips,)),
        DMA((chips,)),
        DMA((n,)),
        DMA((n,)),
    ]


def comm_call(kernel, ident, outs, out_specs, in_specs, scratch, micros, *args):
    return pl.pallas_call(
        kernel,
        out_shape=outs,
        in_specs=in_specs,
        out_specs=out_specs,
        scratch_shapes=scratch,
        compiler_params=pltpu.CompilerParams(
            collective_id=ident, has_side_effects=True, vmem_limit_bytes=VMEM_LIMIT
        ),
        cost_estimate=pl.CostEstimate(
            flops=0, transcendentals=0, bytes_accessed=int(micros * 3.0e6)
        ),
    )(*args)


def swap_all(n, src, out, send, recv, local):
    me = lax.axis_index("ctx")
    own = pltpu.make_async_copy(src.at[me], out.at[me], local)
    own.start()
    copies = []
    for s in range(n - 1, 0, -1):
        peer = flip(me, s, n)
        copies.append(push(src.at[peer], out.at[me], send.at[s], recv.at[s], "ctx", peer))
        copies[-1].start()
    return own, copies


class RowSwap:
    def __init__(self, n, n_dp, src, dst, send, recv, spread):
        self.me = lax.axis_index("ctx")
        self.dst, self.send, self.recv, self.n_dp = dst, send, recv, n_dp
        self.entries = []
        for k in range(n_dp):
            flat = self.me * n_dp + k if spread else k * n + self.me
            peer = flat % n if spread else flat // n_dp
            slot = flat // n if spread else flat % n_dp
            far = push(src.at[k], dst.at[slot], send.at[k], recv.at[slot], "ctx", peer)
            near = pltpu.make_async_copy(src.at[k], dst.at[slot], recv.at[slot])
            self.entries.append((peer, far, near))

    def start(self):
        for peer, far, near in self.entries:
            pl.when(peer != self.me)(far.start)
            pl.when(peer == self.me)(near.start)

    def arrive(self):
        for slot in range(self.n_dp):
            block = self.dst.at[slot]
            pltpu.make_async_copy(block, block, self.recv.at[slot]).wait()

    def finish(self):
        for peer, far, near in self.entries:
            pl.when(peer != self.me)(far.wait_send)


def meet_all(n):
    me = lax.axis_index("ctx")
    meet([("ctx", flip(me, s, n)) for s in range(1, n)])


class Pack:
    def __init__(self, e, sources, buffers, sems):
        self.buffers = buffers
        self.loads = [
            pltpu.make_async_copy(source.at[e], buffer, sems.at[k])
            for k, (source, buffer) in enumerate(zip(sources, buffers))
        ]

    def start(self):
        for load in self.loads:
            load.start()

    def write(self, cuts, outs):
        for load in self.loads:
            load.wait()
        gate, up, down = self.buffers
        cut = gate.shape[0]
        for (low, high), out in zip(cuts, outs):
            out[:cut, :] = gate[:, low:high]
            out[cut : 2 * cut, :] = up[:, low:high]
            out[2 * cut :, :] = jnp.transpose(down[low:high, :].astype(F32)).astype(BF16)


def pack_scratch(weights):
    return [pltpu.VMEM(w.shape[1:], BF16) for w in weights] + [DMA((3,))]


def pack_shapes(cuts, weights):
    cut = weights[0].shape[1]
    return [jax.ShapeDtypeStruct((3 * cut, high - low), BF16) for low, high in cuts]


def prep_kernel(n, n_dp, cuts, cols_ref, small_ref, *rest):
    sources, rest = rest[:3], rest[3:]
    out_ref, all_ref, rest = rest[0], rest[1], rest[2:]
    packed, rest = rest[: len(cuts)], rest[len(cuts) :]
    pack = Pack(0, sources, rest[:3], rest[3])
    pack.start()
    send, recv, local, gsend, grecv, zsend, zrecv = rest[4:]
    me, row = lax.axis_index("ctx"), lax.axis_index("dp")
    meet(
        [("ctx", flip(me, s, n)) for s in range(1, n)]
        + [("dp", flip(row, s, n_dp)) for s in range(1, n_dp)]
    )
    all_ref[row, me] = small_ref[...]
    smalls = []
    for s in range(1, n):
        peer = flip(me, s, n)
        smalls.append(push(small_ref, all_ref.at[row, me], gsend.at[s], grecv.at[s], "ctx", peer))
        smalls[-1].start()
    own, copies = swap_all(n, cols_ref, out_ref, send, recv, local)
    pack.write(cuts, packed)
    for copy in smalls:
        copy.wait_recv()
    planes = []
    for s in range(1, n_dp):
        peer = flip(row, s, n_dp)
        planes.append(push(all_ref.at[row], all_ref.at[row], zsend.at[s], zrecv.at[s], "dp", peer))
        planes[-1].start()
    for copy in copies + planes:
        copy.wait_recv()
    for copy in copies + planes + smalls:
        copy.wait_send()
    own.wait()


class Gains:
    def __init__(self, n, n_dp, small, landed, mid, second, gsend, grecv, zsend, zrecv):
        self.me, self.row = lax.axis_index("ctx"), lax.axis_index("dp")
        self.small, self.landed, self.mid, self.second = small, landed, mid, second
        self.near, self.far = [], []
        for s in range(1, n):
            peer = flip(self.me, s, n)
            self.near.append(push(small.at[peer], landed.at[s], gsend.at[s], grecv.at[s], "ctx", peer))
        for s in range(1, n_dp):
            peer = flip(self.row, s, n_dp)
            self.far.append(push(mid.at[peer], second.at[s], zsend.at[s], zrecv.at[s], "dp", peer))

    def start(self):
        for copy in self.near:
            copy.start()

    def middle(self):
        value = self.small[self.me]
        for s, copy in enumerate(self.near, 1):
            copy.wait_recv()
            value = value + self.landed[s]
        self.mid[...] = value
        for copy in self.far:
            copy.start()

    def finish(self):
        value = self.mid[self.row]
        for s, copy in enumerate(self.far, 1):
            copy.wait_recv()
            value = value + self.second[s]
        for copy in self.near + self.far:
            copy.wait_send()
        return value


def post_kernel(n, src_ref, query_ref, key_ref, value_ref, blocks, send, recv, local):
    me = lax.axis_index("ctx")
    meet([("ctx", flip(me, s, n)) for s in range(1, n)])
    own, copies = swap_all(n, src_ref, blocks, send, recv, local)
    for copy in copies:
        copy.wait_recv()
    own.wait()
    share = n // KV
    qw = HQ * HD // n
    for c in range(n):
        query_ref[:, c * qw : (c + 1) * qw] = blocks[c, :, :qw].astype(F32)
    for g in range(KV):
        for out, kind in ((key_ref, 0), (value_ref, 1)):
            total = blocks[g * share + kind, :, qw:].astype(F32)
            for c in range(2 + kind, share, 2):
                total = total + blocks[g * share + c, :, qw:].astype(F32)
            out[:, g * HD : (g + 1) * HD] = total
    for copy in copies:
        copy.wait_send()


def swap_sems(n, n_dp):
    return [DMA((n,)), DMA((n,)), DMA(()), DMA((n,)), DMA((n,)), DMA((n_dp,)), DMA((n_dp,))]


def prep(n, n_dp, cols, small, cuts, weights):
    shape = jax.ShapeDtypeStruct
    return comm_call(
        functools.partial(prep_kernel, n, n_dp, cuts),
        0,
        [shape(cols.shape, cols.dtype), shape((n_dp, n) + small.shape, F32)]
        + pack_shapes(cuts, weights),
        [ANY, VM] + [VM] * len(cuts),
        [ANY, VM, ANY, ANY, ANY],
        pack_scratch(weights) + swap_sems(n, n_dp),
        8,
        cols,
        small,
        *weights,
    )


def post(n, cols):
    shape = jax.ShapeDtypeStruct
    depth = cols.shape[1]
    return comm_call(
        functools.partial(post_kernel, n),
        1,
        [
            shape((depth, HQ * HD), F32),
            shape((depth, KV * HD), F32),
            shape((depth, KV * HD), F32),
        ],
        [VM] * 3,
        [VM],
        [pltpu.VMEM(cols.shape, BF16), DMA((n,)), DMA((n,)), DMA(())],
        10,
        cols,
    )


def first_kernel(
    n, cuts, x_ref, gain_ref, info_ref, grad_ref, *rest
):
    sources, rest = rest[:3], rest[3:]
    nall_ref, iall_ref, gall_ref, rest = rest[0], rest[1], rest[2], rest[3:]
    packed, rest = rest[: len(cuts)], rest[len(cuts) :]
    pack = Pack(1, sources, rest[:3], rest[3])
    low, sems = rest[4], rest[5:]
    pack.start()
    plane = Plane(n)
    plane.meet()
    infos = Gather(plane, info_ref, iall_ref, *sems[0:3])
    infos.start()

    def norm(at):
        value = x_ref[at, :].astype(F32)
        low[at, :] = (value * rms_parts(value) * gain_ref[...]).astype(BF16)

    by_rows(x_ref.shape[0], norm)
    normed = gather_of(plane, low, nall_ref, *sems[3:6])
    normed.start()
    grads = gather_of(plane, grad_ref, gall_ref, *sems[6:9])
    grads.start()
    pack.write(cuts, packed)
    infos.forward()
    normed.forward()
    grads.forward()
    infos.finish()
    normed.finish()
    grads.finish()


def first(n, x, gain, info, grad, cuts, weights):
    shape = jax.ShapeDtypeStruct
    many = lambda array, kind: shape((n,) + array.shape, kind)
    return comm_call(
        functools.partial(first_kernel, n, cuts),
        2,
        [many(x, BF16), many(info, F32), many(grad, BF16)] + pack_shapes(cuts, weights),
        [ANY] * 3 + [VM] * len(cuts),
        [VM] * 4 + [ANY] * 3,
        pack_scratch(weights)
        + [pltpu.VMEM(x.shape, BF16)]
        + [DMA((n,)), DMA((n,)), DMA(())]
        + gather_sems(n)
        + gather_sems(n),
        90,
        x,
        gain,
        info,
        grad,
        *weights,
    )


def middle_kernel(
    n, attn_ref, wout_ref, x_ref, gain_ref, after_ref, all_ref, low, *scratch
):
    plane = Plane(n)
    plane.meet()
    rows = x_ref.shape[0]

    def value(block, at):
        left = attn_ref[pl.ds(pl.multiple_of(block * rows, rows), rows), :]
        return dot(left, wout_ref[:, at])

    sums = Product(plane, value, *scratch[:8])
    sums.start()
    sums.run()

    def norm(at):
        value = x_ref[at, :].astype(F32) + sums.total(at)
        after_ref[at, :] = value
        low[at, :] = (value * rms_parts(value) * gain_ref[...]).astype(BF16)

    by_rows(rows, norm)
    normed = gather_of(plane, low, all_ref, *scratch[8:])
    normed.start()
    normed.forward()
    sums.finish()
    normed.finish()


def middle(n, attn, wout, x, gain):
    shape = jax.ShapeDtypeStruct
    return comm_call(
        functools.partial(middle_kernel, n),
        3,
        [shape(x.shape, F32), shape((n,) + x.shape, BF16)],
        [VM, ANY],
        [VM, VM, VM, VM],
        [pltpu.VMEM(x.shape, BF16)]
        + product_scratch(n, *x.shape)
        + gather_sems(n),
        105,
        attn,
        wout,
        x,
        gain,
    )


def turn_kernel(
    n, part_ref, after_ref, grad_ref, gain_ref, mid_ref, fpart_ref, all_ref, low, *scratch
):
    plane = Plane(n)
    plane.meet()
    sums = Scatter(plane, part_ref, *scratch[:8])
    sums.start()
    fpart_ref[...] = jnp.zeros_like(fpart_ref)
    sums.run()

    def norm(at):
        value = after_ref[at, :]
        inv = rms_parts(value)
        unit = value * inv
        grad = sums.total(at)
        fpart_ref[0:1, :] += jnp.sum(grad * unit, axis=0, keepdims=True)
        mid = grad_ref[at, :].astype(F32) + rms_back(grad, unit, inv, gain_ref[...])
        mid_ref[at, :] = mid
        low[at, :] = mid.astype(BF16)

    by_rows(after_ref.shape[0], norm)
    branch = gather_of(plane, low, all_ref, *scratch[8:])
    branch.start()
    branch.forward()
    sums.finish()
    branch.finish()


def turn(n, part, after, grad, gain):
    shape = jax.ShapeDtypeStruct
    return comm_call(
        functools.partial(turn_kernel, n),
        4,
        [
            shape(after.shape, F32),
            shape((8, after.shape[1]), F32),
            shape((n,) + after.shape, BF16),
        ],
        [VM, VM, ANY],
        [ANY, VM, VM, VM],
        [pltpu.VMEM(after.shape, BF16)] + scatter_scratch(n, *after.shape) + gather_sems(n),
        95,
        part,
        after,
        grad,
        gain,
    )


def halfway_kernel(
    n,
    n_dp,
    part_ref,
    n2_ref,
    gg_ref,
    ug_ref,
    after_ref,
    grad_ref,
    gain_ref,
    mid_ref,
    fpart_ref,
    low_ref,
    wgrad_ref,
    n2,
    gg,
    ug,
    wgrad,
    lsem,
    wsem,
    *scratch,
):
    loads = [
        pltpu.make_async_copy(src, dst, lsem.at[k])
        for k, (src, dst) in enumerate(((n2_ref, n2), (gg_ref, gg), (ug_ref, ug)))
    ]
    plane = Plane(n)
    plane.meet()
    sums = Scatter(plane, part_ref, *scratch)
    sums.start()
    for load in loads:
        load.start()
    fpart_ref[...] = jnp.zeros_like(fpart_ref)
    sums.pairs()
    for load in loads:
        load.wait()
    cut = wgrad.shape[1] // 2

    def weights(kind, source):
        copies = []
        for z in range(n_dp):
            here = slice(z * cut, (z + 1) * cut)
            there = slice(kind * cut, (kind + 1) * cut)
            wgrad[z, there, :] = dot(n2[:, here], source[...], TN).astype(BF16)
            copies.append(
                pltpu.make_async_copy(
                    wgrad.at[z, pl.ds(kind * cut, cut), :],
                    wgrad_ref.at[z, pl.ds(kind * cut, cut), :],
                    wsem.at[kind, z],
                )
            )
            copies[-1].start()
        return copies

    copies = weights(0, gg)
    sums.spread.relay()
    copies += weights(1, ug)
    sums.spread.gathered()

    def norm(at):
        value = after_ref[at, :]
        inv = rms_parts(value)
        unit = value * inv
        grad = sums.total(at)
        fpart_ref[0:1, :] += jnp.sum(grad * unit, axis=0, keepdims=True)
        mid = grad_ref[at, :].astype(F32) + rms_back(grad, unit, inv, gain_ref[...])
        mid_ref[at, :] = mid
        low_ref[at, :] = mid.astype(BF16)

    by_rows(after_ref.shape[0], norm)
    sums.finish()
    for copy in copies:
        copy.wait()


def halfway(n, n_dp, part, n2, gg, ug, after, grad, gain):
    shape = jax.ShapeDtypeStruct
    width, hidden = n2.shape[1], gg.shape[1]
    out = (n_dp, 2 * width // n_dp, hidden)
    return comm_call(
        functools.partial(halfway_kernel, n, n_dp),
        4,
        [
            shape(after.shape, F32),
            shape((8, after.shape[1]), F32),
            shape(after.shape, BF16),
            shape(out, BF16),
        ],
        [VM, VM, VM, ANY],
        [ANY, ANY, ANY, ANY, VM, VM, VM],
        [
            pltpu.VMEM(n2.shape, BF16),
            pltpu.VMEM(gg.shape, BF16),
            pltpu.VMEM(gg.shape, BF16),
            pltpu.VMEM(out, BF16),
            DMA((3,)),
            DMA((2, n_dp)),
        ]
        + scatter_scratch(n, *after.shape),
        50,
        part,
        n2,
        gg,
        ug,
        after,
        grad,
        gain,
    )


def share_kernel(n, low_ref, all_ref, *sems):
    plane = Plane(n)
    plane.meet()
    gather = gather_of(plane, low_ref, all_ref, *sems)
    gather.start()
    gather.forward()
    gather.finish()


def share_rows(n, low):
    return comm_call(
        functools.partial(share_kernel, n),
        10,
        jax.ShapeDtypeStruct((n,) + low.shape, BF16),
        ANY,
        [VM],
        gather_sems(n),
        45,
        low,
    )


def last_kernel(n, grad_ref, wqkv_ref, x_ref, mid_ref, gain_ref, out_ref, apart_ref, *scratch):
    plane = Plane(n)
    plane.meet()
    apart_ref[...] = jnp.zeros_like(apart_ref)
    rows = x_ref.shape[0]

    def value(block, at):
        left = grad_ref[pl.ds(pl.multiple_of(block * rows, rows), rows), :]
        return dot(left, wqkv_ref[at, :], NT)

    sums = Product(plane, value, *scratch[:8])
    sums.start()
    sums.run()

    def norm(at):
        value = x_ref[at, :].astype(F32)
        inv = rms_parts(value)
        unit = value * inv
        grad = sums.total(at)
        apart_ref[0:1, :] += jnp.sum(grad * unit, axis=0, keepdims=True)
        out_ref[at, :] = mid_ref[at, :] + rms_back(grad, unit, inv, gain_ref[...])

    by_rows(rows, norm)
    sums.finish()


def last(n, grad, wqkv, x, mid, gain):
    shape = jax.ShapeDtypeStruct
    return comm_call(
        functools.partial(last_kernel, n),
        5,
        [shape(mid.shape, F32), shape((8, mid.shape[1]), F32)],
        [VM, VM],
        [VM] * 5,
        product_scratch(n, *mid.shape),
        60,
        grad,
        wqkv,
        x,
        mid,
        gain,
    )


def gains_kernel(n, n_dp, small_ref, sum_ref, *scratch):
    meet(
        [("ctx", flip(lax.axis_index("ctx"), s, n)) for s in range(1, n)]
        + [("dp", flip(lax.axis_index("dp"), s, n_dp)) for s in range(1, n_dp)]
    )
    gains = Gains(n, n_dp, small_ref, *scratch)
    gains.start()
    gains.middle()
    sum_ref[...] = gains.finish()


def gains_sum(n, n_dp, small):
    tile = small.shape[2:]
    return comm_call(
        functools.partial(gains_kernel, n, n_dp),
        8,
        jax.ShapeDtypeStruct(tile, F32),
        VM,
        [VM],
        [
            pltpu.VMEM((n, n_dp) + tile, F32),
            pltpu.VMEM((n_dp,) + tile, F32),
            pltpu.VMEM((n_dp,) + tile, F32),
            DMA((n,)),
            DMA((n,)),
            DMA((n_dp,)),
            DMA((n_dp,)),
        ],
        10,
        small,
    )


def attn_forward_kernel(
    n,
    n_dp,
    heads,
    back,
    normed_ref,
    wqkv_ref,
    cos_ref,
    sin_ref,
    qgain_ref,
    kgain_ref,
    docc_ref,
    docr_ref,
    rows_ref,
    qlin_ref,
    klin_ref,
    q_ref,
    k_ref,
    v_ref,
    attn_ref,
    total_ref,
    wout_ref,
    acc_ref,
    sum_ref,
    mate_ref,
    *sems,
):
    step = pl.program_id(0)

    @pl.when(step == 0)
    def _():
        meet_all(n)
        copy = push(
            wqkv_ref.at[:, pl.ds(heads * HD, HD)],
            mate_ref,
            sems[2],
            sems[3],
            "ctx",
            Plane(n).mate,
        )
        copy.start()
        RowSwap(n, n_dp, rows_ref, wout_ref, *sems[:2], False).start()
        copy.wait_recv()
        copy.wait_send()

    rows = normed_ref.shape[0]
    lin = dot(normed_ref[...], wqkv_ref[...])
    here = pl.ds(step * rows, rows)
    cosine = cos_ref[...]
    sine = sin_ref[...]
    qw = heads * HD
    for head in range(heads):
        cols = slice(head * HD, (head + 1) * HD)
        part = lin[:, cols]
        qlin_ref[:, cols] = part
        q_ref[:, cols] = head_forward(part, qgain_ref[...], cosine, sine).astype(BF16)
    own = lin[:, qw:]
    other = dot(normed_ref[...], mate_ref[...])
    first_core = lax.axis_index("ctx") % 2 == 0
    key_lin = jnp.where(first_core, own, other)
    klin_ref[...] = key_lin
    k_ref[here, :] = head_forward(key_lin, kgain_ref[...], cosine, sine).astype(BF16)
    v_ref[here, :] = jnp.where(first_core, other, own).astype(BF16)
    acc_ref[...] = jnp.zeros_like(acc_ref)
    sum_ref[...] = jnp.zeros_like(sum_ref)
    row_pos = step * rows + lax.broadcasted_iota(jnp.int32, (rows, rows), 0)
    col_off = lax.broadcasted_iota(jnp.int32, (rows, rows), 1)

    def one(block, carry):
        at = pl.ds(pl.multiple_of(block * rows, rows), rows)
        key = k_ref[at, :]
        val = v_ref[at, :]
        allowed = (docc_ref[...] == docr_ref[:, at]) & (block * rows + col_off <= row_pos)
        for head in range(heads):
            cols = slice(head * HD, (head + 1) * HD)
            score = dot(q_ref[:, cols], key, NT) * SCALE2
            expo = jnp.where(allowed, jnp.exp2(score), 0.0)
            folded = expo[:, :HD]
            for piece in range(1, rows // HD):
                folded = folded + expo[:, piece * HD : (piece + 1) * HD]
            sum_ref[:, cols] += folded
            acc_ref[:, cols] += dot(expo.astype(BF16), val)
        return carry

    lax.fori_loop(jnp.maximum(step - back, 0), step + 1, one, 0)
    lane = lax.broadcasted_iota(jnp.int32, (rows, HD), 1)
    totals = jnp.ones((rows, HD), F32)
    for head in range(heads):
        cols = slice(head * HD, (head + 1) * HD)
        total = jnp.sum(sum_ref[:, cols], axis=-1, keepdims=True)
        totals = jnp.where(lane == head, total, totals)
        attn_ref[:, cols] = (acc_ref[:, cols] / total).astype(BF16)
    total_ref[...] = totals

    @pl.when(step == pl.num_programs(0) - 1)
    def _():
        swap = RowSwap(n, n_dp, rows_ref, wout_ref, *sems[:2], False)
        swap.arrive()
        swap.finish()


def attn_forward(n, n_dp, normed, wqkv, cosine, sine, qgain, kgain, doc, wrows, rows):
    length, width = normed.shape
    qw = wqkv.shape[1] - HD
    heads = qw // HD
    blk = lambda cols: pl.BlockSpec((rows, cols), lambda i: (i, 0))
    whole = lambda shape: pl.BlockSpec(shape, lambda i: (0, 0))
    shape = jax.ShapeDtypeStruct
    return pl.pallas_call(
        functools.partial(attn_forward_kernel, n, n_dp, heads, MOST // rows),
        grid=(length // rows,),
        in_specs=[
            blk(width),
            whole(wqkv.shape),
            blk(HD),
            blk(HD),
            whole((1, HD)),
            whole((1, HD)),
            blk(1),
            whole((1, length)),
            ANY,
        ],
        out_specs=[
            blk(qw),
            blk(HD),
            blk(qw),
            whole((length, HD)),
            whole((length, HD)),
            blk(qw),
            blk(HD),
            ANY,
        ],
        out_shape=[
            shape((length, qw), F32),
            shape((length, HD), F32),
            shape((length, qw), BF16),
            shape((length, HD), BF16),
            shape((length, HD), BF16),
            shape((length, qw), BF16),
            shape((length, HD), F32),
            shape(wrows.shape, BF16),
        ],
        scratch_shapes=[
            pltpu.VMEM((rows, qw), F32),
            pltpu.VMEM((rows, qw), F32),
            pltpu.VMEM((width, HD), BF16),
        ]
        + [DMA((n_dp,)), DMA((n_dp,)), DMA(()), DMA(())],
        compiler_params=pltpu.CompilerParams(
            collective_id=7, has_side_effects=True, vmem_limit_bytes=VMEM_LIMIT
        ),
        cost_estimate=pl.CostEstimate(
            flops=35 * 10**9, transcendentals=0, bytes_accessed=30 * 2**20
        ),
        name="attn_forward",
    )(normed, wqkv, cosine, sine, qgain, kgain, doc[:, None], doc[None, :], wrows)


def attn_backward_kernel(
    n,
    n_dp,
    heads,
    back,
    branch_ref,
    wout_ref,
    attn_ref,
    total_ref,
    q_ref,
    k_ref,
    v_ref,
    qlin_ref,
    klin_ref,
    cos_ref,
    sin_ref,
    qgain_ref,
    kgain_ref,
    docc_ref,
    docr_ref,
    wgrad_ref,
    moe_ref,
    after_ref,
    dqkv_ref,
    gains_ref,
    swapped_ref,
    final_ref,
    dk_ref,
    dv_ref,
    dqa_ref,
    give_ref,
    take_ref,
    *sems,
):
    step = pl.program_id(0)

    steps = pl.num_programs(0)

    def scatter():
        return Scatter(Plane(n), moe_ref, *sems[2:10])

    @pl.when(step == 0)
    def _():
        meet_all(n)
        scatter().start()
        RowSwap(n, n_dp, wgrad_ref, swapped_ref, *sems[:2], True).start()

    @pl.when(step == 2)
    def _():
        scatter().pairs()

    @pl.when(step == steps - 2)
    def _():
        scatter().spread.relay()

    rows = branch_ref.shape[0]
    here = pl.ds(pl.multiple_of(step * rows, rows), rows)

    @pl.when(step == 0)
    def _():
        gains_ref[...] = jnp.zeros_like(gains_ref)

    dk_ref[here, :] = jnp.zeros((rows, HD), F32)
    dv_ref[here, :] = jnp.zeros((rows, HD), F32)
    dqa_ref[...] = jnp.zeros_like(dqa_ref)
    attn_grad = dot(branch_ref[...], wout_ref[...], NT)
    grads = []
    shifts = []
    for head in range(heads):
        cols = slice(head * HD, (head + 1) * HD)
        part = attn_grad[:, cols]
        inv_total = 1.0 / total_ref[:, head : head + 1]
        delta = jnp.sum(part * attn_ref[:, cols].astype(F32), axis=-1, keepdims=True)
        grads.append((part * inv_total).astype(BF16))
        shifts.append(delta * inv_total)
    row_pos = step * rows + lax.broadcasted_iota(jnp.int32, (rows, rows), 0)
    col_off = lax.broadcasted_iota(jnp.int32, (rows, rows), 1)

    def one(block, carry):
        at = pl.ds(pl.multiple_of(block * rows, rows), rows)
        key = k_ref[at, :]
        val = v_ref[at, :]
        allowed = (docc_ref[...] == docr_ref[:, at]) & (block * rows + col_off <= row_pos)
        columns = [slice(head * HD, (head + 1) * HD) for head in range(heads)]
        queries = [q_ref[:, cols] for cols in columns]
        scores = [dot(query, key, NT) for query in queries]
        prods = [dot(grad, val, NT) for grad in grads]
        expos = [jnp.where(allowed, jnp.exp2(score * SCALE2), 0.0) for score in scores]
        score_grads = [
            (expo * (prod - shift)).astype(BF16) for expo, prod, shift in zip(expos, prods, shifts)
        ]
        expos = [expo.astype(BF16) for expo in expos]
        dv = sum(dot(expo, grad, TN) for expo, grad in zip(expos, grads))
        dk = sum(dot(each, query, TN) for each, query in zip(score_grads, queries))
        for cols, each in zip(columns, score_grads):
            dqa_ref[:, cols] += dot(each, key)
        dk_ref[at, :] += dk
        dv_ref[at, :] += dv
        return carry

    lax.fori_loop(jnp.maximum(step - back, 0), step + 1, one, 0)
    cosine = cos_ref[here, :]
    sine = sin_ref[here, :]
    for head in range(heads):
        cols = slice(head * HD, (head + 1) * HD)
        grad, gain_part = head_backward(
            qlin_ref[:, cols], qgain_ref[...], cosine, sine, dqa_ref[:, cols] * SCALE
        )
        dqkv_ref[here, cols] = grad.astype(BF16)
        gains_ref[0:1, :] += gain_part

    @pl.when(step == pl.num_programs(0) - 1)
    def _():
        def finish(block, carry):
            at = pl.ds(pl.multiple_of(block * rows, rows), rows)
            grad, gain_part = head_backward(
                klin_ref[at, :], kgain_ref[...], cos_ref[at, :], sin_ref[at, :], dk_ref[at, :] * SCALE
            )
            first_core = lax.axis_index("ctx") % 2 == 0
            dk_ref[at, :] = jnp.where(first_core, grad, dv_ref[at, :])
            give_ref[at, :] = jnp.where(first_core, dv_ref[at, :], grad).astype(BF16)
            gains_ref[1:2, :] += gain_part
            return carry

        lax.fori_loop(0, pl.num_programs(0), finish, 0)
        trade = push(give_ref, take_ref, sems[10], sems[11], "ctx", Plane(n).mate)
        trade.start()
        sums = scatter()
        sums.spread.gathered()

        def add(at):
            final_ref[at, :] = (after_ref[at, :] + sums.total(at)).astype(BF16)

        by_rows(rows, add)
        sums.finish()
        trade.wait_recv()

        def join(block, carry):
            at = pl.ds(pl.multiple_of(block * rows, rows), rows)
            total = dk_ref[at, :] + take_ref[at, :].astype(F32)
            dqkv_ref[at, heads * HD :] = total.astype(BF16)
            return carry

        lax.fori_loop(0, pl.num_programs(0), join, 0)
        trade.wait_send()
        swap = RowSwap(n, n_dp, wgrad_ref, swapped_ref, *sems[:2], True)
        swap.arrive()
        swap.finish()


def attn_backward(n, n_dp, wgrad, moe, after, branch, wout, attn, total, q, k, v, qlin, klin, cosine, sine, qgain, kgain, doc, rows):
    length, width = branch.shape
    qw = wout.shape[0]
    heads = qw // HD
    blk = lambda cols: pl.BlockSpec((rows, cols), lambda i: (i, 0))
    whole = lambda shape: pl.BlockSpec(shape, lambda i: (0, 0), pipeline_mode=pl.Buffered(1))
    shape = jax.ShapeDtypeStruct
    full = whole((length, HD))
    return pl.pallas_call(
        functools.partial(attn_backward_kernel, n, n_dp, heads, MOST // rows),
        grid=(length // rows,),
        in_specs=[
            blk(width),
            whole(wout.shape),
            blk(qw),
            blk(HD),
            blk(qw),
            full,
            full,
            blk(qw),
            full,
            full,
            full,
            whole((1, HD)),
            whole((1, HD)),
            blk(1),
            whole((1, length)),
            ANY,
            ANY,
            whole(after.shape),
        ],
        out_specs=[whole((length, qw + HD)), whole((8, HD)), ANY, whole(after.shape)],
        out_shape=[
            shape((length, qw + HD), BF16),
            shape((8, HD), F32),
            shape(wgrad.shape, BF16),
            shape(after.shape, BF16),
        ],
        scratch_shapes=[
            pltpu.VMEM((length, HD), F32),
            pltpu.VMEM((length, HD), F32),
            pltpu.VMEM((rows, qw), F32),
            pltpu.VMEM((length, HD), BF16),
            pltpu.VMEM((length, HD), BF16),
            DMA((n_dp,)),
            DMA((n_dp,)),
        ]
        + scatter_scratch(n, *after.shape)
        + [DMA(()), DMA(())],
        compiler_params=pltpu.CompilerParams(
            collective_id=9, has_side_effects=True, vmem_limit_bytes=VMEM_LIMIT
        ),
        cost_estimate=pl.CostEstimate(
            flops=60 * 10**9, transcendentals=0, bytes_accessed=30 * 2**20
        ),
        name="attn_backward",
    )(branch, wout, attn, total, q, k, v, qlin, klin, cosine, sine, qgain, kgain, doc[:, None], doc[None, :], wgrad, moe, after)


def expert_kernel(chained, low, aliased, split, plan, z_ref, n2_ref, top_ref, prob_ref, *rest):
    if aliased:
        rest = rest[1:]
    if chained:
        moe_in, row_in = rest[:2]
        rest = rest[2:]
    sources, rest = rest[: len(plan)], rest[len(plan) :]
    moe_ref, row_ref, rest = rest[0], rest[1], rest[2:]
    if split:
        gg_ref, ug_ref, rest = rest[0], rest[1], rest[2:]
    grads_ref, wg_ref, wu_ref, wd_ref, rest = *rest[:4], rest[4:]
    sums, (stage, wsem, sem) = rest[:-3], rest[-3:]
    ad_ref = sums[-1]
    step = pl.program_id(0)
    rows, width = n2_ref.shape
    parts, cut, hidden = wd_ref.shape
    weights = (wg_ref, wu_ref, wd_ref)

    @pl.when(step == 0)
    def _():
        z = z_ref[0]
        for source, (kind, amount, start) in zip(sources, plan):
            count = source.shape[-2] // cut
            for k in range(parts) if kind == "all" else [amount]:
                if kind == "all":
                    src, owner, wanted = source.at[k], k, None
                elif kind == "up":
                    src, owner, wanted = source, z - k, z >= k
                else:
                    src, owner, wanted = source, z + k, z + k < parts

                def load(src=src, owner=owner, start=start, count=count):
                    for piece in range(count):
                        pltpu.make_async_copy(
                            src.at[pl.ds(piece * cut, cut), :],
                            weights[start + piece].at[owner],
                            wsem.at[start + piece, owner],
                        ).start()

                if wanted is None:
                    load()
                else:
                    pl.when(wanted)(load)
        for each in sums:
            each[...] = jnp.zeros_like(each)
        for index in range(3):
            for owner in range(parts):
                block = weights[index].at[owner]
                pltpu.make_async_copy(block, block, wsem.at[index, owner]).wait()

    n2 = n2_ref[...]
    prob = prob_ref[...]
    wg = wg_ref[...].reshape(width, hidden)
    wu = wu_ref[...].reshape(width, hidden)
    gate = dot(n2, wg)
    up = dot(n2, wu)
    sig = 1.0 / (1.0 + jnp.exp(-gate))
    silu = gate * sig
    act = (silu * up).astype(BF16)
    act_grad = jnp.zeros((rows, hidden), F32)
    for z in range(parts):
        cols = slice(z * cut, (z + 1) * cut)
        out = dot(act, wd_ref[z], NT).astype(BF16).astype(F32) * prob
        if chained:
            out = out + moe_in[:, cols].astype(F32)
        moe_ref[:, cols] = out.astype(BF16)
        route = (top_ref[:, cols].astype(F32) * prob).astype(BF16)
        act_grad += dot(route, wd_ref[z])
        ad_ref[z] += dot(route, act, TN)
    gate_grad = (act_grad * up * sig * (1.0 + gate * (1.0 - sig))).astype(BF16)
    up_grad = (act_grad * silu).astype(BF16)
    row = dot(gate_grad, wg, NT) + dot(up_grad, wu, NT)
    if chained:
        row = row + row_in[...].astype(F32)
    row_ref[...] = row.astype(BF16)
    if split:
        gg_ref[...] = gate_grad
        ug_ref[...] = up_grad
    else:
        sums[0][...] += dot(n2, gate_grad, TN).reshape(parts, cut, hidden)
        sums[1][...] += dot(n2, up_grad, TN).reshape(parts, cut, hidden)

    @pl.when(step == pl.num_programs(0) - 1)
    def _():
        copies = []
        pieces = [
            (acc, place, z) for z in range(parts) for place, acc in enumerate(sums)
        ]
        for index, (acc, place, z) in enumerate(pieces):
            slot = index % 2
            if index >= 2:
                copies[index - 2].wait()
            stage[slot] = acc[z].astype(BF16)
            copies.append(
                pltpu.make_async_copy(
                    stage.at[slot],
                    grads_ref.at[z, pl.ds(place * cut, cut), pl.ds(low, acc.shape[2])],
                    sem.at[slot],
                )
            )
            copies[-1].start()
        copies[-2].wait()
        copies[-1].wait()


def expert(z, n2, top, prob, n_dp, sources, before, rows, low, full, grads, split):
    length, width = n2.shape
    cut = width // n_dp
    hidden = sources[0][0].shape[-1]
    blk = pl.BlockSpec((rows, width), lambda i: (i, 0))
    col = pl.BlockSpec((rows, 1), lambda i: (i, 0))
    thin = pl.BlockSpec((rows, hidden), lambda i: (i, 0))
    shape = jax.ShapeDtypeStruct
    plan = tuple(entry[1:] for entry in sources)
    weight = pltpu.VMEM((n_dp, cut, hidden), BF16)
    total = pltpu.VMEM((n_dp, cut, hidden), F32)
    return pl.pallas_call(
        functools.partial(expert_kernel, len(before) > 0, low, len(grads) > 0, split, plan),
        grid=(length // rows,),
        in_specs=[pl.BlockSpec(memory_space=pltpu.SMEM), blk, blk, col]
        + [ANY] * len(grads)
        + [blk] * len(before)
        + [ANY] * len(sources),
        out_specs=[blk, blk] + [thin] * (2 * split) + [ANY],
        out_shape=[
            shape((length, width), BF16),
            shape((length, width), BF16),
        ]
        + [shape((length, hidden), BF16)] * (2 * split)
        + [shape((n_dp, cut if split else 3 * cut, full), BF16)],
        input_output_aliases={4: 2} if grads else {},
        scratch_shapes=[weight] * 3
        + [total] * (1 if split else 3)
        + [pltpu.VMEM((2, cut, hidden), BF16), DMA((3, n_dp)), DMA((2,))],
        compiler_params=pltpu.CompilerParams(vmem_limit_bytes=VMEM_LIMIT),
        cost_estimate=pl.CostEstimate(
            flops=18 * length * width * hidden,
            transcendentals=length * hidden,
            bytes_accessed=5 * length * width * 2,
        ),
        name="expert",
    )(z, n2, top, prob, *grads, *before, *[entry[0] for entry in sources])


def unpack_kernel(
    z_ref, pair_ref, down_one_ref, all_ref, up0_ref, down0_ref, up1_ref, down1_ref, dg_ref, du_ref, dd_ref, own, sem
):
    copy = pltpu.make_async_copy(all_ref.at[z_ref[0]], own, sem)
    copy.start()
    cut = dg_ref.shape[1]
    half = up0_ref.shape[0]
    piece = [slice(k * cut, (k + 1) * cut) for k in range(2)]
    dg_ref[1] = pair_ref[piece[0], :].astype(F32)
    du_ref[1] = pair_ref[piece[1], :].astype(F32)
    dd_ref[1] = jnp.transpose(down_one_ref[...].astype(F32))
    copy.wait()

    def total(low, high):
        shift, up, down = (0, up0_ref, down0_ref) if high <= half else (half, up1_ref, down1_ref)
        there = slice(low - shift, high - shift)
        value = own[low:high, :].astype(F32)
        return value + up[there, :].astype(F32) + down[there, :].astype(F32)

    dg_ref[0] = total(0, cut)
    du_ref[0, : half - cut] = total(cut, half)
    du_ref[0, half - cut :] = total(half, 2 * cut)
    dd_ref[0] = jnp.transpose(total(2 * cut, 3 * cut))


def unpack(z, pair, one, grads, got):
    cut, hidden = one.shape
    rows = 3 * cut
    shape = jax.ShapeDtypeStruct
    return pl.pallas_call(
        unpack_kernel,
        in_specs=[pl.BlockSpec(memory_space=pltpu.SMEM), VM, VM, ANY, VM, VM, VM, VM],
        out_specs=[VM] * 3,
        out_shape=[
            shape((2, cut, hidden), F32),
            shape((2, cut, hidden), F32),
            shape((2, hidden, cut), F32),
        ],
        scratch_shapes=[pltpu.VMEM((rows, hidden), BF16), DMA(())],
        compiler_params=pltpu.CompilerParams(vmem_limit_bytes=VMEM_LIMIT),
        name="unpack",
    )(z, pair, one, grads, *got)


def line_hop(block_up, block_down, n_dp, hop):
    up = [(i, i + 1) for i in range(hop - 1, n_dp - 1)]
    down = [(i + 1, i) for i in range(n_dp - hop)]
    return lax.ppermute(block_up, "dp", up), lax.ppermute(block_down, "dp", down)


def reduce_hop(grads, got, n_dp, hop, rows, before):
    place = lax.axis_index("dp")
    reach = n_dp - hop
    zero = jnp.int32(0)
    size = (1, rows[1] - rows[0], grads.shape[2])
    spots = (jnp.minimum(place + reach, n_dp - 1), jnp.maximum(place - reach, 0))
    if got is not None:
        got = lax.optimization_barrier((*got, *before))[:2]
    elif before:
        grads = after_of(grads, *before)
    blocks = [
        lax.dynamic_slice(grads, (spot.astype(jnp.int32), jnp.int32(rows[0]), zero), size)[0]
        for spot in spots
    ]
    if got is not None:
        blocks = [(b.astype(F32) + g.astype(F32)).astype(BF16) for b, g in zip(blocks, got)]
    up = [(i, i + 1) for i in range(hop)]
    down = [(i, i - 1) for i in range(n_dp - hop, n_dp)]
    sent = lax.ppermute(blocks[0], "dp", up), lax.ppermute(blocks[1], "dp", down)
    return sent, tuple(blocks)


def after_of(value, *others):
    return lax.optimization_barrier((value,) + others)[0]


def per_device(
    layer_input,
    doc_ids,
    route_ids,
    route_probs,
    attn_gain,
    ffn_gain,
    query_gain,
    key_gain,
    w_query,
    w_key,
    w_value,
    w_out,
    w_gate,
    w_up,
    w_down,
    out_grad,
):
    tokens, width = layer_input.shape[1:]
    n_dp = lax.axis_size("dp")
    n_ctx = lax.axis_size("ctx")
    ctx_index = lax.axis_index("ctx")
    length = tokens * n_ctx
    heads = HQ // n_ctx
    share = n_ctx // KV
    qw = heads * HD
    depth = w_query.shape[0]
    own_e = w_gate.shape[0]

    cut = attn_gain.shape[0]
    hcut = query_gain.shape[0]
    kinds = 2 * (cut + hcut)
    small = jnp.concatenate([attn_gain, ffn_gain, query_gain, key_gain]).astype(F32)
    small = jnp.pad(small, (0, 1024 - kinds)).reshape(8, HD)
    even = (jnp.arange(n_ctx) % 2 == 0)[None, :, None]
    wide = [jnp.repeat(w.reshape(depth, KV, HD), share, axis=1) for w in (w_key, w_value)]
    cols = jnp.concatenate(
        [w_query.reshape(depth, n_ctx, qw), jnp.where(even, wide[0], wide[1])], axis=2
    ).transpose(1, 0, 2)
    hidden = w_gate.shape[2]
    cuts = ((0, 256), (256, hidden))
    cols, small, *blocks0 = prep(
        n_ctx, n_dp, cols, small, cuts, (w_gate, w_up, w_down)
    )
    small = small.reshape(n_dp * n_ctx, 1024)
    gain_attn = small[:, :cut].reshape(1, width)
    gain_ffn = small[:, cut : 2 * cut].reshape(1, width)
    gain_query = small[:, 2 * cut : 2 * cut + hcut].reshape(1, HD)
    gain_key = small[:, 2 * cut + hcut : kinds].reshape(1, HD)
    wqkv = lax.all_gather(cols.reshape(n_ctx * depth, qw + HD), "dp", axis=0, tiled=True)
    wrows = lax.all_gather(w_out, "dp", axis=0, tiled=False)

    inputs = layer_input.reshape(tokens, width)
    top_own = out_grad.reshape(tokens, width)
    n_experts = own_e * n_ctx
    match = route_ids.reshape(1, tokens, TOP) == jnp.arange(n_experts, dtype=jnp.int32)[:, None, None]
    probs = jnp.sum(jnp.where(match, route_probs.reshape(1, tokens, TOP), 0.0), axis=2)
    info = jnp.concatenate(
        [probs, doc_ids.reshape(1, tokens).astype(F32), jnp.zeros((7, tokens), F32)], axis=0
    )
    normed, info, top_all, block1 = first(
        n_ctx, inputs, gain_attn, info, top_own, ((0, hidden),), (w_gate, w_up, w_down)
    )
    normed = normed.reshape(length, width)
    doc = info[:, n_experts].reshape(length).astype(jnp.int32)
    my_probs = lax.dynamic_slice_in_dim(info, ctx_index * own_e, own_e, 1)
    my_probs = my_probs.transpose(0, 2, 1).reshape(length, own_e)

    inverse = 1.0 / ROPE_BASE ** (jnp.arange(HD // 2, dtype=F32) * 2.0 / HD)
    angles = jnp.arange(length, dtype=F32)[:, None] * inverse[None, :]
    cosine = jnp.cos(angles)
    sine = jnp.sin(angles)
    cosine = jnp.concatenate([cosine, cosine], axis=1)
    sine = jnp.concatenate([-sine, sine], axis=1)
    qlin, klin, q, k, v, attn, total, wout = attn_forward(
        n_ctx, n_dp, normed, wqkv, cosine, sine, gain_query, gain_key, doc, wrows, tokens
    )
    wout = wout.reshape(qw, width)
    top_all = top_all.reshape(length, width)
    blocks = (n_ctx, tokens, width)
    after, normed2 = middle(n_ctx, attn, wout, inputs, gain_ffn)
    normed2 = normed2.reshape(length, width)

    z = lax.axis_index("dp").astype(jnp.int32).reshape(1)
    hidden = w_gate.shape[2]

    def run(e, sources, carried, low, grads, split=False):
        moe, rows_grad, *grads = expert(
            z,
            normed2,
            top_all,
            my_probs[:, e : e + 1],
            n_dp,
            sources,
            carried,
            tokens,
            low,
            hidden,
            grads,
            split,
        )
        return (moe, rows_grad), grads

    carried, grads0 = (), ()
    for index, (low, high) in enumerate(cuts):
        full = lax.all_gather(blocks0[index], "dp", axis=0, tiled=False)
        if index == 1:
            sources1 = [(block1, "up", 0, 0)]
            up = down = after_of(block1, full)
            up, down = line_hop(up, down, n_dp, 1)
            sources1 += [(up, "up", 1, 0), (down, "down", 1, 0)]
        carried, (grads,) = run(0, [(full, "all", 0, 0)], carried, low, grads0)
        grads0 = (grads,)
    rows_all = 3 * (width // n_dp)
    spans = {"a": (0, rows_all // 2), "b": (rows_all // 2, rows_all)}
    got, before = {tag: None for tag in spans}, ()
    for hop in range(2, n_dp + 1):
        if hop < n_dp:
            up, down = line_hop(up, down, n_dp, hop)
            sources1 += [(up, "up", hop, 0), (down, "down", hop, 0)]
        for tag, rows in spans.items():
            got[tag], before = reduce_hop(grads, got[tag], n_dp, hop - 1, rows, before)
    split = n_ctx == 8
    (moe, rows_grad), grads1 = run(1, sources1, carried, 0, (), split)
    rows_grad = rows_grad.reshape(blocks)
    if split:
        gate_grad, up_grad, down_grad = grads1
        done_d = lax.psum_scatter(
            down_grad.reshape(width, hidden), "dp", scatter_dimension=0, tiled=True
        )
        mid, ffn_part, low_mid, pair_grad = halfway(
            n_ctx, n_dp, rows_grad, normed2, gate_grad, up_grad, after, top_own, gain_ffn
        )
        done_gu = lax.psum_scatter(
            pair_grad.reshape(2 * width, hidden), "dp", scatter_dimension=0, tiled=True
        )
        branch = share_rows(n_ctx, low_mid)
    else:
        done = lax.psum_scatter(
            grads1[0].reshape(3 * width, hidden), "dp", scatter_dimension=0, tiled=True
        )
        done_gu, done_d = done[: 2 * width // n_dp], done[2 * width // n_dp :]
        mid, ffn_part, branch = turn(n_ctx, rows_grad, after, top_own, gain_ffn)
    branch = branch.reshape(length, width)

    out_w = dot(attn, branch, TN).astype(BF16).reshape(n_dp, qw // n_dp, width)
    dqkv, gains, out_w, layer_output = attn_backward(
        n_ctx,
        n_dp,
        out_w,
        moe.reshape(blocks),
        after,
        branch,
        wout,
        attn,
        total,
        q,
        k,
        v,
        qlin,
        klin,
        cosine,
        sine,
        gain_query,
        gain_key,
        doc,
        tokens,
    )
    qkv_w = dot(normed, dqkv, TN).astype(BF16)
    qkv_w = lax.psum_scatter(qkv_w, "dp", scatter_dimension=0, tiled=True)
    out_w = lax.psum_scatter(out_w.reshape(qw, width), "dp", scatter_dimension=0, tiled=True)
    out_w = out_w.astype(F32)
    input_grad, attn_part = last(n_ctx, dqkv, wqkv, inputs, mid, gain_attn)
    n_all = n_dp * n_ctx
    packed = jnp.concatenate(
        [
            attn_part[0].reshape(n_all, cut),
            ffn_part[0].reshape(n_all, cut),
            gains[0].reshape(n_all, hcut),
            gains[1].reshape(n_all, hcut),
            jnp.zeros((n_all, 1024 - kinds), F32),
        ],
        axis=1,
    )
    packed = packed.reshape(n_dp, n_ctx, 8, HD).transpose(1, 0, 2, 3)
    packed = gains_sum(n_ctx, n_dp, packed)
    packed = packed.reshape(1024)
    query_w, key_w, value_w = post(n_ctx, qkv_w.reshape(n_ctx, depth, qw + HD))
    gate_w, up_w, down_w = unpack(z, done_gu, done_d, grads, got["a"] + got["b"])
    return (
        layer_output.reshape(1, tokens, width),
        input_grad.reshape(1, tokens, width),
        packed[:cut],
        packed[cut : 2 * cut],
        packed[2 * cut : 2 * cut + hcut],
        packed[2 * cut + hcut : kinds],
        query_w,
        key_w,
        value_w,
        out_w,
        gate_w,
        up_w,
        down_w,
    )


def solution(mesh):
    both = ("dp", "ctx")
    seq = P("dp", "ctx", None)
    in_specs = (
        seq,
        P("dp", "ctx"),
        seq,
        seq,
        P(both),
        P(both),
        P(both),
        P(both),
        P(both, None),
        P(both, None),
        P(both, None),
        P(both, None),
        P("ctx", "dp", None),
        P("ctx", "dp", None),
        P("ctx", None, "dp"),
        seq,
    )
    out_specs = (
        seq,
        seq,
        P(both),
        P(both),
        P(both),
        P(both),
        P(both, None),
        P(both, None),
        P(both, None),
        P(both, None),
        P("ctx", "dp", None),
        P("ctx", "dp", None),
        P("ctx", None, "dp"),
    )

    return jax.shard_map(
        per_device, mesh=mesh, in_specs=in_specs, out_specs=out_specs, check_vma=False
    )
```

```python
import functools
import math

import jax
import jax.numpy as jnp
from jax import lax
from jax.experimental import pallas as pl
from jax.experimental.pallas import tpu as pltpu
from jax.sharding import PartitionSpec as P


HQ = 32
KV = 4
HD = 128
TOP = 8
MOST = 1024
EPS = 1e-06
ROPE_BASE = 1000000.0
F32 = jnp.float32
BF16 = jnp.bfloat16
SCALE = 1.0 / math.sqrt(HD)
SCALE2 = SCALE / math.log(2.0)
VMEM_LIMIT = 60 * 1024 * 1024


def dot(left, right, dims=((1,), (0,))):
    return lax.dot_general(left, right, (dims, ((), ())), preferred_element_type=F32)


NT = ((1,), (1,))
TN = ((0,), (0,))


def rms_parts(values):
    return lax.rsqrt(jnp.mean(values * values, axis=-1, keepdims=True) + EPS)


def rms_back(grad, unit, inv, gain):
    scaled = grad * gain
    return inv * (scaled - unit * jnp.mean(scaled * unit, axis=-1, keepdims=True))


def head_forward(lin, gain, cosine, sine):
    unit = lin * rms_parts(lin) * gain
    return unit * cosine + pltpu.roll(unit, HD // 2, 1) * sine


def head_backward(lin, gain, cosine, sine, rot_grad):
    grad = rot_grad * cosine + pltpu.roll(rot_grad * sine, HD // 2, 1)
    inv = rms_parts(lin)
    unit = lin * inv
    return rms_back(grad, unit, inv, gain), jnp.sum(grad * unit, axis=0, keepdims=True)


MESH = pl.DeviceIdType.MESH
ANY = pl.BlockSpec(memory_space=pl.ANY)
VM = pl.BlockSpec(memory_space=pltpu.VMEM)
DMA = pltpu.SemaphoreType.DMA
CHUNK = 32


def flip(index, mask, count):
    result, bit = 0, 1
    while bit < count:
        digit = (index // bit) % 2
        result = result + bit * ((1 - digit) if mask & bit else digit)
        bit *= 2
    return result


def push(src, dst, send, recv, axis, peer):
    return pltpu.make_async_remote_copy(
        src_ref=src,
        dst_ref=dst,
        send_sem=send,
        recv_sem=recv,
        device_id={axis: peer},
        device_id_type=MESH,
    )


def meet(peers):
    barrier = pltpu.get_barrier_semaphore()
    for axis, peer in peers:
        pl.semaphore_signal(barrier, inc=1, device_id={axis: peer}, device_id_type=MESH)
    pl.semaphore_wait(barrier, len(peers))


class Plane:
    def __init__(self, n):
        self.chips = n // 2
        self.me = lax.axis_index("ctx")
        self.core = self.me % 2
        self.chip = self.me // 2
        self.mate = self.me + 1 - 2 * self.core

    def same(self, s):
        return 2 * flip(self.chip, s, self.chips) + self.core

    def meet(self):
        meet([("ctx", self.same(s)) for s in range(1, self.chips)] + [("ctx", self.mate)])


def far_first(chips):
    return sorted(range(1, chips), key=lambda s: -bin(s).count("1"))


class Gather:
    def __init__(self, plane, src, out, send, recv, local):
        self.plane, self.out, self.send, self.recv = plane, out, send, recv
        self.own = pltpu.make_async_copy(src, out.at[plane.me], local)
        self.far = [
            push(src, out.at[plane.me], send.at[s], recv.at[s], "ctx", plane.same(s))
            for s in far_first(plane.chips)
        ]
        self.near = push(src, out.at[plane.me], send.at[0], recv.at[0], "ctx", plane.mate)

    def start(self):
        for copy in self.far:
            copy.start()
        self.near.start()
        self.own.start()

    def forward(self):
        plane, out = self.plane, self.out
        self.passed = []
        for s in sorted(range(1, plane.chips), key=lambda s: bin(s).count("1")):
            block = out.at[plane.same(s)]
            push(block, block, self.send.at[s], self.recv.at[s], "ctx", plane.mate).wait_recv()
            slot = plane.chips + s
            copy = push(block, block, self.send.at[slot], self.recv.at[slot], "ctx", plane.mate)
            copy.start()
            self.passed.append(copy)

    def finish(self):
        for copy in self.far:
            copy.wait_send()
        self.near.wait_send()
        self.near.wait_recv()
        for copy in self.passed:
            copy.wait_send()
            copy.wait_recv()
        self.own.wait()


def by_rows(rows, body):
    def one(index, carry):
        body(pl.ds(pl.multiple_of(index * CHUNK, CHUNK), CHUNK))
        return carry

    lax.fori_loop(0, rows // CHUNK, one, 0)


class SquareGather:
    def __init__(self, plane, src, out, send, recv, local):
        self.plane, self.out, self.send, self.recv = plane, out, send, recv
        half = src.shape[0] // 2
        self.halves = [pl.ds(0, half), pl.ds(half, half)]
        mine = out.at[plane.me]
        self.own = pltpu.make_async_copy(src, mine, local)
        self.near = push(src, mine, send.at[0], recv.at[0], "ctx", plane.mate)
        self.far = []
        for s, h in ((1, 0), (2, 1), (1, 1), (2, 0)):
            part, slot = self.halves[h], 2 * s + h
            self.far.append(
                push(
                    src.at[part, :],
                    mine.at[part, :],
                    send.at[slot],
                    recv.at[slot],
                    "ctx",
                    plane.same(s),
                )
            )

    def start(self):
        for copy in self.far:
            copy.start()
        self.near.start()
        self.own.start()

    def arrived(self, s, h):
        block = self.out.at[self.plane.same(s)].at[self.halves[h], :]
        slot = 2 * s + h
        push(block, block, self.send.at[slot], self.recv.at[slot], "ctx", self.plane.mate).wait_recv()
        return block

    def forward(self):
        plane = self.plane
        self.passed = []
        for s, h in ((1, 0), (2, 1)):
            block = self.arrived(s, h)
            slot = 6 + h
            copy = push(block, block, self.send.at[slot], self.recv.at[slot], "ctx", plane.same(3 - s))
            copy.start()
            self.far.append(copy)
        for s in (1, 2, 3):
            if s < 3:
                self.arrived(s, 2 - s)
            else:
                self.arrived(3, 0)
                self.arrived(3, 1)
            block, slot = self.out.at[plane.same(s)], 7 + s
            copy = push(block, block, self.send.at[slot], self.recv.at[slot], "ctx", plane.mate)
            copy.start()
            self.passed.append(copy)

    def finish(self):
        for copy in self.far:
            copy.wait_send()
        self.near.wait_send()
        self.near.wait_recv()
        for copy in self.passed:
            copy.wait_send()
            copy.wait_recv()
        self.own.wait()


def gather_of(plane, src, out, send, recv, local):
    kind = SquareGather if plane.chips == 4 else Gather
    return kind(plane, src, out, send, recv, local)


class Spread:
    def __init__(self, plane, mine, landed, send, recv):
        self.plane, self.mine, self.landed = plane, mine, landed
        self.square = plane.chips == 4
        self.order = [3, 1, 2, 0] if self.square else far_first(plane.chips) + [0]
        self.send, self.recv = send, recv
        half = mine.shape[1] // 2
        self.halves = [pl.ds(0, half), pl.ds(half, half)]

    def copy(self, s, h, to):
        part, slot = self.halves[h], 2 * s + h
        return push(
            self.mine.at[s].at[part, :],
            self.landed.at[s].at[part, :],
            self.send.at[slot],
            self.recv.at[slot],
            "ctx",
            self.plane.same(to),
        )

    def go(self, s, h, to):
        self.copy(s, h, to).start()

    def ready(self, s):
        if self.square:
            if s == 3:
                self.go(3, 0, 1)
                self.go(3, 1, 2)
            elif s == 1:
                self.go(1, 0, 1)
            elif s == 2:
                self.go(2, 1, 2)
        elif s:
            push(
                self.mine.at[s],
                self.landed.at[s],
                self.send.at[s],
                self.recv.at[s],
                "ctx",
                self.plane.same(s),
            ).start()

    def sends(self):
        if self.square:
            hops = ((3, 0, 1), (3, 1, 2), (1, 0, 1), (2, 1, 2), (2, 0, 2), (1, 1, 1))
            return [self.copy(*hop) for hop in hops]
        return [
            push(
                self.mine.at[s],
                self.landed.at[s],
                self.send.at[s],
                self.recv.at[s],
                "ctx",
                self.plane.same(s),
            )
            for s in self.order
            if s
        ]

    def relay(self):
        mine, landed = self.mine, self.landed
        half = mine.shape[1] // 2
        if not self.square:
            return
        for s, h in ((2, 0), (1, 1)):
            self.copy(3, h, 1).wait_recv()

            def add(at, s=s, h=h):
                rows = pl.ds(h * half + at.start, CHUNK)
                total = mine[s, rows, :].astype(F32) + landed[3, rows, :].astype(F32)
                mine[s, rows, :] = total.astype(BF16)

            by_rows(half, add)
            self.copy(s, h, s).start()

    def gathered(self):
        if not self.square:
            for copy in self.sends():
                copy.wait_recv()
            return
        for s in (1, 2):
            for h in (0, 1):
                self.copy(s, h, s).wait_recv()

    def settle(self, extra=None):
        self.relay()
        if extra is not None:
            extra()
        self.gathered()

    def total(self, at):
        value = self.mine[0, at, :].astype(F32)
        for s in (1, 2) if self.square else range(1, self.plane.chips):
            value = value + self.landed[s, at, :].astype(F32)
        return value

    def finish(self):
        for copy in self.sends():
            copy.wait_send()


class Scatter:
    def __init__(self, plane, part, mine, other, landed, send, recv, send2, recv2, local):
        self.plane, self.mine, self.other = plane, mine, other
        self.spread = Spread(plane, mine, landed, send2, recv2)
        self.order = self.spread.order
        self.loads, self.across = {}, {}
        for s in self.order:
            block = plane.same(s)
            self.loads[s] = pltpu.make_async_copy(part.at[block], mine.at[s], local.at[s])
            self.across[s] = push(
                part.at[block + 1 - 2 * plane.core],
                other.at[s],
                send.at[s],
                recv.at[s],
                "ctx",
                plane.mate,
            )

    def start(self):
        for s in self.order:
            self.across[s].start()
            self.loads[s].start()

    def pairs(self):
        mine, other = self.mine, self.other
        for s in self.order:
            self.loads[s].wait()
            self.across[s].wait_recv()

            def add(at, s=s):
                total = mine[s, at, :].astype(F32) + other[s, at, :].astype(F32)
                mine[s, at, :] = total.astype(BF16)

            by_rows(mine.shape[1], add)
            self.spread.ready(s)

    def run(self):
        self.pairs()
        self.spread.settle()

    def total(self, at):
        return self.spread.total(at)

    def finish(self):
        for s in self.order:
            self.across[s].wait_send()
        self.spread.finish()


class Product:
    def __init__(self, plane, value, mine, other, landed, given, send, recv, send2, recv2):
        self.plane, self.value = plane, value
        self.mine, self.other, self.given = mine, other, given
        self.spread = Spread(plane, mine, landed, send2, recv2)
        self.order = self.spread.order
        self.across = {
            s: push(given.at[s], other.at[s], send.at[s], recv.at[s], "ctx", plane.mate)
            for s in self.order
        }

    def start(self):
        plane = self.plane
        for s in self.order:
            block = plane.same(s) + 1 - 2 * plane.core

            def fill(at, s=s, block=block):
                self.given[s, :, at] = self.value(block, at).astype(BF16)

            by_cols(self.mine.shape[2], fill)
            self.across[s].start()

    def run(self, extra=None):
        plane, mine, other = self.plane, self.mine, self.other
        for s in self.order:
            block = plane.same(s)
            self.across[s].wait_recv()

            def fill(at, s=s, block=block):
                total = self.value(block, at) + other[s, :, at].astype(F32)
                mine[s, :, at] = total.astype(BF16)

            by_cols(mine.shape[2], fill)
            self.spread.ready(s)
        self.spread.settle(extra)

    total = Scatter.total
    finish = Scatter.finish


def by_cols(width, body):
    span = 512

    def one(index, carry):
        body(pl.ds(pl.multiple_of(index * span, span), span))
        return carry

    lax.fori_loop(0, width // span, one, 0)


def gather_sems(n):
    return [DMA((12 if n == 8 else n,)), DMA((12 if n == 8 else n,)), DMA(())]


def scatter_scratch(n, rows, width):
    chips = n // 2
    return (
        [pltpu.VMEM((chips, rows, width), BF16)] * 3
        + [DMA((chips,)), DMA((chips,)), DMA((n,)), DMA((n,))]
        + [DMA((chips,))]
    )


def product_scratch(n, rows, width):
    chips = n // 2
    return [pltpu.VMEM((chips, rows, width), BF16)] * 4 + [
        DMA((chips,)),
        DMA((chips,)),
        DMA((n,)),
        DMA((n,)),
    ]


def comm_call(kernel, ident, outs, out_specs, in_specs, scratch, micros, *args):
    return pl.pallas_call(
        kernel,
        out_shape=outs,
        in_specs=in_specs,
        out_specs=out_specs,
        scratch_shapes=scratch,
        compiler_params=pltpu.CompilerParams(
            collective_id=ident, has_side_effects=True, vmem_limit_bytes=VMEM_LIMIT
        ),
        cost_estimate=pl.CostEstimate(
            flops=0, transcendentals=0, bytes_accessed=int(micros * 3.0e6)
        ),
    )(*args)


def swap_all(n, src, out, send, recv, local):
    me = lax.axis_index("ctx")
    own = pltpu.make_async_copy(src.at[me], out.at[me], local)
    own.start()
    copies = []
    for s in range(n - 1, 0, -1):
        peer = flip(me, s, n)
        copies.append(push(src.at[peer], out.at[me], send.at[s], recv.at[s], "ctx", peer))
        copies[-1].start()
    return own, copies


class RowSwap:
    def __init__(self, n, n_dp, src, dst, send, recv, spread):
        self.me = lax.axis_index("ctx")
        self.dst, self.send, self.recv, self.n_dp = dst, send, recv, n_dp
        self.entries = []
        for k in range(n_dp):
            flat = self.me * n_dp + k if spread else k * n + self.me
            peer = flat % n if spread else flat // n_dp
            slot = flat // n if spread else flat % n_dp
            far = push(src.at[k], dst.at[slot], send.at[k], recv.at[slot], "ctx", peer)
            near = pltpu.make_async_copy(src.at[k], dst.at[slot], recv.at[slot])
            self.entries.append((peer, far, near))

    def start(self):
        for peer, far, near in self.entries:
            pl.when(peer != self.me)(far.start)
            pl.when(peer == self.me)(near.start)

    def arrive(self):
        for slot in range(self.n_dp):
            block = self.dst.at[slot]
            pltpu.make_async_copy(block, block, self.recv.at[slot]).wait()

    def finish(self):
        for peer, far, near in self.entries:
            pl.when(peer != self.me)(far.wait_send)


def meet_all(n):
    me = lax.axis_index("ctx")
    meet([("ctx", flip(me, s, n)) for s in range(1, n)])


class Pack:
    def __init__(self, e, sources, buffers, sems):
        self.buffers = buffers
        self.loads = [
            pltpu.make_async_copy(source.at[e], buffer, sems.at[k])
            for k, (source, buffer) in enumerate(zip(sources, buffers))
        ]

    def start(self):
        for load in self.loads:
            load.start()

    def write(self, cuts, outs):
        for load in self.loads:
            load.wait()
        gate, up, down = self.buffers
        cut = gate.shape[0]
        for (low, high), out in zip(cuts, outs):
            out[:cut, :] = gate[:, low:high]
            out[cut : 2 * cut, :] = up[:, low:high]
            out[2 * cut :, :] = jnp.transpose(down[low:high, :].astype(F32)).astype(BF16)


def pack_scratch(weights):
    return [pltpu.VMEM(w.shape[1:], BF16) for w in weights] + [DMA((3,))]


def pack_shapes(cuts, weights):
    cut = weights[0].shape[1]
    return [jax.ShapeDtypeStruct((3 * cut, high - low), BF16) for low, high in cuts]


def prep_kernel(n, n_dp, cuts, cols_ref, small_ref, *rest):
    sources, rest = rest[:3], rest[3:]
    out_ref, all_ref, rest = rest[0], rest[1], rest[2:]
    packed, rest = rest[: len(cuts)], rest[len(cuts) :]
    pack = Pack(0, sources, rest[:3], rest[3])
    pack.start()
    send, recv, local, gsend, grecv, zsend, zrecv = rest[4:]
    me, row = lax.axis_index("ctx"), lax.axis_index("dp")
    meet(
        [("ctx", flip(me, s, n)) for s in range(1, n)]
        + [("dp", flip(row, s, n_dp)) for s in range(1, n_dp)]
    )
    all_ref[row, me] = small_ref[...]
    smalls = []
    for s in range(1, n):
        peer = flip(me, s, n)
        smalls.append(push(small_ref, all_ref.at[row, me], gsend.at[s], grecv.at[s], "ctx", peer))
        smalls[-1].start()
    own, copies = swap_all(n, cols_ref, out_ref, send, recv, local)
    pack.write(cuts, packed)
    for copy in smalls:
        copy.wait_recv()
    planes = []
    for s in range(1, n_dp):
        peer = flip(row, s, n_dp)
        planes.append(push(all_ref.at[row], all_ref.at[row], zsend.at[s], zrecv.at[s], "dp", peer))
        planes[-1].start()
    for copy in copies + planes:
        copy.wait_recv()
    for copy in copies + planes + smalls:
        copy.wait_send()
    own.wait()


class Gains:
    def __init__(self, n, n_dp, small, landed, mid, second, gsend, grecv, zsend, zrecv):
        self.me, self.row = lax.axis_index("ctx"), lax.axis_index("dp")
        self.small, self.landed, self.mid, self.second = small, landed, mid, second
        self.near, self.far = [], []
        for s in range(1, n):
            peer = flip(self.me, s, n)
            self.near.append(push(small.at[peer], landed.at[s], gsend.at[s], grecv.at[s], "ctx", peer))
        for s in range(1, n_dp):
            peer = flip(self.row, s, n_dp)
            self.far.append(push(mid.at[peer], second.at[s], zsend.at[s], zrecv.at[s], "dp", peer))

    def start(self):
        for copy in self.near:
            copy.start()

    def middle(self):
        value = self.small[self.me]
        for s, copy in enumerate(self.near, 1):
            copy.wait_recv()
            value = value + self.landed[s]
        self.mid[...] = value
        for copy in self.far:
            copy.start()

    def finish(self):
        value = self.mid[self.row]
        for s, copy in enumerate(self.far, 1):
            copy.wait_recv()
            value = value + self.second[s]
        for copy in self.near + self.far:
            copy.wait_send()
        return value


def post_kernel(n, src_ref, query_ref, key_ref, value_ref, blocks, send, recv, local):
    me = lax.axis_index("ctx")
    meet([("ctx", flip(me, s, n)) for s in range(1, n)])
    own, copies = swap_all(n, src_ref, blocks, send, recv, local)
    for copy in copies:
        copy.wait_recv()
    own.wait()
    share = n // KV
    qw = HQ * HD // n
    for c in range(n):
        query_ref[:, c * qw : (c + 1) * qw] = blocks[c, :, :qw].astype(F32)
    for g in range(KV):
        for out, kind in ((key_ref, 0), (value_ref, 1)):
            total = blocks[g * share + kind, :, qw:].astype(F32)
            for c in range(2 + kind, share, 2):
                total = total + blocks[g * share + c, :, qw:].astype(F32)
            out[:, g * HD : (g + 1) * HD] = total
    for copy in copies:
        copy.wait_send()


def swap_sems(n, n_dp):
    return [DMA((n,)), DMA((n,)), DMA(()), DMA((n,)), DMA((n,)), DMA((n_dp,)), DMA((n_dp,))]


def prep(n, n_dp, cols, small, cuts, weights):
    shape = jax.ShapeDtypeStruct
    return comm_call(
        functools.partial(prep_kernel, n, n_dp, cuts),
        0,
        [shape(cols.shape, cols.dtype), shape((n_dp, n) + small.shape, F32)]
        + pack_shapes(cuts, weights),
        [ANY, VM] + [VM] * len(cuts),
        [ANY, VM, ANY, ANY, ANY],
        pack_scratch(weights) + swap_sems(n, n_dp),
        8,
        cols,
        small,
        *weights,
    )


def post(n, cols):
    shape = jax.ShapeDtypeStruct
    depth = cols.shape[1]
    return comm_call(
        functools.partial(post_kernel, n),
        1,
        [
            shape((depth, HQ * HD), F32),
            shape((depth, KV * HD), F32),
            shape((depth, KV * HD), F32),
        ],
        [VM] * 3,
        [VM],
        [pltpu.VMEM(cols.shape, BF16), DMA((n,)), DMA((n,)), DMA(())],
        10,
        cols,
    )


def first_kernel(
    n, cuts, x_ref, gain_ref, info_ref, grad_ref, *rest
):
    sources, rest = rest[:3], rest[3:]
    nall_ref, iall_ref, gall_ref, rest = rest[0], rest[1], rest[2], rest[3:]
    packed, rest = rest[: len(cuts)], rest[len(cuts) :]
    pack = Pack(1, sources, rest[:3], rest[3])
    low, sems = rest[4], rest[5:]
    pack.start()
    plane = Plane(n)
    plane.meet()
    infos = Gather(plane, info_ref, iall_ref, *sems[0:3])
    infos.start()

    def norm(at):
        value = x_ref[at, :].astype(F32)
        low[at, :] = (value * rms_parts(value) * gain_ref[...]).astype(BF16)

    by_rows(x_ref.shape[0], norm)
    normed = gather_of(plane, low, nall_ref, *sems[3:6])
    normed.start()
    grads = gather_of(plane, grad_ref, gall_ref, *sems[6:9])
    grads.start()
    pack.write(cuts, packed)
    infos.forward()
    normed.forward()
    grads.forward()
    infos.finish()
    normed.finish()
    grads.finish()


def first(n, x, gain, info, grad, cuts, weights):
    shape = jax.ShapeDtypeStruct
    many = lambda array, kind: shape((n,) + array.shape, kind)
    return comm_call(
        functools.partial(first_kernel, n, cuts),
        2,
        [many(x, BF16), many(info, F32), many(grad, BF16)] + pack_shapes(cuts, weights),
        [ANY] * 3 + [VM] * len(cuts),
        [VM] * 4 + [ANY] * 3,
        pack_scratch(weights)
        + [pltpu.VMEM(x.shape, BF16)]
        + [DMA((n,)), DMA((n,)), DMA(())]
        + gather_sems(n)
        + gather_sems(n),
        90,
        x,
        gain,
        info,
        grad,
        *weights,
    )


def middle_kernel(
    n, attn_ref, wout_ref, x_ref, gain_ref, after_ref, all_ref, low, *scratch
):
    plane = Plane(n)
    plane.meet()
    rows = x_ref.shape[0]

    def value(block, at):
        left = attn_ref[pl.ds(pl.multiple_of(block * rows, rows), rows), :]
        return dot(left, wout_ref[:, at])

    sums = Product(plane, value, *scratch[:8])
    sums.start()
    sums.run()

    def norm(at):
        value = x_ref[at, :].astype(F32) + sums.total(at)
        after_ref[at, :] = value
        low[at, :] = (value * rms_parts(value) * gain_ref[...]).astype(BF16)

    by_rows(rows, norm)
    normed = gather_of(plane, low, all_ref, *scratch[8:])
    normed.start()
    normed.forward()
    sums.finish()
    normed.finish()


def middle(n, attn, wout, x, gain):
    shape = jax.ShapeDtypeStruct
    return comm_call(
        functools.partial(middle_kernel, n),
        3,
        [shape(x.shape, F32), shape((n,) + x.shape, BF16)],
        [VM, ANY],
        [VM, VM, VM, VM],
        [pltpu.VMEM(x.shape, BF16)]
        + product_scratch(n, *x.shape)
        + gather_sems(n),
        105,
        attn,
        wout,
        x,
        gain,
    )


def turn_kernel(
    n, part_ref, after_ref, grad_ref, gain_ref, mid_ref, fpart_ref, all_ref, low, *scratch
):
    plane = Plane(n)
    plane.meet()
    sums = Scatter(plane, part_ref, *scratch[:8])
    sums.start()
    fpart_ref[...] = jnp.zeros_like(fpart_ref)
    sums.run()

    def norm(at):
        value = after_ref[at, :]
        inv = rms_parts(value)
        unit = value * inv
        grad = sums.total(at)
        fpart_ref[0:1, :] += jnp.sum(grad * unit, axis=0, keepdims=True)
        mid = grad_ref[at, :].astype(F32) + rms_back(grad, unit, inv, gain_ref[...])
        mid_ref[at, :] = mid
        low[at, :] = mid.astype(BF16)

    by_rows(after_ref.shape[0], norm)
    branch = gather_of(plane, low, all_ref, *scratch[8:])
    branch.start()
    branch.forward()
    sums.finish()
    branch.finish()


def turn(n, part, after, grad, gain):
    shape = jax.ShapeDtypeStruct
    return comm_call(
        functools.partial(turn_kernel, n),
        4,
        [
            shape(after.shape, F32),
            shape((8, after.shape[1]), F32),
            shape((n,) + after.shape, BF16),
        ],
        [VM, VM, ANY],
        [ANY, VM, VM, VM],
        [pltpu.VMEM(after.shape, BF16)] + scatter_scratch(n, *after.shape) + gather_sems(n),
        95,
        part,
        after,
        grad,
        gain,
    )


def halfway_kernel(
    n,
    n_dp,
    part_ref,
    n2_ref,
    gg_ref,
    ug_ref,
    after_ref,
    grad_ref,
    gain_ref,
    mid_ref,
    fpart_ref,
    low_ref,
    wgrad_ref,
    n2,
    gg,
    ug,
    wgrad,
    lsem,
    wsem,
    *scratch,
):
    loads = [
        pltpu.make_async_copy(src, dst, lsem.at[k])
        for k, (src, dst) in enumerate(((n2_ref, n2), (gg_ref, gg), (ug_ref, ug)))
    ]
    plane = Plane(n)
    plane.meet()
    sums = Scatter(plane, part_ref, *scratch)
    sums.start()
    for load in loads:
        load.start()
    fpart_ref[...] = jnp.zeros_like(fpart_ref)
    sums.pairs()
    for load in loads:
        load.wait()
    cut = wgrad.shape[1] // 2

    def weights(kind, source):
        copies = []
        for z in range(n_dp):
            here = slice(z * cut, (z + 1) * cut)
            there = slice(kind * cut, (kind + 1) * cut)
            wgrad[z, there, :] = dot(n2[:, here], source[...], TN).astype(BF16)
            copies.append(
                pltpu.make_async_copy(
                    wgrad.at[z, pl.ds(kind * cut, cut), :],
                    wgrad_ref.at[z, pl.ds(kind * cut, cut), :],
                    wsem.at[kind, z],
                )
            )
            copies[-1].start()
        return copies

    copies = weights(0, gg)
    sums.spread.relay()
    copies += weights(1, ug)
    sums.spread.gathered()

    def norm(at):
        value = after_ref[at, :]
        inv = rms_parts(value)
        unit = value * inv
        grad = sums.total(at)
        fpart_ref[0:1, :] += jnp.sum(grad * unit, axis=0, keepdims=True)
        mid = grad_ref[at, :].astype(F32) + rms_back(grad, unit, inv, gain_ref[...])
        mid_ref[at, :] = mid
        low_ref[at, :] = mid.astype(BF16)

    by_rows(after_ref.shape[0], norm)
    sums.finish()
    for copy in copies:
        copy.wait()


def halfway(n, n_dp, part, n2, gg, ug, after, grad, gain):
    shape = jax.ShapeDtypeStruct
    width, hidden = n2.shape[1], gg.shape[1]
    out = (n_dp, 2 * width // n_dp, hidden)
    return comm_call(
        functools.partial(halfway_kernel, n, n_dp),
        4,
        [
            shape(after.shape, F32),
            shape((8, after.shape[1]), F32),
            shape(after.shape, BF16),
            shape(out, BF16),
        ],
        [VM, VM, VM, ANY],
        [ANY, ANY, ANY, ANY, VM, VM, VM],
        [
            pltpu.VMEM(n2.shape, BF16),
            pltpu.VMEM(gg.shape, BF16),
            pltpu.VMEM(gg.shape, BF16),
            pltpu.VMEM(out, BF16),
            DMA((3,)),
            DMA((2, n_dp)),
        ]
        + scatter_scratch(n, *after.shape),
        50,
        part,
        n2,
        gg,
        ug,
        after,
        grad,
        gain,
    )


def share_kernel(
    n, low_ref, act_ref, deep_ref, prob_ref, moe_ref, all_ref, out_ref, act, deep, moe, lsem, osem, *sems
):
    loads = [
        pltpu.make_async_copy(src, dst, lsem.at[k])
        for k, (src, dst) in enumerate(((act_ref, act), (deep_ref, deep), (moe_ref, moe)))
    ]
    plane = Plane(n)
    plane.meet()
    gather = gather_of(plane, low_ref, all_ref, *sems)
    gather.start()
    for load in loads:
        load.start()
    rows = low_ref.shape[0]
    parts, cut = deep.shape[:2]
    stores = [
        pltpu.make_async_copy(moe.at[pl.ds(k * rows, rows), :], out_ref.at[pl.ds(k * rows, rows), :], osem.at[k])
        for k in range(n)
    ]

    def product(k):
        here = slice(k * rows, (k + 1) * rows)
        for z in range(parts):
            cols = slice(z * cut, (z + 1) * cut)
            out = dot(act[here, :], deep[z], NT).astype(BF16).astype(F32) * prob_ref[here, :]
            moe[here, cols] = (moe[here, cols].astype(F32) + out).astype(BF16)
        stores[k].start()

    for load in loads:
        load.wait()
    for k in range(n // 2):
        product(k)
    gather.forward()
    for k in range(n // 2, n):
        product(k)
    gather.finish()
    for store in stores:
        store.wait()


def share_rows(n, low, act, deep, prob, moe):
    shape = jax.ShapeDtypeStruct
    return comm_call(
        functools.partial(share_kernel, n),
        10,
        [shape((n,) + low.shape, BF16), shape(moe.shape, BF16)],
        [ANY, ANY],
        [VM, ANY, ANY, VM, ANY],
        [
            pltpu.VMEM(act.shape, BF16),
            pltpu.VMEM(deep.shape, BF16),
            pltpu.VMEM(moe.shape, BF16),
            DMA((3,)),
            DMA((n,)),
        ]
        + gather_sems(n),
        45,
        low,
        act,
        deep,
        prob,
        moe,
    )


def last_kernel(n, grad_ref, wqkv_ref, x_ref, mid_ref, gain_ref, out_ref, apart_ref, *scratch):
    plane = Plane(n)
    plane.meet()
    apart_ref[...] = jnp.zeros_like(apart_ref)
    rows = x_ref.shape[0]

    def value(block, at):
        left = grad_ref[pl.ds(pl.multiple_of(block * rows, rows), rows), :]
        return dot(left, wqkv_ref[at, :], NT)

    sums = Product(plane, value, *scratch[:8])
    sums.start()
    sums.run()

    def norm(at):
        value = x_ref[at, :].astype(F32)
        inv = rms_parts(value)
        unit = value * inv
        grad = sums.total(at)
        apart_ref[0:1, :] += jnp.sum(grad * unit, axis=0, keepdims=True)
        out_ref[at, :] = mid_ref[at, :] + rms_back(grad, unit, inv, gain_ref[...])

    by_rows(rows, norm)
    sums.finish()


def last(n, grad, wqkv, x, mid, gain):
    shape = jax.ShapeDtypeStruct
    return comm_call(
        functools.partial(last_kernel, n),
        5,
        [shape(mid.shape, F32), shape((8, mid.shape[1]), F32)],
        [VM, VM],
        [VM] * 5,
        product_scratch(n, *mid.shape),
        60,
        grad,
        wqkv,
        x,
        mid,
        gain,
    )


def gains_kernel(n, n_dp, small_ref, sum_ref, *scratch):
    meet(
        [("ctx", flip(lax.axis_index("ctx"), s, n)) for s in range(1, n)]
        + [("dp", flip(lax.axis_index("dp"), s, n_dp)) for s in range(1, n_dp)]
    )
    gains = Gains(n, n_dp, small_ref, *scratch)
    gains.start()
    gains.middle()
    sum_ref[...] = gains.finish()


def gains_sum(n, n_dp, small):
    tile = small.shape[2:]
    return comm_call(
        functools.partial(gains_kernel, n, n_dp),
        8,
        jax.ShapeDtypeStruct(tile, F32),
        VM,
        [VM],
        [
            pltpu.VMEM((n, n_dp) + tile, F32),
            pltpu.VMEM((n_dp,) + tile, F32),
            pltpu.VMEM((n_dp,) + tile, F32),
            DMA((n,)),
            DMA((n,)),
            DMA((n_dp,)),
            DMA((n_dp,)),
        ],
        10,
        small,
    )


def attn_forward_kernel(
    n,
    n_dp,
    heads,
    back,
    normed_ref,
    wqkv_ref,
    cos_ref,
    sin_ref,
    qgain_ref,
    kgain_ref,
    docc_ref,
    docr_ref,
    rows_ref,
    qlin_ref,
    klin_ref,
    q_ref,
    k_ref,
    v_ref,
    attn_ref,
    total_ref,
    wout_ref,
    acc_ref,
    sum_ref,
    mate_ref,
    *sems,
):
    step = pl.program_id(0)

    @pl.when(step == 0)
    def _():
        meet_all(n)
        copy = push(
            wqkv_ref.at[:, pl.ds(heads * HD, HD)],
            mate_ref,
            sems[2],
            sems[3],
            "ctx",
            Plane(n).mate,
        )
        copy.start()
        RowSwap(n, n_dp, rows_ref, wout_ref, *sems[:2], False).start()
        copy.wait_recv()
        copy.wait_send()

    rows = normed_ref.shape[0]
    lin = dot(normed_ref[...], wqkv_ref[...])
    here = pl.ds(step * rows, rows)
    cosine = cos_ref[...]
    sine = sin_ref[...]
    qw = heads * HD
    for head in range(heads):
        cols = slice(head * HD, (head + 1) * HD)
        part = lin[:, cols]
        qlin_ref[:, cols] = part
        q_ref[:, cols] = head_forward(part, qgain_ref[...], cosine, sine).astype(BF16)
    own = lin[:, qw:]
    other = dot(normed_ref[...], mate_ref[...])
    first_core = lax.axis_index("ctx") % 2 == 0
    key_lin = jnp.where(first_core, own, other)
    klin_ref[...] = key_lin
    k_ref[here, :] = head_forward(key_lin, kgain_ref[...], cosine, sine).astype(BF16)
    v_ref[here, :] = jnp.where(first_core, other, own).astype(BF16)
    acc_ref[...] = jnp.zeros_like(acc_ref)
    sum_ref[...] = jnp.zeros_like(sum_ref)
    row_pos = step * rows + lax.broadcasted_iota(jnp.int32, (rows, rows), 0)
    col_off = lax.broadcasted_iota(jnp.int32, (rows, rows), 1)

    def one(block, carry):
        at = pl.ds(pl.multiple_of(block * rows, rows), rows)
        key = k_ref[at, :]
        val = v_ref[at, :]
        allowed = (docc_ref[...] == docr_ref[:, at]) & (block * rows + col_off <= row_pos)
        for head in range(heads):
            cols = slice(head * HD, (head + 1) * HD)
            score = dot(q_ref[:, cols], key, NT) * SCALE2
            expo = jnp.where(allowed, jnp.exp2(score), 0.0)
            folded = expo[:, :HD]
            for piece in range(1, rows // HD):
                folded = folded + expo[:, piece * HD : (piece + 1) * HD]
            sum_ref[:, cols] += folded
            acc_ref[:, cols] += dot(expo.astype(BF16), val)
        return carry

    lax.fori_loop(jnp.maximum(step - back, 0), step + 1, one, 0)
    lane = lax.broadcasted_iota(jnp.int32, (rows, HD), 1)
    totals = jnp.ones((rows, HD), F32)
    for head in range(heads):
        cols = slice(head * HD, (head + 1) * HD)
        total = jnp.sum(sum_ref[:, cols], axis=-1, keepdims=True)
        totals = jnp.where(lane == head, total, totals)
        attn_ref[:, cols] = (acc_ref[:, cols] / total).astype(BF16)
    total_ref[...] = totals

    @pl.when(step == pl.num_programs(0) - 1)
    def _():
        swap = RowSwap(n, n_dp, rows_ref, wout_ref, *sems[:2], False)
        swap.arrive()
        swap.finish()


def attn_forward(n, n_dp, normed, wqkv, cosine, sine, qgain, kgain, doc, wrows, rows):
    length, width = normed.shape
    qw = wqkv.shape[1] - HD
    heads = qw // HD
    blk = lambda cols: pl.BlockSpec((rows, cols), lambda i: (i, 0))
    whole = lambda shape: pl.BlockSpec(shape, lambda i: (0, 0))
    shape = jax.ShapeDtypeStruct
    return pl.pallas_call(
        functools.partial(attn_forward_kernel, n, n_dp, heads, MOST // rows),
        grid=(length // rows,),
        in_specs=[
            blk(width),
            whole(wqkv.shape),
            blk(HD),
            blk(HD),
            whole((1, HD)),
            whole((1, HD)),
            blk(1),
            whole((1, length)),
            ANY,
        ],
        out_specs=[
            blk(qw),
            blk(HD),
            blk(qw),
            whole((length, HD)),
            whole((length, HD)),
            blk(qw),
            blk(HD),
            ANY,
        ],
        out_shape=[
            shape((length, qw), F32),
            shape((length, HD), F32),
            shape((length, qw), BF16),
            shape((length, HD), BF16),
            shape((length, HD), BF16),
            shape((length, qw), BF16),
            shape((length, HD), F32),
            shape(wrows.shape, BF16),
        ],
        scratch_shapes=[
            pltpu.VMEM((rows, qw), F32),
            pltpu.VMEM((rows, qw), F32),
            pltpu.VMEM((width, HD), BF16),
        ]
        + [DMA((n_dp,)), DMA((n_dp,)), DMA(()), DMA(())],
        compiler_params=pltpu.CompilerParams(
            collective_id=7, has_side_effects=True, vmem_limit_bytes=VMEM_LIMIT
        ),
        cost_estimate=pl.CostEstimate(
            flops=35 * 10**9, transcendentals=0, bytes_accessed=30 * 2**20
        ),
        name="attn_forward",
    )(normed, wqkv, cosine, sine, qgain, kgain, doc[:, None], doc[None, :], wrows)


def attn_backward_kernel(
    n,
    n_dp,
    heads,
    back,
    branch_ref,
    wout_ref,
    attn_ref,
    total_ref,
    q_ref,
    k_ref,
    v_ref,
    qlin_ref,
    klin_ref,
    cos_ref,
    sin_ref,
    qgain_ref,
    kgain_ref,
    docc_ref,
    docr_ref,
    wgrad_ref,
    moe_ref,
    after_ref,
    dqkv_ref,
    gains_ref,
    swapped_ref,
    final_ref,
    dk_ref,
    dv_ref,
    dqa_ref,
    give_ref,
    take_ref,
    *sems,
):
    step = pl.program_id(0)

    steps = pl.num_programs(0)

    def scatter():
        return Scatter(Plane(n), moe_ref, *sems[2:10])

    @pl.when(step == 0)
    def _():
        meet_all(n)
        scatter().start()
        RowSwap(n, n_dp, wgrad_ref, swapped_ref, *sems[:2], True).start()

    @pl.when(step == 2)
    def _():
        scatter().pairs()

    @pl.when(step == steps - 2)
    def _():
        scatter().spread.relay()

    rows = branch_ref.shape[0]
    here = pl.ds(pl.multiple_of(step * rows, rows), rows)

    @pl.when(step == 0)
    def _():
        gains_ref[...] = jnp.zeros_like(gains_ref)

    dk_ref[here, :] = jnp.zeros((rows, HD), F32)
    dv_ref[here, :] = jnp.zeros((rows, HD), F32)
    dqa_ref[...] = jnp.zeros_like(dqa_ref)
    attn_grad = dot(branch_ref[...], wout_ref[...], NT)
    grads = []
    shifts = []
    for head in range(heads):
        cols = slice(head * HD, (head + 1) * HD)
        part = attn_grad[:, cols]
        inv_total = 1.0 / total_ref[:, head : head + 1]
        delta = jnp.sum(part * attn_ref[:, cols].astype(F32), axis=-1, keepdims=True)
        grads.append((part * inv_total).astype(BF16))
        shifts.append(delta * inv_total)
    row_pos = step * rows + lax.broadcasted_iota(jnp.int32, (rows, rows), 0)
    col_off = lax.broadcasted_iota(jnp.int32, (rows, rows), 1)

    def one(block, carry):
        at = pl.ds(pl.multiple_of(block * rows, rows), rows)
        key = k_ref[at, :]
        val = v_ref[at, :]
        allowed = (docc_ref[...] == docr_ref[:, at]) & (block * rows + col_off <= row_pos)
        columns = [slice(head * HD, (head + 1) * HD) for head in range(heads)]
        queries = [q_ref[:, cols] for cols in columns]
        scores = [dot(query, key, NT) for query in queries]
        prods = [dot(grad, val, NT) for grad in grads]
        expos = [jnp.where(allowed, jnp.exp2(score * SCALE2), 0.0) for score in scores]
        score_grads = [
            (expo * (prod - shift)).astype(BF16) for expo, prod, shift in zip(expos, prods, shifts)
        ]
        expos = [expo.astype(BF16) for expo in expos]
        dv = sum(dot(expo, grad, TN) for expo, grad in zip(expos, grads))
        dk = sum(dot(each, query, TN) for each, query in zip(score_grads, queries))
        for cols, each in zip(columns, score_grads):
            dqa_ref[:, cols] += dot(each, key)
        dk_ref[at, :] += dk
        dv_ref[at, :] += dv
        return carry

    lax.fori_loop(jnp.maximum(step - back, 0), step + 1, one, 0)
    cosine = cos_ref[here, :]
    sine = sin_ref[here, :]
    for head in range(heads):
        cols = slice(head * HD, (head + 1) * HD)
        grad, gain_part = head_backward(
            qlin_ref[:, cols], qgain_ref[...], cosine, sine, dqa_ref[:, cols] * SCALE
        )
        dqkv_ref[here, cols] = grad.astype(BF16)
        gains_ref[0:1, :] += gain_part

    @pl.when(step == pl.num_programs(0) - 1)
    def _():
        def finish(block, carry):
            at = pl.ds(pl.multiple_of(block * rows, rows), rows)
            grad, gain_part = head_backward(
                klin_ref[at, :], kgain_ref[...], cos_ref[at, :], sin_ref[at, :], dk_ref[at, :] * SCALE
            )
            first_core = lax.axis_index("ctx") % 2 == 0
            dk_ref[at, :] = jnp.where(first_core, grad, dv_ref[at, :])
            give_ref[at, :] = jnp.where(first_core, dv_ref[at, :], grad).astype(BF16)
            gains_ref[1:2, :] += gain_part
            return carry

        lax.fori_loop(0, pl.num_programs(0), finish, 0)
        trade = push(give_ref, take_ref, sems[10], sems[11], "ctx", Plane(n).mate)
        trade.start()
        sums = scatter()
        sums.spread.gathered()

        def add(at):
            final_ref[at, :] = (after_ref[at, :] + sums.total(at)).astype(BF16)

        by_rows(rows, add)
        sums.finish()
        trade.wait_recv()

        def join(block, carry):
            at = pl.ds(pl.multiple_of(block * rows, rows), rows)
            total = dk_ref[at, :] + take_ref[at, :].astype(F32)
            dqkv_ref[at, heads * HD :] = total.astype(BF16)
            return carry

        lax.fori_loop(0, pl.num_programs(0), join, 0)
        trade.wait_send()
        swap = RowSwap(n, n_dp, wgrad_ref, swapped_ref, *sems[:2], True)
        swap.arrive()
        swap.finish()


def attn_backward(n, n_dp, wgrad, moe, after, branch, wout, attn, total, q, k, v, qlin, klin, cosine, sine, qgain, kgain, doc, rows):
    length, width = branch.shape
    qw = wout.shape[0]
    heads = qw // HD
    blk = lambda cols: pl.BlockSpec((rows, cols), lambda i: (i, 0))
    whole = lambda shape: pl.BlockSpec(shape, lambda i: (0, 0), pipeline_mode=pl.Buffered(1))
    shape = jax.ShapeDtypeStruct
    full = whole((length, HD))
    return pl.pallas_call(
        functools.partial(attn_backward_kernel, n, n_dp, heads, MOST // rows),
        grid=(length // rows,),
        in_specs=[
            blk(width),
            whole(wout.shape),
            blk(qw),
            blk(HD),
            blk(qw),
            full,
            full,
            blk(qw),
            full,
            full,
            full,
            whole((1, HD)),
            whole((1, HD)),
            blk(1),
            whole((1, length)),
            ANY,
            ANY,
            whole(after.shape),
        ],
        out_specs=[whole((length, qw + HD)), whole((8, HD)), ANY, whole(after.shape)],
        out_shape=[
            shape((length, qw + HD), BF16),
            shape((8, HD), F32),
            shape(wgrad.shape, BF16),
            shape(after.shape, BF16),
        ],
        scratch_shapes=[
            pltpu.VMEM((length, HD), F32),
            pltpu.VMEM((length, HD), F32),
            pltpu.VMEM((rows, qw), F32),
            pltpu.VMEM((length, HD), BF16),
            pltpu.VMEM((length, HD), BF16),
            DMA((n_dp,)),
            DMA((n_dp,)),
        ]
        + scatter_scratch(n, *after.shape)
        + [DMA(()), DMA(())],
        compiler_params=pltpu.CompilerParams(
            collective_id=9, has_side_effects=True, vmem_limit_bytes=VMEM_LIMIT
        ),
        cost_estimate=pl.CostEstimate(
            flops=60 * 10**9, transcendentals=0, bytes_accessed=30 * 2**20
        ),
        name="attn_backward",
    )(branch, wout, attn, total, q, k, v, qlin, klin, cosine, sine, qgain, kgain, doc[:, None], doc[None, :], wgrad, moe, after)


def expert_kernel(chained, low, aliased, split, plan, z_ref, n2_ref, top_ref, prob_ref, *rest):
    if aliased:
        rest = rest[1:]
    if chained and split:
        row_in, rest = rest[0], rest[1:]
    elif chained:
        moe_in, row_in = rest[:2]
        rest = rest[2:]
    sources, rest = rest[: len(plan)], rest[len(plan) :]
    moe_ref, row_ref, rest = rest[0], rest[1], rest[2:]
    if split:
        act_ref = moe_ref
        gg_ref, ug_ref, deep_ref, rest = *rest[:3], rest[3:]
    grads_ref, wg_ref, wu_ref, wd_ref, rest = *rest[:4], rest[4:]
    if split:
        deep_sem, rest = rest[-1], rest[:-1]
    sums, (stage, wsem, sem) = rest[:-3], rest[-3:]
    ad_ref = sums[-1]
    step = pl.program_id(0)
    rows, width = n2_ref.shape
    parts, cut, hidden = wd_ref.shape
    weights = (wg_ref, wu_ref, wd_ref)

    @pl.when(step == 0)
    def _():
        z = z_ref[0]
        for source, (kind, amount, start) in zip(sources, plan):
            count = source.shape[-2] // cut
            for k in range(parts) if kind == "all" else [amount]:
                if kind == "all":
                    src, owner, wanted = source.at[k], k, None
                elif kind == "up":
                    src, owner, wanted = source, z - k, z >= k
                else:
                    src, owner, wanted = source, z + k, z + k < parts

                def load(src=src, owner=owner, start=start, count=count):
                    for piece in range(count):
                        pltpu.make_async_copy(
                            src.at[pl.ds(piece * cut, cut), :],
                            weights[start + piece].at[owner],
                            wsem.at[start + piece, owner],
                        ).start()

                if wanted is None:
                    load()
                else:
                    pl.when(wanted)(load)
        for each in sums:
            each[...] = jnp.zeros_like(each)
        for index in range(3):
            for owner in range(parts):
                block = weights[index].at[owner]
                pltpu.make_async_copy(block, block, wsem.at[index, owner]).wait()
        if split:
            pltpu.make_async_copy(wd_ref, deep_ref, deep_sem).start()

    n2 = n2_ref[...]
    prob = prob_ref[...]
    wg = wg_ref[...].reshape(width, hidden)
    wu = wu_ref[...].reshape(width, hidden)
    gate = dot(n2, wg)
    up = dot(n2, wu)
    sig = 1.0 / (1.0 + jnp.exp(-gate))
    silu = gate * sig
    act = (silu * up).astype(BF16)
    act_grad = jnp.zeros((rows, hidden), F32)
    for z in range(parts):
        cols = slice(z * cut, (z + 1) * cut)
        if not split:
            out = dot(act, wd_ref[z], NT).astype(BF16).astype(F32) * prob
            if chained:
                out = out + moe_in[:, cols].astype(F32)
            moe_ref[:, cols] = out.astype(BF16)
        route = (top_ref[:, cols].astype(F32) * prob).astype(BF16)
        act_grad += dot(route, wd_ref[z])
        ad_ref[z] += dot(route, act, TN)
    gate_grad = (act_grad * up * sig * (1.0 + gate * (1.0 - sig))).astype(BF16)
    up_grad = (act_grad * silu).astype(BF16)
    row = dot(gate_grad, wg, NT) + dot(up_grad, wu, NT)
    if chained:
        row = row + row_in[...].astype(F32)
    row_ref[...] = row.astype(BF16)
    if split:
        act_ref[...] = act
        gg_ref[...] = gate_grad
        ug_ref[...] = up_grad
    else:
        sums[0][...] += dot(n2, gate_grad, TN).reshape(parts, cut, hidden)
        sums[1][...] += dot(n2, up_grad, TN).reshape(parts, cut, hidden)

    @pl.when(step == pl.num_programs(0) - 1)
    def _():
        copies = []
        pieces = [
            (acc, place, z) for z in range(parts) for place, acc in enumerate(sums)
        ]
        for index, (acc, place, z) in enumerate(pieces):
            slot = index % 2
            if index >= 2:
                copies[index - 2].wait()
            stage[slot] = acc[z].astype(BF16)
            copies.append(
                pltpu.make_async_copy(
                    stage.at[slot],
                    grads_ref.at[z, pl.ds(place * cut, cut), pl.ds(low, acc.shape[2])],
                    sem.at[slot],
                )
            )
            copies[-1].start()
        copies[-2].wait()
        copies[-1].wait()
        if split:
            pltpu.make_async_copy(wd_ref, deep_ref, deep_sem).wait()


def expert(z, n2, top, prob, n_dp, sources, before, rows, low, full, grads, split):
    length, width = n2.shape
    cut = width // n_dp
    hidden = sources[0][0].shape[-1]
    blk = pl.BlockSpec((rows, width), lambda i: (i, 0))
    col = pl.BlockSpec((rows, 1), lambda i: (i, 0))
    thin = pl.BlockSpec((rows, hidden), lambda i: (i, 0))
    shape = jax.ShapeDtypeStruct
    plan = tuple(entry[1:] for entry in sources)
    weight = pltpu.VMEM((n_dp, cut, hidden), BF16)
    total = pltpu.VMEM((n_dp, cut, hidden), F32)
    return pl.pallas_call(
        functools.partial(expert_kernel, len(before) > 0, low, len(grads) > 0, split, plan),
        grid=(length // rows,),
        in_specs=[pl.BlockSpec(memory_space=pltpu.SMEM), blk, blk, col]
        + [ANY] * len(grads)
        + [blk] * len(before)
        + [ANY] * len(sources),
        out_specs=[thin if split else blk, blk] + ([thin, thin, ANY] if split else []) + [ANY],
        out_shape=[
            shape((length, hidden if split else width), BF16),
            shape((length, width), BF16),
        ]
        + [shape((length, hidden), BF16)] * (2 * split)
        + [shape((n_dp, cut, hidden), BF16)] * split
        + [shape((n_dp, cut if split else 3 * cut, full), BF16)],
        input_output_aliases={4: 2} if grads else {},
        scratch_shapes=[weight] * 3
        + [total] * (1 if split else 3)
        + [pltpu.VMEM((2, cut, hidden), BF16), DMA((3, n_dp)), DMA((2,))]
        + [DMA(())] * split,
        compiler_params=pltpu.CompilerParams(vmem_limit_bytes=VMEM_LIMIT),
        cost_estimate=pl.CostEstimate(
            flops=18 * length * width * hidden,
            transcendentals=length * hidden,
            bytes_accessed=5 * length * width * 2,
        ),
        name="expert",
    )(z, n2, top, prob, *grads, *before, *[entry[0] for entry in sources])


def unpack_kernel(
    z_ref, pair_ref, down_one_ref, all_ref, up0_ref, down0_ref, up1_ref, down1_ref, dg_ref, du_ref, dd_ref, own, sem
):
    copy = pltpu.make_async_copy(all_ref.at[z_ref[0]], own, sem)
    copy.start()
    cut = dg_ref.shape[1]
    half = up0_ref.shape[0]
    piece = [slice(k * cut, (k + 1) * cut) for k in range(2)]
    dg_ref[1] = pair_ref[piece[0], :].astype(F32)
    du_ref[1] = pair_ref[piece[1], :].astype(F32)
    dd_ref[1] = jnp.transpose(down_one_ref[...].astype(F32))
    copy.wait()

    def total(low, high):
        shift, up, down = (0, up0_ref, down0_ref) if high <= half else (half, up1_ref, down1_ref)
        there = slice(low - shift, high - shift)
        value = own[low:high, :].astype(F32)
        return value + up[there, :].astype(F32) + down[there, :].astype(F32)

    dg_ref[0] = total(0, cut)
    du_ref[0, : half - cut] = total(cut, half)
    du_ref[0, half - cut :] = total(half, 2 * cut)
    dd_ref[0] = jnp.transpose(total(2 * cut, 3 * cut))


def unpack(z, pair, one, grads, got):
    cut, hidden = one.shape
    rows = 3 * cut
    shape = jax.ShapeDtypeStruct
    return pl.pallas_call(
        unpack_kernel,
        in_specs=[pl.BlockSpec(memory_space=pltpu.SMEM), VM, VM, ANY, VM, VM, VM, VM],
        out_specs=[VM] * 3,
        out_shape=[
            shape((2, cut, hidden), F32),
            shape((2, cut, hidden), F32),
            shape((2, hidden, cut), F32),
        ],
        scratch_shapes=[pltpu.VMEM((rows, hidden), BF16), DMA(())],
        compiler_params=pltpu.CompilerParams(vmem_limit_bytes=VMEM_LIMIT),
        name="unpack",
    )(z, pair, one, grads, *got)


def line_hop(block_up, block_down, n_dp, hop):
    up = [(i, i + 1) for i in range(hop - 1, n_dp - 1)]
    down = [(i + 1, i) for i in range(n_dp - hop)]
    return lax.ppermute(block_up, "dp", up), lax.ppermute(block_down, "dp", down)


def reduce_hop(grads, got, n_dp, hop, rows, before):
    place = lax.axis_index("dp")
    reach = n_dp - hop
    zero = jnp.int32(0)
    size = (1, rows[1] - rows[0], grads.shape[2])
    spots = (jnp.minimum(place + reach, n_dp - 1), jnp.maximum(place - reach, 0))
    if got is not None:
        got = lax.optimization_barrier((*got, *before))[:2]
    elif before:
        grads = after_of(grads, *before)
    blocks = [
        lax.dynamic_slice(grads, (spot.astype(jnp.int32), jnp.int32(rows[0]), zero), size)[0]
        for spot in spots
    ]
    if got is not None:
        blocks = [(b.astype(F32) + g.astype(F32)).astype(BF16) for b, g in zip(blocks, got)]
    up = [(i, i + 1) for i in range(hop)]
    down = [(i, i - 1) for i in range(n_dp - hop, n_dp)]
    sent = lax.ppermute(blocks[0], "dp", up), lax.ppermute(blocks[1], "dp", down)
    return sent, tuple(blocks)


def after_of(value, *others):
    return lax.optimization_barrier((value,) + others)[0]


def per_device(
    layer_input,
    doc_ids,
    route_ids,
    route_probs,
    attn_gain,
    ffn_gain,
    query_gain,
    key_gain,
    w_query,
    w_key,
    w_value,
    w_out,
    w_gate,
    w_up,
    w_down,
    out_grad,
):
    tokens, width = layer_input.shape[1:]
    n_dp = lax.axis_size("dp")
    n_ctx = lax.axis_size("ctx")
    ctx_index = lax.axis_index("ctx")
    length = tokens * n_ctx
    heads = HQ // n_ctx
    share = n_ctx // KV
    qw = heads * HD
    depth = w_query.shape[0]
    own_e = w_gate.shape[0]

    cut = attn_gain.shape[0]
    hcut = query_gain.shape[0]
    kinds = 2 * (cut + hcut)
    small = jnp.concatenate([attn_gain, ffn_gain, query_gain, key_gain]).astype(F32)
    small = jnp.pad(small, (0, 1024 - kinds)).reshape(8, HD)
    even = (jnp.arange(n_ctx) % 2 == 0)[None, :, None]
    wide = [jnp.repeat(w.reshape(depth, KV, HD), share, axis=1) for w in (w_key, w_value)]
    cols = jnp.concatenate(
        [w_query.reshape(depth, n_ctx, qw), jnp.where(even, wide[0], wide[1])], axis=2
    ).transpose(1, 0, 2)
    hidden = w_gate.shape[2]
    cuts = ((0, 256), (256, hidden))
    cols, small, *blocks0 = prep(
        n_ctx, n_dp, cols, small, cuts, (w_gate, w_up, w_down)
    )
    small = small.reshape(n_dp * n_ctx, 1024)
    gain_attn = small[:, :cut].reshape(1, width)
    gain_ffn = small[:, cut : 2 * cut].reshape(1, width)
    gain_query = small[:, 2 * cut : 2 * cut + hcut].reshape(1, HD)
    gain_key = small[:, 2 * cut + hcut : kinds].reshape(1, HD)
    wqkv = lax.all_gather(cols.reshape(n_ctx * depth, qw + HD), "dp", axis=0, tiled=True)
    wrows = lax.all_gather(w_out, "dp", axis=0, tiled=False)

    inputs = layer_input.reshape(tokens, width)
    top_own = out_grad.reshape(tokens, width)
    n_experts = own_e * n_ctx
    match = route_ids.reshape(1, tokens, TOP) == jnp.arange(n_experts, dtype=jnp.int32)[:, None, None]
    probs = jnp.sum(jnp.where(match, route_probs.reshape(1, tokens, TOP), 0.0), axis=2)
    info = jnp.concatenate(
        [probs, doc_ids.reshape(1, tokens).astype(F32), jnp.zeros((7, tokens), F32)], axis=0
    )
    normed, info, top_all, block1 = first(
        n_ctx, inputs, gain_attn, info, top_own, ((0, hidden),), (w_gate, w_up, w_down)
    )
    normed = normed.reshape(length, width)
    doc = info[:, n_experts].reshape(length).astype(jnp.int32)
    my_probs = lax.dynamic_slice_in_dim(info, ctx_index * own_e, own_e, 1)
    my_probs = my_probs.transpose(0, 2, 1).reshape(length, own_e)

    inverse = 1.0 / ROPE_BASE ** (jnp.arange(HD // 2, dtype=F32) * 2.0 / HD)
    angles = jnp.arange(length, dtype=F32)[:, None] * inverse[None, :]
    cosine = jnp.cos(angles)
    sine = jnp.sin(angles)
    cosine = jnp.concatenate([cosine, cosine], axis=1)
    sine = jnp.concatenate([-sine, sine], axis=1)
    qlin, klin, q, k, v, attn, total, wout = attn_forward(
        n_ctx, n_dp, normed, wqkv, cosine, sine, gain_query, gain_key, doc, wrows, tokens
    )
    wout = wout.reshape(qw, width)
    top_all = top_all.reshape(length, width)
    blocks = (n_ctx, tokens, width)
    after, normed2 = middle(n_ctx, attn, wout, inputs, gain_ffn)
    normed2 = normed2.reshape(length, width)

    z = lax.axis_index("dp").astype(jnp.int32).reshape(1)
    hidden = w_gate.shape[2]

    def run(e, sources, carried, low, grads, split=False):
        moe, rows_grad, *grads = expert(
            z,
            normed2,
            top_all,
            my_probs[:, e : e + 1],
            n_dp,
            sources,
            carried,
            tokens,
            low,
            hidden,
            grads,
            split,
        )
        return (moe, rows_grad), grads

    carried, grads0 = (), ()
    for index, (low, high) in enumerate(cuts):
        full = lax.all_gather(blocks0[index], "dp", axis=0, tiled=False)
        if index == 1:
            sources1 = [(block1, "up", 0, 0)]
            up = down = after_of(block1, full)
            up, down = line_hop(up, down, n_dp, 1)
            sources1 += [(up, "up", 1, 0), (down, "down", 1, 0)]
        carried, (grads,) = run(0, [(full, "all", 0, 0)], carried, low, grads0)
        grads0 = (grads,)
    rows_all = 3 * (width // n_dp)
    spans = {"a": (0, rows_all // 2), "b": (rows_all // 2, rows_all)}
    got, before = {tag: None for tag in spans}, ()
    for hop in range(2, n_dp + 1):
        if hop < n_dp:
            up, down = line_hop(up, down, n_dp, hop)
            sources1 += [(up, "up", hop, 0), (down, "down", hop, 0)]
        for tag, rows in spans.items():
            got[tag], before = reduce_hop(grads, got[tag], n_dp, hop - 1, rows, before)
    split = n_ctx == 8
    earlier = carried[1:] if split else carried
    (moe, rows_grad), grads1 = run(1, sources1, earlier, 0, (), split)
    rows_grad = rows_grad.reshape(blocks)
    if split:
        gate_grad, up_grad, deep, down_grad = grads1
        done_d = lax.psum_scatter(
            down_grad.reshape(width, hidden), "dp", scatter_dimension=0, tiled=True
        )
        mid, ffn_part, low_mid, pair_grad = halfway(
            n_ctx, n_dp, rows_grad, normed2, gate_grad, up_grad, after, top_own, gain_ffn
        )
        done_gu = lax.psum_scatter(
            pair_grad.reshape(2 * width, hidden), "dp", scatter_dimension=0, tiled=True
        )
        branch, moe = share_rows(n_ctx, low_mid, moe, deep, my_probs[:, 1:2], carried[0])
    else:
        done = lax.psum_scatter(
            grads1[0].reshape(3 * width, hidden), "dp", scatter_dimension=0, tiled=True
        )
        done_gu, done_d = done[: 2 * width // n_dp], done[2 * width // n_dp :]
        mid, ffn_part, branch = turn(n_ctx, rows_grad, after, top_own, gain_ffn)
    branch = branch.reshape(length, width)

    out_w = dot(attn, branch, TN).astype(BF16).reshape(n_dp, qw // n_dp, width)
    dqkv, gains, out_w, layer_output = attn_backward(
        n_ctx,
        n_dp,
        out_w,
        moe.reshape(blocks),
        after,
        branch,
        wout,
        attn,
        total,
        q,
        k,
        v,
        qlin,
        klin,
        cosine,
        sine,
        gain_query,
        gain_key,
        doc,
        tokens,
    )
    qkv_w = dot(normed, dqkv, TN).astype(BF16)
    qkv_w = lax.psum_scatter(qkv_w, "dp", scatter_dimension=0, tiled=True)
    out_w = lax.psum_scatter(out_w.reshape(qw, width), "dp", scatter_dimension=0, tiled=True)
    out_w = out_w.astype(F32)
    input_grad, attn_part = last(n_ctx, dqkv, wqkv, inputs, mid, gain_attn)
    n_all = n_dp * n_ctx
    packed = jnp.concatenate(
        [
            attn_part[0].reshape(n_all, cut),
            ffn_part[0].reshape(n_all, cut),
            gains[0].reshape(n_all, hcut),
            gains[1].reshape(n_all, hcut),
            jnp.zeros((n_all, 1024 - kinds), F32),
        ],
        axis=1,
    )
    packed = packed.reshape(n_dp, n_ctx, 8, HD).transpose(1, 0, 2, 3)
    packed = gains_sum(n_ctx, n_dp, packed)
    packed = packed.reshape(1024)
    query_w, key_w, value_w = post(n_ctx, qkv_w.reshape(n_ctx, depth, qw + HD))
    gate_w, up_w, down_w = unpack(z, done_gu, done_d, grads, got["a"] + got["b"])
    return (
        layer_output.reshape(1, tokens, width),
        input_grad.reshape(1, tokens, width),
        packed[:cut],
        packed[cut : 2 * cut],
        packed[2 * cut : 2 * cut + hcut],
        packed[2 * cut + hcut : kinds],
        query_w,
        key_w,
        value_w,
        out_w,
        gate_w,
        up_w,
        down_w,
    )


def solution(mesh):
    both = ("dp", "ctx")
    seq = P("dp", "ctx", None)
    in_specs = (
        seq,
        P("dp", "ctx"),
        seq,
        seq,
        P(both),
        P(both),
        P(both),
        P(both),
        P(both, None),
        P(both, None),
        P(both, None),
        P(both, None),
        P("ctx", "dp", None),
        P("ctx", "dp", None),
        P("ctx", None, "dp"),
        seq,
    )
    out_specs = (
        seq,
        seq,
        P(both),
        P(both),
        P(both),
        P(both),
        P(both, None),
        P(both, None),
        P(both, None),
        P(both, None),
        P("ctx", "dp", None),
        P("ctx", "dp", None),
        P("ctx", None, "dp"),
    )

    return jax.shard_map(
        per_device, mesh=mesh, in_specs=in_specs, out_specs=out_specs, check_vma=False
    )
```
